8 devices in a mesh: dp: 1 (over z), yz: 2 (over y), x: 4 (over x, core).
Axes of the slice: x: 2, y: 2, z: 1, core: 2. Of those that a mesh axis runs over, the one named last changes fastest.
Arguments:
- hidden: bfloat16 [256, 6144], P('dp', ('x', 'yz'))
- norm_gain: bfloat16 [1, 6144], P(None, 'x')
- w_q: bfloat16 [1, 6144, 6144], P(None, 'x', 'yz')
- w_kv: bfloat16 [1, 6144, 256], P(None, 'x', 'yz')
- w_gate: bfloat16 [1, 6144, 24576], P(None, 'x', 'yz')
- w_up: bfloat16 [1, 6144, 24576], P(None, 'x', 'yz')
- w_o: bfloat16 [1, 6144, 6144], P(None, 'yz', 'x')
- w_down: bfloat16 [1, 24576, 6144], P(None, 'yz', 'x')
- k_cache: bfloat16 [1, 256, 2048, 128], P(None, ('dp', 'x', 'yz'))
- v_cache: bfloat16 [1, 256, 2048, 128], P(None, ('dp', 'x', 'yz'))
- seq_len: int32 [256], P(('dp', 'x', 'yz'))
Outputs:
- output 1: bfloat16 [256, 6144], P('dp', ('x', 'yz'))
- output 2: bfloat16 [1, 256, 2048, 128], P(None, ('dp', 'x', 'yz'))
- output 3: bfloat16 [1, 256, 2048, 128], P(None, ('dp', 'x', 'yz'))
All inputs are finite; a program needn't handle non-finite values.
Results may differ from the reference program's by a relative error of at most 0.0163719.
Values are sent between devices in bfloat16 or wider.
A program may use at most 1 GiB of HBM per device.

```python
import math
import jax
import jax.numpy as jnp
from jax import lax

D_MODEL = 6144
N_HEADS = 48
HEAD_DIM = 128
D_FF = 24576
LAYERS = 1
BATCH_SIZE = 256
CACHE_LEN = 2048

NORM_EPS = 1e-6
QUERY_COLS = N_HEADS * HEAD_DIM
KEY_SCALE = math.sqrt(math.log(CACHE_LEN / 16.0))


def setup_inputs(seed: int = 0, part: int = 0) -> dict:
    base_key = jax.random.key(seed)
    shared = jax.random.split(base_key, 7)
    part_keys = jax.random.split(jax.random.fold_in(base_key, part), 5)
    col_ramp = 0.4 + 1.2 * jnp.arange(D_MODEL, dtype=jnp.float32) / D_MODEL
    hidden = jax.random.normal(part_keys[0], (BATCH_SIZE, D_MODEL), jnp.float32) * col_ramp
    norm_gain = 1.0 + 0.4 * jax.random.normal(shared[0], (LAYERS, D_MODEL), jnp.float32)
    w_q = jax.random.normal(shared[1], (LAYERS, D_MODEL, QUERY_COLS), jnp.float32) * D_MODEL ** -0.5
    kv_scale = jnp.concatenate([jnp.full((HEAD_DIM,), KEY_SCALE, jnp.float32), jnp.ones((HEAD_DIM,), jnp.float32)])
    w_kv = jax.random.normal(shared[2], (LAYERS, D_MODEL, 2 * HEAD_DIM), jnp.float32) * kv_scale * D_MODEL ** -0.5
    w_gate = jax.random.normal(shared[3], (LAYERS, D_MODEL, D_FF), jnp.float32) * D_MODEL ** -0.5
    w_up = jax.random.normal(shared[4], (LAYERS, D_MODEL, D_FF), jnp.float32) * D_MODEL ** -0.5
    w_o = jax.random.normal(shared[5], (LAYERS, QUERY_COLS, D_MODEL), jnp.float32) * 2.0 * QUERY_COLS ** -0.5
    w_down = jax.random.normal(shared[6], (LAYERS, D_FF, D_MODEL), jnp.float32) * 1.5 * D_FF ** -0.5
    k_cache = jax.random.normal(part_keys[1], (LAYERS, BATCH_SIZE, CACHE_LEN, HEAD_DIM), jnp.float32) * KEY_SCALE
    v_cache = jax.random.normal(part_keys[2], (LAYERS, BATCH_SIZE, CACHE_LEN, HEAD_DIM), jnp.float32)
    drawn_len = jax.random.randint(part_keys[3], (BATCH_SIZE,), 1, CACHE_LEN, dtype=jnp.int32)
    longest_at = jax.random.randint(part_keys[4], (), 0, BATCH_SIZE, dtype=jnp.int32)
    seq_len = jnp.where(jnp.arange(BATCH_SIZE) == longest_at, CACHE_LEN - 1, drawn_len).astype(jnp.int32)
    return {
        "hidden": hidden.astype(jnp.bfloat16),
        "norm_gain": norm_gain.astype(jnp.bfloat16),
        "w_q": w_q.astype(jnp.bfloat16),
        "w_kv": w_kv.astype(jnp.bfloat16),
        "w_gate": w_gate.astype(jnp.bfloat16),
        "w_up": w_up.astype(jnp.bfloat16),
        "w_o": w_o.astype(jnp.bfloat16),
        "w_down": w_down.astype(jnp.bfloat16),
        "k_cache": k_cache.astype(jnp.bfloat16),
        "v_cache": v_cache.astype(jnp.bfloat16),
        "seq_len": seq_len,
    }


def rms_scale(hidden, norm_gain):
    hidden_f32 = hidden.astype(jnp.float32)
    inv_rms = lax.rsqrt(jnp.mean(hidden_f32 * hidden_f32, axis=-1, keepdims=True) + NORM_EPS)
    return (hidden_f32 * inv_rms * norm_gain.astype(jnp.float32)).astype(jnp.bfloat16)


def attend_one(packed):
    query_row, keys_row, values_row, length = packed
    scores = jnp.dot(query_row, keys_row.T, preferred_element_type=jnp.float32) * HEAD_DIM ** -0.5
    visible = jnp.arange(CACHE_LEN) <= length
    scores = jnp.where(visible[None, :], scores, -1e30)
    weights = jnp.exp(scores - jnp.max(scores, axis=-1, keepdims=True))
    probs_bf = (weights / jnp.sum(weights, axis=-1, keepdims=True)).astype(jnp.bfloat16)
    return jnp.dot(probs_bf, values_row, preferred_element_type=jnp.float32).astype(jnp.bfloat16)


def reference(hidden, norm_gain, w_q, w_kv, w_gate, w_up, w_o, w_down, k_cache, v_cache, seq_len):
    slot_hit = (jnp.arange(CACHE_LEN)[None, :] == seq_len[:, None])[:, :, None]

    def layer_step(residual, layer_args):
        l_gain, l_wq, l_wkv, l_wgate, l_wup, l_wo, l_wdown, l_kc, l_vc = layer_args
        normed = rms_scale(residual, l_gain)
        query_heads = jnp.dot(normed, l_wq, preferred_element_type=jnp.float32).astype(jnp.bfloat16).reshape(BATCH_SIZE, N_HEADS, HEAD_DIM)
        kv_new = jnp.dot(normed, l_wkv, preferred_element_type=jnp.float32).astype(jnp.bfloat16)
        gate_act = jnp.dot(normed, l_wgate, preferred_element_type=jnp.float32).astype(jnp.bfloat16)
        up_act = jnp.dot(normed, l_wup, preferred_element_type=jnp.float32).astype(jnp.bfloat16)
        new_k = jnp.where(slot_hit, kv_new[:, None, :HEAD_DIM], l_kc)
        new_v = jnp.where(slot_hit, kv_new[:, None, HEAD_DIM:], l_vc)
        attn_out = lax.map(attend_one, (query_heads, new_k, new_v, seq_len))
        mlp_act = (jax.nn.silu(gate_act.astype(jnp.float32)) * up_act.astype(jnp.float32)).astype(jnp.bfloat16)
        update = jnp.dot(attn_out.reshape(BATCH_SIZE, QUERY_COLS), l_wo, preferred_element_type=jnp.float32) + jnp.dot(mlp_act, l_wdown, preferred_element_type=jnp.float32)
        return (residual.astype(jnp.float32) + update).astype(jnp.bfloat16), (new_k, new_v)

    hidden_out, (k_out, v_out) = lax.scan(layer_step, hidden, (norm_gain, w_q, w_kv, w_gate, w_up, w_o, w_down, k_cache, v_cache))
    return hidden_out, k_out, v_out
```

```python
import functools

import jax
import jax.numpy as jnp
from jax import lax
from jax.experimental import pallas as pl
from jax.experimental.pallas import tpu as pltpu
from jax.sharding import PartitionSpec as P

NORM_EPS = 1e-6
W = 512
NBUF1 = 4
NBUF3 = 10
EARLY = 10
SEQ_STEP = 2
VMEM_LIMIT = 64_000_000
F32 = jnp.float32
BF16 = jnp.bfloat16
LOG2E = 1.4426950408889634
MASKED = -1e30


def dev(**axes):
    return dict(device_id=axes, device_id_type=pl.DeviceIdType.MESH)


def silu_mul(gate, up):
    gate = gate.astype(BF16).astype(F32)
    up = up.astype(BF16).astype(F32)
    return (jax.nn.silu(gate) * up).astype(BF16)


def project_kernel(
    n_q, n_ff, d_model, hidden, gain, wq, wkv, wg, wu,
    qkv_out, m_out, keep_out, send_out,
    h_other, u, sq_all, wbuf, wkv_buf, part, part_kv, near, near_kv, keep, keep_kv, far_src, far_src_kv,
    far, far_kv, z_rows, z_other,
    w_sem, wkv_sem, h_sems, sq_send, sq_recv, near_send, near_recv, far_send, far_recv, y_sems, out_sem,
):
    xi = lax.axis_index("x")
    yj = lax.axis_index("yz")
    core = lax.rem(xi, 2)
    chip = xi // 2
    mate = xi + 1 - 2 * core
    across = lax.rem(xi + 2, 4)
    other_y = 1 - yj
    me = xi * 2 + yj
    half = hidden.shape[1]
    n_all = n_q + n_ff

    def weight_copies(g, slot):
        return g, slot

    def start_weights(g):
        slot = lax.rem(g, NBUF1)

        @pl.when(g < n_q)
        def _():
            for k in range(2):
                cols = pl.ds(pl.multiple_of((2 * g + k) * W, W), W)
                pltpu.make_async_copy(wq.at[0, :, cols], wbuf.at[slot, k], w_sem.at[slot, k]).start()

        @pl.when(g >= n_q)
        def _():
            cols = pl.ds(pl.multiple_of((g - n_q) * W, W), W)
            pltpu.make_async_copy(wg.at[0, :, cols], wbuf.at[slot, 0], w_sem.at[slot, 0]).start()
            pltpu.make_async_copy(wu.at[0, :, cols], wbuf.at[slot, 1], w_sem.at[slot, 1]).start()

    for g in range(NBUF1):
        start_weights(jnp.int32(g))
    kv_copy = pltpu.make_async_copy(wkv.at[0], wkv_buf, wkv_sem)
    kv_copy.start()

    barrier = pltpu.get_barrier_semaphore()
    for k in range(1, 8):
        peer = lax.rem(me + k, 8)
        pl.semaphore_signal(barrier, inc=1, **dev(x=peer // 2, yz=lax.rem(peer, 2)))
    pl.semaphore_wait(barrier, 7)

    h_copy = pltpu.make_async_remote_copy(
        src_ref=hidden, dst_ref=h_other, send_sem=h_sems.at[0], recv_sem=h_sems.at[1], **dev(x=xi, yz=other_y))
    h_copy.start()

    h_f32 = hidden[...].astype(F32)
    sq_all[me] = lax.dot_general(
        jnp.ones((8, half), F32), h_f32 * h_f32, (((1,), (1,)), ((), ())),
        precision=lax.Precision.HIGHEST, preferred_element_type=F32)

    def sq_copy(peer, src):
        return pltpu.make_async_remote_copy(
            src_ref=sq_all.at[src], dst_ref=sq_all.at[src], send_sem=sq_send.at[peer], recv_sem=sq_recv.at[src],
            **dev(x=peer // 2, yz=lax.rem(peer, 2)))

    for k in range(1, 8):
        sq_copy(lax.rem(me + k, 8), me).start()
    for k in range(1, 8):
        peer = lax.rem(me + k, 8)
        sq_copy(peer, peer).wait_recv()
    total = jnp.sum(sq_all[...], axis=0)
    inv = lax.rsqrt(total / d_model + NORM_EPS)
    inv_col = jnp.transpose(jnp.concatenate([inv] * 16, axis=0))[:, :1]

    def norm_half(values, which):
        cols = pl.ds(pl.multiple_of(which * half, 128), half)
        u[:, cols] = (values.astype(F32) * inv_col * gain[:, cols].astype(F32)).astype(BF16)

    norm_half(hidden[...], yj)
    h_copy.wait_recv()
    norm_half(h_other[...], other_y)

    def near_copy(g):
        return pltpu.make_async_remote_copy(
            src_ref=part.at[g, :, 1 - core], dst_ref=near.at[g], send_sem=near_send.at[g], recv_sem=near_recv.at[g],
            **dev(x=mate, yz=yj))

    def near_copy_kv():
        return pltpu.make_async_remote_copy(
            src_ref=part_kv.at[:, 1 - core], dst_ref=near_kv, send_sem=near_send.at[n_all],
            recv_sem=near_recv.at[n_all], **dev(x=mate, yz=yj))

    def far_copy(g):
        return pltpu.make_async_remote_copy(
            src_ref=far_src.at[g], dst_ref=far.at[g], send_sem=far_send.at[g], recv_sem=far_recv.at[g],
            **dev(x=across, yz=yj))

    def far_copy_kv():
        return pltpu.make_async_remote_copy(
            src_ref=far_src_kv, dst_ref=far_kv, send_sem=far_send.at[n_q + EARLY],
            recv_sem=far_recv.at[n_q + EARLY], **dev(x=across, yz=yj))

    def out_copies(g):
        k = g - (n_q + EARLY)
        return (
            pltpu.make_async_copy(keep.at[g], keep_out.at[k], out_sem.at[k, 0]),
            pltpu.make_async_copy(far_src.at[g], send_out.at[k], out_sem.at[k, 1]),
        )

    def multiply(g):
        slot = lax.rem(g, NBUF1)
        for k in range(2):
            pltpu.make_async_copy(wq.at[0, :, pl.ds(0, W)], wbuf.at[slot, k], w_sem.at[slot, k]).wait()
            res = jnp.dot(u[...], wbuf[slot, k], preferred_element_type=F32).astype(BF16)
            part[g, :, :, :, k * W:(k + 1) * W] = res.reshape(2, 2, 64, W)
        near_copy(g).start()

        @pl.when(g + NBUF1 < n_all)
        def _():
            start_weights(g + NBUF1)

    def reduce_near(g, send):
        near_copy(g).wait_recv()
        keep[g] = (part[g, chip, core].astype(F32) + near[g, chip].astype(F32)).astype(BF16)
        far_src[g] = (part[g, 1 - chip, core].astype(F32) + near[g, 1 - chip].astype(F32)).astype(BF16)
        if send:
            far_copy(g).start()
        else:
            for copy in out_copies(g):
                copy.start()

    @pl.loop(0, n_q)
    def _(g):
        multiply(g)

        @pl.when(g >= 1)
        def _():
            reduce_near(g - 1, True)

    kv_copy.wait()
    res = jnp.dot(u[...], wkv_buf[...], preferred_element_type=F32).astype(BF16)
    part_kv[...] = res.reshape(2, 2, 64, res.shape[1])
    near_copy_kv().start()
    reduce_near(n_q - 1, True)
    near_copy_kv().wait_recv()
    keep_kv[...] = (part_kv[chip, core].astype(F32) + near_kv[chip].astype(F32)).astype(BF16)
    far_src_kv[...] = (part_kv[1 - chip, core].astype(F32) + near_kv[1 - chip].astype(F32)).astype(BF16)
    far_copy_kv().start()

    @pl.loop(n_q, n_q + EARLY)
    def _(g):
        multiply(g)

        @pl.when(g >= n_q + 1)
        def _():
            reduce_near(g - 1, True)

    q_cols = n_q * 2 * W
    for g in range(n_q):
        far_copy(g).wait_recv()
        z = (keep[g].astype(F32) + far[g].astype(F32)).astype(BF16)
        z_rows[:, :, g * 2 * W:(g + 1) * 2 * W] = z.reshape(2, 32, 2 * W)
    far_copy_kv().wait_recv()
    z = (keep_kv[...].astype(F32) + far_kv[...].astype(F32)).astype(BF16)
    z_rows[:, :, q_cols:] = z.reshape(2, 32, z.shape[1])
    y_copy = pltpu.make_async_remote_copy(
        src_ref=z_rows.at[other_y], dst_ref=z_other, send_sem=y_sems.at[0], recv_sem=y_sems.at[1],
        **dev(x=xi, yz=other_y))
    y_copy.start()
    qkv_out[yj] = z_rows[yj]

    multiply(n_q + EARLY)
    reduce_near(n_q + EARLY - 1, True)

    @pl.loop(n_q + EARLY + 1, n_all)
    def _(g):
        multiply(g)
        reduce_near(g - 1, False)

    reduce_near(n_all - 1, False)
    y_copy.wait_recv()
    qkv_out[other_y] = z_other[...]

    @pl.loop(n_q, n_q + EARLY)
    def _(g):
        far_copy(g).wait_recv()
        z = keep[g].astype(F32) + far[g].astype(F32)
        m_out[g - n_q] = silu_mul(z[:, :W], z[:, W:])

    h_copy.wait_send()
    for k in range(1, 8):
        sq_copy(lax.rem(me + k, 8), me).wait_send()
    y_copy.wait_send()
    near_copy_kv().wait_send()
    far_copy_kv().wait_send()

    @pl.loop(0, n_all)
    def _(g):
        near_copy(g).wait_send()

    @pl.loop(0, n_q + EARLY)
    def _(g):
        far_copy(g).wait_send()

    @pl.loop(n_q + EARLY, n_all)
    def _(g):
        for copy in out_copies(g):
            copy.wait()


def project(hidden, gain, w_q, w_kv, w_gate, w_up, d_model):
    rows, half = hidden.shape
    feats = w_q.shape[1]
    kv = w_kv.shape[2]
    n_q = w_q.shape[2] // (2 * W)
    n_ff = w_gate.shape[2] // W
    n_all = n_q + n_ff
    n_far = n_q + EARLY
    late = n_ff - EARLY
    dma = pltpu.SemaphoreType.DMA
    any_spec = pl.BlockSpec(memory_space=pl.ANY)
    vmem = pl.BlockSpec(memory_space=pltpu.VMEM)
    cols = w_q.shape[2] + kv
    flops = 2 * rows * feats * (w_q.shape[2] + kv + 2 * w_gate.shape[2])
    return pl.pallas_call(
        functools.partial(project_kernel, n_q, n_ff, d_model),
        name="project",
        out_shape=(
            jax.ShapeDtypeStruct((2, 32, cols), BF16),
            jax.ShapeDtypeStruct((EARLY, 64, W), BF16),
            jax.ShapeDtypeStruct((late, 64, 2 * W), BF16),
            jax.ShapeDtypeStruct((late, 64, 2 * W), BF16),
        ),
        in_specs=[vmem, vmem, any_spec, any_spec, any_spec, any_spec],
        out_specs=(vmem, vmem, any_spec, any_spec),
        scratch_shapes=[
            pltpu.VMEM((rows, half), BF16),
            pltpu.VMEM((rows, feats), BF16),
            pltpu.VMEM((8, 8, rows), F32),
            pltpu.VMEM((NBUF1, 2, feats, W), BF16),
            pltpu.VMEM((feats, kv), BF16),
            pltpu.VMEM((n_all, 2, 2, 64, 2 * W), BF16),
            pltpu.VMEM((2, 2, 64, kv), BF16),
            pltpu.VMEM((n_all, 2, 64, 2 * W), BF16),
            pltpu.VMEM((2, 64, kv), BF16),
            pltpu.VMEM((n_all, 64, 2 * W), BF16),
            pltpu.VMEM((64, kv), BF16),
            pltpu.VMEM((n_all, 64, 2 * W), BF16),
            pltpu.VMEM((64, kv), BF16),
            pltpu.VMEM((n_far, 64, 2 * W), BF16),
            pltpu.VMEM((64, kv), BF16),
            pltpu.VMEM((2, 32, cols), BF16),
            pltpu.VMEM((32, cols), BF16),
            dma((NBUF1, 2)),
            dma,
            dma((2,)),
            dma((8,)),
            dma((8,)),
            dma((n_all + 1,)),
            dma((n_all + 1,)),
            dma((n_far + 1,)),
            dma((n_far + 1,)),
            dma((2,)),
            dma((late, 2)),
        ],
        compiler_params=pltpu.CompilerParams(collective_id=0, has_side_effects=True, vmem_limit_bytes=VMEM_LIMIT),
        cost_estimate=pl.CostEstimate(flops=flops, bytes_accessed=feats * (flops // (rows * feats)), transcendentals=0),
    )(hidden, gain, w_q, w_kv, w_gate, w_up)


def attend_kernel(lens, q_ref, kv_ref, k_ref, v_ref, k_out, v_out, o_ref):
    step = pl.program_id(0)
    n_pos = k_ref.shape[2]
    scale = q_ref.shape[2] ** -0.5 * LOG2E
    for s in range(SEQ_STEP):
        length = lens[step * SEQ_STEP + s]
        base = pl.multiple_of((length // 16) * 16, 16)
        k_out[0, s] = k_ref[0, s]
        v_out[0, s] = v_ref[0, s]
        hit = lax.broadcasted_iota(jnp.int32, (16, k_ref.shape[3]), 0) == length - base
        for src, dst, which in ((k_ref, k_out, 0), (v_ref, v_out, 1)):
            old = src[0, s, pl.ds(base, 16), :].astype(F32)
            new = kv_ref[s, which:which + 1, :].astype(F32)
            dst[0, s, pl.ds(base, 16), :] = jnp.where(hit, new, old).astype(BF16)
        scores = lax.dot_general(q_ref[s], k_out[0, s], (((1,), (1,)), ((), ())), preferred_element_type=F32) * scale
        visible = lax.broadcasted_iota(jnp.int32, scores.shape, 1) <= length
        scores = jnp.where(visible, scores, MASKED)
        weights = jnp.exp2(scores - jnp.max(scores, axis=1, keepdims=True))
        probs = (weights * (1.0 / jnp.sum(weights, axis=1, keepdims=True))).astype(BF16)
        o_ref[s] = jnp.dot(probs, v_out[0, s], preferred_element_type=F32).astype(BF16)


def attend(lens, q, kv, k_cache, v_cache):
    seqs, heads, dim = q.shape
    n_pos = k_cache.shape[2]
    cache_spec = pl.BlockSpec((1, SEQ_STEP, n_pos, dim), lambda b, lens: (0, b, 0, 0))
    q_spec = pl.BlockSpec((SEQ_STEP, heads, dim), lambda b, lens: (b, 0, 0))
    return pl.pallas_call(
        attend_kernel,
        name="attend",
        out_shape=(
            jax.ShapeDtypeStruct(k_cache.shape, BF16),
            jax.ShapeDtypeStruct(v_cache.shape, BF16),
            jax.ShapeDtypeStruct(q.shape, BF16),
        ),
        grid_spec=pltpu.PrefetchScalarGridSpec(
            num_scalar_prefetch=1,
            grid=(seqs // SEQ_STEP,),
            in_specs=[q_spec, pl.BlockSpec((SEQ_STEP, 2, dim), lambda b, lens: (b, 0, 0)), cache_spec, cache_spec],
            out_specs=(cache_spec, cache_spec, q_spec),
        ),
        compiler_params=pltpu.CompilerParams(dimension_semantics=("arbitrary",), vmem_limit_bytes=40_000_000),
        cost_estimate=pl.CostEstimate(
            flops=10**10, bytes_accessed=8 * k_cache.size, transcendentals=seqs * heads * n_pos),
    )(lens, q, kv, k_cache, v_cache)


def output_kernel(
    n_ff, n_o, o_in, m_in, keep, recv, hidden, w_o, w_down, out,
    acts, wbuf, acc, y_src, y_dst,
    w_sem, o_sems, far_send, far_recv, near_send, near_recv, y_sems,
):
    xi = lax.axis_index("x")
    yj = lax.axis_index("yz")
    core = lax.rem(xi, 2)
    mate = xi + 1 - 2 * core
    across = lax.rem(xi + 2, 4)
    other_y = 1 - yj
    n_m2 = n_ff // 2
    n2 = n_m2 + n_o // 2
    d_out = w_down.shape[2]
    half = d_out // 2

    def start_weights(g):
        slot = lax.rem(g, NBUF3)

        @pl.when(g < n_m2)
        def _():
            pltpu.make_async_copy(
                w_down.at[0, pl.ds(pl.multiple_of(g * 2 * W, W), 2 * W)], wbuf.at[slot], w_sem.at[slot]).start()

        @pl.when(g >= n_m2)
        def _():
            pltpu.make_async_copy(
                w_o.at[0, pl.ds(pl.multiple_of((g - n_m2) * 2 * W, W), 2 * W)], wbuf.at[slot], w_sem.at[slot]).start()

    for g in range(NBUF3):
        start_weights(jnp.int32(g))

    barrier = pltpu.get_barrier_semaphore()
    for x_, y_ in ((mate, yj), (across, yj), (xi, other_y)):
        pl.semaphore_signal(barrier, inc=1, **dev(x=x_, yz=y_))
    pl.semaphore_wait(barrier, 3)

    def rows_of(block):
        return pl.ds(pl.multiple_of(block * 64, 64), 64)

    def o_rows(j):
        return acts.at[pl.ds(n_ff, n_o), pl.ds(pl.multiple_of(xi * 64 + j * 32, 32), 32)]

    o_copy = pltpu.make_async_remote_copy(
        src_ref=o_in.at[other_y], dst_ref=o_rows(yj), send_sem=o_sems.at[0], recv_sem=o_sems.at[1],
        **dev(x=xi, yz=other_y))
    o_copy.start()

    def far_copy(g):
        block = acts.at[pl.ds(2 * g, 2), rows_of(xi)]
        return pltpu.make_async_remote_copy(
            src_ref=block, dst_ref=block, send_sem=far_send.at[g], recv_sem=far_recv.at[g], **dev(x=across, yz=yj))

    def near_copy(g, which):
        block = acts.at[pl.ds(2 * g, 2), rows_of(xi if which == 0 else across)]
        return pltpu.make_async_remote_copy(
            src_ref=block, dst_ref=block, send_sem=near_send.at[g, which], recv_sem=near_recv.at[g, which],
            **dev(x=mate, yz=yj))

    def give(g):
        far_copy(g).start()
        near_copy(g, 0).start()

    @pl.loop(0, EARLY // 2)
    def _(g):
        for k in range(2):
            acts[2 * g + k, rows_of(xi)] = m_in[2 * g + k]
        give(g)

    @pl.loop(EARLY // 2, n_m2)
    def _(g):
        for k in range(2):
            t = 2 * g + k - EARLY
            z = keep[t].astype(F32) + recv[t].astype(F32)
            acts[2 * g + k, rows_of(xi)] = silu_mul(z[:, :W], z[:, W:])
        give(g)

    for k in range(n_o):
        acts[n_ff + k, pl.ds(pl.multiple_of(xi * 64 + yj * 32, 32), 32)] = o_in[yj, k]
    o_copy.wait_recv()

    @pl.loop(n_m2, n2)
    def _(g):
        give(g)

    acc[...] = jnp.zeros_like(acc)

    def forward(g):
        far_copy(g).wait_recv()
        near_copy(g, 1).start()

    def multiply(g):
        slot = lax.rem(g, NBUF3)
        pltpu.make_async_copy(w_down.at[0, pl.ds(0, 2 * W)], wbuf.at[slot], w_sem.at[slot]).wait()
        near_copy(g, 0).wait_recv()
        near_copy(g, 1).wait_recv()
        for n in range(d_out // W):
            cols = slice(n * W, (n + 1) * W)
            acc[:, cols] += jnp.dot(acts[2 * g], wbuf[slot, :W, cols], preferred_element_type=F32) + jnp.dot(
                acts[2 * g + 1], wbuf[slot, W:, cols], preferred_element_type=F32)

        @pl.when(g + NBUF3 < n2)
        def _():
            start_weights(g + NBUF3)

    forward(0)

    @pl.loop(1, n2)
    def _(g):
        forward(g)
        multiply(g - 1)

    multiply(n2 - 1)

    def cols_of(j):
        return pl.ds(pl.multiple_of(j * half, 128), half)

    y_src[...] = acc[:, cols_of(other_y)].astype(BF16)
    y_copy = pltpu.make_async_remote_copy(
        src_ref=y_src, dst_ref=y_dst, send_sem=y_sems.at[0], recv_sem=y_sems.at[1], **dev(x=xi, yz=other_y))
    y_copy.start()
    acc[:, cols_of(yj)] += hidden[...].astype(F32)
    y_copy.wait_recv()
    out[...] = (acc[:, cols_of(yj)] + y_dst[...].astype(F32)).astype(BF16)

    y_copy.wait_send()
    o_copy.wait_send()

    @pl.loop(0, n2)
    def _(g):
        far_copy(g).wait_send()
        near_copy(g, 0).wait_send()
        near_copy(g, 1).wait_send()


def finish(o, m_early, keep, recv, hidden, w_o, w_down):
    rows, half = hidden.shape
    n_ff = w_down.shape[1] // W
    n_o = w_o.shape[1] // W
    n2 = (n_ff + n_o) // 2
    d_out = w_down.shape[2]
    dma = pltpu.SemaphoreType.DMA
    any_spec = pl.BlockSpec(memory_space=pl.ANY)
    vmem = pl.BlockSpec(memory_space=pltpu.VMEM)
    flops = 2 * rows * d_out * (w_down.shape[1] + w_o.shape[1])
    return pl.pallas_call(
        functools.partial(output_kernel, n_ff, n_o),
        name="finish",
        out_shape=jax.ShapeDtypeStruct((rows, half), BF16),
        in_specs=[vmem, vmem, vmem, vmem, vmem, any_spec, any_spec],
        out_specs=vmem,
        scratch_shapes=[
            pltpu.VMEM((n_ff + n_o, rows, W), BF16),
            pltpu.VMEM((NBUF3, 2 * W, d_out), BF16),
            pltpu.VMEM((rows, d_out), F32),
            pltpu.VMEM((rows, half), BF16),
            pltpu.VMEM((rows, half), BF16),
            dma((NBUF3,)),
            dma((2,)),
            dma((n2,)),
            dma((n2,)),
            dma((n2, 2)),
            dma((n2, 2)),
            dma((2,)),
        ],
        compiler_params=pltpu.CompilerParams(collective_id=1, has_side_effects=True, vmem_limit_bytes=VMEM_LIMIT),
        cost_estimate=pl.CostEstimate(flops=flops, bytes_accessed=2 * d_out * (w_down.shape[1] + w_o.shape[1]), transcendentals=0),
    )(o, m_early, keep, recv, hidden, w_o, w_down)


def solution(mesh):
    x_size = mesh.shape["x"]
    y_size = mesh.shape["yz"]
    row_spec = P("dp", ("x", "yz"))
    tile_in = P(None, "x", "yz")
    tile_out = P(None, "yz", "x")
    cache_spec = P(None, ("dp", "x", "yz"))
    len_spec = P(("dp", "x", "yz"))

    def device_step(hidden, norm_gain, w_q, w_kv, w_gate, w_up, w_o, w_down, k_cache, v_cache, seq_len):
        d_model = hidden.shape[1] * x_size * y_size
        seqs = k_cache.shape[1]
        dim = k_cache.shape[3]
        q_cols = w_q.shape[2]
        heads = q_cols // dim
        qkv, m_early, keep, send = project(hidden, norm_gain, w_q, w_kv, w_gate, w_up, d_model)
        recv = lax.ppermute(send, "x", [(i, (i + x_size // 2) % x_size) for i in range(x_size)])
        q = qkv[:, :, :q_cols].reshape(y_size, seqs, heads, dim).transpose(1, 0, 2, 3).reshape(seqs, y_size * heads, dim)
        kv = qkv[:, :, q_cols:].transpose(1, 0, 2)
        k_new, v_new, o = attend(seq_len, q, kv, k_cache, v_cache)
        o = o.reshape(seqs, y_size, q_cols // W, W).transpose(1, 2, 0, 3)
        hidden_out = finish(o, m_early, keep, recv, hidden, w_o, w_down)
        return hidden_out, k_new, v_new

    return jax.shard_map(
        device_step,
        mesh=mesh,
        in_specs=(row_spec, P(None, "x"), tile_in, tile_in, tile_in, tile_in, tile_out, tile_out, cache_spec, cache_spec, len_spec),
        out_specs=(row_spec, cache_spec, cache_spec),
        check_vma=False,
    )
```

```python
import functools

import jax
import jax.numpy as jnp
from jax import lax
from jax.experimental import pallas as pl
from jax.experimental.pallas import tpu as pltpu
from jax.sharding import PartitionSpec as P

NORM_EPS = 1e-6
W = 512
NBUF1 = 4
NBUF3 = 6
GROUP = 3
EARLY = 12
SEQ_STEP = 2
VMEM_LIMIT = 64_000_000
F32 = jnp.float32
BF16 = jnp.bfloat16
LOG2E = 1.4426950408889634
MASKED = -1e30


def dev(**axes):
    return dict(device_id=axes, device_id_type=pl.DeviceIdType.MESH)


def silu_mul(gate, up):
    gate = gate.astype(BF16).astype(F32)
    up = up.astype(BF16).astype(F32)
    return (jax.nn.silu(gate) * up).astype(BF16)


def project_kernel(
    n_q, n_ff, d_model, hidden, gain, wq, wkv, wg, wu,
    qkv_out, m_out, keep_out, send_out,
    h_other, u, inv_all, sq_all, wbuf, wkv_buf, part, part_kv, near, near_kv, keep, keep_kv, far_src, far_src_kv,
    far, far_kv, z_rows, z_other, m_rows,
    w_sem, wkv_sem, h_sems, sq_send, sq_recv, near_send, near_recv, far_send, far_recv, y_sems, out_sem, m_sem, qkv_sem,
):
    xi = lax.axis_index("x")
    yj = lax.axis_index("yz")
    core = lax.rem(xi, 2)
    chip = xi // 2
    mate = xi + 1 - 2 * core
    across = lax.rem(xi + 2, 4)
    other_y = 1 - yj
    me = xi * 2 + yj
    half = hidden.shape[1]
    n_all = n_q + n_ff
    n_far = n_q + EARLY

    barrier = pltpu.get_barrier_semaphore()
    for k in range(1, 8):
        peer = lax.rem(me + k, 8)
        pl.semaphore_signal(barrier, inc=1, **dev(x=peer // 2, yz=lax.rem(peer, 2)))

    def start_weights(g):
        slot = lax.rem(g, NBUF1)

        @pl.when(g < n_q)
        def _():
            for k in range(2):
                cols = pl.ds(pl.multiple_of((2 * g + k) * W, W), W)
                pltpu.make_async_copy(wq.at[0, :, cols], wbuf.at[slot, k], w_sem.at[slot, k]).start()

        @pl.when(g >= n_q)
        def _():
            cols = pl.ds(pl.multiple_of((g - n_q) * W, W), W)
            pltpu.make_async_copy(wg.at[0, :, cols], wbuf.at[slot, 0], w_sem.at[slot, 0]).start()
            pltpu.make_async_copy(wu.at[0, :, cols], wbuf.at[slot, 1], w_sem.at[slot, 1]).start()

    def wait_weights(slot, k):
        pltpu.make_async_copy(wq.at[0, :, pl.ds(0, W)], wbuf.at[slot, k], w_sem.at[slot, k]).wait()

    for g in range(NBUF1):
        start_weights(jnp.int32(g))
    kv_copy = pltpu.make_async_copy(wkv.at[0], wkv_buf, wkv_sem)
    kv_copy.start()

    h_f32 = hidden[...].astype(F32)
    sq_all[me] = lax.dot_general(
        jnp.ones((8, half), F32), h_f32 * h_f32, (((1,), (1,)), ((), ())),
        precision=lax.Precision.HIGHEST, preferred_element_type=F32)
    pl.semaphore_wait(barrier, 7)

    def sq_copy(peer, src):
        return pltpu.make_async_remote_copy(
            src_ref=sq_all.at[src], dst_ref=sq_all.at[src], send_sem=sq_send.at[peer], recv_sem=sq_recv.at[src],
            **dev(x=peer // 2, yz=lax.rem(peer, 2)))

    def rows_of(which):
        return pl.ds(pl.multiple_of((1 - chip if which == 0 else chip) * 128, 128), 128)

    def h_copy(which):
        return pltpu.make_async_remote_copy(
            src_ref=hidden.at[rows_of(which)], dst_ref=h_other.at[rows_of(which)],
            send_sem=h_sems.at[which, 0], recv_sem=h_sems.at[which, 1], **dev(x=xi, yz=other_y))

    for k in range(1, 8):
        sq_copy(lax.rem(me + k, 8), me).start()
    h_copy(0).start()
    h_copy(1).start()
    for k in range(1, 8):
        peer = lax.rem(me + k, 8)
        sq_copy(peer, peer).wait_recv()
    total = jnp.sum(sq_all[...], axis=0)
    inv = lax.rsqrt(total / d_model + NORM_EPS)
    inv_all[...] = jnp.transpose(jnp.concatenate([inv] * 16, axis=0))

    def normalize(values, rows, which):
        cols = pl.ds(pl.multiple_of(which * half, 128), half)
        u[rows, cols] = (
            values[rows].astype(F32) * inv_all[rows, :1] * gain[:, cols].astype(F32)).astype(BF16)

    def near_copy(g):
        return pltpu.make_async_remote_copy(
            src_ref=part.at[g, :, 1 - core], dst_ref=near.at[g], send_sem=near_send.at[g], recv_sem=near_recv.at[g],
            **dev(x=mate, yz=yj))

    def near_copy_q(g, which):
        side = 1 - chip if which == 0 else chip
        sem = g + which * (n_all + 1)
        return pltpu.make_async_remote_copy(
            src_ref=part.at[g, side, 1 - core], dst_ref=near.at[g, side], send_sem=near_send.at[sem],
            recv_sem=near_recv.at[sem], **dev(x=mate, yz=yj))

    def near_copy_kv(which):
        side = 1 - chip if which == 0 else chip
        sem = n_all + which * (n_q + 1)
        return pltpu.make_async_remote_copy(
            src_ref=part_kv.at[side, 1 - core], dst_ref=near_kv.at[side], send_sem=near_send.at[sem],
            recv_sem=near_recv.at[sem], **dev(x=mate, yz=yj))

    def far_copy(g):
        return pltpu.make_async_remote_copy(
            src_ref=far_src.at[g], dst_ref=far.at[g], send_sem=far_send.at[g], recv_sem=far_recv.at[g],
            **dev(x=across, yz=yj))

    def far_copy_kv():
        return pltpu.make_async_remote_copy(
            src_ref=far_src_kv, dst_ref=far_kv, send_sem=far_send.at[n_far],
            recv_sem=far_recv.at[n_far], **dev(x=across, yz=yj))

    def out_copies(g):
        k = g - n_far
        return (
            pltpu.make_async_copy(keep.at[g], keep_out.at[k], out_sem.at[k, 0]),
            pltpu.make_async_copy(far_src.at[g], send_out.at[k], out_sem.at[k, 1]),
        )

    def add(a, b):
        return (a.astype(F32) + b.astype(F32)).astype(BF16)

    def multiply(g):
        slot = lax.rem(g, NBUF1)
        for k in range(2):
            wait_weights(slot, k)
            res = jnp.dot(u[...], wbuf[slot, k], preferred_element_type=F32).astype(BF16)
            part[g, :, :, :, k * W:(k + 1) * W] = res.reshape(2, 2, 64, W)
        near_copy(g).start()

        @pl.when(g + NBUF1 < n_all)
        def _():
            start_weights(g + NBUF1)

    def reduce_near(g, send):
        near_copy(g).wait_recv()
        keep[g] = add(part[g, chip, core], near[g, chip])
        far_src[g] = add(part[g, 1 - chip, core], near[g, 1 - chip])
        if send:
            far_copy(g).start()
        else:
            for copy in out_copies(g):
                copy.start()

    for which in range(2):
        side = 1 - chip if which == 0 else chip
        rows = rows_of(which)
        normalize(hidden, rows, yj)
        h_copy(which).wait_recv()
        normalize(h_other, rows, other_y)

        def reduce_q(g):
            near_copy_q(g, which).wait_recv()
            total_q = add(part[g, side, core], near[g, side])
            if which == 0:
                far_src[g] = total_q
                far_copy(g).start()
            else:
                keep[g] = total_q

        for g in range(n_q):
            for k in range(2):
                if which == 0:
                    wait_weights(g, k)
                res = jnp.dot(u[rows], wbuf[g, k], preferred_element_type=F32).astype(BF16)
                part[g, side, :, :, k * W:(k + 1) * W] = res.reshape(2, 64, W)
            near_copy_q(g, which).start()
            if which == 1:
                start_weights(jnp.int32(g + NBUF1))
            if g >= 1:
                reduce_q(g - 1)
        if which == 0:
            kv_copy.wait()
        res = jnp.dot(u[rows], wkv_buf[...], preferred_element_type=F32).astype(BF16)
        part_kv[side] = res.reshape(2, 64, res.shape[1])
        near_copy_kv(which).start()
        reduce_q(n_q - 1)
        near_copy_kv(which).wait_recv()
        total_kv = add(part_kv[side, core], near_kv[side])
        if which == 0:
            far_src_kv[...] = total_kv
            far_copy_kv().start()
        else:
            keep_kv[...] = total_kv

    @pl.loop(n_q, n_far)
    def _(g):
        multiply(g)

        @pl.when(g >= n_q + 1)
        def _():
            reduce_near(g - 1, True)

    q_cols = n_q * 2 * W
    for g in range(n_q):
        far_copy(g).wait_recv()
        z_rows[:, :, g * 2 * W:(g + 1) * 2 * W] = add(keep[g], far[g]).reshape(2, 32, 2 * W)
    far_copy_kv().wait_recv()
    z_kv = add(keep_kv[...], far_kv[...])
    z_rows[:, :, q_cols:] = z_kv.reshape(2, 32, z_kv.shape[1])
    y_copy = pltpu.make_async_remote_copy(
        src_ref=z_rows.at[other_y], dst_ref=z_other, send_sem=y_sems.at[0], recv_sem=y_sems.at[1],
        **dev(x=xi, yz=other_y))
    y_copy.start()
    qkv_own = pltpu.make_async_copy(z_rows.at[yj], qkv_out.at[yj], qkv_sem.at[0])
    qkv_own.start()

    multiply(n_far)
    reduce_near(n_far - 1, True)

    @pl.loop(n_far + 1, n_all)
    def _(g):
        multiply(g)
        reduce_near(g - 1, False)

    reduce_near(n_all - 1, False)
    y_copy.wait_recv()
    qkv_other = pltpu.make_async_copy(z_other, qkv_out.at[other_y], qkv_sem.at[1])
    qkv_other.start()

    def m_copy(g):
        return pltpu.make_async_copy(m_rows.at[g - n_q], m_out.at[g - n_q], m_sem.at[g - n_q])

    @pl.loop(n_q, n_far)
    def _(g):
        far_copy(g).wait_recv()
        z = keep[g].astype(F32) + far[g].astype(F32)
        m_rows[g - n_q] = silu_mul(z[:, :W], z[:, W:])
        m_copy(g).start()

    for which in range(2):
        h_copy(which).wait_send()
        near_copy_kv(which).wait_send()
        for g in range(n_q):
            near_copy_q(g, which).wait_send()
    for k in range(1, 8):
        sq_copy(lax.rem(me + k, 8), me).wait_send()
    y_copy.wait_send()
    far_copy_kv().wait_send()
    qkv_own.wait()
    qkv_other.wait()

    @pl.loop(n_q, n_all)
    def _(g):
        near_copy(g).wait_send()

    @pl.loop(0, n_far)
    def _(g):
        far_copy(g).wait_send()

    @pl.loop(n_far, n_all)
    def _(g):
        for copy in out_copies(g):
            copy.wait()

    @pl.loop(n_q, n_far)
    def _(g):
        m_copy(g).wait()


def project(hidden, gain, w_q, w_kv, w_gate, w_up, d_model):
    rows, half = hidden.shape
    feats = w_q.shape[1]
    kv = w_kv.shape[2]
    n_q = w_q.shape[2] // (2 * W)
    n_ff = w_gate.shape[2] // W
    n_all = n_q + n_ff
    n_far = n_q + EARLY
    late = n_ff - EARLY
    dma = pltpu.SemaphoreType.DMA
    any_spec = pl.BlockSpec(memory_space=pl.ANY)
    vmem = pl.BlockSpec(memory_space=pltpu.VMEM)
    cols = w_q.shape[2] + kv
    flops = 2 * rows * feats * (w_q.shape[2] + kv + 2 * w_gate.shape[2])
    return pl.pallas_call(
        functools.partial(project_kernel, n_q, n_ff, d_model),
        name="project",
        out_shape=(
            jax.ShapeDtypeStruct((2, 32, cols), BF16),
            jax.ShapeDtypeStruct((EARLY, 64, W), BF16),
            jax.ShapeDtypeStruct((late, 64, 2 * W), BF16),
            jax.ShapeDtypeStruct((late, 64, 2 * W), BF16),
        ),
        in_specs=[vmem, vmem, any_spec, any_spec, any_spec, any_spec],
        out_specs=(any_spec, any_spec, any_spec, any_spec),
        scratch_shapes=[
            pltpu.VMEM((rows, half), BF16),
            pltpu.VMEM((rows, feats), BF16),
            pltpu.VMEM((rows, 128), F32),
            pltpu.VMEM((8, 8, rows), F32),
            pltpu.VMEM((NBUF1, 2, feats, W), BF16),
            pltpu.VMEM((feats, kv), BF16),
            pltpu.VMEM((n_all, 2, 2, 64, 2 * W), BF16),
            pltpu.VMEM((2, 2, 64, kv), BF16),
            pltpu.VMEM((n_all, 2, 64, 2 * W), BF16),
            pltpu.VMEM((2, 64, kv), BF16),
            pltpu.VMEM((n_all, 64, 2 * W), BF16),
            pltpu.VMEM((64, kv), BF16),
            pltpu.VMEM((n_all, 64, 2 * W), BF16),
            pltpu.VMEM((64, kv), BF16),
            pltpu.VMEM((n_far, 64, 2 * W), BF16),
            pltpu.VMEM((64, kv), BF16),
            pltpu.VMEM((2, 32, cols), BF16),
            pltpu.VMEM((32, cols), BF16),
            pltpu.VMEM((EARLY, 64, W), BF16),
            dma((NBUF1, 2)),
            dma,
            dma((2, 2)),
            dma((8,)),
            dma((8,)),
            dma((n_all + n_q + 2,)),
            dma((n_all + n_q + 2,)),
            dma((n_far + 1,)),
            dma((n_far + 1,)),
            dma((2,)),
            dma((late, 2)),
            dma((EARLY,)),
            dma((2,)),
        ],
        compiler_params=pltpu.CompilerParams(collective_id=0, has_side_effects=True, vmem_limit_bytes=VMEM_LIMIT),
        cost_estimate=pl.CostEstimate(flops=flops, bytes_accessed=feats * (flops // (rows * feats)), transcendentals=0),
    )(hidden, gain, w_q, w_kv, w_gate, w_up)


def attend_kernel(lens, q_ref, kv_ref, k_ref, v_ref, k_out, v_out, o_ref):
    step = pl.program_id(0)
    n_pos = k_ref.shape[2]
    scale = q_ref.shape[2] ** -0.5 * LOG2E
    for s in range(SEQ_STEP):
        length = lens[step * SEQ_STEP + s]
        base = pl.multiple_of((length // 16) * 16, 16)
        k_out[0, s] = k_ref[0, s]
        v_out[0, s] = v_ref[0, s]
        hit = lax.broadcasted_iota(jnp.int32, (16, k_ref.shape[3]), 0) == length - base
        for src, dst, which in ((k_ref, k_out, 0), (v_ref, v_out, 1)):
            old = src[0, s, pl.ds(base, 16), :].astype(F32)
            new = kv_ref[s, which:which + 1, :].astype(F32)
            dst[0, s, pl.ds(base, 16), :] = jnp.where(hit, new, old).astype(BF16)
        scores = lax.dot_general(q_ref[s], k_out[0, s], (((1,), (1,)), ((), ())), preferred_element_type=F32) * scale
        visible = lax.broadcasted_iota(jnp.int32, scores.shape, 1) <= length
        scores = jnp.where(visible, scores, MASKED)
        weights = jnp.exp2(scores - jnp.max(scores, axis=1, keepdims=True))
        probs = (weights * (1.0 / jnp.sum(weights, axis=1, keepdims=True))).astype(BF16)
        o_ref[s] = jnp.dot(probs, v_out[0, s], preferred_element_type=F32).astype(BF16)


def attend(lens, q, kv, k_cache, v_cache):
    seqs, heads, dim = q.shape
    n_pos = k_cache.shape[2]
    cache_spec = pl.BlockSpec((1, SEQ_STEP, n_pos, dim), lambda b, lens: (0, b, 0, 0))
    q_spec = pl.BlockSpec((SEQ_STEP, heads, dim), lambda b, lens: (b, 0, 0))
    return pl.pallas_call(
        attend_kernel,
        name="attend",
        out_shape=(
            jax.ShapeDtypeStruct(k_cache.shape, BF16),
            jax.ShapeDtypeStruct(v_cache.shape, BF16),
            jax.ShapeDtypeStruct(q.shape, BF16),
        ),
        grid_spec=pltpu.PrefetchScalarGridSpec(
            num_scalar_prefetch=1,
            grid=(seqs // SEQ_STEP,),
            in_specs=[q_spec, pl.BlockSpec((SEQ_STEP, 2, dim), lambda b, lens: (b, 0, 0)), cache_spec, cache_spec],
            out_specs=(cache_spec, cache_spec, q_spec),
        ),
        compiler_params=pltpu.CompilerParams(dimension_semantics=("arbitrary",), vmem_limit_bytes=60_000_000),
        cost_estimate=pl.CostEstimate(
            flops=10**10, bytes_accessed=8 * k_cache.size, transcendentals=seqs * heads * n_pos),
    )(lens, q, kv, k_cache, v_cache)


def output_kernel(
    n_ff, n_o, o_in, m_in, keep, recv, hidden, w_o, w_down, out,
    acts, wbuf, acc, keep_v, recv_v, h_v, y_src, y_dst,
    w_sem, in_sems, m_sem, o_sems, far_send, far_recv, near_send, near_recv, y_sems,
):
    xi = lax.axis_index("x")
    yj = lax.axis_index("yz")
    core = lax.rem(xi, 2)
    mate = xi + 1 - 2 * core
    across = lax.rem(xi + 2, 4)
    other_y = 1 - yj
    n_m = n_ff // GROUP
    n_g = n_m + n_o // GROUP
    n_early = EARLY // GROUP
    depth = GROUP * W
    d_out = w_down.shape[2]
    half = d_out // 2

    barrier = pltpu.get_barrier_semaphore()
    for x_, y_ in ((mate, yj), (across, yj), (xi, other_y)):
        pl.semaphore_signal(barrier, inc=1, **dev(x=x_, yz=y_))

    def block(h, g, owner):
        return acts.at[h, pl.ds(GROUP * g, GROUP), pl.ds(pl.multiple_of(owner * 32, 32), 32)]

    def m_block(h, g):
        return m_in.at[pl.ds(GROUP * g, GROUP), pl.ds(32 * h, 32)]

    def m_copy(h, g):
        return pltpu.make_async_copy(m_block(h, g), block(h, g, xi), m_sem.at[h, g])

    def o_block(h):
        return acts.at[h, pl.ds(n_ff, n_o), pl.ds(pl.multiple_of(xi * 32, 32), 32)]

    keep_copy = pltpu.make_async_copy(keep, keep_v, in_sems.at[0])
    recv_copy = pltpu.make_async_copy(recv, recv_v, in_sems.at[1])
    h_copy = pltpu.make_async_copy(hidden, h_v, in_sems.at[2])
    o_own = pltpu.make_async_copy(o_in.at[yj], o_block(yj), in_sems.at[3])

    def start_weights(s):
        slot = lax.rem(s, NBUF3)
        g = lax.rem(s, n_g)

        @pl.when(g < n_m)
        def _():
            pltpu.make_async_copy(
                w_down.at[0, pl.ds(pl.multiple_of(g * depth, W), depth)], wbuf.at[slot], w_sem.at[slot]).start()

        @pl.when(g >= n_m)
        def _():
            pltpu.make_async_copy(
                w_o.at[0, pl.ds(pl.multiple_of((g - n_m) * depth, W), depth)], wbuf.at[slot], w_sem.at[slot]).start()

    pl.semaphore_wait(barrier, 3)

    def far_copy(h, g, src):
        return pltpu.make_async_remote_copy(
            src_ref=src, dst_ref=block(h, g, xi), send_sem=far_send.at[h, g], recv_sem=far_recv.at[h, g],
            **dev(x=across, yz=yj))

    def near_copy(h, g, which, src):
        return pltpu.make_async_remote_copy(
            src_ref=src, dst_ref=block(h, g, xi if which == 0 else across), send_sem=near_send.at[h, g, which],
            recv_sem=near_recv.at[h, g, which], **dev(x=mate, yz=yj))

    o_copy = pltpu.make_async_remote_copy(
        src_ref=o_in.at[other_y], dst_ref=o_block(yj), send_sem=o_sems.at[0], recv_sem=o_sems.at[1],
        **dev(x=xi, yz=other_y))

    def give(h, g, src):
        far_copy(h, g, src).start()
        near_copy(h, g, 0, src).start()

    def give_early(h):
        @pl.loop(0, n_early)
        def _(g):
            give(h, g, m_block(h, g))

    def give_late(h):
        @pl.loop(n_early, n_m)
        def _(g):
            for k in range(GROUP):
                t = GROUP * g + k - EARLY
                rows = slice(32 * h, 32 * h + 32)
                z = keep_v[t, rows].astype(F32) + recv_v[t, rows].astype(F32)
                acts[h, GROUP * g + k, pl.ds(pl.multiple_of(xi * 32, 32), 32)] = silu_mul(z[:, :W], z[:, W:])
            give(h, g, block(h, g, xi))

    def give_o(h):
        @pl.loop(n_m, n_g)
        def _(g):
            give(h, g, block(h, g, xi))

    give_early(0)
    o_copy.start()
    o_own.start()
    keep_copy.start()
    recv_copy.start()
    for h in range(2):
        for g in range(n_early):
            m_copy(h, g).start()
    for s in range(NBUF3):
        start_weights(jnp.int32(s))
    h_copy.start()
    keep_copy.wait()
    recv_copy.wait()
    give_late(0)
    acc[...] = jnp.zeros_like(acc)
    o_own.wait()
    o_copy.wait_recv()
    give_o(0)
    give_early(1)
    give_late(1)
    give_o(1)
    for h in range(2):
        for g in range(n_early):
            m_copy(h, g).wait()

    def forward(h, g):
        far_copy(h, g, block(h, g, xi)).wait_recv()
        near_copy(h, g, 1, block(h, g, across)).start()

    def multiply(h, g):
        s = h * n_g + g
        slot = lax.rem(s, NBUF3)
        pltpu.make_async_copy(w_down.at[0, pl.ds(0, depth)], wbuf.at[slot], w_sem.at[slot]).wait()
        near_copy(h, g, 0, block(h, g, xi)).wait_recv()
        near_copy(h, g, 1, block(h, g, across)).wait_recv()
        for n in range(d_out // W):
            cols = slice(n * W, (n + 1) * W)
            total = acc[h, :, cols]
            for k in range(GROUP):
                total += jnp.dot(
                    acts[h, GROUP * g + k], wbuf[slot, k * W:(k + 1) * W, cols], preferred_element_type=F32)
            acc[h, :, cols] = total

        @pl.when(s + NBUF3 < 2 * n_g)
        def _():
            start_weights(s + NBUF3)

    def cols_of(j):
        return pl.ds(pl.multiple_of(j * half, 128), half)

    def y_copy(h):
        return pltpu.make_async_remote_copy(
            src_ref=y_src.at[h], dst_ref=y_dst.at[h], send_sem=y_sems.at[h, 0], recv_sem=y_sems.at[h, 1],
            **dev(x=xi, yz=other_y))

    def exchange(h):
        y_src[h] = acc[h, :, cols_of(other_y)].astype(BF16)
        y_copy(h).start()

    def finalize(h):
        y_copy(h).wait_recv()
        total = acc[h, :, cols_of(yj)] + y_dst[h].astype(F32)
        out[:, h] = (h_v[:, h].astype(F32) + total.reshape(4, 32, half)).astype(BF16)

    forward(0, 0)

    @pl.loop(1, n_g)
    def _(g):
        forward(0, g)
        multiply(0, g - 1)

    forward(1, 0)
    multiply(0, n_g - 1)
    exchange(0)
    h_copy.wait()

    @pl.loop(1, n_g)
    def _(g):
        forward(1, g)
        multiply(1, g - 1)

    multiply(1, n_g - 1)
    exchange(1)
    finalize(0)
    finalize(1)

    o_copy.wait_send()
    for h in range(2):
        y_copy(h).wait_send()

        @pl.loop(0, n_g)
        def _(g):
            far_copy(h, g, block(h, g, xi)).wait_send()
            near_copy(h, g, 0, block(h, g, xi)).wait_send()
            near_copy(h, g, 1, block(h, g, across)).wait_send()


def finish(o, m_early, keep, recv, hidden, w_o, w_down):
    rows, half = hidden.shape
    n_ff = w_down.shape[1] // W
    n_o = w_o.shape[1] // W
    n_g = (n_ff + n_o) // GROUP
    d_out = w_down.shape[2]
    dma = pltpu.SemaphoreType.DMA
    any_spec = pl.BlockSpec(memory_space=pl.ANY)
    vmem = pl.BlockSpec(memory_space=pltpu.VMEM)
    flops = 2 * rows * d_out * (w_down.shape[1] + w_o.shape[1])
    out = pl.pallas_call(
        functools.partial(output_kernel, n_ff, n_o),
        name="finish",
        out_shape=jax.ShapeDtypeStruct((4, 2, 32, half), BF16),
        in_specs=[any_spec] * 7,
        out_specs=vmem,
        scratch_shapes=[
            pltpu.VMEM((2, n_ff + n_o, rows // 2, W), BF16),
            pltpu.VMEM((NBUF3, GROUP * W, d_out), BF16),
            pltpu.VMEM((2, rows // 2, d_out), F32),
            pltpu.VMEM(keep.shape, BF16),
            pltpu.VMEM(recv.shape, BF16),
            pltpu.VMEM((4, 2, 32, half), BF16),
            pltpu.VMEM((2, rows // 2, half), BF16),
            pltpu.VMEM((2, rows // 2, half), BF16),
            dma((NBUF3,)),
            dma((4,)),
            dma((2, EARLY // GROUP)),
            dma((2,)),
            dma((2, n_g)),
            dma((2, n_g)),
            dma((2, n_g, 2)),
            dma((2, n_g, 2)),
            dma((2, 2)),
        ],
        compiler_params=pltpu.CompilerParams(collective_id=1, has_side_effects=True, vmem_limit_bytes=56_000_000),
        cost_estimate=pl.CostEstimate(flops=flops, bytes_accessed=2 * d_out * (w_down.shape[1] + w_o.shape[1]), transcendentals=0),
    )(o, m_early, keep, recv, hidden.reshape(4, 2, 32, half), w_o, w_down)
    return out.reshape(rows, half)


def solution(mesh):
    x_size = mesh.shape["x"]
    y_size = mesh.shape["yz"]
    row_spec = P("dp", ("x", "yz"))
    tile_in = P(None, "x", "yz")
    tile_out = P(None, "yz", "x")
    cache_spec = P(None, ("dp", "x", "yz"))
    len_spec = P(("dp", "x", "yz"))

    def device_step(hidden, norm_gain, w_q, w_kv, w_gate, w_up, w_o, w_down, k_cache, v_cache, seq_len):
        d_model = hidden.shape[1] * x_size * y_size
        seqs = k_cache.shape[1]
        dim = k_cache.shape[3]
        q_cols = w_q.shape[2]
        heads = q_cols // dim
        qkv, m_early, keep, send = project(hidden, norm_gain, w_q, w_kv, w_gate, w_up, d_model)
        recv = lax.ppermute(send, "x", [(i, (i + x_size // 2) % x_size) for i in range(x_size)])
        q = qkv[:, :, :q_cols].reshape(y_size, seqs, heads, dim).transpose(1, 0, 2, 3).reshape(seqs, y_size * heads, dim)
        kv = qkv[:, :, q_cols:].transpose(1, 0, 2)
        k_new, v_new, o = attend(seq_len, q, kv, k_cache, v_cache)
        o = o.reshape(seqs, y_size, q_cols // W, W).transpose(1, 2, 0, 3)
        hidden_out = finish(o, m_early, keep, recv, hidden, w_o, w_down)
        return hidden_out, k_new, v_new

    return jax.shard_map(
        device_step,
        mesh=mesh,
        in_specs=(row_spec, P(None, "x"), tile_in, tile_in, tile_in, tile_in, tile_out, tile_out, cache_spec, cache_spec, len_spec),
        out_specs=(row_spec, cache_spec, cache_spec),
        check_vma=False,
    )
```

```python
import functools

import jax
import jax.numpy as jnp
from jax import lax
from jax.experimental import pallas as pl
from jax.experimental.pallas import tpu as pltpu
from jax.sharding import PartitionSpec as P

NORM_EPS = 1e-6
W = 512
NBUF1 = 4
NBUF3 = 6
GROUP = 3
PARTS = ((0, 32), (32, 16), (48, 16))
EARLY = 12
SEQ_STEP = 2
VMEM_LIMIT = 64_000_000
F32 = jnp.float32
BF16 = jnp.bfloat16
LOG2E = 1.4426950408889634
MASKED = -1e30


def dev(**axes):
    return dict(device_id=axes, device_id_type=pl.DeviceIdType.MESH)


def silu_mul(gate, up):
    gate = gate.astype(BF16).astype(F32)
    up = up.astype(BF16).astype(F32)
    return (jax.nn.silu(gate) * up).astype(BF16)


def project_kernel(
    n_q, n_ff, d_model, hidden, gain, wq, wkv, wg, wu,
    qkv_out, keep_out, recv_out, send_out,
    h_own, h_other, u, inv_all, sq_all, wbuf, wkv_buf, part, part_kv, near, near_kv, keep, keep_kv, far_src,
    far_src_kv, far_q, far_kv, z_rows, z_other,
    w_sem, wkv_sem, h_in, h_sems, sq_send, sq_recv, near_send, near_recv, qn_send, qn_recv, kn_send, kn_recv,
    far_send, far_recv, qf_send, qf_recv, kf_send, kf_recv, y_sems, out_sem, qkv_sem,
):
    xi = lax.axis_index("x")
    yj = lax.axis_index("yz")
    core = lax.rem(xi, 2)
    chip = xi // 2
    mate = xi + 1 - 2 * core
    across = lax.rem(xi + 2, 4)
    other_y = 1 - yj
    me = xi * 2 + yj
    half = hidden.shape[-1]
    n_all = n_q + n_ff
    to_mate = dev(x=mate, yz=yj)
    to_across = dev(x=across, yz=yj)

    barrier = pltpu.get_barrier_semaphore()
    for k in range(1, 8):
        peer = lax.rem(me + k, 8)
        pl.semaphore_signal(barrier, inc=1, **dev(x=peer // 2, yz=lax.rem(peer, 2)))
    h_load = pltpu.make_async_copy(hidden, h_own, h_in)
    h_load.start()

    def start_weights(g):
        slot = lax.rem(g, NBUF1)

        @pl.when(g < n_q)
        def _():
            for k in range(2):
                cols = pl.ds(pl.multiple_of((2 * g + k) * W, W), W)
                pltpu.make_async_copy(wq.at[0, :, cols], wbuf.at[slot, k], w_sem.at[slot, k]).start()

        @pl.when(g >= n_q)
        def _():
            cols = pl.ds(pl.multiple_of((g - n_q) * W, W), W)
            pltpu.make_async_copy(wg.at[0, :, cols], wbuf.at[slot, 0], w_sem.at[slot, 0]).start()
            pltpu.make_async_copy(wu.at[0, :, cols], wbuf.at[slot, 1], w_sem.at[slot, 1]).start()

    def wait_weights(slot, k):
        pltpu.make_async_copy(wq.at[0, :, pl.ds(0, W)], wbuf.at[slot, k], w_sem.at[slot, k]).wait()

    for g in range(NBUF1):
        start_weights(jnp.int32(g))
    kv_copy = pltpu.make_async_copy(wkv.at[0], wkv_buf, wkv_sem)
    kv_copy.start()

    h_load.wait()
    h_f32 = h_own[...].reshape(256, half).astype(F32)
    sq_all[me] = lax.dot_general(
        jnp.ones((8, half), F32), h_f32 * h_f32, (((1,), (1,)), ((), ())),
        precision=lax.Precision.HIGHEST, preferred_element_type=F32)
    pl.semaphore_wait(barrier, 7)

    def sq_copy(peer, src):
        return pltpu.make_async_remote_copy(
            src_ref=sq_all.at[src], dst_ref=sq_all.at[src], send_sem=sq_send.at[peer], recv_sem=sq_recv.at[src],
            **dev(x=peer // 2, yz=lax.rem(peer, 2)))

    def side_of(step):
        return 1 - chip if step < 2 else chip

    def h_copy(step):
        block = (side_of(step), slice(None), step % 2)
        return pltpu.make_async_remote_copy(
            src_ref=h_own.at[block], dst_ref=h_other.at[block],
            send_sem=h_sems.at[step, 0], recv_sem=h_sems.at[step, 1], **dev(x=xi, yz=other_y))

    for k in range(1, 8):
        sq_copy(lax.rem(me + k, 8), me).start()
    for step in range(4):
        h_copy(step).start()
    for k in range(1, 8):
        peer = lax.rem(me + k, 8)
        sq_copy(peer, peer).wait_recv()
    total = jnp.sum(sq_all[...], axis=0)
    inv = lax.rsqrt(total / d_model + NORM_EPS)
    inv_all[...] = jnp.transpose(jnp.concatenate([inv] * 16, axis=0)).reshape(inv_all.shape)

    def normalize(values, step, which):
        cols = pl.ds(pl.multiple_of(which * half, 128), half)
        side, piece = side_of(step), step % 2
        inv_rows = inv_all[side, :, piece].reshape(64, 128)[:, :1]
        res = (values[side, :, piece].reshape(64, half).astype(F32) * inv_rows
               * gain[:, cols].astype(F32)).astype(BF16)
        u[side, piece, :, cols] = res

    def near_copy(g):
        return pltpu.make_async_remote_copy(
            src_ref=part.at[g, :, :, 1 - core], dst_ref=near.at[g], send_sem=near_send.at[g],
            recv_sem=near_recv.at[g], **to_mate)

    def near_copy_q(g, step):
        side, piece = side_of(step), step % 2
        return pltpu.make_async_remote_copy(
            src_ref=part.at[g, side, piece, 1 - core], dst_ref=near.at[g, side, piece],
            send_sem=qn_send.at[g, step], recv_sem=qn_recv.at[g, step], **to_mate)

    def near_copy_kv(step):
        side, piece = side_of(step), step % 2
        return pltpu.make_async_remote_copy(
            src_ref=part_kv.at[side, piece, 1 - core], dst_ref=near_kv.at[side, piece],
            send_sem=kn_send.at[step], recv_sem=kn_recv.at[step], **to_mate)

    def far_copy(g):
        return pltpu.make_async_remote_copy(
            src_ref=far_src.at[g], dst_ref=recv_out.at[g - n_q], send_sem=far_send.at[g - n_q],
            recv_sem=far_recv.at[g - n_q], **to_across)

    def far_copy_q(g, step):
        rows = slice(32 * step, 32 * step + 32)
        return pltpu.make_async_remote_copy(
            src_ref=far_src.at[g, rows], dst_ref=far_q.at[g, rows], send_sem=qf_send.at[g, step],
            recv_sem=qf_recv.at[g, step], **to_across)

    def far_copy_kv(step):
        rows = slice(32 * step, 32 * step + 32)
        return pltpu.make_async_remote_copy(
            src_ref=far_src_kv.at[rows], dst_ref=far_kv.at[rows], send_sem=kf_send.at[step],
            recv_sem=kf_recv.at[step], **to_across)

    def keep_copy(g):
        return pltpu.make_async_copy(keep.at[g], keep_out.at[g - n_q], out_sem.at[g - n_q, 0])

    def send_copy(g):
        k = g - n_q
        return pltpu.make_async_copy(far_src.at[g], send_out.at[k - EARLY], out_sem.at[k, 1])

    def add(a, b):
        return (a.astype(F32) + b.astype(F32)).astype(BF16)

    def multiply(g):
        slot = lax.rem(g, NBUF1)
        for k in range(2):
            wait_weights(slot, k)
            res = jnp.dot(u[...].reshape(256, u.shape[-1]), wbuf[slot, k], preferred_element_type=F32).astype(BF16)
            part[g, :, :, :, :, k * W:(k + 1) * W] = res.reshape(2, 2, 2, 32, W)
        near_copy(g).start()

        @pl.when(g + NBUF1 < n_all)
        def _():
            start_weights(g + NBUF1)

    def reduce_near(g, send):
        near_copy(g).wait_recv()
        far_src[g] = add(part[g, 1 - chip, :, core], near[g, 1 - chip]).reshape(64, 2 * W)
        if send:
            far_copy(g).start()
        else:
            send_copy(g).start()
        keep[g] = add(part[g, chip, :, core], near[g, chip]).reshape(64, 2 * W)
        keep_copy(g).start()

    for step in range(4):
        side, piece = side_of(step), step % 2
        rows = slice(32 * piece, 32 * piece + 32)
        normalize(h_own, step, yj)
        h_copy(step).wait_recv()
        normalize(h_other, step, other_y)

        def reduce_q(g):
            near_copy_q(g, step).wait_recv()
            total_q = add(part[g, side, piece, core], near[g, side, piece])
            if step < 2:
                far_src[g, rows] = total_q
                far_copy_q(g, step).start()
            else:
                keep[g, rows] = total_q

        for g in range(n_q):
            for k in range(2):
                if step == 0:
                    wait_weights(g, k)
                res = jnp.dot(u[side, piece], wbuf[g, k], preferred_element_type=F32).astype(BF16)
                part[g, side, piece, :, :, k * W:(k + 1) * W] = res.reshape(2, 32, W)
            near_copy_q(g, step).start()
            if step == 3:
                start_weights(jnp.int32(g + NBUF1))
            if g >= 1:
                reduce_q(g - 1)
        if step == 0:
            kv_copy.wait()
        res = jnp.dot(u[side, piece], wkv_buf[...], preferred_element_type=F32).astype(BF16)
        part_kv[side, piece] = res.reshape(2, 32, res.shape[1])
        near_copy_kv(step).start()
        reduce_q(n_q - 1)
        near_copy_kv(step).wait_recv()
        total_kv = add(part_kv[side, piece, core], near_kv[side, piece])
        if step < 2:
            far_src_kv[rows] = total_kv
            far_copy_kv(step).start()
        else:
            keep_kv[rows] = total_kv

    n_far = n_q + EARLY

    @pl.loop(n_q, n_far)
    def _(g):
        multiply(g)

        @pl.when(g >= n_q + 1)
        def _():
            reduce_near(g - 1, True)

    q_cols = n_q * 2 * W
    for g in range(n_q):
        for step in range(2):
            far_copy_q(g, step).wait_recv()
        z_rows[:, :, g * 2 * W:(g + 1) * 2 * W] = add(keep[g], far_q[g]).reshape(2, 32, 2 * W)
    for step in range(2):
        far_copy_kv(step).wait_recv()
    z_kv = add(keep_kv[...], far_kv[...])
    z_rows[:, :, q_cols:] = z_kv.reshape(2, 32, z_kv.shape[1])
    y_copy = pltpu.make_async_remote_copy(
        src_ref=z_rows.at[other_y], dst_ref=z_other, send_sem=y_sems.at[0], recv_sem=y_sems.at[1],
        **dev(x=xi, yz=other_y))
    y_copy.start()
    qkv_own = pltpu.make_async_copy(z_rows.at[yj], qkv_out.at[yj], qkv_sem.at[0])
    qkv_own.start()

    multiply(n_far)
    reduce_near(n_far - 1, True)

    @pl.loop(n_far + 1, n_all)
    def _(g):
        multiply(g)
        reduce_near(g - 1, False)

    reduce_near(n_all - 1, False)
    y_copy.wait_recv()
    qkv_other = pltpu.make_async_copy(z_other, qkv_out.at[other_y], qkv_sem.at[1])
    qkv_other.start()

    for step in range(4):
        h_copy(step).wait_send()
        near_copy_kv(step).wait_send()
        for g in range(n_q):
            near_copy_q(g, step).wait_send()
    for step in range(2):
        far_copy_kv(step).wait_send()
        for g in range(n_q):
            far_copy_q(g, step).wait_send()
    for k in range(1, 8):
        sq_copy(lax.rem(me + k, 8), me).wait_send()
    y_copy.wait_send()

    @pl.loop(n_q, n_all)
    def _(g):
        near_copy(g).wait_send()
        keep_copy(g).wait()

    @pl.loop(n_far, n_all)
    def _(g):
        send_copy(g).wait()

    qkv_own.wait()
    qkv_other.wait()

    @pl.loop(n_q, n_far)
    def _(g):
        far_copy(g).wait_send()
        far_copy(g).wait_recv()


def project(hidden, gain, w_q, w_kv, w_gate, w_up, d_model):
    rows, half = hidden.shape
    feats = w_q.shape[1]
    kv = w_kv.shape[2]
    n_q = w_q.shape[2] // (2 * W)
    n_ff = w_gate.shape[2] // W
    n_all = n_q + n_ff
    late = n_ff - EARLY
    dma = pltpu.SemaphoreType.DMA
    any_spec = pl.BlockSpec(memory_space=pl.ANY)
    vmem = pl.BlockSpec(memory_space=pltpu.VMEM)
    cols = w_q.shape[2] + kv
    flops = 2 * rows * feats * (w_q.shape[2] + kv + 2 * w_gate.shape[2])
    h_shape = (2, 2, 2, 32, half)
    return pl.pallas_call(
        functools.partial(project_kernel, n_q, n_ff, d_model),
        name="project",
        out_shape=(
            jax.ShapeDtypeStruct((2, 32, cols), BF16),
            jax.ShapeDtypeStruct((n_ff, 64, 2 * W), BF16),
            jax.ShapeDtypeStruct((EARLY, 64, 2 * W), BF16),
            jax.ShapeDtypeStruct((late, 64, 2 * W), BF16),
        ),
        in_specs=[any_spec, vmem, any_spec, any_spec, any_spec, any_spec],
        out_specs=(any_spec, any_spec, any_spec, any_spec),
        scratch_shapes=[
            pltpu.VMEM(h_shape, BF16),
            pltpu.VMEM(h_shape, BF16),
            pltpu.VMEM((2, 2, 64, feats), BF16),
            pltpu.VMEM((2, 2, 2, 32, 128), F32),
            pltpu.VMEM((8, 8, rows), F32),
            pltpu.VMEM((NBUF1, 2, feats, W), BF16),
            pltpu.VMEM((feats, kv), BF16),
            pltpu.VMEM((n_all, 2, 2, 2, 32, 2 * W), BF16),
            pltpu.VMEM((2, 2, 2, 32, kv), BF16),
            pltpu.VMEM((n_all, 2, 2, 32, 2 * W), BF16),
            pltpu.VMEM((2, 2, 32, kv), BF16),
            pltpu.VMEM((n_all, 64, 2 * W), BF16),
            pltpu.VMEM((64, kv), BF16),
            pltpu.VMEM((n_all, 64, 2 * W), BF16),
            pltpu.VMEM((64, kv), BF16),
            pltpu.VMEM((n_q, 64, 2 * W), BF16),
            pltpu.VMEM((64, kv), BF16),
            pltpu.VMEM((2, 32, cols), BF16),
            pltpu.VMEM((32, cols), BF16),
            dma((NBUF1, 2)),
            dma,
            dma,
            dma((4, 2)),
            dma((8,)),
            dma((8,)),
            dma((n_all,)),
            dma((n_all,)),
            dma((n_q, 4)),
            dma((n_q, 4)),
            dma((4,)),
            dma((4,)),
            dma((EARLY,)),
            dma((EARLY,)),
            dma((n_q, 2)),
            dma((n_q, 2)),
            dma((2,)),
            dma((2,)),
            dma((2,)),
            dma((n_ff, 2)),
            dma((2,)),
        ],
        compiler_params=pltpu.CompilerParams(collective_id=0, has_side_effects=True, vmem_limit_bytes=VMEM_LIMIT),
        cost_estimate=pl.CostEstimate(flops=flops, bytes_accessed=feats * (flops // (rows * feats)), transcendentals=0),
    )(hidden.reshape(h_shape), gain, w_q, w_kv, w_gate, w_up)


def attend_kernel(lens, q_ref, kv_ref, k_ref, v_ref, k_out, v_out, o_ref):
    step = pl.program_id(0)
    n_pos = k_ref.shape[2]
    scale = q_ref.shape[2] ** -0.5 * LOG2E
    for s in range(SEQ_STEP):
        length = lens[step * SEQ_STEP + s]
        base = pl.multiple_of((length // 16) * 16, 16)
        k_out[0, s] = k_ref[0, s]
        v_out[0, s] = v_ref[0, s]
        hit = lax.broadcasted_iota(jnp.int32, (16, k_ref.shape[3]), 0) == length - base
        for src, dst, which in ((k_ref, k_out, 0), (v_ref, v_out, 1)):
            old = src[0, s, pl.ds(base, 16), :].astype(F32)
            new = kv_ref[s, which:which + 1, :].astype(F32)
            dst[0, s, pl.ds(base, 16), :] = jnp.where(hit, new, old).astype(BF16)
        scores = lax.dot_general(q_ref[s], k_out[0, s], (((1,), (1,)), ((), ())), preferred_element_type=F32) * scale
        visible = lax.broadcasted_iota(jnp.int32, scores.shape, 1) <= length
        scores = jnp.where(visible, scores, MASKED)
        weights = jnp.exp2(scores - jnp.max(scores, axis=1, keepdims=True))
        probs = (weights * (1.0 / jnp.sum(weights, axis=1, keepdims=True))).astype(BF16)
        o_ref[s] = jnp.dot(probs, v_out[0, s], preferred_element_type=F32).astype(BF16)


def attend(lens, q, kv, k_cache, v_cache):
    seqs, heads, dim = q.shape
    n_pos = k_cache.shape[2]
    cache_spec = pl.BlockSpec((1, SEQ_STEP, n_pos, dim), lambda b, lens: (0, b, 0, 0))
    q_spec = pl.BlockSpec((SEQ_STEP, heads, dim), lambda b, lens: (b, 0, 0))
    return pl.pallas_call(
        attend_kernel,
        name="attend",
        out_shape=(
            jax.ShapeDtypeStruct(k_cache.shape, BF16),
            jax.ShapeDtypeStruct(v_cache.shape, BF16),
            jax.ShapeDtypeStruct(q.shape, BF16),
        ),
        grid_spec=pltpu.PrefetchScalarGridSpec(
            num_scalar_prefetch=1,
            grid=(seqs // SEQ_STEP,),
            in_specs=[q_spec, pl.BlockSpec((SEQ_STEP, 2, dim), lambda b, lens: (b, 0, 0)), cache_spec, cache_spec],
            out_specs=(cache_spec, cache_spec, q_spec),
        ),
        compiler_params=pltpu.CompilerParams(dimension_semantics=("arbitrary",), vmem_limit_bytes=66_000_000),
        cost_estimate=pl.CostEstimate(
            flops=10**10, bytes_accessed=8 * k_cache.size, transcendentals=seqs * heads * n_pos),
    )(lens, q, kv, k_cache, v_cache)


def output_kernel(
    n_ff, n_o, o_in, keep, recv_e, recv_l, hidden, w_o, w_down, out,
    acts, wbuf, acc, keep_v, recv_v, h_v, y_src, y_dst,
    w_sem, keep_sem, recv_sem, h_sem, oo_sems, on_send, on_recv, far_send, far_recv, near_send, near_recv, y_sems,
):
    xi = lax.axis_index("x")
    yj = lax.axis_index("yz")
    core = lax.rem(xi, 2)
    mate = xi + 1 - 2 * core
    across = lax.rem(xi + 2, 4)
    other_y = 1 - yj
    n_m = n_ff // GROUP
    n_g = n_m + n_o // GROUP
    n_early = EARLY // GROUP
    depth = GROUP * W
    d_out = w_down.shape[2]
    half = d_out // 2

    barrier = pltpu.get_barrier_semaphore()
    for x_, y_ in ((mate, yj), (across, yj), (xi, other_y)):
        pl.semaphore_signal(barrier, inc=1, **dev(x=x_, yz=y_))

    def keep_copy(g):
        return pltpu.make_async_copy(
            keep.at[pl.ds(GROUP * g, GROUP)], keep_v.at[pl.ds(GROUP * g, GROUP)], keep_sem.at[g])

    def recv_copy(g):
        src = recv_e.at[pl.ds(GROUP * g, GROUP)] if g < n_early else recv_l.at[pl.ds(GROUP * (g - n_early), GROUP)]
        return pltpu.make_async_copy(src, recv_v.at[pl.ds(GROUP * g, GROUP)], recv_sem.at[g])

    for g in range(n_m):
        keep_copy(g).start()
        recv_copy(g).start()

    def rows_of(p, owner):
        off, size = PARTS[p]
        return pl.ds(pl.multiple_of(4 * off + owner * size, 16), size)

    def block(p, g, owner):
        return acts.at[pl.ds(GROUP * g, GROUP), rows_of(p, owner)]

    def o_rows(s):
        row = (1 - yj) * (32 * xi + 16 * s) + yj * (128 + 64 * s + 16 * xi)
        return acts.at[pl.ds(n_ff, n_o), pl.ds(pl.multiple_of(row, 16), 16)]

    def o_own(s):
        return pltpu.make_async_copy(o_in.at[yj, :, pl.ds(16 * s, 16)], o_rows(s), oo_sems.at[s])

    def o_copy(s):
        return pltpu.make_async_remote_copy(
            src_ref=o_in.at[other_y, :, pl.ds(16 * s, 16)], dst_ref=o_rows(s), send_sem=on_send.at[s],
            recv_sem=on_recv.at[s], **dev(x=xi, yz=other_y))

    h_load = pltpu.make_async_copy(hidden, h_v, h_sem)

    def load_weights(g):
        slot = lax.rem(g, NBUF3)

        @pl.when(g < n_m)
        def _():
            pltpu.make_async_copy(
                w_down.at[0, pl.ds(pl.multiple_of(g * depth, W), depth)], wbuf.at[slot], w_sem.at[slot]).start()

        @pl.when(g >= n_m)
        def _():
            pltpu.make_async_copy(
                w_o.at[0, pl.ds(pl.multiple_of((g - n_m) * depth, W), depth)], wbuf.at[slot], w_sem.at[slot]).start()

    def far_copy(p, g):
        return pltpu.make_async_remote_copy(
            src_ref=block(p, g, xi), dst_ref=block(p, g, xi), send_sem=far_send.at[p, g], recv_sem=far_recv.at[p, g],
            **dev(x=across, yz=yj))

    def near_copy(p, g, which):
        rows = block(p, g, xi if which == 0 else across)
        return pltpu.make_async_remote_copy(
            src_ref=rows, dst_ref=rows, send_sem=near_send.at[p, g, which], recv_sem=near_recv.at[p, g, which],
            **dev(x=mate, yz=yj))

    def give(p, g):
        far_copy(p, g).start()
        near_copy(p, g, 0).start()

    def give_m(p, g):
        off, size = PARTS[p]
        for k in range(GROUP):
            t = GROUP * g + k
            z = keep_v[t, off:off + size].astype(F32) + recv_v[t, off:off + size].astype(F32)
            acts[t, rows_of(p, xi)] = silu_mul(z[:, :W], z[:, W:])
        give(p, g)

    pl.semaphore_wait(barrier, 3)
    for g in range(n_m):
        keep_copy(g).wait()
        recv_copy(g).wait()
        give_m(0, g)
        if g == 0:
            for s in range(2):
                o_copy(s).start()
                o_own(s).start()
            for s in range(NBUF3):
                load_weights(jnp.int32(s))
            h_load.start()
    acc[...] = jnp.zeros_like(acc)
    for s in range(2):
        o_own(s).wait()
        o_copy(s).wait_recv()

    def chunk(p, k):
        return k if p % 2 == 0 else n_g - 1 - k

    for g in range(n_m, n_g):
        give(0, g)
    for p in range(1, len(PARTS)):
        @pl.loop(0, n_g)
        def _(k):
            g = chunk(p, k)

            @pl.when(g < n_m)
            def _():
                give_m(p, g)

            @pl.when(g >= n_m)
            def _():
                give(p, g)

    def forward(p, k):
        g = chunk(p, k)
        far_copy(p, g).wait_recv()
        near_copy(p, g, 1).start()

    def multiply(p, k):
        g = chunk(p, k)
        slot = lax.rem(g, NBUF3)

        @pl.when(k >= (0 if p == 0 else NBUF3))
        def _():
            pltpu.make_async_copy(w_down.at[0, pl.ds(0, depth)], wbuf.at[slot], w_sem.at[slot]).wait()

        near_copy(p, g, 0).wait_recv()
        near_copy(p, g, 1).wait_recv()
        off, size = PARTS[p]
        rows = slice(4 * off, 4 * (off + size))
        for n in range(d_out // W):
            cols = slice(n * W, (n + 1) * W)
            total = acc[rows, cols]
            for j in range(GROUP):
                total += jnp.dot(
                    acts[GROUP * g + j, rows], wbuf[slot, j * W:(j + 1) * W, cols], preferred_element_type=F32)
            acc[rows, cols] = total

        @pl.when(k + NBUF3 < n_g)
        def _():
            load_weights(chunk(p, k + NBUF3))

    def cols_of(j):
        return pl.ds(pl.multiple_of(j * half, 128), half)

    def y_copy(p):
        rows = slice(4 * PARTS[p][0], 4 * sum(PARTS[p]))
        return pltpu.make_async_remote_copy(
            src_ref=y_src.at[rows], dst_ref=y_dst.at[rows], send_sem=y_sems.at[p, 0], recv_sem=y_sems.at[p, 1],
            **dev(x=xi, yz=other_y))

    def exchange(p):
        rows = slice(4 * PARTS[p][0], 4 * sum(PARTS[p]))
        y_src[rows] = acc[rows, cols_of(other_y)].astype(BF16)
        y_copy(p).start()

    def finalize(p):
        off, size = PARTS[p]
        rows = slice(4 * off, 4 * (off + size))
        y_copy(p).wait_recv()
        total = (acc[rows, cols_of(yj)] + y_dst[rows].astype(F32)).reshape(4, size, half)
        out[:, off:off + size] = (h_v[:, off:off + size].astype(F32) + total).astype(BF16)

    for p in range(len(PARTS)):
        forward(p, jnp.int32(0))
        if p > 0:
            multiply(p - 1, jnp.int32(n_g - 1))
            exchange(p - 1)
        if p == 1:
            h_load.wait()

        @pl.loop(1, n_g)
        def _(k):
            forward(p, k)
            multiply(p, k - 1)

        if p > 0:
            finalize(p - 1)

    last = len(PARTS) - 1
    multiply(last, jnp.int32(n_g - 1))
    exchange(last)
    for s in range(2):
        o_copy(s).wait_send()
    for p in range(len(PARTS)):
        @pl.loop(0, n_g)
        def _(g):
            far_copy(p, g).wait_send()
            near_copy(p, g, 0).wait_send()
            near_copy(p, g, 1).wait_send()

    finalize(last)
    for p in range(len(PARTS)):
        y_copy(p).wait_send()


def finish(o, keep, recv_e, recv_l, hidden, w_o, w_down):
    rows, half = hidden.shape
    n_ff = w_down.shape[1] // W
    n_o = w_o.shape[1] // W
    n_m = n_ff // GROUP
    n_g = n_m + n_o // GROUP
    n_p = len(PARTS)
    d_out = w_down.shape[2]
    dma = pltpu.SemaphoreType.DMA
    any_spec = pl.BlockSpec(memory_space=pl.ANY)
    vmem = pl.BlockSpec(memory_space=pltpu.VMEM)
    flops = 2 * rows * d_out * (w_down.shape[1] + w_o.shape[1])
    out = pl.pallas_call(
        functools.partial(output_kernel, n_ff, n_o),
        name="finish",
        out_shape=jax.ShapeDtypeStruct((4, 64, half), BF16),
        in_specs=[any_spec] * 7,
        out_specs=vmem,
        scratch_shapes=[
            pltpu.VMEM((n_ff + n_o, rows, W), BF16),
            pltpu.VMEM((NBUF3, GROUP * W, d_out), BF16),
            pltpu.VMEM((rows, d_out), F32),
            pltpu.VMEM(keep.shape, BF16),
            pltpu.VMEM(keep.shape, BF16),
            pltpu.VMEM((4, 64, half), BF16),
            pltpu.VMEM((rows, half), BF16),
            pltpu.VMEM((rows, half), BF16),
            dma((NBUF3,)),
            dma((n_m,)),
            dma((n_m,)),
            dma,
            dma((2,)),
            dma((2,)),
            dma((2,)),
            dma((n_p, n_g)),
            dma((n_p, n_g)),
            dma((n_p, n_g, 2)),
            dma((n_p, n_g, 2)),
            dma((n_p, 2)),
        ],
        compiler_params=pltpu.CompilerParams(collective_id=1, has_side_effects=True, vmem_limit_bytes=56_000_000),
        cost_estimate=pl.CostEstimate(flops=flops, bytes_accessed=2 * d_out * (w_down.shape[1] + w_o.shape[1]), transcendentals=0),
    )(o, keep, recv_e, recv_l, hidden.reshape(4, 64, half), w_o, w_down)
    return out.reshape(rows, half)


def solution(mesh):
    x_size = mesh.shape["x"]
    y_size = mesh.shape["yz"]
    row_spec = P("dp", ("x", "yz"))
    tile_in = P(None, "x", "yz")
    tile_out = P(None, "yz", "x")
    cache_spec = P(None, ("dp", "x", "yz"))
    len_spec = P(("dp", "x", "yz"))

    def device_step(hidden, norm_gain, w_q, w_kv, w_gate, w_up, w_o, w_down, k_cache, v_cache, seq_len):
        d_model = hidden.shape[1] * x_size * y_size
        seqs = k_cache.shape[1]
        dim = k_cache.shape[3]
        q_cols = w_q.shape[2]
        heads = q_cols // dim
        qkv, keep, recv_e, send = project(hidden, norm_gain, w_q, w_kv, w_gate, w_up, d_model)
        recv_l = lax.ppermute(send, "x", [(i, (i + x_size // 2) % x_size) for i in range(x_size)])
        q = qkv[:, :, :q_cols].reshape(y_size, seqs, heads, dim).transpose(1, 0, 2, 3).reshape(seqs, y_size * heads, dim)
        kv = qkv[:, :, q_cols:].transpose(1, 0, 2)
        k_new, v_new, o = attend(seq_len, q, kv, k_cache, v_cache)
        o = o.reshape(seqs, y_size, q_cols // W, W).transpose(1, 2, 0, 3)
        hidden_out = finish(o, keep, recv_e, recv_l, hidden, w_o, w_down)
        return hidden_out, k_new, v_new

    return jax.shard_map(
        device_step,
        mesh=mesh,
        in_specs=(row_spec, P(None, "x"), tile_in, tile_in, tile_in, tile_in, tile_out, tile_out, cache_spec, cache_spec, len_spec),
        out_specs=(row_spec, cache_spec, cache_spec),
        check_vma=False,
    )
```

```python
import functools

import jax
import jax.numpy as jnp
from jax import lax
from jax.experimental import pallas as pl
from jax.experimental.pallas import tpu as pltpu
from jax.sharding import PartitionSpec as P

NORM_EPS = 1e-6
W = 512
NBUF1 = 6
NBUF3 = 6
GROUP = 3
PARTS = ((0, 32), (32, 16), (48, 16))
EARLY = 12
SEQ_STEP = 2
VMEM_LIMIT = 64_000_000
F32 = jnp.float32
BF16 = jnp.bfloat16
LOG2E = 1.4426950408889634
MASKED = -1e30


def dev(**axes):
    return dict(device_id=axes, device_id_type=pl.DeviceIdType.MESH)


def silu_mul(gate, up):
    gate = gate.astype(BF16).astype(F32)
    up = up.astype(BF16).astype(F32)
    return (jax.nn.silu(gate) * up).astype(BF16)


def project_kernel(
    n_q, n_ff, d_model, hidden, gain, wq, wkv, wg, wu,
    qkv_out, keep_out, recv_out, send_out,
    h_own, h_other, u, inv_all, sq_all, wbuf, wkv_buf, part, part_kv, near, near_kv, keep, keep_kv, far_src,
    far_src_kv, far_q, far_kv, z_rows, z_other,
    w_sem, wkv_sem, h_in, h_sems, sq_send, sq_recv, near_send, near_recv, qn_send, qn_recv, kn_send, kn_recv,
    far_send, far_recv, qf_send, qf_recv, kf_send, kf_recv, y_sems, out_sem, qkv_sem,
):
    xi = lax.axis_index("x")
    yj = lax.axis_index("yz")
    core = lax.rem(xi, 2)
    chip = xi // 2
    mate = xi + 1 - 2 * core
    across = lax.rem(xi + 2, 4)
    other_y = 1 - yj
    me = xi * 2 + yj
    half = hidden.shape[-1]
    n_all = n_q + n_ff
    n_far = n_q + EARLY
    to_mate = dev(x=mate, yz=yj)
    to_across = dev(x=across, yz=yj)

    barrier = pltpu.get_barrier_semaphore()
    for k in range(1, 8):
        peer = lax.rem(me + k, 8)
        pl.semaphore_signal(barrier, inc=1, **dev(x=peer // 2, yz=lax.rem(peer, 2)))
    h_load = pltpu.make_async_copy(hidden, h_own, h_in)
    h_load.start()

    def start_weights(g):
        slot = lax.rem(g, NBUF1)

        @pl.when(g < n_q)
        def _():
            for k in range(2):
                cols = pl.ds(pl.multiple_of((2 * g + k) * W, W), W)
                pltpu.make_async_copy(wq.at[0, :, cols], wbuf.at[slot, k], w_sem.at[slot, k]).start()

        @pl.when(g >= n_q)
        def _():
            cols = pl.ds(pl.multiple_of((g - n_q) * W, W), W)
            pltpu.make_async_copy(wg.at[0, :, cols], wbuf.at[slot, 0], w_sem.at[slot, 0]).start()
            pltpu.make_async_copy(wu.at[0, :, cols], wbuf.at[slot, 1], w_sem.at[slot, 1]).start()

    def wait_weights(slot, k):
        pltpu.make_async_copy(wq.at[0, :, pl.ds(0, W)], wbuf.at[slot, k], w_sem.at[slot, k]).wait()

    for g in range(NBUF1):
        start_weights(jnp.int32(g))
    kv_copy = pltpu.make_async_copy(wkv.at[0], wkv_buf, wkv_sem)
    kv_copy.start()

    h_load.wait()
    h_f32 = h_own[...].reshape(256, half).astype(F32)
    sq_all[me] = lax.dot_general(
        jnp.ones((8, half), F32), h_f32 * h_f32, (((1,), (1,)), ((), ())),
        precision=lax.Precision.HIGHEST, preferred_element_type=F32)
    pl.semaphore_wait(barrier, 7)

    def sq_copy(peer, src):
        return pltpu.make_async_remote_copy(
            src_ref=sq_all.at[src], dst_ref=sq_all.at[src], send_sem=sq_send.at[peer], recv_sem=sq_recv.at[src],
            **dev(x=peer // 2, yz=lax.rem(peer, 2)))

    def side_of(step):
        return 1 - chip if step < 2 else chip

    def h_copy(step):
        block = (side_of(step), slice(None), step % 2)
        return pltpu.make_async_remote_copy(
            src_ref=h_own.at[block], dst_ref=h_other.at[block],
            send_sem=h_sems.at[step, 0], recv_sem=h_sems.at[step, 1], **dev(x=xi, yz=other_y))

    for k in range(1, 8):
        sq_copy(lax.rem(me + k, 8), me).start()
    for step in range(4):
        h_copy(step).start()
    for k in range(1, 8):
        peer = lax.rem(me + k, 8)
        sq_copy(peer, peer).wait_recv()
    total = jnp.sum(sq_all[...], axis=0)
    inv = lax.rsqrt(total / d_model + NORM_EPS)
    inv_all[...] = jnp.transpose(jnp.concatenate([inv] * 16, axis=0)).reshape(inv_all.shape)

    def normalize(values, step, which):
        cols = pl.ds(pl.multiple_of(which * half, 128), half)
        side, piece = side_of(step), step % 2
        inv_rows = inv_all[side, :, piece].reshape(64, 128)[:, :1]
        res = (values[side, :, piece].reshape(64, half).astype(F32) * inv_rows
               * gain[:, cols].astype(F32)).astype(BF16)
        u[side, piece, :, cols] = res

    def near_copy(g):
        return pltpu.make_async_remote_copy(
            src_ref=part.at[g, :, :, 1 - core], dst_ref=near.at[g], send_sem=near_send.at[g],
            recv_sem=near_recv.at[g], **to_mate)

    def near_copy_q(g, step):
        side, piece = side_of(step), step % 2
        return pltpu.make_async_remote_copy(
            src_ref=part.at[g, side, piece, 1 - core], dst_ref=near.at[g, side, piece],
            send_sem=qn_send.at[g, step], recv_sem=qn_recv.at[g, step], **to_mate)

    def near_copy_kv(step):
        side, piece = side_of(step), step % 2
        return pltpu.make_async_remote_copy(
            src_ref=part_kv.at[side, piece, 1 - core], dst_ref=near_kv.at[side, piece],
            send_sem=kn_send.at[step], recv_sem=kn_recv.at[step], **to_mate)

    def far_copy(g):
        return pltpu.make_async_remote_copy(
            src_ref=far_src.at[g], dst_ref=recv_out.at[g - n_q], send_sem=far_send.at[g - n_q],
            recv_sem=far_recv.at[g - n_q], **to_across)

    def far_copy_q(g, step):
        rows = slice(32 * step, 32 * step + 32)
        return pltpu.make_async_remote_copy(
            src_ref=far_src.at[g, rows], dst_ref=far_q.at[g, rows], send_sem=qf_send.at[g, step],
            recv_sem=qf_recv.at[g, step], **to_across)

    def far_copy_kv(step):
        rows = slice(32 * step, 32 * step + 32)
        return pltpu.make_async_remote_copy(
            src_ref=far_src_kv.at[rows], dst_ref=far_kv.at[rows], send_sem=kf_send.at[step],
            recv_sem=kf_recv.at[step], **to_across)

    def keep_copy(g):
        return pltpu.make_async_copy(keep.at[g], keep_out.at[g - n_q], out_sem.at[g - n_q, 0])

    def send_copy(g):
        k = g - n_q
        return pltpu.make_async_copy(far_src.at[g], send_out.at[k - EARLY], out_sem.at[k, 1])

    def add(a, b):
        return (a.astype(F32) + b.astype(F32)).astype(BF16)

    def multiply(g):
        slot = lax.rem(g, NBUF1)
        for k in range(2):
            wait_weights(slot, k)
            res = jnp.dot(u[...].reshape(256, u.shape[-1]), wbuf[slot, k], preferred_element_type=F32).astype(BF16)
            part[g, :, :, :, :, k * W:(k + 1) * W] = res.reshape(2, 2, 2, 32, W)
        near_copy(g).start()

        @pl.when(g + NBUF1 < n_all)
        def _():
            start_weights(g + NBUF1)

    def reduce_near(g):
        near_copy(g).wait_recv()
        far_src[g] = add(part[g, 1 - chip, :, core], near[g, 1 - chip]).reshape(64, 2 * W)

        @pl.when(g < n_far)
        def _():
            far_copy(g).start()

        @pl.when(g >= n_far)
        def _():
            send_copy(g).start()

        keep[g] = add(part[g, chip, :, core], near[g, chip]).reshape(64, 2 * W)
        keep_copy(g).start()

    def multiply_q(step, g):
        side, piece = side_of(step), step % 2
        if g == n_q:
            if step == 0:
                kv_copy.wait()
            res = jnp.dot(u[side, piece], wkv_buf[...], preferred_element_type=F32).astype(BF16)
            part_kv[side, piece] = res.reshape(2, 32, res.shape[1])
            near_copy_kv(step).start()
            return
        for k in range(2):
            if step == 0:
                wait_weights(g, k)
            res = jnp.dot(u[side, piece], wbuf[g, k], preferred_element_type=F32).astype(BF16)
            part[g, side, piece, :, :, k * W:(k + 1) * W] = res.reshape(2, 32, W)
        near_copy_q(g, step).start()
        if step == 3:
            start_weights(jnp.int32(g + NBUF1))

    def reduce_q(step, g):
        side, piece = side_of(step), step % 2
        rows = slice(32 * piece, 32 * piece + 32)
        if g == n_q:
            near_copy_kv(step).wait_recv()
            total_q = add(part_kv[side, piece, core], near_kv[side, piece])
            if step < 2:
                far_src_kv[rows] = total_q
                far_copy_kv(step).start()
            else:
                keep_kv[rows] = total_q
            return
        near_copy_q(g, step).wait_recv()
        total_q = add(part[g, side, piece, core], near[g, side, piece])
        if step < 2:
            far_src[g, rows] = total_q
            far_copy_q(g, step).start()
        else:
            keep[g, rows] = total_q

    for step in range(4):
        normalize(h_own, step, yj)
        h_copy(step).wait_recv()
        normalize(h_other, step, other_y)
        for g in range(n_q + 1):
            multiply_q(step, g)
            if step == 0 and g >= 2:
                reduce_q(0, g - 2)
            if step == 2:
                reduce_q(1, g)
        if step == 0:
            reduce_q(0, n_q - 1)
            reduce_q(0, n_q)

    @pl.loop(n_q, n_far)
    def _(g):
        multiply(g)

        @pl.when(g >= n_q + 2)
        def _():
            reduce_near(g - 2)

    q_cols = n_q * 2 * W
    for g in range(n_q + 1):
        reduce_q(2, g)
        reduce_q(3, g)
    for g in range(n_q):
        for step in range(2):
            far_copy_q(g, step).wait_recv()
        z_rows[:, :, g * 2 * W:(g + 1) * 2 * W] = add(keep[g], far_q[g]).reshape(2, 32, 2 * W)
    for step in range(2):
        far_copy_kv(step).wait_recv()
    z_kv = add(keep_kv[...], far_kv[...])
    z_rows[:, :, q_cols:] = z_kv.reshape(2, 32, z_kv.shape[1])
    y_copy = pltpu.make_async_remote_copy(
        src_ref=z_rows.at[other_y], dst_ref=z_other, send_sem=y_sems.at[0], recv_sem=y_sems.at[1],
        **dev(x=xi, yz=other_y))
    y_copy.start()
    qkv_own = pltpu.make_async_copy(z_rows.at[yj], qkv_out.at[yj], qkv_sem.at[0])
    qkv_own.start()

    @pl.loop(n_far, n_all)
    def _(g):
        multiply(g)
        reduce_near(g - 2)

    reduce_near(jnp.int32(n_all - 2))
    reduce_near(jnp.int32(n_all - 1))
    y_copy.wait_recv()
    qkv_other = pltpu.make_async_copy(z_other, qkv_out.at[other_y], qkv_sem.at[1])
    qkv_other.start()

    for step in range(4):
        h_copy(step).wait_send()
        near_copy_kv(step).wait_send()
        for g in range(n_q):
            near_copy_q(g, step).wait_send()
    for step in range(2):
        far_copy_kv(step).wait_send()
        for g in range(n_q):
            far_copy_q(g, step).wait_send()
    for k in range(1, 8):
        sq_copy(lax.rem(me + k, 8), me).wait_send()
    y_copy.wait_send()

    @pl.loop(n_q, n_all)
    def _(g):
        near_copy(g).wait_send()
        keep_copy(g).wait()

    @pl.loop(n_far, n_all)
    def _(g):
        send_copy(g).wait()

    qkv_own.wait()
    qkv_other.wait()

    @pl.loop(n_q, n_far)
    def _(g):
        far_copy(g).wait_send()
        far_copy(g).wait_recv()


def project(hidden, gain, w_q, w_kv, w_gate, w_up, d_model):
    rows, half = hidden.shape
    feats = w_q.shape[1]
    kv = w_kv.shape[2]
    n_q = w_q.shape[2] // (2 * W)
    n_ff = w_gate.shape[2] // W
    n_all = n_q + n_ff
    late = n_ff - EARLY
    dma = pltpu.SemaphoreType.DMA
    any_spec = pl.BlockSpec(memory_space=pl.ANY)
    vmem = pl.BlockSpec(memory_space=pltpu.VMEM)
    cols = w_q.shape[2] + kv
    flops = 2 * rows * feats * (w_q.shape[2] + kv + 2 * w_gate.shape[2])
    h_shape = (2, 2, 2, 32, half)
    return pl.pallas_call(
        functools.partial(project_kernel, n_q, n_ff, d_model),
        name="project",
        out_shape=(
            jax.ShapeDtypeStruct((2, 32, cols), BF16),
            jax.ShapeDtypeStruct((n_ff, 64, 2 * W), BF16),
            jax.ShapeDtypeStruct((EARLY, 64, 2 * W), BF16),
            jax.ShapeDtypeStruct((late, 64, 2 * W), BF16),
        ),
        in_specs=[any_spec, vmem, any_spec, any_spec, any_spec, any_spec],
        out_specs=(any_spec, any_spec, any_spec, any_spec),
        scratch_shapes=[
            pltpu.VMEM(h_shape, BF16),
            pltpu.VMEM(h_shape, BF16),
            pltpu.VMEM((2, 2, 64, feats), BF16),
            pltpu.VMEM((2, 2, 2, 32, 128), F32),
            pltpu.VMEM((8, 8, rows), F32),
            pltpu.VMEM((NBUF1, 2, feats, W), BF16),
            pltpu.VMEM((feats, kv), BF16),
            pltpu.VMEM((n_all, 2, 2, 2, 32, 2 * W), BF16),
            pltpu.VMEM((2, 2, 2, 32, kv), BF16),
            pltpu.VMEM((n_all, 2, 2, 32, 2 * W), BF16),
            pltpu.VMEM((2, 2, 32, kv), BF16),
            pltpu.VMEM((n_all, 64, 2 * W), BF16),
            pltpu.VMEM((64, kv), BF16),
            pltpu.VMEM((n_all, 64, 2 * W), BF16),
            pltpu.VMEM((64, kv), BF16),
            pltpu.VMEM((n_q, 64, 2 * W), BF16),
            pltpu.VMEM((64, kv), BF16),
            pltpu.VMEM((2, 32, cols), BF16),
            pltpu.VMEM((32, cols), BF16),
            dma((NBUF1, 2)),
            dma,
            dma,
            dma((4, 2)),
            dma((8,)),
            dma((8,)),
            dma((n_all,)),
            dma((n_all,)),
            dma((n_q, 4)),
            dma((n_q, 4)),
            dma((4,)),
            dma((4,)),
            dma((EARLY,)),
            dma((EARLY,)),
            dma((n_q, 2)),
            dma((n_q, 2)),
            dma((2,)),
            dma((2,)),
            dma((2,)),
            dma((n_ff, 2)),
            dma((2,)),
        ],
        compiler_params=pltpu.CompilerParams(collective_id=0, has_side_effects=True, vmem_limit_bytes=VMEM_LIMIT),
        cost_estimate=pl.CostEstimate(flops=flops, bytes_accessed=feats * (flops // (rows * feats)), transcendentals=0),
    )(hidden.reshape(h_shape), gain, w_q, w_kv, w_gate, w_up)


def attend_kernel(lens, q_ref, kv_ref, k_ref, v_ref, k_out, v_out, o_ref):
    step = pl.program_id(0)
    n_pos = k_ref.shape[2]
    scale = q_ref.shape[2] ** -0.5 * LOG2E
    for s in range(SEQ_STEP):
        length = lens[step * SEQ_STEP + s]
        base = pl.multiple_of((length // 16) * 16, 16)
        k_out[0, s] = k_ref[0, s]
        v_out[0, s] = v_ref[0, s]
        hit = lax.broadcasted_iota(jnp.int32, (16, k_ref.shape[3]), 0) == length - base
        for src, dst, which in ((k_ref, k_out, 0), (v_ref, v_out, 1)):
            old = src[0, s, pl.ds(base, 16), :].astype(F32)
            new = kv_ref[s, which:which + 1, :].astype(F32)
            dst[0, s, pl.ds(base, 16), :] = jnp.where(hit, new, old).astype(BF16)
        scores = lax.dot_general(q_ref[s], k_out[0, s], (((1,), (1,)), ((), ())), preferred_element_type=F32) * scale
        visible = lax.broadcasted_iota(jnp.int32, scores.shape, 1) <= length
        scores = jnp.where(visible, scores, MASKED)
        weights = jnp.exp2(scores - jnp.max(scores, axis=1, keepdims=True))
        probs = (weights * (1.0 / jnp.sum(weights, axis=1, keepdims=True))).astype(BF16)
        o_ref[s] = jnp.dot(probs, v_out[0, s], preferred_element_type=F32).astype(BF16)


def attend(lens, q, kv, k_cache, v_cache):
    seqs, heads, dim = q.shape
    n_pos = k_cache.shape[2]
    cache_spec = pl.BlockSpec((1, SEQ_STEP, n_pos, dim), lambda b, lens: (0, b, 0, 0))
    q_spec = pl.BlockSpec((SEQ_STEP, heads, dim), lambda b, lens: (b, 0, 0))
    return pl.pallas_call(
        attend_kernel,
        name="attend",
        out_shape=(
            jax.ShapeDtypeStruct(k_cache.shape, BF16),
            jax.ShapeDtypeStruct(v_cache.shape, BF16),
            jax.ShapeDtypeStruct(q.shape, BF16),
        ),
        grid_spec=pltpu.PrefetchScalarGridSpec(
            num_scalar_prefetch=1,
            grid=(seqs // SEQ_STEP,),
            in_specs=[q_spec, pl.BlockSpec((SEQ_STEP, 2, dim), lambda b, lens: (b, 0, 0)), cache_spec, cache_spec],
            out_specs=(cache_spec, cache_spec, q_spec),
        ),
        compiler_params=pltpu.CompilerParams(dimension_semantics=("arbitrary",), vmem_limit_bytes=66_000_000),
        cost_estimate=pl.CostEstimate(
            flops=10**10, bytes_accessed=8 * k_cache.size, transcendentals=seqs * heads * n_pos),
    )(lens, q, kv, k_cache, v_cache)


def output_kernel(
    n_ff, n_o, o_in, keep, recv_e, recv_l, hidden, w_o, w_down, out,
    acts, wbuf, acc, keep_v, recv_v, h_v, y_src, y_dst,
    w_sem, keep_sem, recv_sem, h_sem, oo_sems, on_send, on_recv, far_send, far_recv, near_send, near_recv, y_sems,
):
    xi = lax.axis_index("x")
    yj = lax.axis_index("yz")
    core = lax.rem(xi, 2)
    mate = xi + 1 - 2 * core
    across = lax.rem(xi + 2, 4)
    other_y = 1 - yj
    n_m = n_ff // GROUP
    n_g = n_m + n_o // GROUP
    n_early = EARLY // GROUP
    depth = GROUP * W
    d_out = w_down.shape[2]
    half = d_out // 2

    barrier = pltpu.get_barrier_semaphore()
    for x_, y_ in ((mate, yj), (across, yj), (xi, other_y)):
        pl.semaphore_signal(barrier, inc=1, **dev(x=x_, yz=y_))

    def keep_copy(g):
        return pltpu.make_async_copy(
            keep.at[pl.ds(GROUP * g, GROUP)], keep_v.at[pl.ds(GROUP * g, GROUP)], keep_sem.at[g])

    def recv_copy(g):
        src = recv_e.at[pl.ds(GROUP * g, GROUP)] if g < n_early else recv_l.at[pl.ds(GROUP * (g - n_early), GROUP)]
        return pltpu.make_async_copy(src, recv_v.at[pl.ds(GROUP * g, GROUP)], recv_sem.at[g])

    for g in range(n_m):
        keep_copy(g).start()
        recv_copy(g).start()

    def rows_of(p, owner):
        off, size = PARTS[p]
        return pl.ds(pl.multiple_of(4 * off + owner * size, 16), size)

    def block(p, g, owner):
        return acts.at[pl.ds(GROUP * g, GROUP), rows_of(p, owner)]

    def o_rows(s):
        row = (1 - yj) * (32 * xi + 16 * s) + yj * (128 + 64 * s + 16 * xi)
        return acts.at[pl.ds(n_ff, n_o), pl.ds(pl.multiple_of(row, 16), 16)]

    def o_own(s):
        return pltpu.make_async_copy(o_in.at[yj, :, pl.ds(16 * s, 16)], o_rows(s), oo_sems.at[s])

    def o_copy(s):
        return pltpu.make_async_remote_copy(
            src_ref=o_in.at[other_y, :, pl.ds(16 * s, 16)], dst_ref=o_rows(s), send_sem=on_send.at[s],
            recv_sem=on_recv.at[s], **dev(x=xi, yz=other_y))

    h_load = pltpu.make_async_copy(hidden, h_v, h_sem)

    def load_weights(g):
        slot = lax.rem(g, NBUF3)

        @pl.when(g < n_m)
        def _():
            pltpu.make_async_copy(
                w_down.at[0, pl.ds(pl.multiple_of(g * depth, W), depth)], wbuf.at[slot], w_sem.at[slot]).start()

        @pl.when(g >= n_m)
        def _():
            pltpu.make_async_copy(
                w_o.at[0, pl.ds(pl.multiple_of((g - n_m) * depth, W), depth)], wbuf.at[slot], w_sem.at[slot]).start()

    def far_copy(p, g):
        return pltpu.make_async_remote_copy(
            src_ref=block(p, g, xi), dst_ref=block(p, g, xi), send_sem=far_send.at[p, g], recv_sem=far_recv.at[p, g],
            **dev(x=across, yz=yj))

    def near_copy(p, g, which):
        rows = block(p, g, xi if which == 0 else across)
        return pltpu.make_async_remote_copy(
            src_ref=rows, dst_ref=rows, send_sem=near_send.at[p, g, which], recv_sem=near_recv.at[p, g, which],
            **dev(x=mate, yz=yj))

    def give(p, g):
        far_copy(p, g).start()
        near_copy(p, g, 0).start()

    def give_m(p, g):
        off, size = PARTS[p]
        for k in range(GROUP):
            t = GROUP * g + k
            z = keep_v[t, off:off + size].astype(F32) + recv_v[t, off:off + size].astype(F32)
            acts[t, rows_of(p, xi)] = silu_mul(z[:, :W], z[:, W:])
        give(p, g)

    pl.semaphore_wait(barrier, 3)
    for g in range(n_m):
        keep_copy(g).wait()
        recv_copy(g).wait()
        give_m(0, g)
        if g == 0:
            for s in range(2):
                o_copy(s).start()
                o_own(s).start()
            for s in range(NBUF3):
                load_weights(jnp.int32(s))
            h_load.start()
    acc[...] = jnp.zeros_like(acc)
    for s in range(2):
        o_own(s).wait()
        o_copy(s).wait_recv()

    def chunk(p, k):
        return k if p % 2 == 0 else n_g - 1 - k

    for g in range(n_m, n_g):
        give(0, g)
    for p in range(1, len(PARTS)):
        @pl.loop(0, n_g)
        def _(k):
            g = chunk(p, k)

            @pl.when(g < n_m)
            def _():
                give_m(p, g)

            @pl.when(g >= n_m)
            def _():
                give(p, g)

    def forward(p, k):
        g = chunk(p, k)
        far_copy(p, g).wait_recv()
        near_copy(p, g, 1).start()

    def multiply(p, k):
        g = chunk(p, k)
        slot = lax.rem(g, NBUF3)

        @pl.when(k >= (0 if p == 0 else NBUF3))
        def _():
            pltpu.make_async_copy(w_down.at[0, pl.ds(0, depth)], wbuf.at[slot], w_sem.at[slot]).wait()

        near_copy(p, g, 0).wait_recv()
        near_copy(p, g, 1).wait_recv()
        off, size = PARTS[p]
        rows = slice(4 * off, 4 * (off + size))
        for n in range(d_out // W):
            cols = slice(n * W, (n + 1) * W)
            total = acc[rows, cols]
            for j in range(GROUP):
                total += jnp.dot(
                    acts[GROUP * g + j, rows], wbuf[slot, j * W:(j + 1) * W, cols], preferred_element_type=F32)
            acc[rows, cols] = total

        @pl.when(k + NBUF3 < n_g)
        def _():
            load_weights(chunk(p, k + NBUF3))

    def cols_of(j):
        return pl.ds(pl.multiple_of(j * half, 128), half)

    def y_copy(p):
        rows = slice(4 * PARTS[p][0], 4 * sum(PARTS[p]))
        return pltpu.make_async_remote_copy(
            src_ref=y_src.at[rows], dst_ref=y_dst.at[rows], send_sem=y_sems.at[p, 0], recv_sem=y_sems.at[p, 1],
            **dev(x=xi, yz=other_y))

    def exchange(p):
        rows = slice(4 * PARTS[p][0], 4 * sum(PARTS[p]))
        y_src[rows] = acc[rows, cols_of(other_y)].astype(BF16)
        y_copy(p).start()

    def finalize(p):
        off, size = PARTS[p]
        rows = slice(4 * off, 4 * (off + size))
        y_copy(p).wait_recv()
        total = (acc[rows, cols_of(yj)] + y_dst[rows].astype(F32)).reshape(4, size, half)
        out[:, off:off + size] = (h_v[:, off:off + size].astype(F32) + total).astype(BF16)

    for p in range(len(PARTS)):
        forward(p, jnp.int32(0))
        if p > 0:
            multiply(p - 1, jnp.int32(n_g - 1))
            exchange(p - 1)
        if p == 1:
            h_load.wait()

        @pl.loop(1, n_g)
        def _(k):
            forward(p, k)
            multiply(p, k - 1)

        if p > 0:
            finalize(p - 1)

    last = len(PARTS) - 1
    multiply(last, jnp.int32(n_g - 1))
    exchange(last)
    for s in range(2):
        o_copy(s).wait_send()
    for p in range(len(PARTS)):
        @pl.loop(0, n_g)
        def _(g):
            far_copy(p, g).wait_send()
            near_copy(p, g, 0).wait_send()
            near_copy(p, g, 1).wait_send()

    finalize(last)
    for p in range(len(PARTS)):
        y_copy(p).wait_send()


def finish(o, keep, recv_e, recv_l, hidden, w_o, w_down):
    rows, half = hidden.shape
    n_ff = w_down.shape[1] // W
    n_o = w_o.shape[1] // W
    n_m = n_ff // GROUP
    n_g = n_m + n_o // GROUP
    n_p = len(PARTS)
    d_out = w_down.shape[2]
    dma = pltpu.SemaphoreType.DMA
    any_spec = pl.BlockSpec(memory_space=pl.ANY)
    vmem = pl.BlockSpec(memory_space=pltpu.VMEM)
    flops = 2 * rows * d_out * (w_down.shape[1] + w_o.shape[1])
    out = pl.pallas_call(
        functools.partial(output_kernel, n_ff, n_o),
        name="finish",
        out_shape=jax.ShapeDtypeStruct((4, 64, half), BF16),
        in_specs=[any_spec] * 7,
        out_specs=vmem,
        scratch_shapes=[
            pltpu.VMEM((n_ff + n_o, rows, W), BF16),
            pltpu.VMEM((NBUF3, GROUP * W, d_out), BF16),
            pltpu.VMEM((rows, d_out), F32),
            pltpu.VMEM(keep.shape, BF16),
            pltpu.VMEM(keep.shape, BF16),
            pltpu.VMEM((4, 64, half), BF16),
            pltpu.VMEM((rows, half), BF16),
            pltpu.VMEM((rows, half), BF16),
            dma((NBUF3,)),
            dma((n_m,)),
            dma((n_m,)),
            dma,
            dma((2,)),
            dma((2,)),
            dma((2,)),
            dma((n_p, n_g)),
            dma((n_p, n_g)),
            dma((n_p, n_g, 2)),
            dma((n_p, n_g, 2)),
            dma((n_p, 2)),
        ],
        compiler_params=pltpu.CompilerParams(collective_id=1, has_side_effects=True, vmem_limit_bytes=56_000_000),
        cost_estimate=pl.CostEstimate(flops=flops, bytes_accessed=2 * d_out * (w_down.shape[1] + w_o.shape[1]), transcendentals=0),
    )(o, keep, recv_e, recv_l, hidden.reshape(4, 64, half), w_o, w_down)
    return out.reshape(rows, half)


def solution(mesh):
    x_size = mesh.shape["x"]
    y_size = mesh.shape["yz"]
    row_spec = P("dp", ("x", "yz"))
    tile_in = P(None, "x", "yz")
    tile_out = P(None, "yz", "x")
    cache_spec = P(None, ("dp", "x", "yz"))
    len_spec = P(("dp", "x", "yz"))

    def device_step(hidden, norm_gain, w_q, w_kv, w_gate, w_up, w_o, w_down, k_cache, v_cache, seq_len):
        d_model = hidden.shape[1] * x_size * y_size
        seqs = k_cache.shape[1]
        dim = k_cache.shape[3]
        q_cols = w_q.shape[2]
        heads = q_cols // dim
        qkv, keep, recv_e, send = project(hidden, norm_gain, w_q, w_kv, w_gate, w_up, d_model)
        recv_l = lax.ppermute(send, "x", [(i, (i + x_size // 2) % x_size) for i in range(x_size)])
        q = qkv[:, :, :q_cols].reshape(y_size, seqs, heads, dim).transpose(1, 0, 2, 3).reshape(seqs, y_size * heads, dim)
        kv = qkv[:, :, q_cols:].transpose(1, 0, 2)
        k_new, v_new, o = attend(seq_len, q, kv, k_cache, v_cache)
        o = o.reshape(seqs, y_size, q_cols // W, W).transpose(1, 2, 0, 3)
        hidden_out = finish(o, keep, recv_e, recv_l, hidden, w_o, w_down)
        return hidden_out, k_new, v_new

    return jax.shard_map(
        device_step,
        mesh=mesh,
        in_specs=(row_spec, P(None, "x"), tile_in, tile_in, tile_in, tile_in, tile_out, tile_out, cache_spec, cache_spec, len_spec),
        out_specs=(row_spec, cache_spec, cache_spec),
        check_vma=False,
    )
```

```python
import functools

import jax
import jax.numpy as jnp
from jax import lax
from jax.experimental import pallas as pl
from jax.experimental.pallas import tpu as pltpu
from jax.sharding import PartitionSpec as P

NORM_EPS = 1e-6
W = 512
NBUF1 = 4
NBUF3 = 6
GROUP = 3
PARTS = ((0, 32), (32, 16), (48, 16))
EARLY = 12
SEQ_STEP = 2
VMEM_LIMIT = 64_000_000
F32 = jnp.float32
BF16 = jnp.bfloat16
LOG2E = 1.4426950408889634
MASKED = -1e30


def dev(**axes):
    return dict(device_id=axes, device_id_type=pl.DeviceIdType.MESH)


def silu_mul(gate, up):
    gate = gate.astype(BF16).astype(F32)
    up = up.astype(BF16).astype(F32)
    return (jax.nn.silu(gate) * up).astype(BF16)


def project_kernel(
    n_q, n_ff, d_model, hidden, gain, wq, wkv, wg, wu,
    qkv_out, keep_out, recv_out, send_out,
    h_own, h_other, u, inv_all, sq_all, wq_buf, wbuf, wkv_buf, part, part_kv, near, near_kv, keep, keep_kv, far_src,
    far_src_kv, far, far_kv, z_rows, z_other,
    wq_sem, w_sem, wkv_sem, h_in, h_sems, sq_send, sq_recv, near_send, near_recv, qn_send, qn_recv, kn_send, kn_recv,
    far_send, far_recv, kf_sems, y_sems, out_sem, recv_sem, qkv_sem,
):
    xi = lax.axis_index("x")
    yj = lax.axis_index("yz")
    core = lax.rem(xi, 2)
    chip = xi // 2
    mate = xi + 1 - 2 * core
    across = lax.rem(xi + 2, 4)
    other_y = 1 - yj
    me = xi * 2 + yj
    half = hidden.shape[-1]
    n_all = n_q + n_ff
    n_far = n_q + EARLY
    to_mate = dev(x=mate, yz=yj)
    to_across = dev(x=across, yz=yj)

    barrier = pltpu.get_barrier_semaphore()
    for k in range(1, 8):
        peer = lax.rem(me + k, 8)
        pl.semaphore_signal(barrier, inc=1, **dev(x=peer // 2, yz=lax.rem(peer, 2)))
    h_load = pltpu.make_async_copy(hidden, h_own, h_in)
    h_load.start()

    def start_weights(g):
        slot = lax.rem(g, NBUF1)
        cols = pl.ds(pl.multiple_of((g - n_q) * W, W), W)
        pltpu.make_async_copy(wg.at[0, :, cols], wbuf.at[slot, 0], w_sem.at[slot, 0]).start()
        pltpu.make_async_copy(wu.at[0, :, cols], wbuf.at[slot, 1], w_sem.at[slot, 1]).start()

    def wait_weights(slot, k):
        pltpu.make_async_copy(wg.at[0, :, pl.ds(0, W)], wbuf.at[slot, k], w_sem.at[slot, k]).wait()

    def wq_copy(g):
        return pltpu.make_async_copy(wq.at[0, :, g * 2 * W:(g + 1) * 2 * W], wq_buf.at[g], wq_sem.at[g])

    for g in range(n_q):
        wq_copy(g).start()
    kv_copy = pltpu.make_async_copy(wkv.at[0], wkv_buf, wkv_sem)
    kv_copy.start()
    for g in range(n_q, n_q + NBUF1):
        start_weights(jnp.int32(g))

    h_load.wait()
    h_f32 = h_own[...].astype(F32)
    sq_all[me] = lax.dot_general(
        jnp.ones((8, half), F32), h_f32 * h_f32, (((1,), (1,)), ((), ())),
        precision=lax.Precision.HIGHEST, preferred_element_type=F32)
    pl.semaphore_wait(barrier, 7)

    def sq_copy(peer, src):
        return pltpu.make_async_remote_copy(
            src_ref=sq_all.at[src], dst_ref=sq_all.at[src], send_sem=sq_send.at[peer], recv_sem=sq_recv.at[src],
            **dev(x=peer // 2, yz=lax.rem(peer, 2)))

    def side_of(step):
        return 1 - chip if step == 0 else chip

    def side_rows(step):
        return pl.ds(pl.multiple_of(side_of(step) * 128, 128), 128)

    def h_copy(step):
        return pltpu.make_async_remote_copy(
            src_ref=h_own.at[side_rows(step)], dst_ref=h_other.at[side_rows(step)],
            send_sem=h_sems.at[step, 0], recv_sem=h_sems.at[step, 1], **dev(x=xi, yz=other_y))

    for k in range(1, 8):
        sq_copy(lax.rem(me + k, 8), me).start()
    for step in range(2):
        h_copy(step).start()
    for k in range(1, 8):
        peer = lax.rem(me + k, 8)
        sq_copy(peer, peer).wait_recv()
    total = jnp.sum(sq_all[...], axis=0)
    inv = lax.rsqrt(total / d_model + NORM_EPS)
    inv_all[...] = jnp.transpose(jnp.concatenate([inv] * 16, axis=0))

    def normalize(values, step, which):
        cols = pl.ds(pl.multiple_of(which * half, 128), half)
        rows = side_rows(step)
        u[rows, cols] = (
            values[rows].astype(F32) * inv_all[rows, :1] * gain[:, cols].astype(F32)).astype(BF16)

    def near_copy(g):
        return pltpu.make_async_remote_copy(
            src_ref=part.at[g, :, 1 - core], dst_ref=near.at[g], send_sem=near_send.at[g],
            recv_sem=near_recv.at[g], **to_mate)

    def near_copy_q(g, step):
        side = side_of(step)
        return pltpu.make_async_remote_copy(
            src_ref=part.at[g, side, 1 - core], dst_ref=near.at[g, side],
            send_sem=qn_send.at[g, step], recv_sem=qn_recv.at[g, step], **to_mate)

    def near_copy_kv(step):
        side = side_of(step)
        return pltpu.make_async_remote_copy(
            src_ref=part_kv.at[side, 1 - core], dst_ref=near_kv.at[side],
            send_sem=kn_send.at[step], recv_sem=kn_recv.at[step], **to_mate)

    def far_copy(g):
        return pltpu.make_async_remote_copy(
            src_ref=far_src.at[g], dst_ref=far.at[g], send_sem=far_send.at[g], recv_sem=far_recv.at[g], **to_across)

    def far_copy_kv():
        return pltpu.make_async_remote_copy(
            src_ref=far_src_kv, dst_ref=far_kv, send_sem=kf_sems.at[0], recv_sem=kf_sems.at[1], **to_across)

    def keep_copy(g):
        return pltpu.make_async_copy(keep.at[g], keep_out.at[g - n_q], out_sem.at[g - n_q, 0])

    def send_copy(g):
        k = g - n_q
        return pltpu.make_async_copy(far_src.at[g], send_out.at[k - EARLY], out_sem.at[k, 1])

    def recv_copy(g):
        return pltpu.make_async_copy(far.at[g], recv_out.at[g - n_q], recv_sem.at[g - n_q])

    def add(a, b):
        return (a.astype(F32) + b.astype(F32)).astype(BF16)

    def multiply(g):
        slot = lax.rem(g, NBUF1)
        for k in range(2):
            wait_weights(slot, k)
            res = jnp.dot(u[...], wbuf[slot, k], preferred_element_type=F32).astype(BF16)
            part[g, :, :, :, k * W:(k + 1) * W] = res.reshape(2, 2, 64, W)
        near_copy(g).start()

        @pl.when(g + NBUF1 < n_all)
        def _():
            start_weights(g + NBUF1)

    def reduce_near(g):
        near_copy(g).wait_recv()
        far_src[g] = add(part[g, 1 - chip, core], near[g, 1 - chip])

        @pl.when(g < n_far)
        def _():
            far_copy(g).start()

        @pl.when(g >= n_far)
        def _():
            send_copy(g).start()

        keep[g] = add(part[g, chip, core], near[g, chip])
        keep_copy(g).start()

    def multiply_q(step):
        side = side_of(step)
        for g in range(n_q):
            if step == 0:
                wq_copy(g).wait()
            for k in range(2):
                res = jnp.dot(
                    u[side_rows(step)], wq_buf[g, :, k * W:(k + 1) * W], preferred_element_type=F32).astype(BF16)
                part[g, side, :, :, k * W:(k + 1) * W] = res.reshape(2, 64, W)
            near_copy_q(g, step).start()
            if step == 0 and g >= 2:
                reduce_q(0, g - 2)
        if step == 0:
            kv_copy.wait()
        res = jnp.dot(u[side_rows(step)], wkv_buf[...], preferred_element_type=F32).astype(BF16)
        part_kv[side] = res.reshape(2, 64, res.shape[1])
        near_copy_kv(step).start()

    def reduce_q(step, g):
        side = side_of(step)
        near_copy_q(g, step).wait_recv()
        total_q = add(part[g, side, core], near[g, side])
        if step == 0:
            far_src[g] = total_q
            far_copy(g).start()
        else:
            keep[g] = total_q

    def reduce_kv(step):
        side = side_of(step)
        near_copy_kv(step).wait_recv()
        total_kv = add(part_kv[side, core], near_kv[side])
        if step == 0:
            far_src_kv[...] = total_kv
            far_copy_kv().start()
        else:
            keep_kv[...] = total_kv

    normalize(h_own, 0, yj)
    h_copy(0).wait_recv()
    normalize(h_other, 0, other_y)
    multiply_q(0)
    for g in range(n_q - 2, n_q):
        reduce_q(0, g)
    reduce_kv(0)
    normalize(h_own, 1, yj)
    h_copy(1).wait_recv()
    normalize(h_other, 1, other_y)

    @pl.loop(n_q, n_far)
    def _(g):
        multiply(g)

        @pl.when(g >= n_q + 2)
        def _():
            reduce_near(g - 2)

    q_cols = n_q * 2 * W
    multiply_q(1)
    for g in range(n_q):
        reduce_q(1, g)
        far_copy(g).wait_recv()
        z_rows[:, :, g * 2 * W:(g + 1) * 2 * W] = add(keep[g], far[g]).reshape(2, 32, 2 * W)
    reduce_kv(1)
    far_copy_kv().wait_recv()
    z_kv = add(keep_kv[...], far_kv[...])
    z_rows[:, :, q_cols:] = z_kv.reshape(2, 32, z_kv.shape[1])
    y_copy = pltpu.make_async_remote_copy(
        src_ref=z_rows.at[other_y], dst_ref=z_other, send_sem=y_sems.at[0], recv_sem=y_sems.at[1],
        **dev(x=xi, yz=other_y))
    y_copy.start()
    qkv_own = pltpu.make_async_copy(z_rows.at[yj], qkv_out.at[yj], qkv_sem.at[0])
    qkv_own.start()

    @pl.loop(n_far, n_all)
    def _(g):
        multiply(g)
        reduce_near(g - 2)

    reduce_near(jnp.int32(n_all - 2))
    reduce_near(jnp.int32(n_all - 1))
    y_copy.wait_recv()
    qkv_other = pltpu.make_async_copy(z_other, qkv_out.at[other_y], qkv_sem.at[1])
    qkv_other.start()

    @pl.loop(n_q, n_far)
    def _(g):
        far_copy(g).wait_recv()
        recv_copy(g).start()

    for step in range(2):
        h_copy(step).wait_send()
        near_copy_kv(step).wait_send()
        for g in range(n_q):
            near_copy_q(g, step).wait_send()
    far_copy_kv().wait_send()
    for k in range(1, 8):
        sq_copy(lax.rem(me + k, 8), me).wait_send()
    y_copy.wait_send()

    @pl.loop(n_q, n_all)
    def _(g):
        near_copy(g).wait_send()
        keep_copy(g).wait()

    @pl.loop(n_far, n_all)
    def _(g):
        send_copy(g).wait()

    @pl.loop(0, n_far)
    def _(g):
        far_copy(g).wait_send()

    qkv_own.wait()
    qkv_other.wait()

    @pl.loop(n_q, n_far)
    def _(g):
        recv_copy(g).wait()


def project(hidden, gain, w_q, w_kv, w_gate, w_up, d_model):
    rows, half = hidden.shape
    feats = w_q.shape[1]
    kv = w_kv.shape[2]
    n_q = w_q.shape[2] // (2 * W)
    n_ff = w_gate.shape[2] // W
    n_all = n_q + n_ff
    late = n_ff - EARLY
    dma = pltpu.SemaphoreType.DMA
    any_spec = pl.BlockSpec(memory_space=pl.ANY)
    vmem = pl.BlockSpec(memory_space=pltpu.VMEM)
    cols = w_q.shape[2] + kv
    flops = 2 * rows * feats * (w_q.shape[2] + kv + 2 * w_gate.shape[2])
    return pl.pallas_call(
        functools.partial(project_kernel, n_q, n_ff, d_model),
        name="project",
        out_shape=(
            jax.ShapeDtypeStruct((2, 32, cols), BF16),
            jax.ShapeDtypeStruct((n_ff, 64, 2 * W), BF16),
            jax.ShapeDtypeStruct((EARLY, 64, 2 * W), BF16),
            jax.ShapeDtypeStruct((late, 64, 2 * W), BF16),
        ),
        in_specs=[any_spec, vmem, any_spec, any_spec, any_spec, any_spec],
        out_specs=(any_spec, any_spec, any_spec, any_spec),
        scratch_shapes=[
            pltpu.VMEM((rows, half), BF16),
            pltpu.VMEM((rows, half), BF16),
            pltpu.VMEM((rows, feats), BF16),
            pltpu.VMEM((rows, 128), F32),
            pltpu.VMEM((8, 8, rows), F32),
            pltpu.VMEM((n_q, feats, 2 * W), BF16),
            pltpu.VMEM((NBUF1, 2, feats, W), BF16),
            pltpu.VMEM((feats, kv), BF16),
            pltpu.VMEM((n_all, 2, 2, 64, 2 * W), BF16),
            pltpu.VMEM((2, 2, 64, kv), BF16),
            pltpu.VMEM((n_all, 2, 64, 2 * W), BF16),
            pltpu.VMEM((2, 64, kv), BF16),
            pltpu.VMEM((n_all, 64, 2 * W), BF16),
            pltpu.VMEM((64, kv), BF16),
            pltpu.VMEM((n_all, 64, 2 * W), BF16),
            pltpu.VMEM((64, kv), BF16),
            pltpu.VMEM((n_q + EARLY, 64, 2 * W), BF16),
            pltpu.VMEM((64, kv), BF16),
            pltpu.VMEM((2, 32, cols), BF16),
            pltpu.VMEM((32, cols), BF16),
            dma((n_q,)),
            dma((NBUF1, 2)),
            dma,
            dma,
            dma((2, 2)),
            dma((8,)),
            dma((8,)),
            dma((n_all,)),
            dma((n_all,)),
            dma((n_q, 2)),
            dma((n_q, 2)),
            dma((2,)),
            dma((2,)),
            dma((n_q + EARLY,)),
            dma((n_q + EARLY,)),
            dma((2,)),
            dma((2,)),
            dma((n_ff, 2)),
            dma((EARLY,)),
            dma((2,)),
        ],
        compiler_params=pltpu.CompilerParams(collective_id=0, has_side_effects=True, vmem_limit_bytes=VMEM_LIMIT),
        cost_estimate=pl.CostEstimate(flops=flops, bytes_accessed=feats * (flops // (rows * feats)), transcendentals=0),
    )(hidden, gain, w_q, w_kv, w_gate, w_up)


def attend_kernel(lens, q_ref, kv_ref, k_ref, v_ref, k_out, v_out, o_ref):
    step = pl.program_id(0)
    n_pos = k_ref.shape[2]
    scale = q_ref.shape[2] ** -0.5 * LOG2E
    for s in range(SEQ_STEP):
        length = lens[step * SEQ_STEP + s]
        base = pl.multiple_of((length // 16) * 16, 16)
        k_out[0, s] = k_ref[0, s]
        v_out[0, s] = v_ref[0, s]
        hit = lax.broadcasted_iota(jnp.int32, (16, k_ref.shape[3]), 0) == length - base
        for src, dst, which in ((k_ref, k_out, 0), (v_ref, v_out, 1)):
            old = src[0, s, pl.ds(base, 16), :].astype(F32)
            new = kv_ref[s, which:which + 1, :].astype(F32)
            dst[0, s, pl.ds(base, 16), :] = jnp.where(hit, new, old).astype(BF16)
        scores = lax.dot_general(q_ref[s], k_out[0, s], (((1,), (1,)), ((), ())), preferred_element_type=F32) * scale
        visible = lax.broadcasted_iota(jnp.int32, scores.shape, 1) <= length
        scores = jnp.where(visible, scores, MASKED)
        weights = jnp.exp2(scores - jnp.max(scores, axis=1, keepdims=True))
        probs = (weights * (1.0 / jnp.sum(weights, axis=1, keepdims=True))).astype(BF16)
        o_ref[s] = jnp.dot(probs, v_out[0, s], preferred_element_type=F32).astype(BF16)


def attend(lens, q, kv, k_cache, v_cache):
    seqs, heads, dim = q.shape
    n_pos = k_cache.shape[2]
    cache_spec = pl.BlockSpec((1, SEQ_STEP, n_pos, dim), lambda b, lens: (0, b, 0, 0))
    q_spec = pl.BlockSpec((SEQ_STEP, heads, dim), lambda b, lens: (b, 0, 0))
    return pl.pallas_call(
        attend_kernel,
        name="attend",
        out_shape=(
            jax.ShapeDtypeStruct(k_cache.shape, BF16),
            jax.ShapeDtypeStruct(v_cache.shape, BF16),
            jax.ShapeDtypeStruct(q.shape, BF16),
        ),
        grid_spec=pltpu.PrefetchScalarGridSpec(
            num_scalar_prefetch=1,
            grid=(seqs // SEQ_STEP,),
            in_specs=[q_spec, pl.BlockSpec((SEQ_STEP, 2, dim), lambda b, lens: (b, 0, 0)), cache_spec, cache_spec],
            out_specs=(cache_spec, cache_spec, q_spec),
        ),
        compiler_params=pltpu.CompilerParams(dimension_semantics=("arbitrary",), vmem_limit_bytes=66_000_000),
        cost_estimate=pl.CostEstimate(
            flops=10**10, bytes_accessed=8 * k_cache.size, transcendentals=seqs * heads * n_pos),
    )(lens, q, kv, k_cache, v_cache)


def output_kernel(
    n_ff, n_o, o_in, keep, recv_e, recv_l, hidden, w_o, w_down, out,
    acts, wbuf, acc, keep_v, recv_v, h_v, y_src, y_dst,
    w_sem, keep_sem, recv_sem, h_sem, oo_sems, on_send, on_recv, far_send, far_recv, near_send, near_recv, y_sems,
):
    xi = lax.axis_index("x")
    yj = lax.axis_index("yz")
    core = lax.rem(xi, 2)
    mate = xi + 1 - 2 * core
    across = lax.rem(xi + 2, 4)
    other_y = 1 - yj
    n_m = n_ff // GROUP
    n_g = n_m + n_o // GROUP
    n_early = EARLY // GROUP
    depth = GROUP * W
    d_out = w_down.shape[2]
    half = d_out // 2

    barrier = pltpu.get_barrier_semaphore()
    for x_, y_ in ((mate, yj), (across, yj), (xi, other_y)):
        pl.semaphore_signal(barrier, inc=1, **dev(x=x_, yz=y_))

    def keep_copy(g):
        return pltpu.make_async_copy(
            keep.at[pl.ds(GROUP * g, GROUP)], keep_v.at[pl.ds(GROUP * g, GROUP)], keep_sem.at[g])

    def recv_copy(g):
        src = recv_e.at[pl.ds(GROUP * g, GROUP)] if g < n_early else recv_l.at[pl.ds(GROUP * (g - n_early), GROUP)]
        return pltpu.make_async_copy(src, recv_v.at[pl.ds(GROUP * g, GROUP)], recv_sem.at[g])

    for g in range(n_m):
        keep_copy(g).start()
        recv_copy(g).start()

    def rows_of(p, owner):
        off, size = PARTS[p]
        return pl.ds(pl.multiple_of(4 * off + owner * size, 16), size)

    def block(p, g, owner):
        return acts.at[pl.ds(GROUP * g, GROUP), rows_of(p, owner)]

    def o_rows(s):
        row = (1 - yj) * (32 * xi + 16 * s) + yj * (128 + 64 * s + 16 * xi)
        return acts.at[pl.ds(n_ff, n_o), pl.ds(pl.multiple_of(row, 16), 16)]

    def o_own(s):
        return pltpu.make_async_copy(o_in.at[yj, :, pl.ds(16 * s, 16)], o_rows(s), oo_sems.at[s])

    def o_copy(s):
        return pltpu.make_async_remote_copy(
            src_ref=o_in.at[other_y, :, pl.ds(16 * s, 16)], dst_ref=o_rows(s), send_sem=on_send.at[s],
            recv_sem=on_recv.at[s], **dev(x=xi, yz=other_y))

    h_load = pltpu.make_async_copy(hidden, h_v, h_sem)

    def load_weights(g):
        slot = lax.rem(g, NBUF3)

        @pl.when(g < n_m)
        def _():
            pltpu.make_async_copy(
                w_down.at[0, pl.ds(pl.multiple_of(g * depth, W), depth)], wbuf.at[slot], w_sem.at[slot]).start()

        @pl.when(g >= n_m)
        def _():
            pltpu.make_async_copy(
                w_o.at[0, pl.ds(pl.multiple_of((g - n_m) * depth, W), depth)], wbuf.at[slot], w_sem.at[slot]).start()

    def far_copy(p, g):
        return pltpu.make_async_remote_copy(
            src_ref=block(p, g, xi), dst_ref=block(p, g, xi), send_sem=far_send.at[p, g], recv_sem=far_recv.at[p, g],
            **dev(x=across, yz=yj))

    def near_copy(p, g, which):
        rows = block(p, g, xi if which == 0 else across)
        return pltpu.make_async_remote_copy(
            src_ref=rows, dst_ref=rows, send_sem=near_send.at[p, g, which], recv_sem=near_recv.at[p, g, which],
            **dev(x=mate, yz=yj))

    def give(p, g):
        far_copy(p, g).start()
        near_copy(p, g, 0).start()

    def give_m(p, g):
        off, size = PARTS[p]
        for k in range(GROUP):
            t = GROUP * g + k
            z = keep_v[t, off:off + size].astype(F32) + recv_v[t, off:off + size].astype(F32)
            acts[t, rows_of(p, xi)] = silu_mul(z[:, :W], z[:, W:])
        give(p, g)

    pl.semaphore_wait(barrier, 3)
    for g in range(n_m):
        keep_copy(g).wait()
        recv_copy(g).wait()
        give_m(0, g)
        if g == 0:
            for s in range(2):
                o_copy(s).start()
                o_own(s).start()
            for s in range(NBUF3):
                load_weights(jnp.int32(s))
            h_load.start()
    acc[...] = jnp.zeros_like(acc)
    for s in range(2):
        o_own(s).wait()
        o_copy(s).wait_recv()

    def chunk(p, k):
        return k if p % 2 == 0 else n_g - 1 - k

    for g in range(n_m, n_g):
        give(0, g)
    for p in range(1, len(PARTS)):
        @pl.loop(0, n_g)
        def _(k):
            g = chunk(p, k)

            @pl.when(g < n_m)
            def _():
                give_m(p, g)

            @pl.when(g >= n_m)
            def _():
                give(p, g)

    def forward(p, k):
        g = chunk(p, k)
        far_copy(p, g).wait_recv()
        near_copy(p, g, 1).start()

    def multiply(p, k):
        g = chunk(p, k)
        slot = lax.rem(g, NBUF3)

        @pl.when(k >= (0 if p == 0 else NBUF3))
        def _():
            pltpu.make_async_copy(w_down.at[0, pl.ds(0, depth)], wbuf.at[slot], w_sem.at[slot]).wait()

        near_copy(p, g, 0).wait_recv()
        near_copy(p, g, 1).wait_recv()
        off, size = PARTS[p]
        rows = slice(4 * off, 4 * (off + size))
        for n in range(d_out // W):
            cols = slice(n * W, (n + 1) * W)
            total = acc[rows, cols]
            for j in range(GROUP):
                total += jnp.dot(
                    acts[GROUP * g + j, rows], wbuf[slot, j * W:(j + 1) * W, cols], preferred_element_type=F32)
            acc[rows, cols] = total

        @pl.when(k + NBUF3 < n_g)
        def _():
            load_weights(chunk(p, k + NBUF3))

    def cols_of(j):
        return pl.ds(pl.multiple_of(j * half, 128), half)

    def y_copy(p):
        rows = slice(4 * PARTS[p][0], 4 * sum(PARTS[p]))
        return pltpu.make_async_remote_copy(
            src_ref=y_src.at[rows], dst_ref=y_dst.at[rows], send_sem=y_sems.at[p, 0], recv_sem=y_sems.at[p, 1],
            **dev(x=xi, yz=other_y))

    def exchange(p):
        rows = slice(4 * PARTS[p][0], 4 * sum(PARTS[p]))
        y_src[rows] = acc[rows, cols_of(other_y)].astype(BF16)
        y_copy(p).start()

    def finalize(p):
        off, size = PARTS[p]
        rows = slice(4 * off, 4 * (off + size))
        y_copy(p).wait_recv()
        total = (acc[rows, cols_of(yj)] + y_dst[rows].astype(F32)).reshape(4, size, half)
        out[:, off:off + size] = (h_v[:, off:off + size].astype(F32) + total).astype(BF16)

    for p in range(len(PARTS)):
        forward(p, jnp.int32(0))
        if p > 0:
            multiply(p - 1, jnp.int32(n_g - 1))
            exchange(p - 1)
        if p == 1:
            h_load.wait()

        @pl.loop(1, n_g)
        def _(k):
            forward(p, k)
            multiply(p, k - 1)

        if p > 0:
            finalize(p - 1)

    last = len(PARTS) - 1
    multiply(last, jnp.int32(n_g - 1))
    exchange(last)
    for s in range(2):
        o_copy(s).wait_send()
    for p in range(len(PARTS)):
        @pl.loop(0, n_g)
        def _(g):
            far_copy(p, g).wait_send()
            near_copy(p, g, 0).wait_send()
            near_copy(p, g, 1).wait_send()

    finalize(last)
    for p in range(len(PARTS)):
        y_copy(p).wait_send()


def finish(o, keep, recv_e, recv_l, hidden, w_o, w_down):
    rows, half = hidden.shape
    n_ff = w_down.shape[1] // W
    n_o = w_o.shape[1] // W
    n_m = n_ff // GROUP
    n_g = n_m + n_o // GROUP
    n_p = len(PARTS)
    d_out = w_down.shape[2]
    dma = pltpu.SemaphoreType.DMA
    any_spec = pl.BlockSpec(memory_space=pl.ANY)
    vmem = pl.BlockSpec(memory_space=pltpu.VMEM)
    flops = 2 * rows * d_out * (w_down.shape[1] + w_o.shape[1])
    out = pl.pallas_call(
        functools.partial(output_kernel, n_ff, n_o),
        name="finish",
        out_shape=jax.ShapeDtypeStruct((4, 64, half), BF16),
        in_specs=[any_spec] * 7,
        out_specs=vmem,
        scratch_shapes=[
            pltpu.VMEM((n_ff + n_o, rows, W), BF16),
            pltpu.VMEM((NBUF3, GROUP * W, d_out), BF16),
            pltpu.VMEM((rows, d_out), F32),
            pltpu.VMEM(keep.shape, BF16),
            pltpu.VMEM(keep.shape, BF16),
            pltpu.VMEM((4, 64, half), BF16),
            pltpu.VMEM((rows, half), BF16),
            pltpu.VMEM((rows, half), BF16),
            dma((NBUF3,)),
            dma((n_m,)),
            dma((n_m,)),
            dma,
            dma((2,)),
            dma((2,)),
            dma((2,)),
            dma((n_p, n_g)),
            dma((n_p, n_g)),
            dma((n_p, n_g, 2)),
            dma((n_p, n_g, 2)),
            dma((n_p, 2)),
        ],
        compiler_params=pltpu.CompilerParams(collective_id=1, has_side_effects=True, vmem_limit_bytes=56_000_000),
        cost_estimate=pl.CostEstimate(flops=flops, bytes_accessed=2 * d_out * (w_down.shape[1] + w_o.shape[1]), transcendentals=0),
    )(o, keep, recv_e, recv_l, hidden.reshape(4, 64, half), w_o, w_down)
    return out.reshape(rows, half)


def solution(mesh):
    x_size = mesh.shape["x"]
    y_size = mesh.shape["yz"]
    row_spec = P("dp", ("x", "yz"))
    tile_in = P(None, "x", "yz")
    tile_out = P(None, "yz", "x")
    cache_spec = P(None, ("dp", "x", "yz"))
    len_spec = P(("dp", "x", "yz"))

    def device_step(hidden, norm_gain, w_q, w_kv, w_gate, w_up, w_o, w_down, k_cache, v_cache, seq_len):
        d_model = hidden.shape[1] * x_size * y_size
        seqs = k_cache.shape[1]
        dim = k_cache.shape[3]
        q_cols = w_q.shape[2]
        heads = q_cols // dim
        qkv, keep, recv_e, send = project(hidden, norm_gain, w_q, w_kv, w_gate, w_up, d_model)
        recv_l = lax.ppermute(send, "x", [(i, (i + x_size // 2) % x_size) for i in range(x_size)])
        q = qkv[:, :, :q_cols].reshape(y_size, seqs, heads, dim).transpose(1, 0, 2, 3).reshape(seqs, y_size * heads, dim)
        kv = qkv[:, :, q_cols:].transpose(1, 0, 2)
        k_new, v_new, o = attend(seq_len, q, kv, k_cache, v_cache)
        o = o.reshape(seqs, y_size, q_cols // W, W).transpose(1, 2, 0, 3)
        hidden_out = finish(o, keep, recv_e, recv_l, hidden, w_o, w_down)
        return hidden_out, k_new, v_new

    return jax.shard_map(
        device_step,
        mesh=mesh,
        in_specs=(row_spec, P(None, "x"), tile_in, tile_in, tile_in, tile_in, tile_out, tile_out, cache_spec, cache_spec, len_spec),
        out_specs=(row_spec, cache_spec, cache_spec),
        check_vma=False,
    )
```

```python
import functools

import jax
import jax.numpy as jnp
from jax import lax
from jax.experimental import pallas as pl
from jax.experimental.pallas import tpu as pltpu
from jax.sharding import PartitionSpec as P

NORM_EPS = 1e-6
W = 512
NBUF1 = 4
NBUF3 = 6
GROUP = 3
PARTS = ((0, 32), (32, 16), (48, 16))
EARLY = 12
SEQ_STEP = 2
VMEM_LIMIT = 64_000_000
F32 = jnp.float32
BF16 = jnp.bfloat16
LOG2E = 1.4426950408889634
MASKED = -1e30


def dev(**axes):
    return dict(device_id=axes, device_id_type=pl.DeviceIdType.MESH)


def silu_mul(gate, up):
    gate = gate.astype(BF16).astype(F32)
    up = up.astype(BF16).astype(F32)
    return (jax.nn.silu(gate) * up).astype(BF16)


def project_kernel(
    n_q, n_ff, d_model, hidden, gain, wq, wkv, wg, wu,
    qkv_out, keep_out, recv_out, send_out,
    h_own, h_other, u, inv_all, sq_all, wq_buf, wbuf, wkv_buf, part, part_kv, near, near_kv, keep, keep_kv, far_src,
    far_src_kv, far, far_kv, z_rows, z_other,
    wq_sem, w_sem, wkv_sem, h_in, h_sems, sq_send, sq_recv, near_send, near_recv, qn_send, qn_recv, kn_send, kn_recv,
    far_send, far_recv, qf_send, qf_recv, kf_send, kf_recv, y_sems, out_sem, recv_sem, qkv_sem,
):
    xi = lax.axis_index("x")
    yj = lax.axis_index("yz")
    core = lax.rem(xi, 2)
    chip = xi // 2
    mate = xi + 1 - 2 * core
    across = lax.rem(xi + 2, 4)
    other_y = 1 - yj
    me = xi * 2 + yj
    half = hidden.shape[-1]
    n_all = n_q + n_ff
    n_far = n_q + EARLY
    to_mate = dev(x=mate, yz=yj)
    to_across = dev(x=across, yz=yj)

    barrier = pltpu.get_barrier_semaphore()
    for k in range(1, 8):
        peer = lax.rem(me + k, 8)
        pl.semaphore_signal(barrier, inc=1, **dev(x=peer // 2, yz=lax.rem(peer, 2)))
    h_load = pltpu.make_async_copy(hidden, h_own, h_in)
    h_load.start()

    def start_weights(g):
        slot = lax.rem(g, NBUF1)
        cols = pl.ds(pl.multiple_of((g - n_q) * W, W), W)
        pltpu.make_async_copy(wg.at[0, :, cols], wbuf.at[slot, 0], w_sem.at[slot, 0]).start()
        pltpu.make_async_copy(wu.at[0, :, cols], wbuf.at[slot, 1], w_sem.at[slot, 1]).start()

    def wait_weights(slot, k):
        pltpu.make_async_copy(wg.at[0, :, pl.ds(0, W)], wbuf.at[slot, k], w_sem.at[slot, k]).wait()

    def wq_copy(g):
        return pltpu.make_async_copy(wq.at[0, :, g * 2 * W:(g + 1) * 2 * W], wq_buf.at[g], wq_sem.at[g])

    h_load.wait()
    for g in range(n_q):
        wq_copy(g).start()
    kv_copy = pltpu.make_async_copy(wkv.at[0], wkv_buf, wkv_sem)
    kv_copy.start()
    for g in range(n_q, n_q + NBUF1):
        start_weights(jnp.int32(g))

    h_f32 = h_own[...].reshape(256, half).astype(F32)
    sq_all[me] = lax.dot_general(
        jnp.ones((8, half), F32), h_f32 * h_f32, (((1,), (1,)), ((), ())),
        precision=lax.Precision.HIGHEST, preferred_element_type=F32)
    pl.semaphore_wait(barrier, 7)

    def sq_copy(peer, src):
        return pltpu.make_async_remote_copy(
            src_ref=sq_all.at[src], dst_ref=sq_all.at[src], send_sem=sq_send.at[peer], recv_sem=sq_recv.at[src],
            **dev(x=peer // 2, yz=lax.rem(peer, 2)))

    def side_of(step):
        return 1 - chip if step < 2 else chip

    def piece(step):
        return pl.ds(32 * step, 32) if step < 2 else pl.ds(0, 64)

    def h_copy(step):
        block = (side_of(step), slice(None), piece(step))
        return pltpu.make_async_remote_copy(
            src_ref=h_own.at[block], dst_ref=h_other.at[block],
            send_sem=h_sems.at[step, 0], recv_sem=h_sems.at[step, 1], **dev(x=xi, yz=other_y))

    for k in range(1, 8):
        sq_copy(lax.rem(me + k, 8), me).start()
    for step in range(3):
        h_copy(step).start()
    for k in range(1, 8):
        peer = lax.rem(me + k, 8)
        sq_copy(peer, peer).wait_recv()
    total = jnp.sum(sq_all[...], axis=0)
    inv = lax.rsqrt(total / d_model + NORM_EPS)
    inv_all[...] = jnp.transpose(jnp.concatenate([inv] * 16, axis=0)).reshape(inv_all.shape)

    def normalize(values, step, which):
        cols = pl.ds(pl.multiple_of(which * half, 128), half)
        side, rows = side_of(step), piece(step)
        u[side, :, rows, cols] = (
            values[side, :, rows].astype(F32) * inv_all[side, :, rows, :1] * gain[:, cols].astype(F32)).astype(BF16)

    def near_copy(g):
        return pltpu.make_async_remote_copy(
            src_ref=part.at[g, :, 1 - core], dst_ref=near.at[g], send_sem=near_send.at[g],
            recv_sem=near_recv.at[g], **to_mate)

    def near_copy_q(g, step):
        side, rows = side_of(step), piece(step)
        return pltpu.make_async_remote_copy(
            src_ref=part.at[g, side, 1 - core, rows], dst_ref=near.at[g, side, rows],
            send_sem=qn_send.at[g, step], recv_sem=qn_recv.at[g, step], **to_mate)

    def near_copy_kv(step):
        side, rows = side_of(step), piece(step)
        return pltpu.make_async_remote_copy(
            src_ref=part_kv.at[side, 1 - core, rows], dst_ref=near_kv.at[side, rows],
            send_sem=kn_send.at[step], recv_sem=kn_recv.at[step], **to_mate)

    def far_copy(g):
        return pltpu.make_async_remote_copy(
            src_ref=far_src.at[g], dst_ref=far.at[g], send_sem=far_send.at[g - n_q], recv_sem=far_recv.at[g - n_q],
            **to_across)

    def far_copy_q(g, step):
        rows = piece(step)
        return pltpu.make_async_remote_copy(
            src_ref=far_src.at[g, rows], dst_ref=far.at[g, rows], send_sem=qf_send.at[g, step],
            recv_sem=qf_recv.at[g, step], **to_across)

    def far_copy_kv(step):
        rows = piece(step)
        return pltpu.make_async_remote_copy(
            src_ref=far_src_kv.at[rows], dst_ref=far_kv.at[rows], send_sem=kf_send.at[step], recv_sem=kf_recv.at[step],
            **to_across)

    def keep_copy(g):
        return pltpu.make_async_copy(keep.at[g], keep_out.at[g - n_q], out_sem.at[g - n_q, 0])

    def send_copy(g):
        k = g - n_q
        return pltpu.make_async_copy(far_src.at[g], send_out.at[k - EARLY], out_sem.at[k, 1])

    def recv_copy(g):
        return pltpu.make_async_copy(far.at[g], recv_out.at[g - n_q], recv_sem.at[g - n_q])

    def add(a, b):
        return (a.astype(F32) + b.astype(F32)).astype(BF16)

    def multiply(g):
        slot = lax.rem(g, NBUF1)
        for k in range(2):
            wait_weights(slot, k)
            res = jnp.dot(u[...].reshape(256, u.shape[-1]), wbuf[slot, k], preferred_element_type=F32).astype(BF16)
            part[g, :, :, :, k * W:(k + 1) * W] = res.reshape(2, 2, 64, W)
        near_copy(g).start()

        @pl.when(g + NBUF1 < n_all)
        def _():
            start_weights(g + NBUF1)

    def reduce_near(g):
        near_copy(g).wait_recv()
        far_src[g] = add(part[g, 1 - chip, core], near[g, 1 - chip])

        @pl.when(g < n_far)
        def _():
            far_copy(g).start()

        @pl.when(g >= n_far)
        def _():
            send_copy(g).start()

        keep[g] = add(part[g, chip, core], near[g, chip])
        keep_copy(g).start()

    def multiply_q(step):
        side, rows = side_of(step), piece(step)
        lhs = u[side, :, rows].reshape(2 * rows.size, u.shape[-1])
        for g in range(n_q):
            if step == 0:
                wq_copy(g).wait()
            for k in range(2):
                res = jnp.dot(lhs, wq_buf[g, :, k * W:(k + 1) * W], preferred_element_type=F32).astype(BF16)
                part[g, side, :, rows, k * W:(k + 1) * W] = res.reshape(2, rows.size, W)
            near_copy_q(g, step).start()
            if step == 0 and g >= 2:
                reduce_q(0, g - 2)
        if step == 0:
            kv_copy.wait()
        res = jnp.dot(lhs, wkv_buf[...], preferred_element_type=F32).astype(BF16)
        part_kv[side, :, rows] = res.reshape(2, rows.size, res.shape[1])
        near_copy_kv(step).start()

    def reduce_q(step, g):
        side, rows = side_of(step), piece(step)
        near_copy_q(g, step).wait_recv()
        total_q = add(part[g, side, core, rows], near[g, side, rows])
        if step < 2:
            far_src[g, rows] = total_q
            far_copy_q(g, step).start()
        else:
            keep[g] = total_q

    def reduce_kv(step):
        side, rows = side_of(step), piece(step)
        near_copy_kv(step).wait_recv()
        total_kv = add(part_kv[side, core, rows], near_kv[side, rows])
        if step < 2:
            far_src_kv[rows] = total_kv
            far_copy_kv(step).start()
        else:
            keep_kv[...] = total_kv

    for step in range(3):
        normalize(h_own, step, yj)
        h_copy(step).wait_recv()
        normalize(h_other, step, other_y)
        if step < 2:
            multiply_q(step)
            for g in range(n_q - 2 if step == 0 else 0, n_q):
                reduce_q(step, g)
            reduce_kv(step)

    @pl.loop(n_q, n_far)
    def _(g):
        multiply(g)

        @pl.when(g >= n_q + 2)
        def _():
            reduce_near(g - 2)

    q_cols = n_q * 2 * W
    multiply_q(2)
    for g in range(n_q):
        reduce_q(2, g)
        for step in range(2):
            far_copy_q(g, step).wait_recv()
        z_rows[:, :, g * 2 * W:(g + 1) * 2 * W] = add(keep[g], far[g]).reshape(2, 32, 2 * W)
    reduce_kv(2)
    for step in range(2):
        far_copy_kv(step).wait_recv()
    z_kv = add(keep_kv[...], far_kv[...])
    z_rows[:, :, q_cols:] = z_kv.reshape(2, 32, z_kv.shape[1])
    y_copy = pltpu.make_async_remote_copy(
        src_ref=z_rows.at[other_y], dst_ref=z_other, send_sem=y_sems.at[0], recv_sem=y_sems.at[1],
        **dev(x=xi, yz=other_y))
    y_copy.start()
    qkv_own = pltpu.make_async_copy(z_rows.at[yj], qkv_out.at[yj], qkv_sem.at[0])
    qkv_own.start()

    @pl.loop(n_far, n_all)
    def _(g):
        multiply(g)
        reduce_near(g - 2)

    reduce_near(jnp.int32(n_all - 2))
    reduce_near(jnp.int32(n_all - 1))
    y_copy.wait_recv()
    qkv_other = pltpu.make_async_copy(z_other, qkv_out.at[other_y], qkv_sem.at[1])
    qkv_other.start()

    @pl.loop(n_q, n_far)
    def _(g):
        far_copy(g).wait_recv()
        recv_copy(g).start()

    for step in range(3):
        h_copy(step).wait_send()
        near_copy_kv(step).wait_send()
        for g in range(n_q):
            near_copy_q(g, step).wait_send()
    for step in range(2):
        far_copy_kv(step).wait_send()
        for g in range(n_q):
            far_copy_q(g, step).wait_send()
    for k in range(1, 8):
        sq_copy(lax.rem(me + k, 8), me).wait_send()
    y_copy.wait_send()

    @pl.loop(n_q, n_all)
    def _(g):
        near_copy(g).wait_send()
        keep_copy(g).wait()

    @pl.loop(n_far, n_all)
    def _(g):
        send_copy(g).wait()

    @pl.loop(n_q, n_far)
    def _(g):
        far_copy(g).wait_send()

    qkv_own.wait()
    qkv_other.wait()

    @pl.loop(n_q, n_far)
    def _(g):
        recv_copy(g).wait()


def project(hidden, gain, w_q, w_kv, w_gate, w_up, d_model):
    rows, half = hidden.shape
    feats = w_q.shape[1]
    kv = w_kv.shape[2]
    n_q = w_q.shape[2] // (2 * W)
    n_ff = w_gate.shape[2] // W
    n_all = n_q + n_ff
    late = n_ff - EARLY
    dma = pltpu.SemaphoreType.DMA
    any_spec = pl.BlockSpec(memory_space=pl.ANY)
    vmem = pl.BlockSpec(memory_space=pltpu.VMEM)
    cols = w_q.shape[2] + kv
    flops = 2 * rows * feats * (w_q.shape[2] + kv + 2 * w_gate.shape[2])
    return pl.pallas_call(
        functools.partial(project_kernel, n_q, n_ff, d_model),
        name="project",
        out_shape=(
            jax.ShapeDtypeStruct((2, 32, cols), BF16),
            jax.ShapeDtypeStruct((n_ff, 64, 2 * W), BF16),
            jax.ShapeDtypeStruct((EARLY, 64, 2 * W), BF16),
            jax.ShapeDtypeStruct((late, 64, 2 * W), BF16),
        ),
        in_specs=[any_spec, vmem, any_spec, any_spec, any_spec, any_spec],
        out_specs=(any_spec, any_spec, any_spec, any_spec),
        scratch_shapes=[
            pltpu.VMEM((2, 2, 64, half), BF16),
            pltpu.VMEM((2, 2, 64, half), BF16),
            pltpu.VMEM((2, 2, 64, feats), BF16),
            pltpu.VMEM((2, 2, 64, 128), F32),
            pltpu.VMEM((8, 8, rows), F32),
            pltpu.VMEM((n_q, feats, 2 * W), BF16),
            pltpu.VMEM((NBUF1, 2, feats, W), BF16),
            pltpu.VMEM((feats, kv), BF16),
            pltpu.VMEM((n_all, 2, 2, 64, 2 * W), BF16),
            pltpu.VMEM((2, 2, 64, kv), BF16),
            pltpu.VMEM((n_all, 2, 64, 2 * W), BF16),
            pltpu.VMEM((2, 64, kv), BF16),
            pltpu.VMEM((n_all, 64, 2 * W), BF16),
            pltpu.VMEM((64, kv), BF16),
            pltpu.VMEM((n_all, 64, 2 * W), BF16),
            pltpu.VMEM((64, kv), BF16),
            pltpu.VMEM((n_q + EARLY, 64, 2 * W), BF16),
            pltpu.VMEM((64, kv), BF16),
            pltpu.VMEM((2, 32, cols), BF16),
            pltpu.VMEM((32, cols), BF16),
            dma((n_q,)),
            dma((NBUF1, 2)),
            dma,
            dma,
            dma((3, 2)),
            dma((8,)),
            dma((8,)),
            dma((n_all,)),
            dma((n_all,)),
            dma((n_q, 3)),
            dma((n_q, 3)),
            dma((3,)),
            dma((3,)),
            dma((EARLY,)),
            dma((EARLY,)),
            dma((n_q, 2)),
            dma((n_q, 2)),
            dma((2,)),
            dma((2,)),
            dma((2,)),
            dma((n_ff, 2)),
            dma((EARLY,)),
            dma((2,)),
        ],
        compiler_params=pltpu.CompilerParams(collective_id=0, has_side_effects=True, vmem_limit_bytes=VMEM_LIMIT),
        cost_estimate=pl.CostEstimate(flops=flops, bytes_accessed=feats * (flops // (rows * feats)), transcendentals=0),
    )(hidden.reshape(2, 2, 64, half), gain, w_q, w_kv, w_gate, w_up)


def attend_kernel(lens, q_ref, kv_ref, k_ref, v_ref, k_out, v_out, o_ref):
    step = pl.program_id(0)
    n_pos = k_ref.shape[2]
    scale = q_ref.shape[2] ** -0.5 * LOG2E
    for s in range(SEQ_STEP):
        length = lens[step * SEQ_STEP + s]
        base = pl.multiple_of((length // 16) * 16, 16)
        k_out[0, s] = k_ref[0, s]
        v_out[0, s] = v_ref[0, s]
        hit = lax.broadcasted_iota(jnp.int32, (16, k_ref.shape[3]), 0) == length - base
        for src, dst, which in ((k_ref, k_out, 0), (v_ref, v_out, 1)):
            old = src[0, s, pl.ds(base, 16), :].astype(F32)
            new = kv_ref[s, which:which + 1, :].astype(F32)
            dst[0, s, pl.ds(base, 16), :] = jnp.where(hit, new, old).astype(BF16)
        scores = lax.dot_general(q_ref[s], k_out[0, s], (((1,), (1,)), ((), ())), preferred_element_type=F32) * scale
        visible = lax.broadcasted_iota(jnp.int32, scores.shape, 1) <= length
        scores = jnp.where(visible, scores, MASKED)
        weights = jnp.exp2(scores - jnp.max(scores, axis=1, keepdims=True))
        probs = (weights * (1.0 / jnp.sum(weights, axis=1, keepdims=True))).astype(BF16)
        o_ref[s] = jnp.dot(probs, v_out[0, s], preferred_element_type=F32).astype(BF16)


def attend(lens, q, kv, k_cache, v_cache):
    seqs, heads, dim = q.shape
    n_pos = k_cache.shape[2]
    cache_spec = pl.BlockSpec((1, SEQ_STEP, n_pos, dim), lambda b, lens: (0, b, 0, 0))
    q_spec = pl.BlockSpec((SEQ_STEP, heads, dim), lambda b, lens: (b, 0, 0))
    return pl.pallas_call(
        attend_kernel,
        name="attend",
        out_shape=(
            jax.ShapeDtypeStruct(k_cache.shape, BF16),
            jax.ShapeDtypeStruct(v_cache.shape, BF16),
            jax.ShapeDtypeStruct(q.shape, BF16),
        ),
        grid_spec=pltpu.PrefetchScalarGridSpec(
            num_scalar_prefetch=1,
            grid=(seqs // SEQ_STEP,),
            in_specs=[q_spec, pl.BlockSpec((SEQ_STEP, 2, dim), lambda b, lens: (b, 0, 0)), cache_spec, cache_spec],
            out_specs=(cache_spec, cache_spec, q_spec),
        ),
        compiler_params=pltpu.CompilerParams(dimension_semantics=("arbitrary",), vmem_limit_bytes=66_000_000),
        cost_estimate=pl.CostEstimate(
            flops=10**10, bytes_accessed=8 * k_cache.size, transcendentals=seqs * heads * n_pos),
    )(lens, q, kv, k_cache, v_cache)


def output_kernel(
    n_ff, n_o, o_in, keep, recv_e, recv_l, hidden, w_o, w_down, out,
    acts, wbuf, acc, keep_v, recv_v, h_v, y_src, y_dst,
    w_sem, keep_sem, recv_sem, h_sem, oo_sems, on_send, on_recv, far_send, far_recv, near_send, near_recv, y_sems,
):
    xi = lax.axis_index("x")
    yj = lax.axis_index("yz")
    core = lax.rem(xi, 2)
    mate = xi + 1 - 2 * core
    across = lax.rem(xi + 2, 4)
    other_y = 1 - yj
    n_m = n_ff // GROUP
    n_g = n_m + n_o // GROUP
    n_early = EARLY // GROUP
    depth = GROUP * W
    d_out = w_down.shape[2]
    half = d_out // 2

    barrier = pltpu.get_barrier_semaphore()
    for x_, y_ in ((mate, yj), (across, yj), (xi, other_y)):
        pl.semaphore_signal(barrier, inc=1, **dev(x=x_, yz=y_))

    def keep_copy(g):
        return pltpu.make_async_copy(
            keep.at[pl.ds(GROUP * g, GROUP)], keep_v.at[pl.ds(GROUP * g, GROUP)], keep_sem.at[g])

    def recv_copy(g):
        src = recv_e.at[pl.ds(GROUP * g, GROUP)] if g < n_early else recv_l.at[pl.ds(GROUP * (g - n_early), GROUP)]
        return pltpu.make_async_copy(src, recv_v.at[pl.ds(GROUP * g, GROUP)], recv_sem.at[g])

    for g in range(n_m):
        keep_copy(g).start()
        recv_copy(g).start()

    def rows_of(p, owner):
        off, size = PARTS[p]
        return pl.ds(pl.multiple_of(4 * off + owner * size, 16), size)

    def block(p, g, owner):
        return acts.at[pl.ds(GROUP * g, GROUP), rows_of(p, owner)]

    def o_rows(s):
        row = (1 - yj) * (32 * xi + 16 * s) + yj * (128 + 64 * s + 16 * xi)
        return acts.at[pl.ds(n_ff, n_o), pl.ds(pl.multiple_of(row, 16), 16)]

    def o_own(s):
        return pltpu.make_async_copy(o_in.at[yj, :, pl.ds(16 * s, 16)], o_rows(s), oo_sems.at[s])

    def o_copy(s):
        return pltpu.make_async_remote_copy(
            src_ref=o_in.at[other_y, :, pl.ds(16 * s, 16)], dst_ref=o_rows(s), send_sem=on_send.at[s],
            recv_sem=on_recv.at[s], **dev(x=xi, yz=other_y))

    h_load = pltpu.make_async_copy(hidden, h_v, h_sem)

    def load_weights(g):
        slot = lax.rem(g, NBUF3)

        @pl.when(g < n_m)
        def _():
            pltpu.make_async_copy(
                w_down.at[0, pl.ds(pl.multiple_of(g * depth, W), depth)], wbuf.at[slot], w_sem.at[slot]).start()

        @pl.when(g >= n_m)
        def _():
            pltpu.make_async_copy(
                w_o.at[0, pl.ds(pl.multiple_of((g - n_m) * depth, W), depth)], wbuf.at[slot], w_sem.at[slot]).start()

    def far_copy(p, g):
        return pltpu.make_async_remote_copy(
            src_ref=block(p, g, xi), dst_ref=block(p, g, xi), send_sem=far_send.at[p, g], recv_sem=far_recv.at[p, g],
            **dev(x=across, yz=yj))

    def near_copy(p, g, which):
        rows = block(p, g, xi if which == 0 else across)
        return pltpu.make_async_remote_copy(
            src_ref=rows, dst_ref=rows, send_sem=near_send.at[p, g, which], recv_sem=near_recv.at[p, g, which],
            **dev(x=mate, yz=yj))

    def give(p, g):
        far_copy(p, g).start()
        near_copy(p, g, 0).start()

    def give_m(p, g):
        off, size = PARTS[p]
        for k in range(GROUP):
            t = GROUP * g + k
            z = keep_v[t, off:off + size].astype(F32) + recv_v[t, off:off + size].astype(F32)
            acts[t, rows_of(p, xi)] = silu_mul(z[:, :W], z[:, W:])
        give(p, g)

    pl.semaphore_wait(barrier, 3)
    for g in range(n_m):
        keep_copy(g).wait()
        recv_copy(g).wait()
        give_m(0, g)
        if g == 0:
            for s in range(2):
                o_copy(s).start()
                o_own(s).start()
            for s in range(NBUF3):
                load_weights(jnp.int32(s))
            h_load.start()
    acc[...] = jnp.zeros_like(acc)
    for s in range(2):
        o_own(s).wait()
        o_copy(s).wait_recv()

    def chunk(p, k):
        return k if p % 2 == 0 else n_g - 1 - k

    for g in range(n_m, n_g):
        give(0, g)
    for p in range(1, len(PARTS)):
        @pl.loop(0, n_g)
        def _(k):
            g = chunk(p, k)

            @pl.when(g < n_m)
            def _():
                give_m(p, g)

            @pl.when(g >= n_m)
            def _():
                give(p, g)

    def forward(p, k):
        g = chunk(p, k)
        far_copy(p, g).wait_recv()
        near_copy(p, g, 1).start()

    def multiply(p, k):
        g = chunk(p, k)
        slot = lax.rem(g, NBUF3)

        @pl.when(k >= (0 if p == 0 else NBUF3))
        def _():
            pltpu.make_async_copy(w_down.at[0, pl.ds(0, depth)], wbuf.at[slot], w_sem.at[slot]).wait()

        near_copy(p, g, 0).wait_recv()
        near_copy(p, g, 1).wait_recv()
        off, size = PARTS[p]
        rows = slice(4 * off, 4 * (off + size))
        for n in range(d_out // W):
            cols = slice(n * W, (n + 1) * W)
            total = acc[rows, cols]
            for j in range(GROUP):
                total += jnp.dot(
                    acts[GROUP * g + j, rows], wbuf[slot, j * W:(j + 1) * W, cols], preferred_element_type=F32)
            acc[rows, cols] = total

        @pl.when(k + NBUF3 < n_g)
        def _():
            load_weights(chunk(p, k + NBUF3))

    def cols_of(j):
        return pl.ds(pl.multiple_of(j * half, 128), half)

    def y_copy(p):
        rows = slice(4 * PARTS[p][0], 4 * sum(PARTS[p]))
        return pltpu.make_async_remote_copy(
            src_ref=y_src.at[rows], dst_ref=y_dst.at[rows], send_sem=y_sems.at[p, 0], recv_sem=y_sems.at[p, 1],
            **dev(x=xi, yz=other_y))

    def exchange(p):
        rows = slice(4 * PARTS[p][0], 4 * sum(PARTS[p]))
        y_src[rows] = acc[rows, cols_of(other_y)].astype(BF16)
        y_copy(p).start()

    def finalize(p):
        off, size = PARTS[p]
        rows = slice(4 * off, 4 * (off + size))
        y_copy(p).wait_recv()
        total = (acc[rows, cols_of(yj)] + y_dst[rows].astype(F32)).reshape(4, size, half)
        out[:, off:off + size] = (h_v[:, off:off + size].astype(F32) + total).astype(BF16)

    for p in range(len(PARTS)):
        forward(p, jnp.int32(0))
        if p > 0:
            multiply(p - 1, jnp.int32(n_g - 1))
            exchange(p - 1)
        if p == 1:
            h_load.wait()

        @pl.loop(1, n_g)
        def _(k):
            forward(p, k)
            multiply(p, k - 1)

        if p > 0:
            finalize(p - 1)

    last = len(PARTS) - 1
    multiply(last, jnp.int32(n_g - 1))
    exchange(last)
    for s in range(2):
        o_copy(s).wait_send()
    for p in range(len(PARTS)):
        @pl.loop(0, n_g)
        def _(g):
            far_copy(p, g).wait_send()
            near_copy(p, g, 0).wait_send()
            near_copy(p, g, 1).wait_send()

    finalize(last)
    for p in range(len(PARTS)):
        y_copy(p).wait_send()


def finish(o, keep, recv_e, recv_l, hidden, w_o, w_down):
    rows, half = hidden.shape
    n_ff = w_down.shape[1] // W
    n_o = w_o.shape[1] // W
    n_m = n_ff // GROUP
    n_g = n_m + n_o // GROUP
    n_p = len(PARTS)
    d_out = w_down.shape[2]
    dma = pltpu.SemaphoreType.DMA
    any_spec = pl.BlockSpec(memory_space=pl.ANY)
    vmem = pl.BlockSpec(memory_space=pltpu.VMEM)
    flops = 2 * rows * d_out * (w_down.shape[1] + w_o.shape[1])
    out = pl.pallas_call(
        functools.partial(output_kernel, n_ff, n_o),
        name="finish",
        out_shape=jax.ShapeDtypeStruct((4, 64, half), BF16),
        in_specs=[any_spec] * 7,
        out_specs=vmem,
        scratch_shapes=[
            pltpu.VMEM((n_ff + n_o, rows, W), BF16),
            pltpu.VMEM((NBUF3, GROUP * W, d_out), BF16),
            pltpu.VMEM((rows, d_out), F32),
            pltpu.VMEM(keep.shape, BF16),
            pltpu.VMEM(keep.shape, BF16),
            pltpu.VMEM((4, 64, half), BF16),
            pltpu.VMEM((rows, half), BF16),
            pltpu.VMEM((rows, half), BF16),
            dma((NBUF3,)),
            dma((n_m,)),
            dma((n_m,)),
            dma,
            dma((2,)),
            dma((2,)),
            dma((2,)),
            dma((n_p, n_g)),
            dma((n_p, n_g)),
            dma((n_p, n_g, 2)),
            dma((n_p, n_g, 2)),
            dma((n_p, 2)),
        ],
        compiler_params=pltpu.CompilerParams(collective_id=1, has_side_effects=True, vmem_limit_bytes=56_000_000),
        cost_estimate=pl.CostEstimate(flops=flops, bytes_accessed=2 * d_out * (w_down.shape[1] + w_o.shape[1]), transcendentals=0),
    )(o, keep, recv_e, recv_l, hidden.reshape(4, 64, half), w_o, w_down)
    return out.reshape(rows, half)


def solution(mesh):
    x_size = mesh.shape["x"]
    y_size = mesh.shape["yz"]
    row_spec = P("dp", ("x", "yz"))
    tile_in = P(None, "x", "yz")
    tile_out = P(None, "yz", "x")
    cache_spec = P(None, ("dp", "x", "yz"))
    len_spec = P(("dp", "x", "yz"))

    def device_step(hidden, norm_gain, w_q, w_kv, w_gate, w_up, w_o, w_down, k_cache, v_cache, seq_len):
        d_model = hidden.shape[1] * x_size * y_size
        seqs = k_cache.shape[1]
        dim = k_cache.shape[3]
        q_cols = w_q.shape[2]
        heads = q_cols // dim
        qkv, keep, recv_e, send = project(hidden, norm_gain, w_q, w_kv, w_gate, w_up, d_model)
        recv_l = lax.ppermute(send, "x", [(i, (i + x_size // 2) % x_size) for i in range(x_size)])
        q = qkv[:, :, :q_cols].reshape(y_size, seqs, heads, dim).transpose(1, 0, 2, 3).reshape(seqs, y_size * heads, dim)
        kv = qkv[:, :, q_cols:].transpose(1, 0, 2)
        k_new, v_new, o = attend(seq_len, q, kv, k_cache, v_cache)
        o = o.reshape(seqs, y_size, q_cols // W, W).transpose(1, 2, 0, 3)
        hidden_out = finish(o, keep, recv_e, recv_l, hidden, w_o, w_down)
        return hidden_out, k_new, v_new

    return jax.shard_map(
        device_step,
        mesh=mesh,
        in_specs=(row_spec, P(None, "x"), tile_in, tile_in, tile_in, tile_in, tile_out, tile_out, cache_spec, cache_spec, len_spec),
        out_specs=(row_spec, cache_spec, cache_spec),
        check_vma=False,
    )
```

```python
import functools

import jax
import jax.numpy as jnp
from jax import lax
from jax.experimental import pallas as pl
from jax.experimental.pallas import tpu as pltpu
from jax.sharding import PartitionSpec as P

NORM_EPS = 1e-6
W = 512
NBUF1 = 4
NBUF3 = 6
GROUP = 3
PARTS = ((0, 32), (32, 16), (48, 16))
EARLY = 12
SEQ_STEP = 2
VMEM_LIMIT = 64_000_000
F32 = jnp.float32
BF16 = jnp.bfloat16
LOG2E = 1.4426950408889634
MASKED = -1e30


def dev(**axes):
    return dict(device_id=axes, device_id_type=pl.DeviceIdType.MESH)


def silu_mul(gate, up):
    gate = gate.astype(BF16).astype(F32)
    up = up.astype(BF16).astype(F32)
    return (jax.nn.silu(gate) * up).astype(BF16)


def project_kernel(
    n_q, n_ff, d_model, hidden, gain, wq, wkv, wg, wu,
    qkv_out, keep_out, recv_out, send_out,
    h_own, h_other, u, inv_all, sq_all, wq_buf, wbuf, wkv_buf, part, part_kv, near, near_kv, keep, keep_kv, far_src,
    far_src_kv, far, far_kv, z_rows, z_other,
    wq_sem, w_sem, wkv_sem, h_in, h_sems, sq_send, sq_recv, near_send, near_recv, qn_send, qn_recv, kn_send, kn_recv,
    far_send, far_recv, qf_send, qf_recv, kf_send, kf_recv, y_sems, out_sem, qkv_sem,
):
    xi = lax.axis_index("x")
    yj = lax.axis_index("yz")
    core = lax.rem(xi, 2)
    chip = xi // 2
    mate = xi + 1 - 2 * core
    across = lax.rem(xi + 2, 4)
    other_y = 1 - yj
    me = xi * 2 + yj
    half = hidden.shape[-1]
    n_all = n_q + n_ff
    n_far = n_q + EARLY
    to_mate = dev(x=mate, yz=yj)
    to_across = dev(x=across, yz=yj)

    barrier = pltpu.get_barrier_semaphore()
    for k in range(1, 8):
        peer = lax.rem(me + k, 8)
        pl.semaphore_signal(barrier, inc=1, **dev(x=peer // 2, yz=lax.rem(peer, 2)))
    h_load = pltpu.make_async_copy(hidden, h_own, h_in)
    h_load.start()

    def start_weights(g):
        slot = lax.rem(g, NBUF1)
        cols = pl.ds(pl.multiple_of((g - n_q) * W, W), W)
        pltpu.make_async_copy(wg.at[0, :, cols], wbuf.at[slot, 0], w_sem.at[slot, 0]).start()
        pltpu.make_async_copy(wu.at[0, :, cols], wbuf.at[slot, 1], w_sem.at[slot, 1]).start()

    def wait_weights(slot, k):
        pltpu.make_async_copy(wg.at[0, :, pl.ds(0, W)], wbuf.at[slot, k], w_sem.at[slot, k]).wait()

    def wq_copy(g):
        return pltpu.make_async_copy(wq.at[0, :, g * 2 * W:(g + 1) * 2 * W], wq_buf.at[g], wq_sem.at[g])

    h_load.wait()
    for g in range(n_q):
        wq_copy(g).start()
    kv_copy = pltpu.make_async_copy(wkv.at[0], wkv_buf, wkv_sem)
    kv_copy.start()

    h_f32 = h_own[...].reshape(256, half).astype(F32)
    sq_all[me] = lax.dot_general(
        jnp.ones((8, half), F32), h_f32 * h_f32, (((1,), (1,)), ((), ())),
        precision=lax.Precision.HIGHEST, preferred_element_type=F32)
    pl.semaphore_wait(barrier, 7)

    def sq_copy(peer, src):
        return pltpu.make_async_remote_copy(
            src_ref=sq_all.at[src], dst_ref=sq_all.at[src], send_sem=sq_send.at[peer], recv_sem=sq_recv.at[src],
            **dev(x=peer // 2, yz=lax.rem(peer, 2)))

    def side_of(step):
        return 1 - chip if step < 2 else chip

    def piece(step):
        return pl.ds(32 * step, 32) if step < 2 else pl.ds(0, 64)

    def h_copy(step):
        block = (side_of(step), slice(None), piece(step))
        return pltpu.make_async_remote_copy(
            src_ref=h_own.at[block], dst_ref=h_other.at[block],
            send_sem=h_sems.at[step, 0], recv_sem=h_sems.at[step, 1], **dev(x=xi, yz=other_y))

    for k in range(1, 8):
        sq_copy(lax.rem(me + k, 8), me).start()
    for step in range(3):
        h_copy(step).start()
    for k in range(1, 8):
        peer = lax.rem(me + k, 8)
        sq_copy(peer, peer).wait_recv()
    total = jnp.sum(sq_all[...], axis=0)
    inv = lax.rsqrt(total / d_model + NORM_EPS)
    inv_all[...] = jnp.transpose(jnp.concatenate([inv] * 16, axis=0)).reshape(inv_all.shape)

    def normalize(values, step, which):
        cols = pl.ds(pl.multiple_of(which * half, 128), half)
        side, rows = side_of(step), piece(step)
        u[side, :, rows, cols] = (
            values[side, :, rows].astype(F32) * inv_all[side, :, rows, :1] * gain[:, cols].astype(F32)).astype(BF16)

    def near_copy(g):
        return pltpu.make_async_remote_copy(
            src_ref=part.at[g, :, 1 - core], dst_ref=near.at[g], send_sem=near_send.at[g],
            recv_sem=near_recv.at[g], **to_mate)

    def near_copy_q(g, step):
        side, rows = side_of(step), piece(step)
        return pltpu.make_async_remote_copy(
            src_ref=part.at[g, side, 1 - core, rows], dst_ref=near.at[g, side, rows],
            send_sem=qn_send.at[g, step], recv_sem=qn_recv.at[g, step], **to_mate)

    def near_copy_kv(step):
        side, rows = side_of(step), piece(step)
        return pltpu.make_async_remote_copy(
            src_ref=part_kv.at[side, 1 - core, rows], dst_ref=near_kv.at[side, rows],
            send_sem=kn_send.at[step], recv_sem=kn_recv.at[step], **to_mate)

    def far_copy(g):
        return pltpu.make_async_remote_copy(
            src_ref=far_src.at[g], dst_ref=recv_out.at[g - n_q], send_sem=far_send.at[g - n_q],
            recv_sem=far_recv.at[g - n_q], **to_across)

    def far_copy_q(g, step):
        rows = piece(step)
        return pltpu.make_async_remote_copy(
            src_ref=far_src.at[g, rows], dst_ref=far.at[g, rows], send_sem=qf_send.at[g, step],
            recv_sem=qf_recv.at[g, step], **to_across)

    def far_copy_kv(step):
        rows = piece(step)
        return pltpu.make_async_remote_copy(
            src_ref=far_src_kv.at[rows], dst_ref=far_kv.at[rows], send_sem=kf_send.at[step], recv_sem=kf_recv.at[step],
            **to_across)

    def keep_copy(g):
        return pltpu.make_async_copy(keep.at[g], keep_out.at[g - n_q], out_sem.at[g - n_q, 0])

    def send_copy(g):
        k = g - n_q
        return pltpu.make_async_copy(far_src.at[g], send_out.at[k - EARLY], out_sem.at[k, 1])

    def add(a, b):
        return (a.astype(F32) + b.astype(F32)).astype(BF16)

    def multiply(g):
        slot = lax.rem(g, NBUF1)
        for k in range(2):
            wait_weights(slot, k)
            res = jnp.dot(u[...].reshape(256, u.shape[-1]), wbuf[slot, k], preferred_element_type=F32).astype(BF16)
            part[g, :, :, :, k * W:(k + 1) * W] = res.reshape(2, 2, 64, W)
        near_copy(g).start()

        @pl.when(g + NBUF1 < n_all)
        def _():
            start_weights(g + NBUF1)

    def reduce_near(g):
        near_copy(g).wait_recv()
        far_src[g] = add(part[g, 1 - chip, core], near[g, 1 - chip])

        @pl.when(g < n_far)
        def _():
            far_copy(g).start()

        @pl.when(g >= n_far)
        def _():
            send_copy(g).start()

        keep[g] = add(part[g, chip, core], near[g, chip])
        keep_copy(g).start()

    def multiply_q(step):
        side, rows = side_of(step), piece(step)
        lhs = u[side, :, rows].reshape(2 * rows.size, u.shape[-1])
        for g in range(n_q):
            if step == 0:
                wq_copy(g).wait()
            for k in range(2):
                res = jnp.dot(lhs, wq_buf[g, :, k * W:(k + 1) * W], preferred_element_type=F32).astype(BF16)
                part[g, side, :, rows, k * W:(k + 1) * W] = res.reshape(2, rows.size, W)
            near_copy_q(g, step).start()
            if step == 0 and g >= 2:
                reduce_q(0, g - 2)
        if step == 0:
            kv_copy.wait()
        res = jnp.dot(lhs, wkv_buf[...], preferred_element_type=F32).astype(BF16)
        part_kv[side, :, rows] = res.reshape(2, rows.size, res.shape[1])
        near_copy_kv(step).start()

    def reduce_q(step, g):
        side, rows = side_of(step), piece(step)
        near_copy_q(g, step).wait_recv()
        total_q = add(part[g, side, core, rows], near[g, side, rows])
        if step < 2:
            far_src[g, rows] = total_q
            far_copy_q(g, step).start()
        else:
            keep[g] = total_q

    def reduce_kv(step):
        side, rows = side_of(step), piece(step)
        near_copy_kv(step).wait_recv()
        total_kv = add(part_kv[side, core, rows], near_kv[side, rows])
        if step < 2:
            far_src_kv[rows] = total_kv
            far_copy_kv(step).start()
        else:
            keep_kv[...] = total_kv

    for step in range(3):
        normalize(h_own, step, yj)
        h_copy(step).wait_recv()
        normalize(h_other, step, other_y)
        if step < 2:
            multiply_q(step)
            for g in range(n_q - 2 if step == 0 else 0, n_q):
                reduce_q(step, g)
            reduce_kv(step)
        if step == 0:
            for g in range(n_q, n_q + NBUF1):
                start_weights(jnp.int32(g))

    @pl.loop(n_q, n_far)
    def _(g):
        multiply(g)

        @pl.when(g >= n_q + 2)
        def _():
            reduce_near(g - 2)

    q_cols = n_q * 2 * W
    multiply_q(2)
    for g in range(n_q):
        reduce_q(2, g)
        for step in range(2):
            far_copy_q(g, step).wait_recv()
        z_rows[:, :, g * 2 * W:(g + 1) * 2 * W] = add(keep[g], far[g]).reshape(2, 32, 2 * W)
    reduce_kv(2)
    for step in range(2):
        far_copy_kv(step).wait_recv()
    z_kv = add(keep_kv[...], far_kv[...])
    z_rows[:, :, q_cols:] = z_kv.reshape(2, 32, z_kv.shape[1])
    y_copy = pltpu.make_async_remote_copy(
        src_ref=z_rows.at[other_y], dst_ref=z_other, send_sem=y_sems.at[0], recv_sem=y_sems.at[1],
        **dev(x=xi, yz=other_y))
    y_copy.start()
    qkv_own = pltpu.make_async_copy(z_rows.at[yj], qkv_out.at[yj], qkv_sem.at[0])
    qkv_own.start()

    @pl.loop(n_far, n_all)
    def _(g):
        multiply(g)
        reduce_near(g - 2)

    reduce_near(jnp.int32(n_all - 2))
    reduce_near(jnp.int32(n_all - 1))
    y_copy.wait_recv()
    qkv_other = pltpu.make_async_copy(z_other, qkv_out.at[other_y], qkv_sem.at[1])
    qkv_other.start()

    for step in range(3):
        h_copy(step).wait_send()
        near_copy_kv(step).wait_send()
        for g in range(n_q):
            near_copy_q(g, step).wait_send()
    for step in range(2):
        far_copy_kv(step).wait_send()
        for g in range(n_q):
            far_copy_q(g, step).wait_send()
    for k in range(1, 8):
        sq_copy(lax.rem(me + k, 8), me).wait_send()
    y_copy.wait_send()

    @pl.loop(n_q, n_all)
    def _(g):
        near_copy(g).wait_send()
        keep_copy(g).wait()

    @pl.loop(n_far, n_all)
    def _(g):
        send_copy(g).wait()

    qkv_own.wait()
    qkv_other.wait()

    @pl.loop(n_q, n_far)
    def _(g):
        far_copy(g).wait_send()
        far_copy(g).wait_recv()


def project(hidden, gain, w_q, w_kv, w_gate, w_up, d_model):
    rows, half = hidden.shape
    feats = w_q.shape[1]
    kv = w_kv.shape[2]
    n_q = w_q.shape[2] // (2 * W)
    n_ff = w_gate.shape[2] // W
    n_all = n_q + n_ff
    late = n_ff - EARLY
    dma = pltpu.SemaphoreType.DMA
    any_spec = pl.BlockSpec(memory_space=pl.ANY)
    vmem = pl.BlockSpec(memory_space=pltpu.VMEM)
    cols = w_q.shape[2] + kv
    flops = 2 * rows * feats * (w_q.shape[2] + kv + 2 * w_gate.shape[2])
    return pl.pallas_call(
        functools.partial(project_kernel, n_q, n_ff, d_model),
        name="project",
        out_shape=(
            jax.ShapeDtypeStruct((2, 32, cols), BF16),
            jax.ShapeDtypeStruct((n_ff, 64, 2 * W), BF16),
            jax.ShapeDtypeStruct((EARLY, 64, 2 * W), BF16),
            jax.ShapeDtypeStruct((late, 64, 2 * W), BF16),
        ),
        in_specs=[any_spec, vmem, any_spec, any_spec, any_spec, any_spec],
        out_specs=(any_spec, any_spec, any_spec, any_spec),
        scratch_shapes=[
            pltpu.VMEM((2, 2, 64, half), BF16),
            pltpu.VMEM((2, 2, 64, half), BF16),
            pltpu.VMEM((2, 2, 64, feats), BF16),
            pltpu.VMEM((2, 2, 64, 128), F32),
            pltpu.VMEM((8, 8, rows), F32),
            pltpu.VMEM((n_q, feats, 2 * W), BF16),
            pltpu.VMEM((NBUF1, 2, feats, W), BF16),
            pltpu.VMEM((feats, kv), BF16),
            pltpu.VMEM((n_all, 2, 2, 64, 2 * W), BF16),
            pltpu.VMEM((2, 2, 64, kv), BF16),
            pltpu.VMEM((n_all, 2, 64, 2 * W), BF16),
            pltpu.VMEM((2, 64, kv), BF16),
            pltpu.VMEM((n_all, 64, 2 * W), BF16),
            pltpu.VMEM((64, kv), BF16),
            pltpu.VMEM((n_all, 64, 2 * W), BF16),
            pltpu.VMEM((64, kv), BF16),
            pltpu.VMEM((n_q, 64, 2 * W), BF16),
            pltpu.VMEM((64, kv), BF16),
            pltpu.VMEM((2, 32, cols), BF16),
            pltpu.VMEM((32, cols), BF16),
            dma((n_q,)),
            dma((NBUF1, 2)),
            dma,
            dma,
            dma((3, 2)),
            dma((8,)),
            dma((8,)),
            dma((n_all,)),
            dma((n_all,)),
            dma((n_q, 3)),
            dma((n_q, 3)),
            dma((3,)),
            dma((3,)),
            dma((EARLY,)),
            dma((EARLY,)),
            dma((n_q, 2)),
            dma((n_q, 2)),
            dma((2,)),
            dma((2,)),
            dma((2,)),
            dma((n_ff, 2)),
            dma((2,)),
        ],
        compiler_params=pltpu.CompilerParams(collective_id=0, has_side_effects=True, vmem_limit_bytes=VMEM_LIMIT),
        cost_estimate=pl.CostEstimate(flops=flops, bytes_accessed=feats * (flops // (rows * feats)), transcendentals=0),
    )(hidden.reshape(2, 2, 64, half), gain, w_q, w_kv, w_gate, w_up)


def attend_kernel(lens, q_ref, kv_ref, k_ref, v_ref, k_out, v_out, o_ref):
    step = pl.program_id(0)
    n_pos = k_ref.shape[2]
    scale = q_ref.shape[2] ** -0.5 * LOG2E
    for s in range(SEQ_STEP):
        length = lens[step * SEQ_STEP + s]
        base = pl.multiple_of((length // 16) * 16, 16)
        k_out[0, s] = k_ref[0, s]
        v_out[0, s] = v_ref[0, s]
        hit = lax.broadcasted_iota(jnp.int32, (16, k_ref.shape[3]), 0) == length - base
        for src, dst, which in ((k_ref, k_out, 0), (v_ref, v_out, 1)):
            old = src[0, s, pl.ds(base, 16), :].astype(F32)
            new = kv_ref[s, which:which + 1, :].astype(F32)
            dst[0, s, pl.ds(base, 16), :] = jnp.where(hit, new, old).astype(BF16)
        scores = lax.dot_general(q_ref[s], k_out[0, s], (((1,), (1,)), ((), ())), preferred_element_type=F32) * scale
        visible = lax.broadcasted_iota(jnp.int32, scores.shape, 1) <= length
        scores = jnp.where(visible, scores, MASKED)
        weights = jnp.exp2(scores - jnp.max(scores, axis=1, keepdims=True))
        probs = (weights * (1.0 / jnp.sum(weights, axis=1, keepdims=True))).astype(BF16)
        o_ref[s] = jnp.dot(probs, v_out[0, s], preferred_element_type=F32).astype(BF16)


def attend(lens, q, kv, k_cache, v_cache):
    seqs, heads, dim = q.shape
    n_pos = k_cache.shape[2]
    cache_spec = pl.BlockSpec((1, SEQ_STEP, n_pos, dim), lambda b, lens: (0, b, 0, 0))
    q_spec = pl.BlockSpec((SEQ_STEP, heads, dim), lambda b, lens: (b, 0, 0))
    return pl.pallas_call(
        attend_kernel,
        name="attend",
        out_shape=(
            jax.ShapeDtypeStruct(k_cache.shape, BF16),
            jax.ShapeDtypeStruct(v_cache.shape, BF16),
            jax.ShapeDtypeStruct(q.shape, BF16),
        ),
        grid_spec=pltpu.PrefetchScalarGridSpec(
            num_scalar_prefetch=1,
            grid=(seqs // SEQ_STEP,),
            in_specs=[q_spec, pl.BlockSpec((SEQ_STEP, 2, dim), lambda b, lens: (b, 0, 0)), cache_spec, cache_spec],
            out_specs=(cache_spec, cache_spec, q_spec),
        ),
        compiler_params=pltpu.CompilerParams(dimension_semantics=("arbitrary",), vmem_limit_bytes=66_000_000),
        cost_estimate=pl.CostEstimate(
            flops=10**10, bytes_accessed=8 * k_cache.size, transcendentals=seqs * heads * n_pos),
    )(lens, q, kv, k_cache, v_cache)


def output_kernel(
    n_ff, n_o, o_in, keep, recv_e, recv_l, hidden, w_o, w_down, out,
    acts, wbuf, acc, keep_v, recv_v, h_v, y_src, y_dst,
    w_sem, keep_sem, recv_sem, h_sem, oo_sems, on_send, on_recv, far_send, far_recv, near_send, near_recv, y_sems,
):
    xi = lax.axis_index("x")
    yj = lax.axis_index("yz")
    core = lax.rem(xi, 2)
    mate = xi + 1 - 2 * core
    across = lax.rem(xi + 2, 4)
    other_y = 1 - yj
    n_m = n_ff // GROUP
    n_g = n_m + n_o // GROUP
    n_early = EARLY // GROUP
    depth = GROUP * W
    d_out = w_down.shape[2]
    half = d_out // 2

    barrier = pltpu.get_barrier_semaphore()
    for x_, y_ in ((mate, yj), (across, yj), (xi, other_y)):
        pl.semaphore_signal(barrier, inc=1, **dev(x=x_, yz=y_))

    def keep_copy(g):
        return pltpu.make_async_copy(
            keep.at[pl.ds(GROUP * g, GROUP)], keep_v.at[pl.ds(GROUP * g, GROUP)], keep_sem.at[g])

    def recv_copy(g):
        src = recv_e.at[pl.ds(GROUP * g, GROUP)] if g < n_early else recv_l.at[pl.ds(GROUP * (g - n_early), GROUP)]
        return pltpu.make_async_copy(src, recv_v.at[pl.ds(GROUP * g, GROUP)], recv_sem.at[g])

    keep_copy(0).start()
    recv_copy(0).start()

    def rows_of(p, owner):
        off, size = PARTS[p]
        return pl.ds(pl.multiple_of(4 * off + owner * size, 16), size)

    def block(p, g, owner):
        return acts.at[pl.ds(GROUP * g, GROUP), rows_of(p, owner)]

    def o_rows(s):
        row = (1 - yj) * (32 * xi + 16 * s) + yj * (128 + 64 * s + 16 * xi)
        return acts.at[pl.ds(n_ff, n_o), pl.ds(pl.multiple_of(row, 16), 16)]

    def o_own(s):
        return pltpu.make_async_copy(o_in.at[yj, :, pl.ds(16 * s, 16)], o_rows(s), oo_sems.at[s])

    def o_copy(s):
        return pltpu.make_async_remote_copy(
            src_ref=o_in.at[other_y, :, pl.ds(16 * s, 16)], dst_ref=o_rows(s), send_sem=on_send.at[s],
            recv_sem=on_recv.at[s], **dev(x=xi, yz=other_y))

    h_load = pltpu.make_async_copy(hidden, h_v, h_sem)

    def load_weights(g):
        slot = lax.rem(g, NBUF3)

        @pl.when(g < n_m)
        def _():
            pltpu.make_async_copy(
                w_down.at[0, pl.ds(pl.multiple_of(g * depth, W), depth)], wbuf.at[slot], w_sem.at[slot]).start()

        @pl.when(g >= n_m)
        def _():
            pltpu.make_async_copy(
                w_o.at[0, pl.ds(pl.multiple_of((g - n_m) * depth, W), depth)], wbuf.at[slot], w_sem.at[slot]).start()

    def far_copy(p, g):
        return pltpu.make_async_remote_copy(
            src_ref=block(p, g, xi), dst_ref=block(p, g, xi), send_sem=far_send.at[p, g], recv_sem=far_recv.at[p, g],
            **dev(x=across, yz=yj))

    def near_copy(p, g, which):
        rows = block(p, g, xi if which == 0 else across)
        return pltpu.make_async_remote_copy(
            src_ref=rows, dst_ref=rows, send_sem=near_send.at[p, g, which], recv_sem=near_recv.at[p, g, which],
            **dev(x=mate, yz=yj))

    def give(p, g):
        far_copy(p, g).start()
        near_copy(p, g, 0).start()

    def give_m(p, g):
        off, size = PARTS[p]
        for k in range(GROUP):
            t = GROUP * g + k
            z = keep_v[t, off:off + size].astype(F32) + recv_v[t, off:off + size].astype(F32)
            acts[t, rows_of(p, xi)] = silu_mul(z[:, :W], z[:, W:])
        give(p, g)

    pl.semaphore_wait(barrier, 3)
    for g in range(n_m):
        keep_copy(g).wait()
        recv_copy(g).wait()
        give_m(0, g)
        if g == 0:
            for s in range(2):
                o_copy(s).start()
                o_own(s).start()
            for k in range(1, n_m):
                keep_copy(k).start()
                recv_copy(k).start()
    for s in range(NBUF3):
        load_weights(jnp.int32(s))
    h_load.start()
    acc[...] = jnp.zeros_like(acc)
    for s in range(2):
        o_own(s).wait()
        o_copy(s).wait_recv()

    def chunk(p, k):
        return k if p % 2 == 0 else n_g - 1 - k

    for g in range(n_m, n_g):
        give(0, g)
    for p in range(1, len(PARTS)):
        @pl.loop(0, n_g)
        def _(k):
            g = chunk(p, k)

            @pl.when(g < n_m)
            def _():
                give_m(p, g)

            @pl.when(g >= n_m)
            def _():
                give(p, g)

    def forward(p, k):
        g = chunk(p, k)
        far_copy(p, g).wait_recv()
        near_copy(p, g, 1).start()

    def multiply(p, k):
        g = chunk(p, k)
        slot = lax.rem(g, NBUF3)

        @pl.when(k >= (0 if p == 0 else NBUF3))
        def _():
            pltpu.make_async_copy(w_down.at[0, pl.ds(0, depth)], wbuf.at[slot], w_sem.at[slot]).wait()

        near_copy(p, g, 0).wait_recv()
        near_copy(p, g, 1).wait_recv()
        off, size = PARTS[p]
        rows = slice(4 * off, 4 * (off + size))
        for n in range(d_out // W):
            cols = slice(n * W, (n + 1) * W)
            total = acc[rows, cols]
            for j in range(GROUP):
                total += jnp.dot(
                    acts[GROUP * g + j, rows], wbuf[slot, j * W:(j + 1) * W, cols], preferred_element_type=F32)
            acc[rows, cols] = total

        @pl.when(k + NBUF3 < n_g)
        def _():
            load_weights(chunk(p, k + NBUF3))

    def cols_of(j):
        return pl.ds(pl.multiple_of(j * half, 128), half)

    def y_copy(p):
        rows = slice(4 * PARTS[p][0], 4 * sum(PARTS[p]))
        return pltpu.make_async_remote_copy(
            src_ref=y_src.at[rows], dst_ref=y_dst.at[rows], send_sem=y_sems.at[p, 0], recv_sem=y_sems.at[p, 1],
            **dev(x=xi, yz=other_y))

    def exchange(p):
        rows = slice(4 * PARTS[p][0], 4 * sum(PARTS[p]))
        y_src[rows] = acc[rows, cols_of(other_y)].astype(BF16)
        y_copy(p).start()

    def finalize(p):
        off, size = PARTS[p]
        rows = slice(4 * off, 4 * (off + size))
        y_copy(p).wait_recv()
        total = (acc[rows, cols_of(yj)] + y_dst[rows].astype(F32)).reshape(4, size, half)
        out[:, off:off + size] = (h_v[:, off:off + size].astype(F32) + total).astype(BF16)

    for p in range(len(PARTS)):
        forward(p, jnp.int32(0))
        if p > 0:
            multiply(p - 1, jnp.int32(n_g - 1))
            exchange(p - 1)
        if p == 1:
            h_load.wait()

        @pl.loop(1, n_g)
        def _(k):
            forward(p, k)
            multiply(p, k - 1)

        if p > 0:
            finalize(p - 1)

    last = len(PARTS) - 1
    multiply(last, jnp.int32(n_g - 1))
    exchange(last)
    for s in range(2):
        o_copy(s).wait_send()
    for p in range(len(PARTS)):
        @pl.loop(0, n_g)
        def _(g):
            far_copy(p, g).wait_send()
            near_copy(p, g, 0).wait_send()
            near_copy(p, g, 1).wait_send()

    finalize(last)
    for p in range(len(PARTS)):
        y_copy(p).wait_send()


def finish(o, keep, recv_e, recv_l, hidden, w_o, w_down):
    rows, half = hidden.shape
    n_ff = w_down.shape[1] // W
    n_o = w_o.shape[1] // W
    n_m = n_ff // GROUP
    n_g = n_m + n_o // GROUP
    n_p = len(PARTS)
    d_out = w_down.shape[2]
    dma = pltpu.SemaphoreType.DMA
    any_spec = pl.BlockSpec(memory_space=pl.ANY)
    vmem = pl.BlockSpec(memory_space=pltpu.VMEM)
    flops = 2 * rows * d_out * (w_down.shape[1] + w_o.shape[1])
    out = pl.pallas_call(
        functools.partial(output_kernel, n_ff, n_o),
        name="finish",
        out_shape=jax.ShapeDtypeStruct((4, 64, half), BF16),
        in_specs=[any_spec] * 7,
        out_specs=vmem,
        scratch_shapes=[
            pltpu.VMEM((n_ff + n_o, rows, W), BF16),
            pltpu.VMEM((NBUF3, GROUP * W, d_out), BF16),
            pltpu.VMEM((rows, d_out), F32),
            pltpu.VMEM(keep.shape, BF16),
            pltpu.VMEM(keep.shape, BF16),
            pltpu.VMEM((4, 64, half), BF16),
            pltpu.VMEM((rows, half), BF16),
            pltpu.VMEM((rows, half), BF16),
            dma((NBUF3,)),
            dma((n_m,)),
            dma((n_m,)),
            dma,
            dma((2,)),
            dma((2,)),
            dma((2,)),
            dma((n_p, n_g)),
            dma((n_p, n_g)),
            dma((n_p, n_g, 2)),
            dma((n_p, n_g, 2)),
            dma((n_p, 2)),
        ],
        compiler_params=pltpu.CompilerParams(collective_id=1, has_side_effects=True, vmem_limit_bytes=56_000_000),
        cost_estimate=pl.CostEstimate(flops=flops, bytes_accessed=2 * d_out * (w_down.shape[1] + w_o.shape[1]), transcendentals=0),
    )(o, keep, recv_e, recv_l, hidden.reshape(4, 64, half), w_o, w_down)
    return out.reshape(rows, half)


def solution(mesh):
    x_size = mesh.shape["x"]
    y_size = mesh.shape["yz"]
    row_spec = P("dp", ("x", "yz"))
    tile_in = P(None, "x", "yz")
    tile_out = P(None, "yz", "x")
    cache_spec = P(None, ("dp", "x", "yz"))
    len_spec = P(("dp", "x", "yz"))

    def device_step(hidden, norm_gain, w_q, w_kv, w_gate, w_up, w_o, w_down, k_cache, v_cache, seq_len):
        d_model = hidden.shape[1] * x_size * y_size
        seqs = k_cache.shape[1]
        dim = k_cache.shape[3]
        q_cols = w_q.shape[2]
        heads = q_cols // dim
        qkv, keep, recv_e, send = project(hidden, norm_gain, w_q, w_kv, w_gate, w_up, d_model)
        recv_l = lax.ppermute(send, "x", [(i, (i + x_size // 2) % x_size) for i in range(x_size)])
        q = qkv[:, :, :q_cols].reshape(y_size, seqs, heads, dim).transpose(1, 0, 2, 3).reshape(seqs, y_size * heads, dim)
        kv = qkv[:, :, q_cols:].transpose(1, 0, 2)
        k_new, v_new, o = attend(seq_len, q, kv, k_cache, v_cache)
        o = o.reshape(seqs, y_size, q_cols // W, W).transpose(1, 2, 0, 3)
        hidden_out = finish(o, keep, recv_e, recv_l, hidden, w_o, w_down)
        return hidden_out, k_new, v_new

    return jax.shard_map(
        device_step,
        mesh=mesh,
        in_specs=(row_spec, P(None, "x"), tile_in, tile_in, tile_in, tile_in, tile_out, tile_out, cache_spec, cache_spec, len_spec),
        out_specs=(row_spec, cache_spec, cache_spec),
        check_vma=False,
    )
```

```python
import functools

import jax
import jax.numpy as jnp
from jax import lax
from jax.experimental import pallas as pl
from jax.experimental.pallas import tpu as pltpu
from jax.sharding import PartitionSpec as P

NORM_EPS = 1e-6
W = 512
NBUF1 = 4
NBUF3 = 6
GROUP = 3
PARTS = ((0, 32), (32, 16), (48, 16))
EARLY = 9
SEQ_STEP = 2
VMEM_LIMIT = 64_000_000
F32 = jnp.float32
BF16 = jnp.bfloat16
LOG2E = 1.4426950408889634
MASKED = -1e30


def dev(**axes):
    return dict(device_id=axes, device_id_type=pl.DeviceIdType.MESH)


def silu_mul(gate, up):
    gate = gate.astype(BF16).astype(F32)
    up = up.astype(BF16).astype(F32)
    return (jax.nn.silu(gate) * up).astype(BF16)


def project_kernel(
    n_q, n_ff, d_model, hidden, gain, wq, wkv, wg, wu,
    qkv_out, keep_out, recv_out, send_out,
    h_own, h_other, u, inv_all, sq_all, wq_buf, wbuf, wkv_buf, part, part_kv, near, near_kv, keep, keep_kv, far_src,
    far_src_kv, far, far_kv, z_rows, z_other,
    wq_sem, w_sem, wkv_sem, h_in, h_sems, sq_send, sq_recv, near_send, near_recv, qn_send, qn_recv, kn_send, kn_recv,
    far_send, far_recv, qf_send, qf_recv, kf_send, kf_recv, y_sems, out_sem, qkv_sem,
):
    xi = lax.axis_index("x")
    yj = lax.axis_index("yz")
    core = lax.rem(xi, 2)
    chip = xi // 2
    mate = xi + 1 - 2 * core
    across = lax.rem(xi + 2, 4)
    other_y = 1 - yj
    me = xi * 2 + yj
    half = hidden.shape[-1]
    n_all = n_q + n_ff
    n_far = n_q + EARLY
    to_mate = dev(x=mate, yz=yj)
    to_across = dev(x=across, yz=yj)

    barrier = pltpu.get_barrier_semaphore()
    for k in range(1, 8):
        peer = lax.rem(me + k, 8)
        pl.semaphore_signal(barrier, inc=1, **dev(x=peer // 2, yz=lax.rem(peer, 2)))
    h_load = pltpu.make_async_copy(hidden, h_own, h_in)
    h_load.start()

    def start_weights(g):
        slot = lax.rem(g, NBUF1)
        cols = pl.ds(pl.multiple_of((g - n_q) * W, W), W)
        pltpu.make_async_copy(wg.at[0, :, cols], wbuf.at[slot, 0], w_sem.at[slot, 0]).start()
        pltpu.make_async_copy(wu.at[0, :, cols], wbuf.at[slot, 1], w_sem.at[slot, 1]).start()

    def wait_weights(slot, k):
        pltpu.make_async_copy(wg.at[0, :, pl.ds(0, W)], wbuf.at[slot, k], w_sem.at[slot, k]).wait()

    def wq_copy(g):
        return pltpu.make_async_copy(wq.at[0, :, g * 2 * W:(g + 1) * 2 * W], wq_buf.at[g], wq_sem.at[g])

    h_load.wait()
    for g in range(n_q):
        wq_copy(g).start()
    kv_copy = pltpu.make_async_copy(wkv.at[0], wkv_buf, wkv_sem)
    kv_copy.start()

    h_f32 = h_own[...].reshape(256, half).astype(F32)
    sq_all[me] = lax.dot_general(
        jnp.ones((8, half), F32), h_f32 * h_f32, (((1,), (1,)), ((), ())),
        precision=lax.Precision.HIGHEST, preferred_element_type=F32)
    pl.semaphore_wait(barrier, 7)

    def sq_copy(peer, src):
        return pltpu.make_async_remote_copy(
            src_ref=sq_all.at[src], dst_ref=sq_all.at[src], send_sem=sq_send.at[peer], recv_sem=sq_recv.at[src],
            **dev(x=peer // 2, yz=lax.rem(peer, 2)))

    def side_of(step):
        return 1 - chip if step < 2 else chip

    def piece(step):
        return pl.ds(32 * step, 32) if step < 2 else pl.ds(0, 64)

    def h_copy(step):
        block = (side_of(step), slice(None), piece(step))
        return pltpu.make_async_remote_copy(
            src_ref=h_own.at[block], dst_ref=h_other.at[block],
            send_sem=h_sems.at[step, 0], recv_sem=h_sems.at[step, 1], **dev(x=xi, yz=other_y))

    for k in range(1, 8):
        sq_copy(lax.rem(me + k, 8), me).start()
    for step in range(3):
        h_copy(step).start()
    for k in range(1, 8):
        peer = lax.rem(me + k, 8)
        sq_copy(peer, peer).wait_recv()
    total = jnp.sum(sq_all[...], axis=0)
    inv = lax.rsqrt(total / d_model + NORM_EPS)
    inv_all[...] = jnp.transpose(jnp.concatenate([inv] * 16, axis=0)).reshape(inv_all.shape)

    def normalize(values, step, which):
        cols = pl.ds(pl.multiple_of(which * half, 128), half)
        side, rows = side_of(step), piece(step)
        u[side, :, rows, cols] = (
            values[side, :, rows].astype(F32) * inv_all[side, :, rows, :1] * gain[:, cols].astype(F32)).astype(BF16)

    def near_copy(g):
        return pltpu.make_async_remote_copy(
            src_ref=part.at[g, :, 1 - core], dst_ref=near.at[g], send_sem=near_send.at[g],
            recv_sem=near_recv.at[g], **to_mate)

    def near_copy_q(g, step):
        side, rows = side_of(step), piece(step)
        return pltpu.make_async_remote_copy(
            src_ref=part.at[g, side, 1 - core, rows], dst_ref=near.at[g, side, rows],
            send_sem=qn_send.at[g, step], recv_sem=qn_recv.at[g, step], **to_mate)

    def near_copy_kv(step):
        side, rows = side_of(step), piece(step)
        return pltpu.make_async_remote_copy(
            src_ref=part_kv.at[side, 1 - core, rows], dst_ref=near_kv.at[side, rows],
            send_sem=kn_send.at[step], recv_sem=kn_recv.at[step], **to_mate)

    def far_copy(g):
        return pltpu.make_async_remote_copy(
            src_ref=far_src.at[g], dst_ref=recv_out.at[g - n_q], send_sem=far_send.at[g - n_q],
            recv_sem=far_recv.at[g - n_q], **to_across)

    def far_copy_q(g, step):
        rows = piece(step)
        return pltpu.make_async_remote_copy(
            src_ref=far_src.at[g, rows], dst_ref=far.at[g, rows], send_sem=qf_send.at[g, step],
            recv_sem=qf_recv.at[g, step], **to_across)

    def far_copy_kv(step):
        rows = piece(step)
        return pltpu.make_async_remote_copy(
            src_ref=far_src_kv.at[rows], dst_ref=far_kv.at[rows], send_sem=kf_send.at[step], recv_sem=kf_recv.at[step],
            **to_across)

    def keep_copy(g):
        return pltpu.make_async_copy(keep.at[g], keep_out.at[g - n_q], out_sem.at[g - n_q, 0])

    def send_copy(g):
        k = g - n_q
        return pltpu.make_async_copy(far_src.at[g], send_out.at[k - EARLY], out_sem.at[k, 1])

    def add(a, b):
        return (a.astype(F32) + b.astype(F32)).astype(BF16)

    def multiply(g):
        slot = lax.rem(g, NBUF1)
        for k in range(2):
            wait_weights(slot, k)
            res = jnp.dot(u[...].reshape(256, u.shape[-1]), wbuf[slot, k], preferred_element_type=F32).astype(BF16)
            part[g, :, :, :, k * W:(k + 1) * W] = res.reshape(2, 2, 64, W)
        near_copy(g).start()

        @pl.when(g + NBUF1 < n_all)
        def _():
            start_weights(g + NBUF1)

    def reduce_near(g):
        near_copy(g).wait_recv()
        far_src[g] = add(part[g, 1 - chip, core], near[g, 1 - chip])

        @pl.when(g < n_far)
        def _():
            far_copy(g).start()

        @pl.when(g >= n_far)
        def _():
            send_copy(g).start()

        keep[g] = add(part[g, chip, core], near[g, chip])
        keep_copy(g).start()

    def multiply_q(step):
        side, rows = side_of(step), piece(step)
        lhs = u[side, :, rows].reshape(2 * rows.size, u.shape[-1])
        for g in range(n_q):
            if step == 0:
                wq_copy(g).wait()
            for k in range(2):
                res = jnp.dot(lhs, wq_buf[g, :, k * W:(k + 1) * W], preferred_element_type=F32).astype(BF16)
                part[g, side, :, rows, k * W:(k + 1) * W] = res.reshape(2, rows.size, W)
            near_copy_q(g, step).start()
            if step == 0 and g >= 2:
                reduce_q(0, g - 2)
        if step == 0:
            kv_copy.wait()
        res = jnp.dot(lhs, wkv_buf[...], preferred_element_type=F32).astype(BF16)
        part_kv[side, :, rows] = res.reshape(2, rows.size, res.shape[1])
        near_copy_kv(step).start()

    def reduce_q(step, g):
        side, rows = side_of(step), piece(step)
        near_copy_q(g, step).wait_recv()
        total_q = add(part[g, side, core, rows], near[g, side, rows])
        if step < 2:
            far_src[g, rows] = total_q
            far_copy_q(g, step).start()
        else:
            keep[g] = total_q

    def reduce_kv(step):
        side, rows = side_of(step), piece(step)
        near_copy_kv(step).wait_recv()
        total_kv = add(part_kv[side, core, rows], near_kv[side, rows])
        if step < 2:
            far_src_kv[rows] = total_kv
            far_copy_kv(step).start()
        else:
            keep_kv[...] = total_kv

    for step in range(3):
        normalize(h_own, step, yj)
        h_copy(step).wait_recv()
        normalize(h_other, step, other_y)
        if step < 2:
            multiply_q(step)
            for g in range(n_q - 2 if step == 0 else 0, n_q):
                reduce_q(step, g)
            reduce_kv(step)
        if step == 0:
            for g in range(n_q, n_q + NBUF1):
                start_weights(jnp.int32(g))

    @pl.loop(n_q, n_far)
    def _(g):
        multiply(g)

        @pl.when(g >= n_q + 2)
        def _():
            reduce_near(g - 2)

    q_cols = n_q * 2 * W
    multiply_q(2)
    for g in range(n_q):
        reduce_q(2, g)
        for step in range(2):
            far_copy_q(g, step).wait_recv()
        z_rows[:, :, g * 2 * W:(g + 1) * 2 * W] = add(keep[g], far[g]).reshape(2, 32, 2 * W)
    reduce_kv(2)
    for step in range(2):
        far_copy_kv(step).wait_recv()
    z_kv = add(keep_kv[...], far_kv[...])
    z_rows[:, :, q_cols:] = z_kv.reshape(2, 32, z_kv.shape[1])
    y_copy = pltpu.make_async_remote_copy(
        src_ref=z_rows.at[other_y], dst_ref=z_other, send_sem=y_sems.at[0], recv_sem=y_sems.at[1],
        **dev(x=xi, yz=other_y))
    y_copy.start()
    qkv_own = pltpu.make_async_copy(z_rows.at[yj], qkv_out.at[yj], qkv_sem.at[0])
    qkv_own.start()

    @pl.loop(n_far, n_all)
    def _(g):
        multiply(g)
        reduce_near(g - 2)

    reduce_near(jnp.int32(n_all - 2))
    reduce_near(jnp.int32(n_all - 1))
    y_copy.wait_recv()
    qkv_other = pltpu.make_async_copy(z_other, qkv_out.at[other_y], qkv_sem.at[1])
    qkv_other.start()

    for step in range(3):
        h_copy(step).wait_send()
        near_copy_kv(step).wait_send()
        for g in range(n_q):
            near_copy_q(g, step).wait_send()
    for step in range(2):
        far_copy_kv(step).wait_send()
        for g in range(n_q):
            far_copy_q(g, step).wait_send()
    for k in range(1, 8):
        sq_copy(lax.rem(me + k, 8), me).wait_send()
    y_copy.wait_send()

    @pl.loop(n_q, n_all)
    def _(g):
        near_copy(g).wait_send()
        keep_copy(g).wait()

    @pl.loop(n_far, n_all)
    def _(g):
        send_copy(g).wait()

    qkv_own.wait()
    qkv_other.wait()

    @pl.loop(n_q, n_far)
    def _(g):
        far_copy(g).wait_send()
        far_copy(g).wait_recv()


def project(hidden, gain, w_q, w_kv, w_gate, w_up, d_model):
    rows, half = hidden.shape
    feats = w_q.shape[1]
    kv = w_kv.shape[2]
    n_q = w_q.shape[2] // (2 * W)
    n_ff = w_gate.shape[2] // W
    n_all = n_q + n_ff
    late = n_ff - EARLY
    dma = pltpu.SemaphoreType.DMA
    any_spec = pl.BlockSpec(memory_space=pl.ANY)
    vmem = pl.BlockSpec(memory_space=pltpu.VMEM)
    cols = w_q.shape[2] + kv
    flops = 2 * rows * feats * (w_q.shape[2] + kv + 2 * w_gate.shape[2])
    return pl.pallas_call(
        functools.partial(project_kernel, n_q, n_ff, d_model),
        name="project",
        out_shape=(
            jax.ShapeDtypeStruct((2, 32, cols), BF16),
            jax.ShapeDtypeStruct((n_ff, 64, 2 * W), BF16),
            jax.ShapeDtypeStruct((EARLY, 64, 2 * W), BF16),
            jax.ShapeDtypeStruct((late, 64, 2 * W), BF16),
        ),
        in_specs=[any_spec, vmem, any_spec, any_spec, any_spec, any_spec],
        out_specs=(any_spec, any_spec, any_spec, any_spec),
        scratch_shapes=[
            pltpu.VMEM((2, 2, 64, half), BF16),
            pltpu.VMEM((2, 2, 64, half), BF16),
            pltpu.VMEM((2, 2, 64, feats), BF16),
            pltpu.VMEM((2, 2, 64, 128), F32),
            pltpu.VMEM((8, 8, rows), F32),
            pltpu.VMEM((n_q, feats, 2 * W), BF16),
            pltpu.VMEM((NBUF1, 2, feats, W), BF16),
            pltpu.VMEM((feats, kv), BF16),
            pltpu.VMEM((n_all, 2, 2, 64, 2 * W), BF16),
            pltpu.VMEM((2, 2, 64, kv), BF16),
            pltpu.VMEM((n_all, 2, 64, 2 * W), BF16),
            pltpu.VMEM((2, 64, kv), BF16),
            pltpu.VMEM((n_all, 64, 2 * W), BF16),
            pltpu.VMEM((64, kv), BF16),
            pltpu.VMEM((n_all, 64, 2 * W), BF16),
            pltpu.VMEM((64, kv), BF16),
            pltpu.VMEM((n_q, 64, 2 * W), BF16),
            pltpu.VMEM((64, kv), BF16),
            pltpu.VMEM((2, 32, cols), BF16),
            pltpu.VMEM((32, cols), BF16),
            dma((n_q,)),
            dma((NBUF1, 2)),
            dma,
            dma,
            dma((3, 2)),
            dma((8,)),
            dma((8,)),
            dma((n_all,)),
            dma((n_all,)),
            dma((n_q, 3)),
            dma((n_q, 3)),
            dma((3,)),
            dma((3,)),
            dma((EARLY,)),
            dma((EARLY,)),
            dma((n_q, 2)),
            dma((n_q, 2)),
            dma((2,)),
            dma((2,)),
            dma((2,)),
            dma((n_ff, 2)),
            dma((2,)),
        ],
        compiler_params=pltpu.CompilerParams(collective_id=0, has_side_effects=True, vmem_limit_bytes=VMEM_LIMIT),
        cost_estimate=pl.CostEstimate(flops=flops, bytes_accessed=feats * (flops // (rows * feats)), transcendentals=0),
    )(hidden.reshape(2, 2, 64, half), gain, w_q, w_kv, w_gate, w_up)


def attend_kernel(lens, q_ref, kv_ref, k_ref, v_ref, k_out, v_out, o_ref):
    step = pl.program_id(0)
    n_pos = k_ref.shape[2]
    scale = q_ref.shape[2] ** -0.5 * LOG2E
    for s in range(SEQ_STEP):
        length = lens[step * SEQ_STEP + s]
        base = pl.multiple_of((length // 16) * 16, 16)
        k_out[0, s] = k_ref[0, s]
        v_out[0, s] = v_ref[0, s]
        hit = lax.broadcasted_iota(jnp.int32, (16, k_ref.shape[3]), 0) == length - base
        for src, dst, which in ((k_ref, k_out, 0), (v_ref, v_out, 1)):
            old = src[0, s, pl.ds(base, 16), :].astype(F32)
            new = kv_ref[s, which:which + 1, :].astype(F32)
            dst[0, s, pl.ds(base, 16), :] = jnp.where(hit, new, old).astype(BF16)
        scores = lax.dot_general(q_ref[s], k_out[0, s], (((1,), (1,)), ((), ())), preferred_element_type=F32) * scale
        visible = lax.broadcasted_iota(jnp.int32, scores.shape, 1) <= length
        scores = jnp.where(visible, scores, MASKED)
        weights = jnp.exp2(scores - jnp.max(scores, axis=1, keepdims=True))
        probs = (weights * (1.0 / jnp.sum(weights, axis=1, keepdims=True))).astype(BF16)
        o_ref[s] = jnp.dot(probs, v_out[0, s], preferred_element_type=F32).astype(BF16)


def attend(lens, q, kv, k_cache, v_cache):
    seqs, heads, dim = q.shape
    n_pos = k_cache.shape[2]
    cache_spec = pl.BlockSpec((1, SEQ_STEP, n_pos, dim), lambda b, lens: (0, b, 0, 0))
    q_spec = pl.BlockSpec((SEQ_STEP, heads, dim), lambda b, lens: (b, 0, 0))
    return pl.pallas_call(
        attend_kernel,
        name="attend",
        out_shape=(
            jax.ShapeDtypeStruct(k_cache.shape, BF16),
            jax.ShapeDtypeStruct(v_cache.shape, BF16),
            jax.ShapeDtypeStruct(q.shape, BF16),
        ),
        grid_spec=pltpu.PrefetchScalarGridSpec(
            num_scalar_prefetch=1,
            grid=(seqs // SEQ_STEP,),
            in_specs=[q_spec, pl.BlockSpec((SEQ_STEP, 2, dim), lambda b, lens: (b, 0, 0)), cache_spec, cache_spec],
            out_specs=(cache_spec, cache_spec, q_spec),
        ),
        compiler_params=pltpu.CompilerParams(dimension_semantics=("arbitrary",), vmem_limit_bytes=66_000_000),
        cost_estimate=pl.CostEstimate(
            flops=10**10, bytes_accessed=8 * k_cache.size, transcendentals=seqs * heads * n_pos),
    )(lens, q, kv, k_cache, v_cache)


def output_kernel(
    n_ff, n_o, o_in, keep, recv_e, recv_l, hidden, w_o, w_down, out,
    acts, wbuf, acc, keep_v, recv_v, h_v, y_src, y_dst,
    w_sem, keep_sem, recv_sem, h_sem, oo_sems, on_send, on_recv, far_send, far_recv, near_send, near_recv, y_sems,
):
    xi = lax.axis_index("x")
    yj = lax.axis_index("yz")
    core = lax.rem(xi, 2)
    mate = xi + 1 - 2 * core
    across = lax.rem(xi + 2, 4)
    other_y = 1 - yj
    n_m = n_ff // GROUP
    n_g = n_m + n_o // GROUP
    n_early = EARLY // GROUP
    depth = GROUP * W
    d_out = w_down.shape[2]
    half = d_out // 2

    barrier = pltpu.get_barrier_semaphore()
    for x_, y_ in ((mate, yj), (across, yj), (xi, other_y)):
        pl.semaphore_signal(barrier, inc=1, **dev(x=x_, yz=y_))

    def keep_copy(g):
        return pltpu.make_async_copy(
            keep.at[pl.ds(GROUP * g, GROUP)], keep_v.at[pl.ds(GROUP * g, GROUP)], keep_sem.at[g])

    def recv_copy(g):
        src = recv_e.at[pl.ds(GROUP * g, GROUP)] if g < n_early else recv_l.at[pl.ds(GROUP * (g - n_early), GROUP)]
        return pltpu.make_async_copy(src, recv_v.at[pl.ds(GROUP * g, GROUP)], recv_sem.at[g])

    keep_copy(0).start()
    recv_copy(0).start()

    def rows_of(p, owner):
        off, size = PARTS[p]
        return pl.ds(pl.multiple_of(4 * off + owner * size, 16), size)

    def block(p, g, owner):
        return acts.at[pl.ds(GROUP * g, GROUP), rows_of(p, owner)]

    def o_rows(s):
        row = (1 - yj) * (32 * xi + 16 * s) + yj * (128 + 64 * s + 16 * xi)
        return acts.at[pl.ds(n_ff, n_o), pl.ds(pl.multiple_of(row, 16), 16)]

    def o_own(s):
        return pltpu.make_async_copy(o_in.at[yj, :, pl.ds(16 * s, 16)], o_rows(s), oo_sems.at[s])

    def o_copy(s):
        return pltpu.make_async_remote_copy(
            src_ref=o_in.at[other_y, :, pl.ds(16 * s, 16)], dst_ref=o_rows(s), send_sem=on_send.at[s],
            recv_sem=on_recv.at[s], **dev(x=xi, yz=other_y))

    h_load = pltpu.make_async_copy(hidden, h_v, h_sem)

    def load_weights(g):
        slot = lax.rem(g, NBUF3)

        @pl.when(g < n_m)
        def _():
            pltpu.make_async_copy(
                w_down.at[0, pl.ds(pl.multiple_of(g * depth, W), depth)], wbuf.at[slot], w_sem.at[slot]).start()

        @pl.when(g >= n_m)
        def _():
            pltpu.make_async_copy(
                w_o.at[0, pl.ds(pl.multiple_of((g - n_m) * depth, W), depth)], wbuf.at[slot], w_sem.at[slot]).start()

    def far_copy(p, g):
        return pltpu.make_async_remote_copy(
            src_ref=block(p, g, xi), dst_ref=block(p, g, xi), send_sem=far_send.at[p, g], recv_sem=far_recv.at[p, g],
            **dev(x=across, yz=yj))

    def near_copy(p, g, which):
        rows = block(p, g, xi if which == 0 else across)
        return pltpu.make_async_remote_copy(
            src_ref=rows, dst_ref=rows, send_sem=near_send.at[p, g, which], recv_sem=near_recv.at[p, g, which],
            **dev(x=mate, yz=yj))

    def give(p, g):
        far_copy(p, g).start()
        near_copy(p, g, 0).start()

    def give_m(p, g):
        off, size = PARTS[p]
        for k in range(GROUP):
            t = GROUP * g + k
            z = keep_v[t, off:off + size].astype(F32) + recv_v[t, off:off + size].astype(F32)
            acts[t, rows_of(p, xi)] = silu_mul(z[:, :W], z[:, W:])
        give(p, g)

    pl.semaphore_wait(barrier, 3)
    for g in range(n_m):
        keep_copy(g).wait()
        recv_copy(g).wait()
        give_m(0, g)
        if g == 0:
            for s in range(2):
                o_copy(s).start()
                o_own(s).start()
            for k in range(1, n_m):
                keep_copy(k).start()
                recv_copy(k).start()
    for s in range(NBUF3):
        load_weights(jnp.int32(s))
    h_load.start()
    acc[...] = jnp.zeros_like(acc)
    for s in range(2):
        o_own(s).wait()
        o_copy(s).wait_recv()

    def chunk(p, k):
        return k if p % 2 == 0 else n_g - 1 - k

    for g in range(n_m, n_g):
        give(0, g)
    for p in range(1, len(PARTS)):
        @pl.loop(0, n_g)
        def _(k):
            g = chunk(p, k)

            @pl.when(g < n_m)
            def _():
                give_m(p, g)

            @pl.when(g >= n_m)
            def _():
                give(p, g)

    def forward(p, k):
        g = chunk(p, k)
        far_copy(p, g).wait_recv()
        near_copy(p, g, 1).start()

    def multiply(p, k):
        g = chunk(p, k)
        slot = lax.rem(g, NBUF3)

        @pl.when(k >= (0 if p == 0 else NBUF3))
        def _():
            pltpu.make_async_copy(w_down.at[0, pl.ds(0, depth)], wbuf.at[slot], w_sem.at[slot]).wait()

        near_copy(p, g, 0).wait_recv()
        near_copy(p, g, 1).wait_recv()
        off, size = PARTS[p]
        rows = slice(4 * off, 4 * (off + size))
        for n in range(d_out // W):
            cols = slice(n * W, (n + 1) * W)
            total = acc[rows, cols]
            for j in range(GROUP):
                total += jnp.dot(
                    acts[GROUP * g + j, rows], wbuf[slot, j * W:(j + 1) * W, cols], preferred_element_type=F32)
            acc[rows, cols] = total

        @pl.when(k + NBUF3 < n_g)
        def _():
            load_weights(chunk(p, k + NBUF3))

    def cols_of(j):
        return pl.ds(pl.multiple_of(j * half, 128), half)

    def y_copy(p):
        rows = slice(4 * PARTS[p][0], 4 * sum(PARTS[p]))
        return pltpu.make_async_remote_copy(
            src_ref=y_src.at[rows], dst_ref=y_dst.at[rows], send_sem=y_sems.at[p, 0], recv_sem=y_sems.at[p, 1],
            **dev(x=xi, yz=other_y))

    def exchange(p):
        rows = slice(4 * PARTS[p][0], 4 * sum(PARTS[p]))
        y_src[rows] = acc[rows, cols_of(other_y)].astype(BF16)
        y_copy(p).start()

    def finalize(p):
        off, size = PARTS[p]
        rows = slice(4 * off, 4 * (off + size))
        y_copy(p).wait_recv()
        total = (acc[rows, cols_of(yj)] + y_dst[rows].astype(F32)).reshape(4, size, half)
        out[:, off:off + size] = (h_v[:, off:off + size].astype(F32) + total).astype(BF16)

    for p in range(len(PARTS)):
        forward(p, jnp.int32(0))
        if p > 0:
            multiply(p - 1, jnp.int32(n_g - 1))
            exchange(p - 1)
        if p == 1:
            h_load.wait()

        @pl.loop(1, n_g)
        def _(k):
            forward(p, k)
            multiply(p, k - 1)

        if p > 0:
            finalize(p - 1)

    last = len(PARTS) - 1
    multiply(last, jnp.int32(n_g - 1))
    exchange(last)
    for s in range(2):
        o_copy(s).wait_send()
    for p in range(len(PARTS)):
        @pl.loop(0, n_g)
        def _(g):
            far_copy(p, g).wait_send()
            near_copy(p, g, 0).wait_send()
            near_copy(p, g, 1).wait_send()

    finalize(last)
    for p in range(len(PARTS)):
        y_copy(p).wait_send()


def finish(o, keep, recv_e, recv_l, hidden, w_o, w_down):
    rows, half = hidden.shape
    n_ff = w_down.shape[1] // W
    n_o = w_o.shape[1] // W
    n_m = n_ff // GROUP
    n_g = n_m + n_o // GROUP
    n_p = len(PARTS)
    d_out = w_down.shape[2]
    dma = pltpu.SemaphoreType.DMA
    any_spec = pl.BlockSpec(memory_space=pl.ANY)
    vmem = pl.BlockSpec(memory_space=pltpu.VMEM)
    flops = 2 * rows * d_out * (w_down.shape[1] + w_o.shape[1])
    out = pl.pallas_call(
        functools.partial(output_kernel, n_ff, n_o),
        name="finish",
        out_shape=jax.ShapeDtypeStruct((4, 64, half), BF16),
        in_specs=[any_spec] * 7,
        out_specs=vmem,
        scratch_shapes=[
            pltpu.VMEM((n_ff + n_o, rows, W), BF16),
            pltpu.VMEM((NBUF3, GROUP * W, d_out), BF16),
            pltpu.VMEM((rows, d_out), F32),
            pltpu.VMEM(keep.shape, BF16),
            pltpu.VMEM(keep.shape, BF16),
            pltpu.VMEM((4, 64, half), BF16),
            pltpu.VMEM((rows, half), BF16),
            pltpu.VMEM((rows, half), BF16),
            dma((NBUF3,)),
            dma((n_m,)),
            dma((n_m,)),
            dma,
            dma((2,)),
            dma((2,)),
            dma((2,)),
            dma((n_p, n_g)),
            dma((n_p, n_g)),
            dma((n_p, n_g, 2)),
            dma((n_p, n_g, 2)),
            dma((n_p, 2)),
        ],
        compiler_params=pltpu.CompilerParams(collective_id=1, has_side_effects=True, vmem_limit_bytes=56_000_000),
        cost_estimate=pl.CostEstimate(flops=flops, bytes_accessed=2 * d_out * (w_down.shape[1] + w_o.shape[1]), transcendentals=0),
    )(o, keep, recv_e, recv_l, hidden.reshape(4, 64, half), w_o, w_down)
    return out.reshape(rows, half)


def solution(mesh):
    x_size = mesh.shape["x"]
    y_size = mesh.shape["yz"]
    row_spec = P("dp", ("x", "yz"))
    tile_in = P(None, "x", "yz")
    tile_out = P(None, "yz", "x")
    cache_spec = P(None, ("dp", "x", "yz"))
    len_spec = P(("dp", "x", "yz"))

    def device_step(hidden, norm_gain, w_q, w_kv, w_gate, w_up, w_o, w_down, k_cache, v_cache, seq_len):
        d_model = hidden.shape[1] * x_size * y_size
        seqs = k_cache.shape[1]
        dim = k_cache.shape[3]
        q_cols = w_q.shape[2]
        heads = q_cols // dim
        qkv, keep, recv_e, send = project(hidden, norm_gain, w_q, w_kv, w_gate, w_up, d_model)
        recv_l = lax.ppermute(send, "x", [(i, (i + x_size // 2) % x_size) for i in range(x_size)])
        q = qkv[:, :, :q_cols].reshape(y_size, seqs, heads, dim).transpose(1, 0, 2, 3).reshape(seqs, y_size * heads, dim)
        kv = qkv[:, :, q_cols:].transpose(1, 0, 2)
        k_new, v_new, o = attend(seq_len, q, kv, k_cache, v_cache)
        o = o.reshape(seqs, y_size, q_cols // W, W).transpose(1, 2, 0, 3)
        hidden_out = finish(o, keep, recv_e, recv_l, hidden, w_o, w_down)
        return hidden_out, k_new, v_new

    return jax.shard_map(
        device_step,
        mesh=mesh,
        in_specs=(row_spec, P(None, "x"), tile_in, tile_in, tile_in, tile_in, tile_out, tile_out, cache_spec, cache_spec, len_spec),
        out_specs=(row_spec, cache_spec, cache_spec),
        check_vma=False,
    )
```

```python
import functools

import jax
import jax.numpy as jnp
from jax import lax
from jax.experimental import pallas as pl
from jax.experimental.pallas import tpu as pltpu
from jax.sharding import PartitionSpec as P

NORM_EPS = 1e-6
W = 512
NBUF1 = 4
FAR = 2
NBUF3 = 3
GROUP = 6
PARTS = ((0, 32), (32, 16), (48, 16))
EARLY = 12
SEQ_STEP = 2
VMEM_LIMIT = 64_000_000
F32 = jnp.float32
BF16 = jnp.bfloat16
LOG2E = 1.4426950408889634
MASKED = -1e30


def dev(**axes):
    return dict(device_id=axes, device_id_type=pl.DeviceIdType.MESH)


def silu_mul(gate, up):
    gate = gate.astype(BF16).astype(F32)
    up = up.astype(BF16).astype(F32)
    return (jax.nn.silu(gate) * up).astype(BF16)


def project_kernel(
    n_q, n_ff, d_model, hidden, gain, wq, wkv, wg, wu,
    qkv_out, keep_out, recv_out, send_out,
    h_own, h_other, u, inv_all, sq_all, wq_buf, wbuf, wkv_buf, part, part_kv, near, near_kv, keep, keep_kv, far_src,
    far_src_kv, far, far_kv, z_rows, z_other,
    wq_sem, w_sem, wkv_sem, h_in, h_sems, sq_send, sq_recv, near_send, near_recv, qn_send, qn_recv, kn_send, kn_recv,
    far_send, far_recv, qf_send, qf_recv, kf_send, kf_recv, y_sems, out_sem, qkv_sem,
):
    xi = lax.axis_index("x")
    yj = lax.axis_index("yz")
    core = lax.rem(xi, 2)
    chip = xi // 2
    mate = xi + 1 - 2 * core
    across = lax.rem(xi + 2, 4)
    other_y = 1 - yj
    me = xi * 2 + yj
    half = hidden.shape[-1]
    n_all = n_q + n_ff
    n_far = n_q + EARLY
    to_mate = dev(x=mate, yz=yj)
    to_across = dev(x=across, yz=yj)

    barrier = pltpu.get_barrier_semaphore()
    for k in range(1, 8):
        peer = lax.rem(me + k, 8)
        pl.semaphore_signal(barrier, inc=1, **dev(x=peer // 2, yz=lax.rem(peer, 2)))
    h_load = pltpu.make_async_copy(hidden, h_own, h_in)
    h_load.start()

    def start_weights(g):
        slot = lax.rem(g, NBUF1)
        cols = pl.ds(pl.multiple_of((g - n_q) * W, W), W)
        pltpu.make_async_copy(wg.at[0, :, cols], wbuf.at[slot, 0], w_sem.at[slot, 0]).start()
        pltpu.make_async_copy(wu.at[0, :, cols], wbuf.at[slot, 1], w_sem.at[slot, 1]).start()

    def wait_weights(slot, k):
        pltpu.make_async_copy(wg.at[0, :, pl.ds(0, W)], wbuf.at[slot, k], w_sem.at[slot, k]).wait()

    def wq_copy(g):
        return pltpu.make_async_copy(wq.at[0, :, g * 2 * W:(g + 1) * 2 * W], wq_buf.at[g], wq_sem.at[g])

    h_load.wait()
    for g in range(n_q):
        wq_copy(g).start()
    kv_copy = pltpu.make_async_copy(wkv.at[0], wkv_buf, wkv_sem)
    kv_copy.start()

    h_f32 = h_own[...].reshape(256, half).astype(F32)
    sq_all[me] = lax.dot_general(
        jnp.ones((8, half), F32), h_f32 * h_f32, (((1,), (1,)), ((), ())),
        precision=lax.Precision.HIGHEST, preferred_element_type=F32)
    pl.semaphore_wait(barrier, 7)

    def sq_copy(peer, src):
        return pltpu.make_async_remote_copy(
            src_ref=sq_all.at[src], dst_ref=sq_all.at[src], send_sem=sq_send.at[peer], recv_sem=sq_recv.at[src],
            **dev(x=peer // 2, yz=lax.rem(peer, 2)))

    def side_of(step):
        return 1 - chip if step < 2 else chip

    def piece(step):
        return pl.ds(32 * step, 32) if step < 2 else pl.ds(0, 64)

    def h_copy(step):
        block = (side_of(step), slice(None), piece(step))
        return pltpu.make_async_remote_copy(
            src_ref=h_own.at[block], dst_ref=h_other.at[block],
            send_sem=h_sems.at[step, 0], recv_sem=h_sems.at[step, 1], **dev(x=xi, yz=other_y))

    for k in range(1, 8):
        sq_copy(lax.rem(me + k, 8), me).start()
    for step in range(3):
        h_copy(step).start()
    for k in range(1, 8):
        peer = lax.rem(me + k, 8)
        sq_copy(peer, peer).wait_recv()
    total = jnp.sum(sq_all[...], axis=0)
    inv = lax.rsqrt(total / d_model + NORM_EPS)
    inv_all[...] = jnp.transpose(jnp.concatenate([inv] * 16, axis=0)).reshape(inv_all.shape)

    def normalize(values, step, which):
        cols = pl.ds(pl.multiple_of(which * half, 128), half)
        side, rows = side_of(step), piece(step)
        u[side, :, rows, cols] = (
            values[side, :, rows].astype(F32) * inv_all[side, :, rows, :1] * gain[:, cols].astype(F32)).astype(BF16)

    def near_copy(g):
        return pltpu.make_async_remote_copy(
            src_ref=part.at[g, :, 1 - core], dst_ref=near.at[g], send_sem=near_send.at[g],
            recv_sem=near_recv.at[g], **to_mate)

    def near_copy_q(g, step):
        side, rows = side_of(step), piece(step)
        return pltpu.make_async_remote_copy(
            src_ref=part.at[g, side, 1 - core, rows], dst_ref=near.at[g, side, rows],
            send_sem=qn_send.at[g, step], recv_sem=qn_recv.at[g, step], **to_mate)

    def near_copy_kv(step):
        side, rows = side_of(step), piece(step)
        return pltpu.make_async_remote_copy(
            src_ref=part_kv.at[side, 1 - core, rows], dst_ref=near_kv.at[side, rows],
            send_sem=kn_send.at[step], recv_sem=kn_recv.at[step], **to_mate)

    def far_copy(k):
        return pltpu.make_async_remote_copy(
            src_ref=far_src.at[pl.ds(n_q + FAR * k, FAR)], dst_ref=recv_out.at[pl.ds(FAR * k, FAR)],
            send_sem=far_send.at[k], recv_sem=far_recv.at[k], **to_across)

    def far_copy_q(g, step):
        rows = piece(step)
        return pltpu.make_async_remote_copy(
            src_ref=far_src.at[g, rows], dst_ref=far.at[g, rows], send_sem=qf_send.at[g, step],
            recv_sem=qf_recv.at[g, step], **to_across)

    def far_copy_kv(step):
        rows = piece(step)
        return pltpu.make_async_remote_copy(
            src_ref=far_src_kv.at[rows], dst_ref=far_kv.at[rows], send_sem=kf_send.at[step], recv_sem=kf_recv.at[step],
            **to_across)

    def keep_copy(g):
        return pltpu.make_async_copy(keep.at[g], keep_out.at[g - n_q], out_sem.at[g - n_q, 0])

    def send_copy(g):
        k = g - n_q
        return pltpu.make_async_copy(far_src.at[g], send_out.at[k - EARLY], out_sem.at[k, 1])

    def add(a, b):
        return (a.astype(F32) + b.astype(F32)).astype(BF16)

    def multiply(g):
        slot = lax.rem(g, NBUF1)
        for k in range(2):
            wait_weights(slot, k)
            res = jnp.dot(u[...].reshape(256, u.shape[-1]), wbuf[slot, k], preferred_element_type=F32).astype(BF16)
            part[g, :, :, :, k * W:(k + 1) * W] = res.reshape(2, 2, 64, W)
        near_copy(g).start()

        @pl.when(g + NBUF1 < n_all)
        def _():
            start_weights(g + NBUF1)

    def reduce_near(g):
        near_copy(g).wait_recv()
        far_src[g] = add(part[g, 1 - chip, core], near[g, 1 - chip])

        @pl.when((g < n_far) & (lax.rem(g - n_q, FAR) == FAR - 1))
        def _():
            far_copy((g - n_q) // FAR).start()

        @pl.when(g >= n_far)
        def _():
            send_copy(g).start()

        keep[g] = add(part[g, chip, core], near[g, chip])
        keep_copy(g).start()

    def multiply_q(step):
        side, rows = side_of(step), piece(step)
        lhs = u[side, :, rows].reshape(2 * rows.size, u.shape[-1])
        for g in range(n_q):
            if step == 0:
                wq_copy(g).wait()
            for k in range(2):
                res = jnp.dot(lhs, wq_buf[g, :, k * W:(k + 1) * W], preferred_element_type=F32).astype(BF16)
                part[g, side, :, rows, k * W:(k + 1) * W] = res.reshape(2, rows.size, W)
            near_copy_q(g, step).start()
            if step == 0 and g >= 2:
                reduce_q(0, g - 2)
        if step == 0:
            kv_copy.wait()
        res = jnp.dot(lhs, wkv_buf[...], preferred_element_type=F32).astype(BF16)
        part_kv[side, :, rows] = res.reshape(2, rows.size, res.shape[1])
        near_copy_kv(step).start()

    def reduce_q(step, g):
        side, rows = side_of(step), piece(step)
        near_copy_q(g, step).wait_recv()
        total_q = add(part[g, side, core, rows], near[g, side, rows])
        if step < 2:
            far_src[g, rows] = total_q
            far_copy_q(g, step).start()
        else:
            keep[g] = total_q

    def reduce_kv(step):
        side, rows = side_of(step), piece(step)
        near_copy_kv(step).wait_recv()
        total_kv = add(part_kv[side, core, rows], near_kv[side, rows])
        if step < 2:
            far_src_kv[rows] = total_kv
            far_copy_kv(step).start()
        else:
            keep_kv[...] = total_kv

    for step in range(3):
        normalize(h_own, step, yj)
        h_copy(step).wait_recv()
        normalize(h_other, step, other_y)
        if step < 2:
            multiply_q(step)
            for g in range(n_q - 2 if step == 0 else 0, n_q):
                reduce_q(step, g)
            reduce_kv(step)
        if step == 0:
            for g in range(n_q, n_q + NBUF1):
                start_weights(jnp.int32(g))

    @pl.loop(n_q, n_far)
    def _(g):
        multiply(g)

        @pl.when(g >= n_q + 1)
        def _():
            reduce_near(g - 1)

    q_cols = n_q * 2 * W
    multiply_q(2)
    for g in range(n_q):
        reduce_q(2, g)
        for step in range(2):
            far_copy_q(g, step).wait_recv()
        z_rows[:, :, g * 2 * W:(g + 1) * 2 * W] = add(keep[g], far[g]).reshape(2, 32, 2 * W)
    reduce_kv(2)
    for step in range(2):
        far_copy_kv(step).wait_recv()
    z_kv = add(keep_kv[...], far_kv[...])
    z_rows[:, :, q_cols:] = z_kv.reshape(2, 32, z_kv.shape[1])
    y_copy = pltpu.make_async_remote_copy(
        src_ref=z_rows.at[other_y], dst_ref=z_other, send_sem=y_sems.at[0], recv_sem=y_sems.at[1],
        **dev(x=xi, yz=other_y))
    y_copy.start()
    qkv_own = pltpu.make_async_copy(z_rows.at[yj], qkv_out.at[yj], qkv_sem.at[0])
    qkv_own.start()

    @pl.loop(n_far, n_all)
    def _(g):
        multiply(g)
        reduce_near(g - 1)

    reduce_near(jnp.int32(n_all - 1))
    y_copy.wait_recv()
    qkv_other = pltpu.make_async_copy(z_other, qkv_out.at[other_y], qkv_sem.at[1])
    qkv_other.start()

    for step in range(3):
        h_copy(step).wait_send()
        near_copy_kv(step).wait_send()
        for g in range(n_q):
            near_copy_q(g, step).wait_send()
    for step in range(2):
        far_copy_kv(step).wait_send()
        for g in range(n_q):
            far_copy_q(g, step).wait_send()
    for k in range(1, 8):
        sq_copy(lax.rem(me + k, 8), me).wait_send()
    y_copy.wait_send()

    @pl.loop(n_q, n_all)
    def _(g):
        near_copy(g).wait_send()
        keep_copy(g).wait()

    @pl.loop(n_far, n_all)
    def _(g):
        send_copy(g).wait()

    qkv_own.wait()
    qkv_other.wait()

    @pl.loop(0, EARLY // FAR)
    def _(k):
        far_copy(k).wait_send()
        far_copy(k).wait_recv()


def project(hidden, gain, w_q, w_kv, w_gate, w_up, d_model):
    rows, half = hidden.shape
    feats = w_q.shape[1]
    kv = w_kv.shape[2]
    n_q = w_q.shape[2] // (2 * W)
    n_ff = w_gate.shape[2] // W
    n_all = n_q + n_ff
    late = n_ff - EARLY
    dma = pltpu.SemaphoreType.DMA
    any_spec = pl.BlockSpec(memory_space=pl.ANY)
    vmem = pl.BlockSpec(memory_space=pltpu.VMEM)
    cols = w_q.shape[2] + kv
    flops = 2 * rows * feats * (w_q.shape[2] + kv + 2 * w_gate.shape[2])
    return pl.pallas_call(
        functools.partial(project_kernel, n_q, n_ff, d_model),
        name="project",
        out_shape=(
            jax.ShapeDtypeStruct((2, 32, cols), BF16),
            jax.ShapeDtypeStruct((n_ff, 64, 2 * W), BF16),
            jax.ShapeDtypeStruct((EARLY, 64, 2 * W), BF16),
            jax.ShapeDtypeStruct((late, 64, 2 * W), BF16),
        ),
        in_specs=[any_spec, vmem, any_spec, any_spec, any_spec, any_spec],
        out_specs=(any_spec, any_spec, any_spec, any_spec),
        scratch_shapes=[
            pltpu.VMEM((2, 2, 64, half), BF16),
            pltpu.VMEM((2, 2, 64, half), BF16),
            pltpu.VMEM((2, 2, 64, feats), BF16),
            pltpu.VMEM((2, 2, 64, 128), F32),
            pltpu.VMEM((8, 8, rows), F32),
            pltpu.VMEM((n_q, feats, 2 * W), BF16),
            pltpu.VMEM((NBUF1, 2, feats, W), BF16),
            pltpu.VMEM((feats, kv), BF16),
            pltpu.VMEM((n_all, 2, 2, 64, 2 * W), BF16),
            pltpu.VMEM((2, 2, 64, kv), BF16),
            pltpu.VMEM((n_all, 2, 64, 2 * W), BF16),
            pltpu.VMEM((2, 64, kv), BF16),
            pltpu.VMEM((n_all, 64, 2 * W), BF16),
            pltpu.VMEM((64, kv), BF16),
            pltpu.VMEM((n_all, 64, 2 * W), BF16),
            pltpu.VMEM((64, kv), BF16),
            pltpu.VMEM((n_q, 64, 2 * W), BF16),
            pltpu.VMEM((64, kv), BF16),
            pltpu.VMEM((2, 32, cols), BF16),
            pltpu.VMEM((32, cols), BF16),
            dma((n_q,)),
            dma((NBUF1, 2)),
            dma,
            dma,
            dma((3, 2)),
            dma((8,)),
            dma((8,)),
            dma((n_all,)),
            dma((n_all,)),
            dma((n_q, 3)),
            dma((n_q, 3)),
            dma((3,)),
            dma((3,)),
            dma((EARLY // FAR,)),
            dma((EARLY // FAR,)),
            dma((n_q, 2)),
            dma((n_q, 2)),
            dma((2,)),
            dma((2,)),
            dma((2,)),
            dma((n_ff, 2)),
            dma((2,)),
        ],
        compiler_params=pltpu.CompilerParams(collective_id=0, has_side_effects=True, vmem_limit_bytes=VMEM_LIMIT),
        cost_estimate=pl.CostEstimate(flops=flops, bytes_accessed=feats * (flops // (rows * feats)), transcendentals=0),
    )(hidden.reshape(2, 2, 64, half), gain, w_q, w_kv, w_gate, w_up)


def attend_kernel(lens, q_ref, kv_ref, k_ref, v_ref, k_out, v_out, o_ref):
    step = pl.program_id(0)
    n_pos = k_ref.shape[2]
    scale = q_ref.shape[2] ** -0.5 * LOG2E
    for s in range(SEQ_STEP):
        length = lens[step * SEQ_STEP + s]
        base = pl.multiple_of((length // 16) * 16, 16)
        k_out[0, s] = k_ref[0, s]
        v_out[0, s] = v_ref[0, s]
        hit = lax.broadcasted_iota(jnp.int32, (16, k_ref.shape[3]), 0) == length - base
        for src, dst, which in ((k_ref, k_out, 0), (v_ref, v_out, 1)):
            old = src[0, s, pl.ds(base, 16), :].astype(F32)
            new = kv_ref[s, which:which + 1, :].astype(F32)
            dst[0, s, pl.ds(base, 16), :] = jnp.where(hit, new, old).astype(BF16)
        scores = lax.dot_general(q_ref[s], k_out[0, s], (((1,), (1,)), ((), ())), preferred_element_type=F32) * scale
        visible = lax.broadcasted_iota(jnp.int32, scores.shape, 1) <= length
        scores = jnp.where(visible, scores, MASKED)
        weights = jnp.exp2(scores - jnp.max(scores, axis=1, keepdims=True))
        probs = (weights * (1.0 / jnp.sum(weights, axis=1, keepdims=True))).astype(BF16)
        o_ref[s] = jnp.dot(probs, v_out[0, s], preferred_element_type=F32).astype(BF16)


def attend(lens, q, kv, k_cache, v_cache):
    seqs, heads, dim = q.shape
    n_pos = k_cache.shape[2]
    cache_spec = pl.BlockSpec((1, SEQ_STEP, n_pos, dim), lambda b, lens: (0, b, 0, 0))
    q_spec = pl.BlockSpec((SEQ_STEP, heads, dim), lambda b, lens: (b, 0, 0))
    return pl.pallas_call(
        attend_kernel,
        name="attend",
        out_shape=(
            jax.ShapeDtypeStruct(k_cache.shape, BF16),
            jax.ShapeDtypeStruct(v_cache.shape, BF16),
            jax.ShapeDtypeStruct(q.shape, BF16),
        ),
        grid_spec=pltpu.PrefetchScalarGridSpec(
            num_scalar_prefetch=1,
            grid=(seqs // SEQ_STEP,),
            in_specs=[q_spec, pl.BlockSpec((SEQ_STEP, 2, dim), lambda b, lens: (b, 0, 0)), cache_spec, cache_spec],
            out_specs=(cache_spec, cache_spec, q_spec),
        ),
        compiler_params=pltpu.CompilerParams(dimension_semantics=("arbitrary",), vmem_limit_bytes=66_000_000),
        cost_estimate=pl.CostEstimate(
            flops=10**10, bytes_accessed=8 * k_cache.size, transcendentals=seqs * heads * n_pos),
    )(lens, q, kv, k_cache, v_cache)


def output_kernel(
    n_ff, n_o, o_in, keep, recv_e, recv_l, hidden, w_o, w_down, out,
    acts, wbuf, acc, keep_v, recv_v, h_v, y_src, y_dst,
    w_sem, keep_sem, recv_sem, h_sem, oo_sems, on_send, on_recv, far_send, far_recv, near_send, near_recv, y_sems,
):
    xi = lax.axis_index("x")
    yj = lax.axis_index("yz")
    core = lax.rem(xi, 2)
    mate = xi + 1 - 2 * core
    across = lax.rem(xi + 2, 4)
    other_y = 1 - yj
    n_m = n_ff // GROUP
    n_g = n_m + n_o // GROUP
    n_early = EARLY // GROUP
    depth = GROUP * W
    d_out = w_down.shape[2]
    half = d_out // 2

    barrier = pltpu.get_barrier_semaphore()
    for x_, y_ in ((mate, yj), (across, yj), (xi, other_y)):
        pl.semaphore_signal(barrier, inc=1, **dev(x=x_, yz=y_))

    def keep_copy(g):
        return pltpu.make_async_copy(
            keep.at[pl.ds(GROUP * g, GROUP)], keep_v.at[pl.ds(GROUP * g, GROUP)], keep_sem.at[g])

    def recv_copy(g):
        src = recv_e.at[pl.ds(GROUP * g, GROUP)] if g < n_early else recv_l.at[pl.ds(GROUP * (g - n_early), GROUP)]
        return pltpu.make_async_copy(src, recv_v.at[pl.ds(GROUP * g, GROUP)], recv_sem.at[g])

    keep_copy(0).start()
    recv_copy(0).start()

    def rows_of(p, owner):
        off, size = PARTS[p]
        return pl.ds(pl.multiple_of(4 * off + owner * size, 16), size)

    def block(p, g, owner):
        return acts.at[pl.ds(GROUP * g, GROUP), rows_of(p, owner)]

    def o_rows(s):
        row = (1 - yj) * (32 * xi + 16 * s) + yj * (128 + 64 * s + 16 * xi)
        return acts.at[pl.ds(n_ff, n_o), pl.ds(pl.multiple_of(row, 16), 16)]

    def o_own(s):
        return pltpu.make_async_copy(o_in.at[yj, :, pl.ds(16 * s, 16)], o_rows(s), oo_sems.at[s])

    def o_copy(s):
        return pltpu.make_async_remote_copy(
            src_ref=o_in.at[other_y, :, pl.ds(16 * s, 16)], dst_ref=o_rows(s), send_sem=on_send.at[s],
            recv_sem=on_recv.at[s], **dev(x=xi, yz=other_y))

    h_load = pltpu.make_async_copy(hidden, h_v, h_sem)

    def load_weights(g):
        slot = lax.rem(g, NBUF3)

        @pl.when(g < n_m)
        def _():
            pltpu.make_async_copy(
                w_down.at[0, pl.ds(pl.multiple_of(g * depth, W), depth)], wbuf.at[slot], w_sem.at[slot]).start()

        @pl.when(g >= n_m)
        def _():
            pltpu.make_async_copy(
                w_o.at[0, pl.ds(pl.multiple_of((g - n_m) * depth, W), depth)], wbuf.at[slot], w_sem.at[slot]).start()

    def far_copy(p, g):
        return pltpu.make_async_remote_copy(
            src_ref=block(p, g, xi), dst_ref=block(p, g, xi), send_sem=far_send.at[p, g], recv_sem=far_recv.at[p, g],
            **dev(x=across, yz=yj))

    def near_copy(p, g, which):
        rows = block(p, g, xi if which == 0 else across)
        return pltpu.make_async_remote_copy(
            src_ref=rows, dst_ref=rows, send_sem=near_send.at[p, g, which], recv_sem=near_recv.at[p, g, which],
            **dev(x=mate, yz=yj))

    def give(p, g):
        far_copy(p, g).start()
        near_copy(p, g, 0).start()

    def give_m(p, g):
        off, size = PARTS[p]
        for k in range(GROUP):
            t = GROUP * g + k
            z = keep_v[t, off:off + size].astype(F32) + recv_v[t, off:off + size].astype(F32)
            acts[t, rows_of(p, xi)] = silu_mul(z[:, :W], z[:, W:])
        give(p, g)

    pl.semaphore_wait(barrier, 3)
    for g in range(n_m):
        keep_copy(g).wait()
        recv_copy(g).wait()
        give_m(0, g)
        if g == 0:
            for s in range(2):
                o_copy(s).start()
                o_own(s).start()
            for k in range(1, n_m):
                keep_copy(k).start()
                recv_copy(k).start()
    for s in range(NBUF3):
        load_weights(jnp.int32(s))
    h_load.start()
    acc[...] = jnp.zeros_like(acc)
    for s in range(2):
        o_own(s).wait()
        o_copy(s).wait_recv()

    def chunk(p, k):
        return k if p % 2 == 0 else n_g - 1 - k

    for g in range(n_m, n_g):
        give(0, g)
    for p in range(1, len(PARTS)):
        @pl.loop(0, n_g)
        def _(k):
            g = chunk(p, k)

            @pl.when(g < n_m)
            def _():
                give_m(p, g)

            @pl.when(g >= n_m)
            def _():
                give(p, g)

    def forward(p, k):
        g = chunk(p, k)
        far_copy(p, g).wait_recv()
        near_copy(p, g, 1).start()

    def multiply(p, k):
        g = chunk(p, k)
        slot = lax.rem(g, NBUF3)

        @pl.when(k >= (0 if p == 0 else NBUF3))
        def _():
            pltpu.make_async_copy(w_down.at[0, pl.ds(0, depth)], wbuf.at[slot], w_sem.at[slot]).wait()

        near_copy(p, g, 0).wait_recv()
        near_copy(p, g, 1).wait_recv()
        off, size = PARTS[p]
        rows = slice(4 * off, 4 * (off + size))
        for n in range(d_out // W):
            cols = slice(n * W, (n + 1) * W)
            total = acc[rows, cols]
            for j in range(GROUP):
                total += jnp.dot(
                    acts[GROUP * g + j, rows], wbuf[slot, j * W:(j + 1) * W, cols], preferred_element_type=F32)
            acc[rows, cols] = total

        @pl.when(k + NBUF3 < n_g)
        def _():
            load_weights(chunk(p, k + NBUF3))

    def cols_of(j):
        return pl.ds(pl.multiple_of(j * half, 128), half)

    def y_copy(p):
        rows = slice(4 * PARTS[p][0], 4 * sum(PARTS[p]))
        return pltpu.make_async_remote_copy(
            src_ref=y_src.at[rows], dst_ref=y_dst.at[rows], send_sem=y_sems.at[p, 0], recv_sem=y_sems.at[p, 1],
            **dev(x=xi, yz=other_y))

    def exchange(p):
        rows = slice(4 * PARTS[p][0], 4 * sum(PARTS[p]))
        y_src[rows] = acc[rows, cols_of(other_y)].astype(BF16)
        y_copy(p).start()

    def finalize(p):
        off, size = PARTS[p]
        rows = slice(4 * off, 4 * (off + size))
        y_copy(p).wait_recv()
        total = (acc[rows, cols_of(yj)] + y_dst[rows].astype(F32)).reshape(4, size, half)
        out[:, off:off + size] = (h_v[:, off:off + size].astype(F32) + total).astype(BF16)

    for p in range(len(PARTS)):
        forward(p, jnp.int32(0))
        if p > 0:
            multiply(p - 1, jnp.int32(n_g - 1))
            exchange(p - 1)
        if p == 1:
            h_load.wait()

        @pl.loop(1, n_g)
        def _(k):
            forward(p, k)
            multiply(p, k - 1)

        if p > 0:
            finalize(p - 1)

    last = len(PARTS) - 1
    multiply(last, jnp.int32(n_g - 1))
    exchange(last)
    for s in range(2):
        o_copy(s).wait_send()
    for p in range(len(PARTS)):
        @pl.loop(0, n_g)
        def _(g):
            far_copy(p, g).wait_send()
            near_copy(p, g, 0).wait_send()
            near_copy(p, g, 1).wait_send()

    finalize(last)
    for p in range(len(PARTS)):
        y_copy(p).wait_send()


def finish(o, keep, recv_e, recv_l, hidden, w_o, w_down):
    rows, half = hidden.shape
    n_ff = w_down.shape[1] // W
    n_o = w_o.shape[1] // W
    n_m = n_ff // GROUP
    n_g = n_m + n_o // GROUP
    n_p = len(PARTS)
    d_out = w_down.shape[2]
    dma = pltpu.SemaphoreType.DMA
    any_spec = pl.BlockSpec(memory_space=pl.ANY)
    vmem = pl.BlockSpec(memory_space=pltpu.VMEM)
    flops = 2 * rows * d_out * (w_down.shape[1] + w_o.shape[1])
    out = pl.pallas_call(
        functools.partial(output_kernel, n_ff, n_o),
        name="finish",
        out_shape=jax.ShapeDtypeStruct((4, 64, half), BF16),
        in_specs=[any_spec] * 7,
        out_specs=vmem,
        scratch_shapes=[
            pltpu.VMEM((n_ff + n_o, rows, W), BF16),
            pltpu.VMEM((NBUF3, GROUP * W, d_out), BF16),
            pltpu.VMEM((rows, d_out), F32),
            pltpu.VMEM(keep.shape, BF16),
            pltpu.VMEM(keep.shape, BF16),
            pltpu.VMEM((4, 64, half), BF16),
            pltpu.VMEM((rows, half), BF16),
            pltpu.VMEM((rows, half), BF16),
            dma((NBUF3,)),
            dma((n_m,)),
            dma((n_m,)),
            dma,
            dma((2,)),
            dma((2,)),
            dma((2,)),
            dma((n_p, n_g)),
            dma((n_p, n_g)),
            dma((n_p, n_g, 2)),
            dma((n_p, n_g, 2)),
            dma((n_p, 2)),
        ],
        compiler_params=pltpu.CompilerParams(collective_id=1, has_side_effects=True, vmem_limit_bytes=56_000_000),
        cost_estimate=pl.CostEstimate(flops=flops, bytes_accessed=2 * d_out * (w_down.shape[1] + w_o.shape[1]), transcendentals=0),
    )(o, keep, recv_e, recv_l, hidden.reshape(4, 64, half), w_o, w_down)
    return out.reshape(rows, half)


def solution(mesh):
    x_size = mesh.shape["x"]
    y_size = mesh.shape["yz"]
    row_spec = P("dp", ("x", "yz"))
    tile_in = P(None, "x", "yz")
    tile_out = P(None, "yz", "x")
    cache_spec = P(None, ("dp", "x", "yz"))
    len_spec = P(("dp", "x", "yz"))

    def device_step(hidden, norm_gain, w_q, w_kv, w_gate, w_up, w_o, w_down, k_cache, v_cache, seq_len):
        d_model = hidden.shape[1] * x_size * y_size
        seqs = k_cache.shape[1]
        dim = k_cache.shape[3]
        q_cols = w_q.shape[2]
        heads = q_cols // dim
        qkv, keep, recv_e, send = project(hidden, norm_gain, w_q, w_kv, w_gate, w_up, d_model)
        recv_l = lax.ppermute(send, "x", [(i, (i + x_size // 2) % x_size) for i in range(x_size)])
        q = qkv[:, :, :q_cols].reshape(y_size, seqs, heads, dim).transpose(1, 0, 2, 3).reshape(seqs, y_size * heads, dim)
        kv = qkv[:, :, q_cols:].transpose(1, 0, 2)
        k_new, v_new, o = attend(seq_len, q, kv, k_cache, v_cache)
        o = o.reshape(seqs, y_size, q_cols // W, W).transpose(1, 2, 0, 3)
        hidden_out = finish(o, keep, recv_e, recv_l, hidden, w_o, w_down)
        return hidden_out, k_new, v_new

    return jax.shard_map(
        device_step,
        mesh=mesh,
        in_specs=(row_spec, P(None, "x"), tile_in, tile_in, tile_in, tile_in, tile_out, tile_out, cache_spec, cache_spec, len_spec),
        out_specs=(row_spec, cache_spec, cache_spec),
        check_vma=False,
    )
```

```python
import functools

import jax
import jax.numpy as jnp
from jax import lax
from jax.experimental import pallas as pl
from jax.experimental.pallas import tpu as pltpu
from jax.sharding import PartitionSpec as P

NORM_EPS = 1e-6
W = 512
NBUF1 = 4
NBUF3 = 6
GROUP = 3
PARTS = ((0, 32), (32, 16), (48, 16))
EARLY = 12
SEQ_STEP = 2
VMEM_LIMIT = 64_000_000
F32 = jnp.float32
BF16 = jnp.bfloat16
LOG2E = 1.4426950408889634
MASKED = -1e30 * LOG2E


def dev(**axes):
    return dict(device_id=axes, device_id_type=pl.DeviceIdType.MESH)


def silu_mul(gate, up):
    gate = gate.astype(BF16).astype(F32)
    up = up.astype(BF16).astype(F32)
    return (jax.nn.silu(gate) * up).astype(BF16)


def project_kernel(
    n_q, n_ff, d_model, hidden, gain_in, wq, wkv, wg, wu,
    qkv_out, keep_out, recv_out, send_out,
    gain, h_own, h_other, u, inv_all, sq_all, wq_buf, wbuf, wkv_buf, part, part_kv, near, near_kv, keep, keep_kv, far_src,
    far_src_kv, far, far_kv, z_rows, z_other,
    wq_sem, w_sem, wkv_sem, h_in, gain_sem, h_sems, sq_send, sq_recv, near_send, near_recv, qn_send, qn_recv, kn_send, kn_recv,
    far_send, far_recv, qf_send, qf_recv, kf_send, kf_recv, y_sems, out_sem, qkv_sem,
):
    xi = lax.axis_index("x")
    yj = lax.axis_index("yz")
    core = lax.rem(xi, 2)
    chip = xi // 2
    mate = xi + 1 - 2 * core
    across = lax.rem(xi + 2, 4)
    other_y = 1 - yj
    me = xi * 2 + yj
    half = hidden.shape[-1]
    n_all = n_q + n_ff
    n_far = n_q + EARLY
    to_mate = dev(x=mate, yz=yj)
    to_across = dev(x=across, yz=yj)

    barrier = pltpu.get_barrier_semaphore()
    for k in range(1, 8):
        peer = lax.rem(me + k, 8)
        pl.semaphore_signal(barrier, inc=1, **dev(x=peer // 2, yz=lax.rem(peer, 2)))
    h_load = pltpu.make_async_copy(hidden, h_own, h_in)
    h_load.start()
    gain_load = pltpu.make_async_copy(gain_in, gain, gain_sem)
    gain_load.start()

    def start_weights(g):
        slot = lax.rem(g, NBUF1)
        cols = pl.ds(pl.multiple_of((g - n_q) * W, W), W)
        pltpu.make_async_copy(wg.at[0, :, cols], wbuf.at[slot, 0], w_sem.at[slot, 0]).start()
        pltpu.make_async_copy(wu.at[0, :, cols], wbuf.at[slot, 1], w_sem.at[slot, 1]).start()

    def wait_weights(slot, k):
        pltpu.make_async_copy(wg.at[0, :, pl.ds(0, W)], wbuf.at[slot, k], w_sem.at[slot, k]).wait()

    def wq_copy(g):
        return pltpu.make_async_copy(wq.at[0, :, g * 2 * W:(g + 1) * 2 * W], wq_buf.at[g], wq_sem.at[g])

    h_load.wait()
    gain_load.wait()
    for g in range(n_q):
        wq_copy(g).start()
    kv_copy = pltpu.make_async_copy(wkv.at[0], wkv_buf, wkv_sem)
    kv_copy.start()

    folded = jnp.zeros((256, 128), F32)
    for k in range(half // 128):
        block = h_own[:, :, :, k * 128:(k + 1) * 128].reshape(256, 128).astype(F32)
        folded += block * block
    sq_all[me] = jnp.broadcast_to(jnp.sum(jnp.transpose(folded), axis=0, keepdims=True), (8, 256))
    pl.semaphore_wait(barrier, 7)

    def sq_copy(peer, src):
        return pltpu.make_async_remote_copy(
            src_ref=sq_all.at[src], dst_ref=sq_all.at[src], send_sem=sq_send.at[peer], recv_sem=sq_recv.at[src],
            **dev(x=peer // 2, yz=lax.rem(peer, 2)))

    def side_of(step):
        return 1 - chip if step < 2 else chip

    def piece(step):
        return pl.ds(32 * step, 32) if step < 2 else pl.ds(0, 64)

    def h_copy(step):
        block = (side_of(step), slice(None), piece(step))
        return pltpu.make_async_remote_copy(
            src_ref=h_own.at[block], dst_ref=h_other.at[block],
            send_sem=h_sems.at[step, 0], recv_sem=h_sems.at[step, 1], **dev(x=xi, yz=other_y))

    for k in range(1, 8):
        sq_copy(lax.rem(me + k, 8), me).start()
    for step in range(3):
        h_copy(step).start()
    for k in range(1, 8):
        peer = lax.rem(me + k, 8)
        sq_copy(peer, peer).wait_recv()
    total = jnp.sum(sq_all[...], axis=0)
    inv = lax.rsqrt(total / d_model + NORM_EPS)
    inv_all[...] = jnp.transpose(jnp.concatenate([inv] * 16, axis=0)).reshape(inv_all.shape)

    def normalize(values, step, which):
        cols = pl.ds(pl.multiple_of(which * half, 128), half)
        side, rows = side_of(step), piece(step)
        u[side, :, rows, cols] = (
            values[side, :, rows].astype(F32) * inv_all[side, :, rows, :1] * gain[:, cols].astype(F32)).astype(BF16)

    def near_copy(g):
        return pltpu.make_async_remote_copy(
            src_ref=part.at[g, :, 1 - core], dst_ref=near.at[g], send_sem=near_send.at[g],
            recv_sem=near_recv.at[g], **to_mate)

    def near_copy_q(g, step):
        side, rows = side_of(step), piece(step)
        return pltpu.make_async_remote_copy(
            src_ref=part.at[g, side, 1 - core, rows], dst_ref=near.at[g, side, rows],
            send_sem=qn_send.at[g, step], recv_sem=qn_recv.at[g, step], **to_mate)

    def near_copy_kv(step):
        side, rows = side_of(step), piece(step)
        return pltpu.make_async_remote_copy(
            src_ref=part_kv.at[side, 1 - core, rows], dst_ref=near_kv.at[side, rows],
            send_sem=kn_send.at[step], recv_sem=kn_recv.at[step], **to_mate)

    def far_copy(g):
        return pltpu.make_async_remote_copy(
            src_ref=far_src.at[g], dst_ref=recv_out.at[g - n_q], send_sem=far_send.at[g - n_q],
            recv_sem=far_recv.at[g - n_q], **to_across)

    def far_copy_q(g, step):
        rows = piece(step)
        return pltpu.make_async_remote_copy(
            src_ref=far_src.at[g, rows], dst_ref=far.at[g, rows], send_sem=qf_send.at[g, step],
            recv_sem=qf_recv.at[g, step], **to_across)

    def far_copy_kv(step):
        rows = piece(step)
        return pltpu.make_async_remote_copy(
            src_ref=far_src_kv.at[rows], dst_ref=far_kv.at[rows], send_sem=kf_send.at[step], recv_sem=kf_recv.at[step],
            **to_across)

    def keep_copy(g):
        return pltpu.make_async_copy(keep.at[g], keep_out.at[g - n_q], out_sem.at[g - n_q, 0])

    def send_copy(g):
        k = g - n_q
        return pltpu.make_async_copy(far_src.at[g], send_out.at[k - EARLY], out_sem.at[k, 1])

    def add(a, b):
        return (a.astype(F32) + b.astype(F32)).astype(BF16)

    def multiply(g):
        slot = lax.rem(g, NBUF1)
        for k in range(2):
            wait_weights(slot, k)
            res = jnp.dot(u[...].reshape(256, u.shape[-1]), wbuf[slot, k], preferred_element_type=F32).astype(BF16)
            part[g, :, :, :, k * W:(k + 1) * W] = res.reshape(2, 2, 64, W)
        near_copy(g).start()

        @pl.when(g + NBUF1 < n_all)
        def _():
            start_weights(g + NBUF1)

    def reduce_near(g):
        near_copy(g).wait_recv()
        far_src[g] = add(part[g, 1 - chip, core], near[g, 1 - chip])

        @pl.when(g < n_far)
        def _():
            far_copy(g).start()

        @pl.when(g >= n_far)
        def _():
            send_copy(g).start()

        keep[g] = add(part[g, chip, core], near[g, chip])
        keep_copy(g).start()

    def multiply_q(step):
        side, rows = side_of(step), piece(step)
        lhs = u[side, :, rows].reshape(2 * rows.size, u.shape[-1])
        for g in range(n_q):
            if step == 0:
                wq_copy(g).wait()
            for k in range(2):
                res = jnp.dot(lhs, wq_buf[g, :, k * W:(k + 1) * W], preferred_element_type=F32).astype(BF16)
                part[g, side, :, rows, k * W:(k + 1) * W] = res.reshape(2, rows.size, W)
            near_copy_q(g, step).start()
            if step == 0 and g >= 1:
                reduce_q(0, g - 1)
        if step == 0:
            kv_copy.wait()
        res = jnp.dot(lhs, wkv_buf[...], preferred_element_type=F32).astype(BF16)
        part_kv[side, :, rows] = res.reshape(2, rows.size, res.shape[1])
        near_copy_kv(step).start()

    def reduce_q(step, g):
        side, rows = side_of(step), piece(step)
        near_copy_q(g, step).wait_recv()
        total_q = add(part[g, side, core, rows], near[g, side, rows])
        if step < 2:
            far_src[g, rows] = total_q
            far_copy_q(g, step).start()
        else:
            keep[g] = total_q

    def reduce_kv(step):
        side, rows = side_of(step), piece(step)
        near_copy_kv(step).wait_recv()
        total_kv = add(part_kv[side, core, rows], near_kv[side, rows])
        if step < 2:
            far_src_kv[rows] = total_kv
            far_copy_kv(step).start()
        else:
            keep_kv[...] = total_kv

    for step in range(3):
        normalize(h_own, step, yj)
        h_copy(step).wait_recv()
        normalize(h_other, step, other_y)
        if step < 2:
            multiply_q(step)
            for g in range(n_q - 1 if step == 0 else 0, n_q):
                reduce_q(step, g)
            reduce_kv(step)
        if step == 0:
            for g in range(n_q, n_q + NBUF1):
                start_weights(jnp.int32(g))

    @pl.loop(n_q, n_far)
    def _(g):
        multiply(g)

        @pl.when(g >= n_q + 2)
        def _():
            reduce_near(g - 2)

    q_cols = n_q * 2 * W
    multiply_q(2)
    for g in range(n_q):
        reduce_q(2, g)
        for step in range(2):
            far_copy_q(g, step).wait_recv()
        z_rows[:, :, g * 2 * W:(g + 1) * 2 * W] = add(keep[g], far[g]).reshape(2, 32, 2 * W)
    reduce_kv(2)
    for step in range(2):
        far_copy_kv(step).wait_recv()
    z_kv = add(keep_kv[...], far_kv[...])
    z_rows[:, :, q_cols:] = z_kv.reshape(2, 32, z_kv.shape[1])
    y_copy = pltpu.make_async_remote_copy(
        src_ref=z_rows.at[other_y], dst_ref=z_other, send_sem=y_sems.at[0], recv_sem=y_sems.at[1],
        **dev(x=xi, yz=other_y))
    y_copy.start()
    qkv_own = pltpu.make_async_copy(z_rows.at[yj], qkv_out.at[yj], qkv_sem.at[0])
    qkv_own.start()

    @pl.loop(n_far, n_all)
    def _(g):
        multiply(g)
        reduce_near(g - 2)

    reduce_near(jnp.int32(n_all - 2))
    reduce_near(jnp.int32(n_all - 1))
    y_copy.wait_recv()
    qkv_other = pltpu.make_async_copy(z_other, qkv_out.at[other_y], qkv_sem.at[1])
    qkv_other.start()

    for step in range(3):
        h_copy(step).wait_send()
        near_copy_kv(step).wait_send()
        for g in range(n_q):
            near_copy_q(g, step).wait_send()
    for step in range(2):
        far_copy_kv(step).wait_send()
        for g in range(n_q):
            far_copy_q(g, step).wait_send()
    for k in range(1, 8):
        sq_copy(lax.rem(me + k, 8), me).wait_send()
    y_copy.wait_send()

    @pl.loop(n_q, n_all)
    def _(g):
        near_copy(g).wait_send()
        keep_copy(g).wait()

    @pl.loop(n_far, n_all)
    def _(g):
        send_copy(g).wait()

    qkv_own.wait()
    qkv_other.wait()

    @pl.loop(n_q, n_far)
    def _(g):
        far_copy(g).wait_send()
        far_copy(g).wait_recv()


def project(hidden, gain, w_q, w_kv, w_gate, w_up, d_model):
    rows, half = hidden.shape
    feats = w_q.shape[1]
    kv = w_kv.shape[2]
    n_q = w_q.shape[2] // (2 * W)
    n_ff = w_gate.shape[2] // W
    n_all = n_q + n_ff
    late = n_ff - EARLY
    dma = pltpu.SemaphoreType.DMA
    any_spec = pl.BlockSpec(memory_space=pl.ANY)
    cols = w_q.shape[2] + kv
    flops = 2 * rows * feats * (w_q.shape[2] + kv + 2 * w_gate.shape[2])
    return pl.pallas_call(
        functools.partial(project_kernel, n_q, n_ff, d_model),
        name="project",
        out_shape=(
            jax.ShapeDtypeStruct((2, 32, cols), BF16),
            jax.ShapeDtypeStruct((n_ff, 64, 2 * W), BF16),
            jax.ShapeDtypeStruct((EARLY, 64, 2 * W), BF16),
            jax.ShapeDtypeStruct((late, 64, 2 * W), BF16),
        ),
        in_specs=[any_spec] * 6,
        out_specs=(any_spec, any_spec, any_spec, any_spec),
        scratch_shapes=[
            pltpu.VMEM((1, feats), BF16),
            pltpu.VMEM((2, 2, 64, half), BF16),
            pltpu.VMEM((2, 2, 64, half), BF16),
            pltpu.VMEM((2, 2, 64, feats), BF16),
            pltpu.VMEM((2, 2, 64, 128), F32),
            pltpu.VMEM((8, 8, rows), F32),
            pltpu.VMEM((n_q, feats, 2 * W), BF16),
            pltpu.VMEM((NBUF1, 2, feats, W), BF16),
            pltpu.VMEM((feats, kv), BF16),
            pltpu.VMEM((n_all, 2, 2, 64, 2 * W), BF16),
            pltpu.VMEM((2, 2, 64, kv), BF16),
            pltpu.VMEM((n_all, 2, 64, 2 * W), BF16),
            pltpu.VMEM((2, 64, kv), BF16),
            pltpu.VMEM((n_all, 64, 2 * W), BF16),
            pltpu.VMEM((64, kv), BF16),
            pltpu.VMEM((n_all, 64, 2 * W), BF16),
            pltpu.VMEM((64, kv), BF16),
            pltpu.VMEM((n_q, 64, 2 * W), BF16),
            pltpu.VMEM((64, kv), BF16),
            pltpu.VMEM((2, 32, cols), BF16),
            pltpu.VMEM((32, cols), BF16),
            dma((n_q,)),
            dma((NBUF1, 2)),
            dma,
            dma,
            dma,
            dma((3, 2)),
            dma((8,)),
            dma((8,)),
            dma((n_all,)),
            dma((n_all,)),
            dma((n_q, 3)),
            dma((n_q, 3)),
            dma((3,)),
            dma((3,)),
            dma((EARLY,)),
            dma((EARLY,)),
            dma((n_q, 2)),
            dma((n_q, 2)),
            dma((2,)),
            dma((2,)),
            dma((2,)),
            dma((n_ff, 2)),
            dma((2,)),
        ],
        compiler_params=pltpu.CompilerParams(collective_id=0, has_side_effects=True, vmem_limit_bytes=VMEM_LIMIT),
        cost_estimate=pl.CostEstimate(flops=flops, bytes_accessed=feats * (flops // (rows * feats)), transcendentals=0),
    )(hidden.reshape(2, 2, 64, half), gain, w_q, w_kv, w_gate, w_up)


def attend_kernel(lens, q_ref, kv_ref, k_ref, v_ref, k_out, v_out, o_ref):
    step = pl.program_id(0)
    n_pos = k_ref.shape[2]
    scale = q_ref.shape[2] ** -0.5 * LOG2E
    for s in range(SEQ_STEP):
        length = lens[step * SEQ_STEP + s]
        base = pl.multiple_of((length // 16) * 16, 16)
        k_out[0, s] = k_ref[0, s]
        v_out[0, s] = v_ref[0, s]
        hit = lax.broadcasted_iota(jnp.int32, (16, k_ref.shape[3]), 0) == length - base
        for src, dst, which in ((k_ref, k_out, 0), (v_ref, v_out, 1)):
            old = src[0, s, pl.ds(base, 16), :].astype(F32)
            new = kv_ref[s, which:which + 1, :].astype(F32)
            dst[0, s, pl.ds(base, 16), :] = jnp.where(hit, new, old).astype(BF16)
        scores = lax.dot_general(q_ref[s], k_out[0, s], (((1,), (1,)), ((), ())), preferred_element_type=F32) * scale
        visible = lax.broadcasted_iota(jnp.int32, scores.shape, 1) <= length
        scores = jnp.where(visible, scores, MASKED)
        weights = jnp.exp2(scores - jnp.max(scores, axis=1, keepdims=True))
        probs = (weights * (1.0 / jnp.sum(weights, axis=1, keepdims=True))).astype(BF16)
        o_ref[s] = jnp.dot(probs, v_out[0, s], preferred_element_type=F32).astype(BF16)


def attend(lens, q, kv, k_cache, v_cache):
    seqs, heads, dim = q.shape
    n_pos = k_cache.shape[2]
    cache_spec = pl.BlockSpec((1, SEQ_STEP, n_pos, dim), lambda b, lens: (0, b, 0, 0))
    q_spec = pl.BlockSpec((SEQ_STEP, heads, dim), lambda b, lens: (b, 0, 0))
    return pl.pallas_call(
        attend_kernel,
        name="attend",
        out_shape=(
            jax.ShapeDtypeStruct(k_cache.shape, BF16),
            jax.ShapeDtypeStruct(v_cache.shape, BF16),
            jax.ShapeDtypeStruct(q.shape, BF16),
        ),
        grid_spec=pltpu.PrefetchScalarGridSpec(
            num_scalar_prefetch=1,
            grid=(seqs // SEQ_STEP,),
            in_specs=[q_spec, pl.BlockSpec((SEQ_STEP, 2, dim), lambda b, lens: (b, 0, 0)), cache_spec, cache_spec],
            out_specs=(cache_spec, cache_spec, q_spec),
        ),
        compiler_params=pltpu.CompilerParams(dimension_semantics=("arbitrary",), vmem_limit_bytes=66_000_000),
        cost_estimate=pl.CostEstimate(
            flops=10**10, bytes_accessed=8 * k_cache.size, transcendentals=seqs * heads * n_pos),
    )(lens, q, kv, k_cache, v_cache)


def output_kernel(
    n_ff, n_o, o_in, keep, recv_e, recv_l, hidden, w_o, w_down, out,
    acts, wbuf, acc, keep_v, recv_v, h_v, y_src, y_dst,
    w_sem, keep_sem, recv_sem, h_sem, oo_sems, on_send, on_recv, far_send, far_recv, near_send, near_recv, y_sems,
):
    xi = lax.axis_index("x")
    yj = lax.axis_index("yz")
    core = lax.rem(xi, 2)
    mate = xi + 1 - 2 * core
    across = lax.rem(xi + 2, 4)
    other_y = 1 - yj
    n_m = n_ff // GROUP
    n_g = n_m + n_o // GROUP
    n_early = EARLY // GROUP
    depth = GROUP * W
    d_out = w_down.shape[2]
    half = d_out // 2

    barrier = pltpu.get_barrier_semaphore()
    for x_, y_ in ((mate, yj), (across, yj), (xi, other_y)):
        pl.semaphore_signal(barrier, inc=1, **dev(x=x_, yz=y_))

    def keep_copy(g):
        return pltpu.make_async_copy(
            keep.at[pl.ds(GROUP * g, GROUP)], keep_v.at[pl.ds(GROUP * g, GROUP)], keep_sem.at[g])

    def recv_copy(g):
        src = recv_e.at[pl.ds(GROUP * g, GROUP)] if g < n_early else recv_l.at[pl.ds(GROUP * (g - n_early), GROUP)]
        return pltpu.make_async_copy(src, recv_v.at[pl.ds(GROUP * g, GROUP)], recv_sem.at[g])

    keep_copy(0).start()
    recv_copy(0).start()

    def rows_of(p, owner):
        off, size = PARTS[p]
        return pl.ds(pl.multiple_of(4 * off + owner * size, 16), size)

    def block(p, g, owner):
        return acts.at[pl.ds(GROUP * g, GROUP), rows_of(p, owner)]

    def o_rows(s):
        row = (1 - yj) * (32 * xi + 16 * s) + yj * (128 + 64 * s + 16 * xi)
        return acts.at[pl.ds(n_ff, n_o), pl.ds(pl.multiple_of(row, 16), 16)]

    def o_own(s):
        return pltpu.make_async_copy(o_in.at[yj, :, pl.ds(16 * s, 16)], o_rows(s), oo_sems.at[s])

    def o_copy(s):
        return pltpu.make_async_remote_copy(
            src_ref=o_in.at[other_y, :, pl.ds(16 * s, 16)], dst_ref=o_rows(s), send_sem=on_send.at[s],
            recv_sem=on_recv.at[s], **dev(x=xi, yz=other_y))

    h_load = pltpu.make_async_copy(hidden, h_v, h_sem)

    def load_weights(g):
        slot = lax.rem(g, NBUF3)

        @pl.when(g < n_m)
        def _():
            pltpu.make_async_copy(
                w_down.at[0, pl.ds(pl.multiple_of(g * depth, W), depth)], wbuf.at[slot], w_sem.at[slot]).start()

        @pl.when(g >= n_m)
        def _():
            pltpu.make_async_copy(
                w_o.at[0, pl.ds(pl.multiple_of((g - n_m) * depth, W), depth)], wbuf.at[slot], w_sem.at[slot]).start()

    def far_copy(p, g):
        return pltpu.make_async_remote_copy(
            src_ref=block(p, g, xi), dst_ref=block(p, g, xi), send_sem=far_send.at[p, g], recv_sem=far_recv.at[p, g],
            **dev(x=across, yz=yj))

    def near_copy(p, g, which):
        rows = block(p, g, xi if which == 0 else across)
        return pltpu.make_async_remote_copy(
            src_ref=rows, dst_ref=rows, send_sem=near_send.at[p, g, which], recv_sem=near_recv.at[p, g, which],
            **dev(x=mate, yz=yj))

    def give(p, g):
        far_copy(p, g).start()
        near_copy(p, g, 0).start()

    def give_m(p, g):
        off, size = PARTS[p]
        for k in range(GROUP):
            t = GROUP * g + k
            z = keep_v[t, off:off + size].astype(F32) + recv_v[t, off:off + size].astype(F32)
            acts[t, rows_of(p, xi)] = silu_mul(z[:, :W], z[:, W:])
        give(p, g)

    pl.semaphore_wait(barrier, 3)
    for g in range(n_m):
        keep_copy(g).wait()
        recv_copy(g).wait()
        give_m(0, g)
        if g == 0:
            for s in range(2):
                o_copy(s).start()
                o_own(s).start()
            for k in range(1, n_m):
                keep_copy(k).start()
                recv_copy(k).start()
    for s in range(NBUF3):
        load_weights(jnp.int32(s))
    h_load.start()
    acc[...] = jnp.zeros_like(acc)
    for s in range(2):
        o_own(s).wait()
        o_copy(s).wait_recv()

    def chunk(p, k):
        return k if p % 2 == 0 else n_g - 1 - k

    for g in range(n_m, n_g):
        give(0, g)
    for p in range(1, len(PARTS)):
        @pl.loop(0, n_g)
        def _(k):
            g = chunk(p, k)

            @pl.when(g < n_m)
            def _():
                give_m(p, g)

            @pl.when(g >= n_m)
            def _():
                give(p, g)

    def forward(p, k):
        g = chunk(p, k)
        far_copy(p, g).wait_recv()
        near_copy(p, g, 1).start()

    def multiply(p, k):
        g = chunk(p, k)
        slot = lax.rem(g, NBUF3)

        @pl.when(k >= (0 if p == 0 else NBUF3))
        def _():
            pltpu.make_async_copy(w_down.at[0, pl.ds(0, depth)], wbuf.at[slot], w_sem.at[slot]).wait()

        near_copy(p, g, 0).wait_recv()
        near_copy(p, g, 1).wait_recv()
        off, size = PARTS[p]
        rows = slice(4 * off, 4 * (off + size))
        for n in range(d_out // W):
            cols = slice(n * W, (n + 1) * W)
            total = acc[rows, cols]
            for j in range(GROUP):
                total += jnp.dot(
                    acts[GROUP * g + j, rows], wbuf[slot, j * W:(j + 1) * W, cols], preferred_element_type=F32)
            acc[rows, cols] = total

        @pl.when(k + NBUF3 < n_g)
        def _():
            load_weights(chunk(p, k + NBUF3))

    def cols_of(j):
        return pl.ds(pl.multiple_of(j * half, 128), half)

    def y_copy(p):
        rows = slice(4 * PARTS[p][0], 4 * sum(PARTS[p]))
        return pltpu.make_async_remote_copy(
            src_ref=y_src.at[rows], dst_ref=y_dst.at[rows], send_sem=y_sems.at[p, 0], recv_sem=y_sems.at[p, 1],
            **dev(x=xi, yz=other_y))

    def exchange(p):
        rows = slice(4 * PARTS[p][0], 4 * sum(PARTS[p]))
        y_src[rows] = acc[rows, cols_of(other_y)].astype(BF16)
        y_copy(p).start()

    def finalize(p):
        off, size = PARTS[p]
        rows = slice(4 * off, 4 * (off + size))
        y_copy(p).wait_recv()
        total = (acc[rows, cols_of(yj)] + y_dst[rows].astype(F32)).reshape(4, size, half)
        out[:, off:off + size] = (h_v[:, off:off + size].astype(F32) + total).astype(BF16)

    for p in range(len(PARTS)):
        forward(p, jnp.int32(0))
        if p > 0:
            multiply(p - 1, jnp.int32(n_g - 1))
            exchange(p - 1)
        if p == 1:
            h_load.wait()

        @pl.loop(1, n_g)
        def _(k):
            forward(p, k)
            multiply(p, k - 1)

        if p > 0:
            finalize(p - 1)

    last = len(PARTS) - 1
    g = chunk(last, n_g - 1)
    if n_g > NBUF3:
        pltpu.make_async_copy(w_down.at[0, pl.ds(0, depth)], wbuf.at[g % NBUF3], w_sem.at[g % NBUF3]).wait()
    near_copy(last, g, 0).wait_recv()
    near_copy(last, g, 1).wait_recv()
    rows = slice(4 * PARTS[last][0], 4 * sum(PARTS[last]))
    for j in (other_y, yj):
        for n in range(half // 256):
            cols = pl.ds(pl.multiple_of(j * half + n * 256, 256), 256)
            total = acc[rows, cols]
            for k in range(GROUP):
                total += jnp.dot(
                    acts[GROUP * g + k, rows], wbuf[g % NBUF3, k * W:(k + 1) * W, cols], preferred_element_type=F32)
            acc[rows, cols] = total
        if j is other_y:
            exchange(last)
    for s in range(2):
        o_copy(s).wait_send()
    for p in range(len(PARTS)):
        @pl.loop(0, n_g)
        def _(g):
            far_copy(p, g).wait_send()
            near_copy(p, g, 0).wait_send()
            near_copy(p, g, 1).wait_send()

    finalize(last)
    for p in range(len(PARTS)):
        y_copy(p).wait_send()


def finish(o, keep, recv_e, recv_l, hidden, w_o, w_down):
    rows, half = hidden.shape
    n_ff = w_down.shape[1] // W
    n_o = w_o.shape[1] // W
    n_m = n_ff // GROUP
    n_g = n_m + n_o // GROUP
    n_p = len(PARTS)
    d_out = w_down.shape[2]
    dma = pltpu.SemaphoreType.DMA
    any_spec = pl.BlockSpec(memory_space=pl.ANY)
    vmem = pl.BlockSpec(memory_space=pltpu.VMEM)
    flops = 2 * rows * d_out * (w_down.shape[1] + w_o.shape[1])
    out = pl.pallas_call(
        functools.partial(output_kernel, n_ff, n_o),
        name="finish",
        out_shape=jax.ShapeDtypeStruct((4, 64, half), BF16),
        in_specs=[any_spec] * 7,
        out_specs=vmem,
        scratch_shapes=[
            pltpu.VMEM((n_ff + n_o, rows, W), BF16),
            pltpu.VMEM((NBUF3, GROUP * W, d_out), BF16),
            pltpu.VMEM((rows, d_out), F32),
            pltpu.VMEM(keep.shape, BF16),
            pltpu.VMEM(keep.shape, BF16),
            pltpu.VMEM((4, 64, half), BF16),
            pltpu.VMEM((rows, half), BF16),
            pltpu.VMEM((rows, half), BF16),
            dma((NBUF3,)),
            dma((n_m,)),
            dma((n_m,)),
            dma,
            dma((2,)),
            dma((2,)),
            dma((2,)),
            dma((n_p, n_g)),
            dma((n_p, n_g)),
            dma((n_p, n_g, 2)),
            dma((n_p, n_g, 2)),
            dma((n_p, 2)),
        ],
        compiler_params=pltpu.CompilerParams(collective_id=1, has_side_effects=True, vmem_limit_bytes=56_000_000),
        cost_estimate=pl.CostEstimate(flops=flops, bytes_accessed=2 * d_out * (w_down.shape[1] + w_o.shape[1]), transcendentals=0),
    )(o, keep, recv_e, recv_l, hidden.reshape(4, 64, half), w_o, w_down)
    return out.reshape(rows, half)


def solution(mesh):
    x_size = mesh.shape["x"]
    y_size = mesh.shape["yz"]
    row_spec = P("dp", ("x", "yz"))
    tile_in = P(None, "x", "yz")
    tile_out = P(None, "yz", "x")
    cache_spec = P(None, ("dp", "x", "yz"))
    len_spec = P(("dp", "x", "yz"))

    def device_step(hidden, norm_gain, w_q, w_kv, w_gate, w_up, w_o, w_down, k_cache, v_cache, seq_len):
        d_model = hidden.shape[1] * x_size * y_size
        seqs = k_cache.shape[1]
        dim = k_cache.shape[3]
        q_cols = w_q.shape[2]
        heads = q_cols // dim
        qkv, keep, recv_e, send = project(hidden, norm_gain, w_q, w_kv, w_gate, w_up, d_model)
        recv_l = lax.ppermute(send, "x", [(i, (i + x_size // 2) % x_size) for i in range(x_size)])
        q = qkv[:, :, :q_cols].reshape(y_size, seqs, heads, dim).transpose(1, 0, 2, 3).reshape(seqs, y_size * heads, dim)
        kv = qkv[:, :, q_cols:].transpose(1, 0, 2)
        k_new, v_new, o = attend(seq_len, q, kv, k_cache, v_cache)
        o = o.reshape(seqs, y_size, q_cols // W, W).transpose(1, 2, 0, 3)
        hidden_out = finish(o, keep, recv_e, recv_l, hidden, w_o, w_down)
        return hidden_out, k_new, v_new

    return jax.shard_map(
        device_step,
        mesh=mesh,
        in_specs=(row_spec, P(None, "x"), tile_in, tile_in, tile_in, tile_in, tile_out, tile_out, cache_spec, cache_spec, len_spec),
        out_specs=(row_spec, cache_spec, cache_spec),
        check_vma=False,
    )
```

```python
import functools

import jax
import jax.numpy as jnp
from jax import lax
from jax.experimental import pallas as pl
from jax.experimental.pallas import tpu as pltpu
from jax.sharding import PartitionSpec as P

NORM_EPS = 1e-6
W = 512
NBUF1 = 4
NBUF3 = 6
GROUP = 3
PARTS = ((0, 32), (32, 16), (48, 16))
EARLY = 12
SEQ_STEP = 4
HELD = 6
RELEASE = 3
VMEM_LIMIT = 64_000_000
F32 = jnp.float32
BF16 = jnp.bfloat16
LOG2E = 1.4426950408889634
MASKED = -1e30 * LOG2E


def dev(**axes):
    return dict(device_id=axes, device_id_type=pl.DeviceIdType.MESH)


def silu_mul(gate, up):
    gate = gate.astype(BF16).astype(F32)
    up = up.astype(BF16).astype(F32)
    return (jax.nn.silu(gate) * up).astype(BF16)


def project_kernel(
    n_q, n_ff, d_model, hidden, gain_in, wq, wkv, wg, wu,
    qkv_out, keep_out, recv_out, send_out,
    gain, h_own, h_other, u, inv_all, sq_all, wq_buf, wbuf, wkv_buf, part, part_kv, near, near_kv, keep, keep_kv, far_src,
    far_src_kv, far, far_kv, z_rows, z_other,
    wq_sem, w_sem, wkv_sem, h_in, gain_sem, h_sems, sq_send, sq_recv, near_send, near_recv, qn_send, qn_recv, kn_send, kn_recv,
    far_send, far_recv, qf_send, qf_recv, kf_send, kf_recv, y_sems, out_sem, qkv_sem,
):
    xi = lax.axis_index("x")
    yj = lax.axis_index("yz")
    core = lax.rem(xi, 2)
    chip = xi // 2
    mate = xi + 1 - 2 * core
    across = lax.rem(xi + 2, 4)
    other_y = 1 - yj
    me = xi * 2 + yj
    half = hidden.shape[-1]
    n_all = n_q + n_ff
    n_far = n_q + EARLY
    to_mate = dev(x=mate, yz=yj)
    to_across = dev(x=across, yz=yj)

    barrier = pltpu.get_barrier_semaphore()
    for k in range(1, 8):
        peer = lax.rem(me + k, 8)
        pl.semaphore_signal(barrier, inc=1, **dev(x=peer // 2, yz=lax.rem(peer, 2)))
    h_load = pltpu.make_async_copy(hidden, h_own, h_in)
    h_load.start()
    gain_load = pltpu.make_async_copy(gain_in, gain, gain_sem)
    gain_load.start()

    def start_weights(g):
        slot = lax.rem(g, NBUF1)
        cols = pl.ds(pl.multiple_of((g - n_q) * W, W), W)
        pltpu.make_async_copy(wg.at[0, :, cols], wbuf.at[slot, 0], w_sem.at[slot, 0]).start()
        pltpu.make_async_copy(wu.at[0, :, cols], wbuf.at[slot, 1], w_sem.at[slot, 1]).start()

    def wait_weights(slot, k):
        pltpu.make_async_copy(wg.at[0, :, pl.ds(0, W)], wbuf.at[slot, k], w_sem.at[slot, k]).wait()

    def wq_copy(g):
        return pltpu.make_async_copy(wq.at[0, :, g * 2 * W:(g + 1) * 2 * W], wq_buf.at[g], wq_sem.at[g])

    h_load.wait()
    gain_load.wait()
    for g in range(n_q):
        wq_copy(g).start()
    kv_copy = pltpu.make_async_copy(wkv.at[0], wkv_buf, wkv_sem)
    kv_copy.start()

    folded = jnp.zeros((256, 128), F32)
    for k in range(half // 128):
        block = h_own[:, :, :, k * 128:(k + 1) * 128].reshape(256, 128).astype(F32)
        folded += block * block
    sq_all[me] = jnp.broadcast_to(jnp.sum(jnp.transpose(folded), axis=0, keepdims=True), (8, 256))
    pl.semaphore_wait(barrier, 7)

    def sq_copy(peer, src):
        return pltpu.make_async_remote_copy(
            src_ref=sq_all.at[src], dst_ref=sq_all.at[src], send_sem=sq_send.at[peer], recv_sem=sq_recv.at[src],
            **dev(x=peer // 2, yz=lax.rem(peer, 2)))

    def side_of(step):
        return 1 - chip if step < 2 else chip

    def piece(step):
        return pl.ds(32 * step, 32) if step < 2 else pl.ds(0, 64)

    def h_copy(step):
        block = (side_of(step), slice(None), piece(step))
        return pltpu.make_async_remote_copy(
            src_ref=h_own.at[block], dst_ref=h_other.at[block],
            send_sem=h_sems.at[step, 0], recv_sem=h_sems.at[step, 1], **dev(x=xi, yz=other_y))

    for k in range(1, 8):
        sq_copy(lax.rem(me + k, 8), me).start()
    for step in range(3):
        h_copy(step).start()
    for k in range(1, 8):
        peer = lax.rem(me + k, 8)
        sq_copy(peer, peer).wait_recv()
    total = jnp.sum(sq_all[...], axis=0)
    inv = lax.rsqrt(total / d_model + NORM_EPS)
    inv_all[...] = jnp.transpose(jnp.concatenate([inv] * 16, axis=0)).reshape(inv_all.shape)

    def normalize(values, step, which):
        cols = pl.ds(pl.multiple_of(which * half, 128), half)
        side, rows = side_of(step), piece(step)
        u[side, :, rows, cols] = (
            values[side, :, rows].astype(F32) * inv_all[side, :, rows, :1] * gain[:, cols].astype(F32)).astype(BF16)

    def near_copy(g):
        return pltpu.make_async_remote_copy(
            src_ref=part.at[g, :, 1 - core], dst_ref=near.at[g], send_sem=near_send.at[g],
            recv_sem=near_recv.at[g], **to_mate)

    def near_copy_q(g, step):
        side, rows = side_of(step), piece(step)
        return pltpu.make_async_remote_copy(
            src_ref=part.at[g, side, 1 - core, rows], dst_ref=near.at[g, side, rows],
            send_sem=qn_send.at[g, step], recv_sem=qn_recv.at[g, step], **to_mate)

    def near_copy_kv(step):
        side, rows = side_of(step), piece(step)
        return pltpu.make_async_remote_copy(
            src_ref=part_kv.at[side, 1 - core, rows], dst_ref=near_kv.at[side, rows],
            send_sem=kn_send.at[step], recv_sem=kn_recv.at[step], **to_mate)

    def far_copy(g):
        return pltpu.make_async_remote_copy(
            src_ref=far_src.at[g], dst_ref=recv_out.at[g - n_q], send_sem=far_send.at[g - n_q],
            recv_sem=far_recv.at[g - n_q], **to_across)

    def far_copy_q(g, step):
        rows = piece(step)
        return pltpu.make_async_remote_copy(
            src_ref=far_src.at[g, rows], dst_ref=far.at[g, rows], send_sem=qf_send.at[g, step],
            recv_sem=qf_recv.at[g, step], **to_across)

    def far_copy_kv(step):
        rows = piece(step)
        return pltpu.make_async_remote_copy(
            src_ref=far_src_kv.at[rows], dst_ref=far_kv.at[rows], send_sem=kf_send.at[step], recv_sem=kf_recv.at[step],
            **to_across)

    def keep_copy(g):
        return pltpu.make_async_copy(keep.at[g], keep_out.at[g - n_q], out_sem.at[g - n_q, 0])

    def send_copy(g):
        k = g - n_q
        return pltpu.make_async_copy(far_src.at[g], send_out.at[k - EARLY], out_sem.at[k, 1])

    def add(a, b):
        return (a.astype(F32) + b.astype(F32)).astype(BF16)

    def multiply(g):
        slot = lax.rem(g, NBUF1)
        for k in range(2):
            wait_weights(slot, k)
            res = jnp.dot(u[...].reshape(256, u.shape[-1]), wbuf[slot, k], preferred_element_type=F32).astype(BF16)
            part[g, :, :, :, k * W:(k + 1) * W] = res.reshape(2, 2, 64, W)
        near_copy(g).start()

        @pl.when(g + NBUF1 < n_all)
        def _():
            start_weights(g + NBUF1)

    def reduce_near(g):
        near_copy(g).wait_recv()
        far_src[g] = add(part[g, 1 - chip, core], near[g, 1 - chip])

        @pl.when((g < n_far) & ((core == 1) | (g < n_far - HELD)))
        def _():
            far_copy(g).start()

        @pl.when(g >= n_far)
        def _():
            send_copy(g).start()

        keep[g] = add(part[g, chip, core], near[g, chip])
        keep_copy(g).start()

    def multiply_q(step):
        side, rows = side_of(step), piece(step)
        lhs = u[side, :, rows].reshape(2 * rows.size, u.shape[-1])
        for g in range(n_q):
            if step == 0:
                wq_copy(g).wait()
            for k in range(2):
                res = jnp.dot(lhs, wq_buf[g, :, k * W:(k + 1) * W], preferred_element_type=F32).astype(BF16)
                part[g, side, :, rows, k * W:(k + 1) * W] = res.reshape(2, rows.size, W)
            near_copy_q(g, step).start()
            if step == 0 and g >= 1:
                reduce_q(0, g - 1)
        if step == 0:
            kv_copy.wait()
        res = jnp.dot(lhs, wkv_buf[...], preferred_element_type=F32).astype(BF16)
        part_kv[side, :, rows] = res.reshape(2, rows.size, res.shape[1])
        near_copy_kv(step).start()

    def reduce_q(step, g):
        side, rows = side_of(step), piece(step)
        near_copy_q(g, step).wait_recv()
        total_q = add(part[g, side, core, rows], near[g, side, rows])
        if step < 2:
            far_src[g, rows] = total_q
            far_copy_q(g, step).start()
        else:
            keep[g] = total_q

    def reduce_kv(step):
        side, rows = side_of(step), piece(step)
        near_copy_kv(step).wait_recv()
        total_kv = add(part_kv[side, core, rows], near_kv[side, rows])
        if step < 2:
            far_src_kv[rows] = total_kv
            far_copy_kv(step).start()
        else:
            keep_kv[...] = total_kv

    for step in range(3):
        normalize(h_own, step, yj)
        h_copy(step).wait_recv()
        normalize(h_other, step, other_y)
        if step < 2:
            multiply_q(step)
            for g in range(n_q - 1 if step == 0 else 0, n_q):
                reduce_q(step, g)
            reduce_kv(step)
        if step == 0:
            for g in range(n_q, n_q + NBUF1):
                start_weights(jnp.int32(g))

    @pl.loop(n_q, n_far)
    def _(g):
        multiply(g)

        @pl.when(g >= n_q + 1)
        def _():
            reduce_near(g - 1)

    q_cols = n_q * 2 * W
    multiply_q(2)
    for g in range(n_q):
        reduce_q(2, g)
        for step in range(2):
            far_copy_q(g, step).wait_recv()
        z_rows[:, :, g * 2 * W:(g + 1) * 2 * W] = add(keep[g], far[g]).reshape(2, 32, 2 * W)
    reduce_kv(2)
    for step in range(2):
        far_copy_kv(step).wait_recv()
    z_kv = add(keep_kv[...], far_kv[...])
    z_rows[:, :, q_cols:] = z_kv.reshape(2, 32, z_kv.shape[1])
    y_copy = pltpu.make_async_remote_copy(
        src_ref=z_rows.at[other_y], dst_ref=z_other, send_sem=y_sems.at[0], recv_sem=y_sems.at[1],
        **dev(x=xi, yz=other_y))
    y_copy.start()
    qkv_own = pltpu.make_async_copy(z_rows.at[yj], qkv_out.at[yj], qkv_sem.at[0])
    qkv_own.start()

    @pl.loop(n_far, n_all)
    def _(g):
        multiply(g)
        reduce_near(g - 1)

        @pl.when((g == n_far + RELEASE) & (core == 0))
        def _():
            @pl.loop(n_far - HELD, n_far)
            def _(k):
                far_copy(k).start()

    reduce_near(jnp.int32(n_all - 1))
    y_copy.wait_recv()
    qkv_other = pltpu.make_async_copy(z_other, qkv_out.at[other_y], qkv_sem.at[1])
    qkv_other.start()

    for step in range(3):
        h_copy(step).wait_send()
        near_copy_kv(step).wait_send()
        for g in range(n_q):
            near_copy_q(g, step).wait_send()
    for step in range(2):
        far_copy_kv(step).wait_send()
        for g in range(n_q):
            far_copy_q(g, step).wait_send()
    for k in range(1, 8):
        sq_copy(lax.rem(me + k, 8), me).wait_send()
    y_copy.wait_send()

    @pl.loop(n_q, n_all)
    def _(g):
        near_copy(g).wait_send()
        keep_copy(g).wait()

    @pl.loop(n_far, n_all)
    def _(g):
        send_copy(g).wait()

    qkv_own.wait()
    qkv_other.wait()

    @pl.loop(n_q, n_far)
    def _(g):
        far_copy(g).wait_send()
        far_copy(g).wait_recv()


def project(hidden, gain, w_q, w_kv, w_gate, w_up, d_model):
    rows, half = hidden.shape
    feats = w_q.shape[1]
    kv = w_kv.shape[2]
    n_q = w_q.shape[2] // (2 * W)
    n_ff = w_gate.shape[2] // W
    n_all = n_q + n_ff
    late = n_ff - EARLY
    dma = pltpu.SemaphoreType.DMA
    any_spec = pl.BlockSpec(memory_space=pl.ANY)
    cols = w_q.shape[2] + kv
    flops = 2 * rows * feats * (w_q.shape[2] + kv + 2 * w_gate.shape[2])
    return pl.pallas_call(
        functools.partial(project_kernel, n_q, n_ff, d_model),
        name="project",
        out_shape=(
            jax.ShapeDtypeStruct((2, 32, cols), BF16),
            jax.ShapeDtypeStruct((n_ff, 64, 2 * W), BF16),
            jax.ShapeDtypeStruct((EARLY, 64, 2 * W), BF16),
            jax.ShapeDtypeStruct((late, 64, 2 * W), BF16),
        ),
        in_specs=[any_spec] * 6,
        out_specs=(any_spec, any_spec, any_spec, any_spec),
        scratch_shapes=[
            pltpu.VMEM((1, feats), BF16),
            pltpu.VMEM((2, 2, 64, half), BF16),
            pltpu.VMEM((2, 2, 64, half), BF16),
            pltpu.VMEM((2, 2, 64, feats), BF16),
            pltpu.VMEM((2, 2, 64, 128), F32),
            pltpu.VMEM((8, 8, rows), F32),
            pltpu.VMEM((n_q, feats, 2 * W), BF16),
            pltpu.VMEM((NBUF1, 2, feats, W), BF16),
            pltpu.VMEM((feats, kv), BF16),
            pltpu.VMEM((n_all, 2, 2, 64, 2 * W), BF16),
            pltpu.VMEM((2, 2, 64, kv), BF16),
            pltpu.VMEM((n_all, 2, 64, 2 * W), BF16),
            pltpu.VMEM((2, 64, kv), BF16),
            pltpu.VMEM((n_all, 64, 2 * W), BF16),
            pltpu.VMEM((64, kv), BF16),
            pltpu.VMEM((n_all, 64, 2 * W), BF16),
            pltpu.VMEM((64, kv), BF16),
            pltpu.VMEM((n_q, 64, 2 * W), BF16),
            pltpu.VMEM((64, kv), BF16),
            pltpu.VMEM((2, 32, cols), BF16),
            pltpu.VMEM((32, cols), BF16),
            dma((n_q,)),
            dma((NBUF1, 2)),
            dma,
            dma,
            dma,
            dma((3, 2)),
            dma((8,)),
            dma((8,)),
            dma((n_all,)),
            dma((n_all,)),
            dma((n_q, 3)),
            dma((n_q, 3)),
            dma((3,)),
            dma((3,)),
            dma((EARLY,)),
            dma((EARLY,)),
            dma((n_q, 2)),
            dma((n_q, 2)),
            dma((2,)),
            dma((2,)),
            dma((2,)),
            dma((n_ff, 2)),
            dma((2,)),
        ],
        compiler_params=pltpu.CompilerParams(collective_id=0, has_side_effects=True, vmem_limit_bytes=VMEM_LIMIT),
        cost_estimate=pl.CostEstimate(flops=flops, bytes_accessed=feats * (flops // (rows * feats)), transcendentals=0),
    )(hidden.reshape(2, 2, 64, half), gain, w_q, w_kv, w_gate, w_up)


def attend_kernel(lens, q_ref, kv_ref, k_ref, v_ref, k_out, v_out, o_ref):
    step = pl.program_id(0)
    n_pos = k_ref.shape[2]
    scale = q_ref.shape[2] ** -0.5 * LOG2E
    for s in range(SEQ_STEP):
        length = lens[step * SEQ_STEP + s]
        base = pl.multiple_of((length // 16) * 16, 16)
        k_out[0, s] = k_ref[0, s]
        v_out[0, s] = v_ref[0, s]
        hit = lax.broadcasted_iota(jnp.int32, (16, k_ref.shape[3]), 0) == length - base
        for src, dst, which in ((k_ref, k_out, 0), (v_ref, v_out, 1)):
            old = src[0, s, pl.ds(base, 16), :].astype(F32)
            new = kv_ref[s, which:which + 1, :].astype(F32)
            dst[0, s, pl.ds(base, 16), :] = jnp.where(hit, new, old).astype(BF16)
        scores = lax.dot_general(q_ref[s], k_out[0, s], (((1,), (1,)), ((), ())), preferred_element_type=F32) * scale
        visible = lax.broadcasted_iota(jnp.int32, scores.shape, 1) <= length
        scores = jnp.where(visible, scores, MASKED)
        weights = jnp.exp2(scores - jnp.max(scores, axis=1, keepdims=True))
        probs = (weights * (1.0 / jnp.sum(weights, axis=1, keepdims=True))).astype(BF16)
        o_ref[s] = jnp.dot(probs, v_out[0, s], preferred_element_type=F32).astype(BF16)


def attend(lens, q, kv, k_cache, v_cache):
    seqs, heads, dim = q.shape
    n_pos = k_cache.shape[2]
    cache_spec = pl.BlockSpec((1, SEQ_STEP, n_pos, dim), lambda b, lens: (0, b, 0, 0))
    q_spec = pl.BlockSpec((SEQ_STEP, heads, dim), lambda b, lens: (b, 0, 0))
    return pl.pallas_call(
        attend_kernel,
        name="attend",
        out_shape=(
            jax.ShapeDtypeStruct(k_cache.shape, BF16),
            jax.ShapeDtypeStruct(v_cache.shape, BF16),
            jax.ShapeDtypeStruct(q.shape, BF16),
        ),
        grid_spec=pltpu.PrefetchScalarGridSpec(
            num_scalar_prefetch=1,
            grid=(seqs // SEQ_STEP,),
            in_specs=[q_spec, pl.BlockSpec((SEQ_STEP, 2, dim), lambda b, lens: (b, 0, 0)), cache_spec, cache_spec],
            out_specs=(cache_spec, cache_spec, q_spec),
        ),
        compiler_params=pltpu.CompilerParams(dimension_semantics=("arbitrary",), vmem_limit_bytes=66_000_000),
        cost_estimate=pl.CostEstimate(
            flops=10**10, bytes_accessed=8 * k_cache.size, transcendentals=seqs * heads * n_pos),
    )(lens, q, kv, k_cache, v_cache)


def output_kernel(
    n_ff, n_o, o_in, keep, recv_e, recv_l, hidden, w_o, w_down, out,
    acts, wbuf, acc, keep_v, recv_v, h_v, y_src, y_dst,
    w_sem, keep_sem, recv_sem, h_sem, oo_sems, on_send, on_recv, far_send, far_recv, near_send, near_recv, y_sems,
):
    xi = lax.axis_index("x")
    yj = lax.axis_index("yz")
    core = lax.rem(xi, 2)
    mate = xi + 1 - 2 * core
    across = lax.rem(xi + 2, 4)
    other_y = 1 - yj
    n_m = n_ff // GROUP
    n_g = n_m + n_o // GROUP
    n_early = EARLY // GROUP
    depth = GROUP * W
    d_out = w_down.shape[2]
    half = d_out // 2

    barrier = pltpu.get_barrier_semaphore()
    for x_, y_ in ((mate, yj), (across, yj), (xi, other_y)):
        pl.semaphore_signal(barrier, inc=1, **dev(x=x_, yz=y_))

    def keep_copy(g):
        return pltpu.make_async_copy(
            keep.at[pl.ds(GROUP * g, GROUP)], keep_v.at[pl.ds(GROUP * g, GROUP)], keep_sem.at[g])

    def recv_copy(g):
        src = recv_e.at[pl.ds(GROUP * g, GROUP)] if g < n_early else recv_l.at[pl.ds(GROUP * (g - n_early), GROUP)]
        return pltpu.make_async_copy(src, recv_v.at[pl.ds(GROUP * g, GROUP)], recv_sem.at[g])

    keep_copy(0).start()
    recv_copy(0).start()

    def rows_of(p, owner):
        off, size = PARTS[p]
        return pl.ds(pl.multiple_of(4 * off + owner * size, 16), size)

    def block(p, g, owner):
        return acts.at[pl.ds(GROUP * g, GROUP), rows_of(p, owner)]

    def o_rows(s):
        row = (1 - yj) * (32 * xi + 16 * s) + yj * (128 + 64 * s + 16 * xi)
        return acts.at[pl.ds(n_ff, n_o), pl.ds(pl.multiple_of(row, 16), 16)]

    def o_own(s):
        return pltpu.make_async_copy(o_in.at[yj, :, pl.ds(16 * s, 16)], o_rows(s), oo_sems.at[s])

    def o_copy(s):
        return pltpu.make_async_remote_copy(
            src_ref=o_in.at[other_y, :, pl.ds(16 * s, 16)], dst_ref=o_rows(s), send_sem=on_send.at[s],
            recv_sem=on_recv.at[s], **dev(x=xi, yz=other_y))

    h_load = pltpu.make_async_copy(hidden, h_v, h_sem)

    def load_weights(g):
        slot = lax.rem(g, NBUF3)

        @pl.when(g < n_m)
        def _():
            pltpu.make_async_copy(
                w_down.at[0, pl.ds(pl.multiple_of(g * depth, W), depth)], wbuf.at[slot], w_sem.at[slot]).start()

        @pl.when(g >= n_m)
        def _():
            pltpu.make_async_copy(
                w_o.at[0, pl.ds(pl.multiple_of((g - n_m) * depth, W), depth)], wbuf.at[slot], w_sem.at[slot]).start()

    def far_copy(p, g):
        return pltpu.make_async_remote_copy(
            src_ref=block(p, g, xi), dst_ref=block(p, g, xi), send_sem=far_send.at[p, g], recv_sem=far_recv.at[p, g],
            **dev(x=across, yz=yj))

    def near_copy(p, g, which):
        rows = block(p, g, xi if which == 0 else across)
        return pltpu.make_async_remote_copy(
            src_ref=rows, dst_ref=rows, send_sem=near_send.at[p, g, which], recv_sem=near_recv.at[p, g, which],
            **dev(x=mate, yz=yj))

    def give(p, g):
        far_copy(p, g).start()
        near_copy(p, g, 0).start()

    def give_m(p, g):
        off, size = PARTS[p]
        for k in range(GROUP):
            t = GROUP * g + k
            z = keep_v[t, off:off + size].astype(F32) + recv_v[t, off:off + size].astype(F32)
            acts[t, rows_of(p, xi)] = silu_mul(z[:, :W], z[:, W:])
        give(p, g)

    pl.semaphore_wait(barrier, 3)
    for g in range(n_m):
        keep_copy(g).wait()
        recv_copy(g).wait()
        give_m(0, g)
        if g == 0:
            for s in range(2):
                o_copy(s).start()
                o_own(s).start()
            for k in range(1, n_m):
                keep_copy(k).start()
                recv_copy(k).start()
    for s in range(NBUF3):
        load_weights(jnp.int32(s))
    h_load.start()
    acc[...] = jnp.zeros_like(acc)
    for s in range(2):
        o_own(s).wait()
        o_copy(s).wait_recv()

    def chunk(p, k):
        return k if p % 2 == 0 else n_g - 1 - k

    for g in range(n_m, n_g):
        give(0, g)
    for p in range(1, len(PARTS)):
        @pl.loop(0, n_g)
        def _(k):
            g = chunk(p, k)

            @pl.when(g < n_m)
            def _():
                give_m(p, g)

            @pl.when(g >= n_m)
            def _():
                give(p, g)

    def forward(p, k):
        g = chunk(p, k)
        far_copy(p, g).wait_recv()
        near_copy(p, g, 1).start()

    def multiply(p, k):
        g = chunk(p, k)
        slot = lax.rem(g, NBUF3)

        @pl.when(k >= (0 if p == 0 else NBUF3))
        def _():
            pltpu.make_async_copy(w_down.at[0, pl.ds(0, depth)], wbuf.at[slot], w_sem.at[slot]).wait()

        near_copy(p, g, 0).wait_recv()
        near_copy(p, g, 1).wait_recv()
        off, size = PARTS[p]
        rows = slice(4 * off, 4 * (off + size))
        for n in range(d_out // W):
            cols = slice(n * W, (n + 1) * W)
            total = acc[rows, cols]
            for j in range(GROUP):
                total += jnp.dot(
                    acts[GROUP * g + j, rows], wbuf[slot, j * W:(j + 1) * W, cols], preferred_element_type=F32)
            acc[rows, cols] = total

        @pl.when(k + NBUF3 < n_g)
        def _():
            load_weights(chunk(p, k + NBUF3))

    def cols_of(j):
        return pl.ds(pl.multiple_of(j * half, 128), half)

    def y_copy(p):
        rows = slice(4 * PARTS[p][0], 4 * sum(PARTS[p]))
        return pltpu.make_async_remote_copy(
            src_ref=y_src.at[rows], dst_ref=y_dst.at[rows], send_sem=y_sems.at[p, 0], recv_sem=y_sems.at[p, 1],
            **dev(x=xi, yz=other_y))

    def exchange(p):
        rows = slice(4 * PARTS[p][0], 4 * sum(PARTS[p]))
        y_src[rows] = acc[rows, cols_of(other_y)].astype(BF16)
        y_copy(p).start()

    def finalize(p):
        off, size = PARTS[p]
        rows = slice(4 * off, 4 * (off + size))
        y_copy(p).wait_recv()
        total = (acc[rows, cols_of(yj)] + y_dst[rows].astype(F32)).reshape(4, size, half)
        out[:, off:off + size] = (h_v[:, off:off + size].astype(F32) + total).astype(BF16)

    for p in range(len(PARTS)):
        forward(p, jnp.int32(0))
        if p > 0:
            multiply(p - 1, jnp.int32(n_g - 1))
            exchange(p - 1)
        if p == 1:
            h_load.wait()

        @pl.loop(1, n_g)
        def _(k):
            forward(p, k)
            multiply(p, k - 1)

        if p > 0:
            finalize(p - 1)

    last = len(PARTS) - 1
    g = chunk(last, n_g - 1)
    if n_g > NBUF3:
        pltpu.make_async_copy(w_down.at[0, pl.ds(0, depth)], wbuf.at[g % NBUF3], w_sem.at[g % NBUF3]).wait()
    near_copy(last, g, 0).wait_recv()
    near_copy(last, g, 1).wait_recv()
    rows = slice(4 * PARTS[last][0], 4 * sum(PARTS[last]))
    for j in (other_y, yj):
        for n in range(half // 256):
            cols = pl.ds(pl.multiple_of(j * half + n * 256, 256), 256)
            total = acc[rows, cols]
            for k in range(GROUP):
                total += jnp.dot(
                    acts[GROUP * g + k, rows], wbuf[g % NBUF3, k * W:(k + 1) * W, cols], preferred_element_type=F32)
            acc[rows, cols] = total
        if j is other_y:
            exchange(last)
    for s in range(2):
        o_copy(s).wait_send()
    for p in range(len(PARTS)):
        @pl.loop(0, n_g)
        def _(g):
            far_copy(p, g).wait_send()
            near_copy(p, g, 0).wait_send()
            near_copy(p, g, 1).wait_send()

    finalize(last)
    for p in range(len(PARTS)):
        y_copy(p).wait_send()


def finish(o, keep, recv_e, recv_l, hidden, w_o, w_down):
    rows, half = hidden.shape
    n_ff = w_down.shape[1] // W
    n_o = w_o.shape[1] // W
    n_m = n_ff // GROUP
    n_g = n_m + n_o // GROUP
    n_p = len(PARTS)
    d_out = w_down.shape[2]
    dma = pltpu.SemaphoreType.DMA
    any_spec = pl.BlockSpec(memory_space=pl.ANY)
    vmem = pl.BlockSpec(memory_space=pltpu.VMEM)
    flops = 2 * rows * d_out * (w_down.shape[1] + w_o.shape[1])
    out = pl.pallas_call(
        functools.partial(output_kernel, n_ff, n_o),
        name="finish",
        out_shape=jax.ShapeDtypeStruct((4, 64, half), BF16),
        in_specs=[any_spec] * 7,
        out_specs=vmem,
        scratch_shapes=[
            pltpu.VMEM((n_ff + n_o, rows, W), BF16),
            pltpu.VMEM((NBUF3, GROUP * W, d_out), BF16),
            pltpu.VMEM((rows, d_out), F32),
            pltpu.VMEM(keep.shape, BF16),
            pltpu.VMEM(keep.shape, BF16),
            pltpu.VMEM((4, 64, half), BF16),
            pltpu.VMEM((rows, half), BF16),
            pltpu.VMEM((rows, half), BF16),
            dma((NBUF3,)),
            dma((n_m,)),
            dma((n_m,)),
            dma,
            dma((2,)),
            dma((2,)),
            dma((2,)),
            dma((n_p, n_g)),
            dma((n_p, n_g)),
            dma((n_p, n_g, 2)),
            dma((n_p, n_g, 2)),
            dma((n_p, 2)),
        ],
        compiler_params=pltpu.CompilerParams(collective_id=1, has_side_effects=True, vmem_limit_bytes=56_000_000),
        cost_estimate=pl.CostEstimate(flops=flops, bytes_accessed=2 * d_out * (w_down.shape[1] + w_o.shape[1]), transcendentals=0),
    )(o, keep, recv_e, recv_l, hidden.reshape(4, 64, half), w_o, w_down)
    return out.reshape(rows, half)


def solution(mesh):
    x_size = mesh.shape["x"]
    y_size = mesh.shape["yz"]
    row_spec = P("dp", ("x", "yz"))
    tile_in = P(None, "x", "yz")
    tile_out = P(None, "yz", "x")
    cache_spec = P(None, ("dp", "x", "yz"))
    len_spec = P(("dp", "x", "yz"))

    def device_step(hidden, norm_gain, w_q, w_kv, w_gate, w_up, w_o, w_down, k_cache, v_cache, seq_len):
        d_model = hidden.shape[1] * x_size * y_size
        seqs = k_cache.shape[1]
        dim = k_cache.shape[3]
        q_cols = w_q.shape[2]
        heads = q_cols // dim
        qkv, keep, recv_e, send = project(hidden, norm_gain, w_q, w_kv, w_gate, w_up, d_model)
        recv_l = lax.ppermute(send, "x", [(i, (i + x_size // 2) % x_size) for i in range(x_size)])
        q = qkv[:, :, :q_cols].reshape(y_size, seqs, heads, dim).transpose(1, 0, 2, 3).reshape(seqs, y_size * heads, dim)
        kv = qkv[:, :, q_cols:].transpose(1, 0, 2)
        k_new, v_new, o = attend(seq_len, q, kv, k_cache, v_cache)
        o = o.reshape(seqs, y_size, q_cols // W, W).transpose(1, 2, 0, 3)
        hidden_out = finish(o, keep, recv_e, recv_l, hidden, w_o, w_down)
        return hidden_out, k_new, v_new

    return jax.shard_map(
        device_step,
        mesh=mesh,
        in_specs=(row_spec, P(None, "x"), tile_in, tile_in, tile_in, tile_in, tile_out, tile_out, cache_spec, cache_spec, len_spec),
        out_specs=(row_spec, cache_spec, cache_spec),
        check_vma=False,
    )
```

```python
import functools

import jax
import jax.numpy as jnp
from jax import lax
from jax.experimental import pallas as pl
from jax.experimental.pallas import tpu as pltpu
from jax.sharding import PartitionSpec as P

NORM_EPS = 1e-6
W = 512
NBUF1 = 4
NBUF3 = 6
GROUP = 3
PARTS = ((0, 32), (32, 16), (48, 16))
EARLY = 12
SEQ_STEP = 2
HELD = 6
RELEASE = 3
VMEM_LIMIT = 64_000_000
F32 = jnp.float32
BF16 = jnp.bfloat16
LOG2E = 1.4426950408889634
MASKED = -1e30 * LOG2E


def dev(**axes):
    return dict(device_id=axes, device_id_type=pl.DeviceIdType.MESH)


def silu_mul(gate, up):
    gate = gate.astype(BF16).astype(F32)
    up = up.astype(BF16).astype(F32)
    return (jax.nn.silu(gate) * up).astype(BF16)


def project_kernel(
    n_q, n_ff, d_model, hidden, gain_in, wq, wkv, wg, wu,
    q_out, kv_out, keep_out, recv_out, send_out,
    gain, h_own, h_other, u, inv_all, sq_all, wq_buf, wbuf, wkv_buf, part, part_kv, near, near_kv, keep, keep_kv, far_src,
    far_src_kv, far, far_kv, z_rows, z_other,
    wq_sem, w_sem, wkv_sem, h_in, gain_sem, h_sems, sq_send, sq_recv, near_send, near_recv, qn_send, qn_recv, kn_send, kn_recv,
    far_send, far_recv, qf_send, qf_recv, kf_send, kf_recv, y_sems, out_sem, qkv_sem,
):
    xi = lax.axis_index("x")
    yj = lax.axis_index("yz")
    core = lax.rem(xi, 2)
    chip = xi // 2
    mate = xi + 1 - 2 * core
    across = lax.rem(xi + 2, 4)
    other_y = 1 - yj
    me = xi * 2 + yj
    half = hidden.shape[-1]
    n_all = n_q + n_ff
    n_far = n_q + EARLY
    to_mate = dev(x=mate, yz=yj)
    to_across = dev(x=across, yz=yj)

    barrier = pltpu.get_barrier_semaphore()
    for k in range(1, 8):
        peer = lax.rem(me + k, 8)
        pl.semaphore_signal(barrier, inc=1, **dev(x=peer // 2, yz=lax.rem(peer, 2)))
    h_load = pltpu.make_async_copy(hidden, h_own, h_in)
    h_load.start()
    gain_load = pltpu.make_async_copy(gain_in, gain, gain_sem)
    gain_load.start()

    def start_weights(g):
        slot = lax.rem(g, NBUF1)
        cols = pl.ds(pl.multiple_of((g - n_q) * W, W), W)
        pltpu.make_async_copy(wg.at[0, :, cols], wbuf.at[slot, 0], w_sem.at[slot, 0]).start()
        pltpu.make_async_copy(wu.at[0, :, cols], wbuf.at[slot, 1], w_sem.at[slot, 1]).start()

    def wait_weights(slot, k):
        pltpu.make_async_copy(wg.at[0, :, pl.ds(0, W)], wbuf.at[slot, k], w_sem.at[slot, k]).wait()

    def wq_copy(g):
        return pltpu.make_async_copy(wq.at[0, :, g * 2 * W:(g + 1) * 2 * W], wq_buf.at[g], wq_sem.at[g])

    h_load.wait()
    gain_load.wait()
    for g in range(n_q):
        wq_copy(g).start()
    kv_copy = pltpu.make_async_copy(wkv.at[0], wkv_buf, wkv_sem)
    kv_copy.start()

    folded = jnp.zeros((256, 128), F32)
    for k in range(half // 128):
        block = h_own[:, :, :, k * 128:(k + 1) * 128].reshape(256, 128).astype(F32)
        folded += block * block
    sq_all[me] = jnp.broadcast_to(jnp.sum(jnp.transpose(folded), axis=0, keepdims=True), (8, 256))
    pl.semaphore_wait(barrier, 7)

    def sq_copy(peer, src):
        return pltpu.make_async_remote_copy(
            src_ref=sq_all.at[src], dst_ref=sq_all.at[src], send_sem=sq_send.at[peer], recv_sem=sq_recv.at[src],
            **dev(x=peer // 2, yz=lax.rem(peer, 2)))

    def side_of(step):
        return 1 - chip if step < 2 else chip

    def piece(step):
        return pl.ds(32 * step, 32) if step < 2 else pl.ds(0, 64)

    def h_copy(step):
        block = (side_of(step), slice(None), piece(step))
        return pltpu.make_async_remote_copy(
            src_ref=h_own.at[block], dst_ref=h_other.at[block],
            send_sem=h_sems.at[step, 0], recv_sem=h_sems.at[step, 1], **dev(x=xi, yz=other_y))

    for k in range(1, 8):
        sq_copy(lax.rem(me + k, 8), me).start()
    for step in range(3):
        h_copy(step).start()
    for k in range(1, 8):
        peer = lax.rem(me + k, 8)
        sq_copy(peer, peer).wait_recv()
    total = jnp.sum(sq_all[...], axis=0)
    inv = lax.rsqrt(total / d_model + NORM_EPS)
    inv_all[...] = jnp.transpose(jnp.concatenate([inv] * 16, axis=0)).reshape(inv_all.shape)

    def normalize(values, step, which):
        cols = pl.ds(pl.multiple_of(which * half, 128), half)
        side, rows = side_of(step), piece(step)
        u[side, :, rows, cols] = (
            values[side, :, rows].astype(F32) * inv_all[side, :, rows, :1] * gain[:, cols].astype(F32)).astype(BF16)

    def near_copy(g):
        return pltpu.make_async_remote_copy(
            src_ref=part.at[g, :, 1 - core], dst_ref=near.at[g], send_sem=near_send.at[g],
            recv_sem=near_recv.at[g], **to_mate)

    def near_copy_q(g, step):
        side, rows = side_of(step), piece(step)
        return pltpu.make_async_remote_copy(
            src_ref=part.at[g, side, 1 - core, rows], dst_ref=near.at[g, side, rows],
            send_sem=qn_send.at[g, step], recv_sem=qn_recv.at[g, step], **to_mate)

    def near_copy_kv(step):
        side, rows = side_of(step), piece(step)
        return pltpu.make_async_remote_copy(
            src_ref=part_kv.at[side, 1 - core, rows], dst_ref=near_kv.at[side, rows],
            send_sem=kn_send.at[step], recv_sem=kn_recv.at[step], **to_mate)

    def far_copy(g):
        return pltpu.make_async_remote_copy(
            src_ref=far_src.at[g], dst_ref=recv_out.at[g - n_q], send_sem=far_send.at[g - n_q],
            recv_sem=far_recv.at[g - n_q], **to_across)

    def far_copy_q(g, step):
        rows = piece(step)
        return pltpu.make_async_remote_copy(
            src_ref=far_src.at[g, rows], dst_ref=far.at[g, rows], send_sem=qf_send.at[g, step],
            recv_sem=qf_recv.at[g, step], **to_across)

    def far_copy_kv(step):
        rows = piece(step)
        return pltpu.make_async_remote_copy(
            src_ref=far_src_kv.at[rows], dst_ref=far_kv.at[rows], send_sem=kf_send.at[step], recv_sem=kf_recv.at[step],
            **to_across)

    def keep_copy(g):
        return pltpu.make_async_copy(keep.at[g], keep_out.at[g - n_q], out_sem.at[g - n_q, 0])

    def send_copy(g):
        k = g - n_q
        return pltpu.make_async_copy(far_src.at[g], send_out.at[k - EARLY], out_sem.at[k, 1])

    def add(a, b):
        return (a.astype(F32) + b.astype(F32)).astype(BF16)

    def multiply(g):
        slot = lax.rem(g, NBUF1)
        for k in range(2):
            wait_weights(slot, k)
            res = jnp.dot(u[...].reshape(256, u.shape[-1]), wbuf[slot, k], preferred_element_type=F32).astype(BF16)
            part[g, :, :, :, k * W:(k + 1) * W] = res.reshape(2, 2, 64, W)
        near_copy(g).start()

        @pl.when(g + NBUF1 < n_all)
        def _():
            start_weights(g + NBUF1)

    def reduce_near(g):
        near_copy(g).wait_recv()
        far_src[g] = add(part[g, 1 - chip, core], near[g, 1 - chip])

        @pl.when((g < n_far) & ((core == 1) | (g < n_far - HELD)))
        def _():
            far_copy(g).start()

        @pl.when(g >= n_far)
        def _():
            send_copy(g).start()

        keep[g] = add(part[g, chip, core], near[g, chip])
        keep_copy(g).start()

    def multiply_q(step):
        side, rows = side_of(step), piece(step)
        lhs = u[side, :, rows].reshape(2 * rows.size, u.shape[-1])
        for g in range(n_q):
            if step == 0:
                wq_copy(g).wait()
            for k in range(2):
                res = jnp.dot(lhs, wq_buf[g, :, k * W:(k + 1) * W], preferred_element_type=F32).astype(BF16)
                part[g, side, :, rows, k * W:(k + 1) * W] = res.reshape(2, rows.size, W)
            near_copy_q(g, step).start()
            if step == 0 and g >= 1:
                reduce_q(0, g - 1)
        if step == 0:
            kv_copy.wait()
        res = jnp.dot(lhs, wkv_buf[...], preferred_element_type=F32).astype(BF16)
        part_kv[side, :, rows] = res.reshape(2, rows.size, res.shape[1])
        near_copy_kv(step).start()

    def reduce_q(step, g):
        side, rows = side_of(step), piece(step)
        near_copy_q(g, step).wait_recv()
        total_q = add(part[g, side, core, rows], near[g, side, rows])
        if step < 2:
            far_src[g, rows] = total_q
            far_copy_q(g, step).start()
        else:
            keep[g] = total_q

    def reduce_kv(step):
        side, rows = side_of(step), piece(step)
        near_copy_kv(step).wait_recv()
        total_kv = add(part_kv[side, core, rows], near_kv[side, rows])
        if step < 2:
            far_src_kv[rows] = total_kv
            far_copy_kv(step).start()
        else:
            keep_kv[...] = total_kv

    for step in range(3):
        normalize(h_own, step, yj)
        h_copy(step).wait_recv()
        normalize(h_other, step, other_y)
        if step < 2:
            multiply_q(step)
            for g in range(n_q - 1 if step == 0 else 0, n_q):
                reduce_q(step, g)
            reduce_kv(step)
        if step == 0:
            for g in range(n_q, n_q + NBUF1):
                start_weights(jnp.int32(g))

    @pl.loop(n_q, n_far)
    def _(g):
        multiply(g)

        @pl.when(g >= n_q + 1)
        def _():
            reduce_near(g - 1)

    q_cols = n_q * 2 * W
    multiply_q(2)
    for g in range(n_q):
        reduce_q(2, g)
        for step in range(2):
            far_copy_q(g, step).wait_recv()
        z_rows[:, :, g * 2 * W:(g + 1) * 2 * W] = add(keep[g], far[g]).reshape(2, 32, 2 * W)
    reduce_kv(2)
    for step in range(2):
        far_copy_kv(step).wait_recv()
    z_kv = add(keep_kv[...], far_kv[...])
    z_rows[:, :, q_cols:] = z_kv.reshape(2, 32, z_kv.shape[1])
    y_copy = pltpu.make_async_remote_copy(
        src_ref=z_rows.at[other_y], dst_ref=z_other, send_sem=y_sems.at[0], recv_sem=y_sems.at[1],
        **dev(x=xi, yz=other_y))
    y_copy.start()
    def qkv_copies(src, which):
        return (
            pltpu.make_async_copy(src.at[:, :q_cols], q_out.at[which], qkv_sem.at[0, 0 if src is z_other else 1]),
            pltpu.make_async_copy(src.at[:, q_cols:], kv_out.at[which], qkv_sem.at[1, 0 if src is z_other else 1]),
        )

    qkv_own = qkv_copies(z_rows.at[yj], yj)
    for copy in qkv_own:
        copy.start()

    @pl.loop(n_far, n_all)
    def _(g):
        multiply(g)
        reduce_near(g - 1)

        @pl.when((g == n_far + RELEASE) & (core == 0))
        def _():
            @pl.loop(n_far - HELD, n_far)
            def _(k):
                far_copy(k).start()

    reduce_near(jnp.int32(n_all - 1))
    y_copy.wait_recv()
    qkv_other = qkv_copies(z_other, other_y)
    for copy in qkv_other:
        copy.start()

    for step in range(3):
        h_copy(step).wait_send()
        near_copy_kv(step).wait_send()
        for g in range(n_q):
            near_copy_q(g, step).wait_send()
    for step in range(2):
        far_copy_kv(step).wait_send()
        for g in range(n_q):
            far_copy_q(g, step).wait_send()
    for k in range(1, 8):
        sq_copy(lax.rem(me + k, 8), me).wait_send()
    y_copy.wait_send()

    @pl.loop(n_q, n_all)
    def _(g):
        near_copy(g).wait_send()
        keep_copy(g).wait()

    @pl.loop(n_far, n_all)
    def _(g):
        send_copy(g).wait()

    for copy in qkv_own + qkv_other:
        copy.wait()

    @pl.loop(n_q, n_far)
    def _(g):
        far_copy(g).wait_send()
        far_copy(g).wait_recv()


def project(hidden, gain, w_q, w_kv, w_gate, w_up, d_model):
    rows, half = hidden.shape
    feats = w_q.shape[1]
    kv = w_kv.shape[2]
    n_q = w_q.shape[2] // (2 * W)
    n_ff = w_gate.shape[2] // W
    n_all = n_q + n_ff
    late = n_ff - EARLY
    dma = pltpu.SemaphoreType.DMA
    any_spec = pl.BlockSpec(memory_space=pl.ANY)
    cols = w_q.shape[2] + kv
    flops = 2 * rows * feats * (w_q.shape[2] + kv + 2 * w_gate.shape[2])
    return pl.pallas_call(
        functools.partial(project_kernel, n_q, n_ff, d_model),
        name="project",
        out_shape=(
            jax.ShapeDtypeStruct((2, 32, cols - kv), BF16),
            jax.ShapeDtypeStruct((2, 32, kv), BF16),
            jax.ShapeDtypeStruct((n_ff, 64, 2 * W), BF16),
            jax.ShapeDtypeStruct((EARLY, 64, 2 * W), BF16),
            jax.ShapeDtypeStruct((late, 64, 2 * W), BF16),
        ),
        in_specs=[any_spec] * 6,
        out_specs=(any_spec,) * 5,
        scratch_shapes=[
            pltpu.VMEM((1, feats), BF16),
            pltpu.VMEM((2, 2, 64, half), BF16),
            pltpu.VMEM((2, 2, 64, half), BF16),
            pltpu.VMEM((2, 2, 64, feats), BF16),
            pltpu.VMEM((2, 2, 64, 128), F32),
            pltpu.VMEM((8, 8, rows), F32),
            pltpu.VMEM((n_q, feats, 2 * W), BF16),
            pltpu.VMEM((NBUF1, 2, feats, W), BF16),
            pltpu.VMEM((feats, kv), BF16),
            pltpu.VMEM((n_all, 2, 2, 64, 2 * W), BF16),
            pltpu.VMEM((2, 2, 64, kv), BF16),
            pltpu.VMEM((n_all, 2, 64, 2 * W), BF16),
            pltpu.VMEM((2, 64, kv), BF16),
            pltpu.VMEM((n_all, 64, 2 * W), BF16),
            pltpu.VMEM((64, kv), BF16),
            pltpu.VMEM((n_all, 64, 2 * W), BF16),
            pltpu.VMEM((64, kv), BF16),
            pltpu.VMEM((n_q, 64, 2 * W), BF16),
            pltpu.VMEM((64, kv), BF16),
            pltpu.VMEM((2, 32, cols), BF16),
            pltpu.VMEM((32, cols), BF16),
            dma((n_q,)),
            dma((NBUF1, 2)),
            dma,
            dma,
            dma,
            dma((3, 2)),
            dma((8,)),
            dma((8,)),
            dma((n_all,)),
            dma((n_all,)),
            dma((n_q, 3)),
            dma((n_q, 3)),
            dma((3,)),
            dma((3,)),
            dma((EARLY,)),
            dma((EARLY,)),
            dma((n_q, 2)),
            dma((n_q, 2)),
            dma((2,)),
            dma((2,)),
            dma((2,)),
            dma((n_ff, 2)),
            dma((2, 2)),
        ],
        compiler_params=pltpu.CompilerParams(collective_id=0, has_side_effects=True, vmem_limit_bytes=VMEM_LIMIT),
        cost_estimate=pl.CostEstimate(flops=flops, bytes_accessed=feats * (flops // (rows * feats)), transcendentals=0),
    )(hidden.reshape(2, 2, 64, half), gain, w_q, w_kv, w_gate, w_up)


def attend_kernel(lens, q_ref, kv_ref, k_ref, v_ref, k_out, v_out, o_ref):
    step = pl.program_id(0)
    n_pos = k_ref.shape[2]
    scale = q_ref.shape[2] ** -0.5 * LOG2E
    for s in range(SEQ_STEP):
        length = lens[step * SEQ_STEP + s]
        base = pl.multiple_of((length // 16) * 16, 16)
        k_out[0, s] = k_ref[0, s]
        v_out[0, s] = v_ref[0, s]
        hit = lax.broadcasted_iota(jnp.int32, (16, k_ref.shape[3]), 0) == length - base
        for src, dst, which in ((k_ref, k_out, 0), (v_ref, v_out, 1)):
            old = src[0, s, pl.ds(base, 16), :].astype(F32)
            fresh = kv_ref[which].astype(F32)
            mine = lax.broadcasted_iota(jnp.int32, fresh.shape, 0) == step * SEQ_STEP + s
            new = jnp.sum(jnp.where(mine, fresh, 0.0), axis=0, keepdims=True)
            dst[0, s, pl.ds(base, 16), :] = jnp.where(hit, new, old).astype(BF16)
        scores = lax.dot_general(q_ref[s], k_out[0, s], (((1,), (1,)), ((), ())), preferred_element_type=F32) * scale
        visible = lax.broadcasted_iota(jnp.int32, scores.shape, 1) <= length
        scores = jnp.where(visible, scores, MASKED)
        weights = jnp.exp2(scores - jnp.max(scores, axis=1, keepdims=True))
        probs = (weights * (1.0 / jnp.sum(weights, axis=1, keepdims=True))).astype(BF16)
        o_ref[s] = jnp.dot(probs, v_out[0, s], preferred_element_type=F32).astype(BF16)


def attend(lens, q, kv, k_cache, v_cache):
    seqs, heads, dim = q.shape
    n_pos = k_cache.shape[2]
    cache_spec = pl.BlockSpec((1, SEQ_STEP, n_pos, dim), lambda b, lens: (0, b, 0, 0))
    q_spec = pl.BlockSpec((SEQ_STEP, heads, dim), lambda b, lens: (b, 0, 0))
    return pl.pallas_call(
        attend_kernel,
        name="attend",
        out_shape=(
            jax.ShapeDtypeStruct(k_cache.shape, BF16),
            jax.ShapeDtypeStruct(v_cache.shape, BF16),
            jax.ShapeDtypeStruct(q.shape, BF16),
        ),
        grid_spec=pltpu.PrefetchScalarGridSpec(
            num_scalar_prefetch=1,
            grid=(seqs // SEQ_STEP,),
            in_specs=[q_spec, pl.BlockSpec((2, seqs, dim), lambda b, lens: (0, 0, 0)), cache_spec, cache_spec],
            out_specs=(cache_spec, cache_spec, q_spec),
        ),
        compiler_params=pltpu.CompilerParams(dimension_semantics=("arbitrary",), vmem_limit_bytes=66_000_000),
        cost_estimate=pl.CostEstimate(
            flops=10**10, bytes_accessed=8 * k_cache.size, transcendentals=seqs * heads * n_pos),
    )(lens, q, kv, k_cache, v_cache)


def output_kernel(
    n_ff, n_o, o_in, keep, recv_e, recv_l, hidden, w_o, w_down, out,
    acts, wbuf, acc, keep_v, recv_v, h_v, y_src, y_dst,
    w_sem, keep_sem, recv_sem, h_sem, oo_sems, on_send, on_recv, far_send, far_recv, near_send, near_recv, y_sems,
):
    xi = lax.axis_index("x")
    yj = lax.axis_index("yz")
    core = lax.rem(xi, 2)
    mate = xi + 1 - 2 * core
    across = lax.rem(xi + 2, 4)
    other_y = 1 - yj
    n_m = n_ff // GROUP
    n_g = n_m + n_o // GROUP
    n_early = EARLY // GROUP
    depth = GROUP * W
    d_out = w_down.shape[2]
    half = d_out // 2

    barrier = pltpu.get_barrier_semaphore()
    for x_, y_ in ((mate, yj), (across, yj), (xi, other_y)):
        pl.semaphore_signal(barrier, inc=1, **dev(x=x_, yz=y_))

    def keep_copy(g):
        return pltpu.make_async_copy(
            keep.at[pl.ds(GROUP * g, GROUP)], keep_v.at[pl.ds(GROUP * g, GROUP)], keep_sem.at[g])

    def recv_copy(g):
        src = recv_e.at[pl.ds(GROUP * g, GROUP)] if g < n_early else recv_l.at[pl.ds(GROUP * (g - n_early), GROUP)]
        return pltpu.make_async_copy(src, recv_v.at[pl.ds(GROUP * g, GROUP)], recv_sem.at[g])

    keep_copy(0).start()
    recv_copy(0).start()

    def rows_of(p, owner):
        off, size = PARTS[p]
        return pl.ds(pl.multiple_of(4 * off + owner * size, 16), size)

    def block(p, g, owner):
        return acts.at[pl.ds(GROUP * g, GROUP), rows_of(p, owner)]

    def o_rows(s):
        row = (1 - yj) * (32 * xi + 16 * s) + yj * (128 + 64 * s + 16 * xi)
        return acts.at[pl.ds(n_ff, n_o), pl.ds(pl.multiple_of(row, 16), 16)]

    def o_own(s):
        return pltpu.make_async_copy(o_in.at[yj, :, pl.ds(16 * s, 16)], o_rows(s), oo_sems.at[s])

    def o_copy(s):
        return pltpu.make_async_remote_copy(
            src_ref=o_in.at[other_y, :, pl.ds(16 * s, 16)], dst_ref=o_rows(s), send_sem=on_send.at[s],
            recv_sem=on_recv.at[s], **dev(x=xi, yz=other_y))

    h_load = pltpu.make_async_copy(hidden, h_v, h_sem)

    def load_weights(g):
        slot = lax.rem(g, NBUF3)

        @pl.when(g < n_m)
        def _():
            pltpu.make_async_copy(
                w_down.at[0, pl.ds(pl.multiple_of(g * depth, W), depth)], wbuf.at[slot], w_sem.at[slot]).start()

        @pl.when(g >= n_m)
        def _():
            pltpu.make_async_copy(
                w_o.at[0, pl.ds(pl.multiple_of((g - n_m) * depth, W), depth)], wbuf.at[slot], w_sem.at[slot]).start()

    def far_copy(p, g):
        return pltpu.make_async_remote_copy(
            src_ref=block(p, g, xi), dst_ref=block(p, g, xi), send_sem=far_send.at[p, g], recv_sem=far_recv.at[p, g],
            **dev(x=across, yz=yj))

    def near_copy(p, g, which):
        rows = block(p, g, xi if which == 0 else across)
        return pltpu.make_async_remote_copy(
            src_ref=rows, dst_ref=rows, send_sem=near_send.at[p, g, which], recv_sem=near_recv.at[p, g, which],
            **dev(x=mate, yz=yj))

    def give(p, g):
        far_copy(p, g).start()
        near_copy(p, g, 0).start()

    def give_m(p, g):
        off, size = PARTS[p]
        for k in range(GROUP):
            t = GROUP * g + k
            z = keep_v[t, off:off + size].astype(F32) + recv_v[t, off:off + size].astype(F32)
            acts[t, rows_of(p, xi)] = silu_mul(z[:, :W], z[:, W:])
        give(p, g)

    pl.semaphore_wait(barrier, 3)
    for g in range(n_m):
        keep_copy(g).wait()
        recv_copy(g).wait()
        give_m(0, g)
        if g == 0:
            for s in range(2):
                o_copy(s).start()
                o_own(s).start()
            for k in range(1, n_m):
                keep_copy(k).start()
                recv_copy(k).start()
    for s in range(NBUF3):
        load_weights(jnp.int32(s))
    h_load.start()
    acc[...] = jnp.zeros_like(acc)
    for s in range(2):
        o_own(s).wait()
        o_copy(s).wait_recv()

    def chunk(p, k):
        return k if p % 2 == 0 else n_g - 1 - k

    for g in range(n_m, n_g):
        give(0, g)
    for p in range(1, len(PARTS)):
        @pl.loop(0, n_g)
        def _(k):
            g = chunk(p, k)

            @pl.when(g < n_m)
            def _():
                give_m(p, g)

            @pl.when(g >= n_m)
            def _():
                give(p, g)

    def forward(p, k):
        g = chunk(p, k)
        far_copy(p, g).wait_recv()
        near_copy(p, g, 1).start()

    def multiply(p, k):
        g = chunk(p, k)
        slot = lax.rem(g, NBUF3)

        @pl.when(k >= (0 if p == 0 else NBUF3))
        def _():
            pltpu.make_async_copy(w_down.at[0, pl.ds(0, depth)], wbuf.at[slot], w_sem.at[slot]).wait()

        near_copy(p, g, 0).wait_recv()
        near_copy(p, g, 1).wait_recv()
        off, size = PARTS[p]
        rows = slice(4 * off, 4 * (off + size))
        for n in range(d_out // W):
            cols = slice(n * W, (n + 1) * W)
            total = acc[rows, cols]
            for j in range(GROUP):
                total += jnp.dot(
                    acts[GROUP * g + j, rows], wbuf[slot, j * W:(j + 1) * W, cols], preferred_element_type=F32)
            acc[rows, cols] = total

        @pl.when(k + NBUF3 < n_g)
        def _():
            load_weights(chunk(p, k + NBUF3))

    def cols_of(j):
        return pl.ds(pl.multiple_of(j * half, 128), half)

    def y_copy(p):
        rows = slice(4 * PARTS[p][0], 4 * sum(PARTS[p]))
        return pltpu.make_async_remote_copy(
            src_ref=y_src.at[rows], dst_ref=y_dst.at[rows], send_sem=y_sems.at[p, 0], recv_sem=y_sems.at[p, 1],
            **dev(x=xi, yz=other_y))

    def exchange(p):
        rows = slice(4 * PARTS[p][0], 4 * sum(PARTS[p]))
        y_src[rows] = acc[rows, cols_of(other_y)].astype(BF16)
        y_copy(p).start()

    def finalize(p):
        off, size = PARTS[p]
        rows = slice(4 * off, 4 * (off + size))
        y_copy(p).wait_recv()
        total = (acc[rows, cols_of(yj)] + y_dst[rows].astype(F32)).reshape(4, size, half)
        out[:, off:off + size] = (h_v[:, off:off + size].astype(F32) + total).astype(BF16)

    for p in range(len(PARTS)):
        forward(p, jnp.int32(0))
        if p > 0:
            multiply(p - 1, jnp.int32(n_g - 1))
            exchange(p - 1)
        if p == 1:
            h_load.wait()

        @pl.loop(1, n_g)
        def _(k):
            forward(p, k)
            multiply(p, k - 1)

        if p > 0:
            finalize(p - 1)

    last = len(PARTS) - 1
    g = chunk(last, n_g - 1)
    if n_g > NBUF3:
        pltpu.make_async_copy(w_down.at[0, pl.ds(0, depth)], wbuf.at[g % NBUF3], w_sem.at[g % NBUF3]).wait()
    near_copy(last, g, 0).wait_recv()
    near_copy(last, g, 1).wait_recv()
    rows = slice(4 * PARTS[last][0], 4 * sum(PARTS[last]))
    for j in (other_y, yj):
        for n in range(half // 256):
            cols = pl.ds(pl.multiple_of(j * half + n * 256, 256), 256)
            total = acc[rows, cols]
            for k in range(GROUP):
                total += jnp.dot(
                    acts[GROUP * g + k, rows], wbuf[g % NBUF3, k * W:(k + 1) * W, cols], preferred_element_type=F32)
            acc[rows, cols] = total
        if j is other_y:
            exchange(last)
    for s in range(2):
        o_copy(s).wait_send()
    for p in range(len(PARTS)):
        @pl.loop(0, n_g)
        def _(g):
            far_copy(p, g).wait_send()
            near_copy(p, g, 0).wait_send()
            near_copy(p, g, 1).wait_send()

    finalize(last)
    for p in range(len(PARTS)):
        y_copy(p).wait_send()


def finish(o, keep, recv_e, recv_l, hidden, w_o, w_down):
    rows, half = hidden.shape
    n_ff = w_down.shape[1] // W
    n_o = w_o.shape[1] // W
    n_m = n_ff // GROUP
    n_g = n_m + n_o // GROUP
    n_p = len(PARTS)
    d_out = w_down.shape[2]
    dma = pltpu.SemaphoreType.DMA
    any_spec = pl.BlockSpec(memory_space=pl.ANY)
    vmem = pl.BlockSpec(memory_space=pltpu.VMEM)
    flops = 2 * rows * d_out * (w_down.shape[1] + w_o.shape[1])
    out = pl.pallas_call(
        functools.partial(output_kernel, n_ff, n_o),
        name="finish",
        out_shape=jax.ShapeDtypeStruct((4, 64, half), BF16),
        in_specs=[any_spec] * 7,
        out_specs=vmem,
        scratch_shapes=[
            pltpu.VMEM((n_ff + n_o, rows, W), BF16),
            pltpu.VMEM((NBUF3, GROUP * W, d_out), BF16),
            pltpu.VMEM((rows, d_out), F32),
            pltpu.VMEM(keep.shape, BF16),
            pltpu.VMEM(keep.shape, BF16),
            pltpu.VMEM((4, 64, half), BF16),
            pltpu.VMEM((rows, half), BF16),
            pltpu.VMEM((rows, half), BF16),
            dma((NBUF3,)),
            dma((n_m,)),
            dma((n_m,)),
            dma,
            dma((2,)),
            dma((2,)),
            dma((2,)),
            dma((n_p, n_g)),
            dma((n_p, n_g)),
            dma((n_p, n_g, 2)),
            dma((n_p, n_g, 2)),
            dma((n_p, 2)),
        ],
        compiler_params=pltpu.CompilerParams(collective_id=1, has_side_effects=True, vmem_limit_bytes=56_000_000),
        cost_estimate=pl.CostEstimate(flops=flops, bytes_accessed=2 * d_out * (w_down.shape[1] + w_o.shape[1]), transcendentals=0),
    )(o, keep, recv_e, recv_l, hidden.reshape(4, 64, half), w_o, w_down)
    return out.reshape(rows, half)


def solution(mesh):
    x_size = mesh.shape["x"]
    y_size = mesh.shape["yz"]
    row_spec = P("dp", ("x", "yz"))
    tile_in = P(None, "x", "yz")
    tile_out = P(None, "yz", "x")
    cache_spec = P(None, ("dp", "x", "yz"))
    len_spec = P(("dp", "x", "yz"))

    def device_step(hidden, norm_gain, w_q, w_kv, w_gate, w_up, w_o, w_down, k_cache, v_cache, seq_len):
        d_model = hidden.shape[1] * x_size * y_size
        seqs = k_cache.shape[1]
        dim = k_cache.shape[3]
        q_cols = w_q.shape[2]
        heads = q_cols // dim
        q, kv, keep, recv_e, send = project(hidden, norm_gain, w_q, w_kv, w_gate, w_up, d_model)
        recv_l = lax.ppermute(send, "x", [(i, (i + x_size // 2) % x_size) for i in range(x_size)])
        q = q.reshape(y_size, seqs, heads, dim).transpose(1, 0, 2, 3).reshape(seqs, y_size * heads, dim)
        k_new, v_new, o = attend(seq_len, q, kv, k_cache, v_cache)
        o = o.reshape(seqs, y_size, q_cols // W, W).transpose(1, 2, 0, 3)
        hidden_out = finish(o, keep, recv_e, recv_l, hidden, w_o, w_down)
        return hidden_out, k_new, v_new

    return jax.shard_map(
        device_step,
        mesh=mesh,
        in_specs=(row_spec, P(None, "x"), tile_in, tile_in, tile_in, tile_in, tile_out, tile_out, cache_spec, cache_spec, len_spec),
        out_specs=(row_spec, cache_spec, cache_spec),
        check_vma=False,
    )
```

```python
import functools

import jax
import jax.numpy as jnp
from jax import lax
from jax.experimental import pallas as pl
from jax.experimental.pallas import tpu as pltpu
from jax.sharding import PartitionSpec as P

NORM_EPS = 1e-6
W = 512
NBUF1 = 4
NBUF3 = 6
GROUP = 3
PARTS = ((0, 32), (32, 16), (48, 16))
EARLY = 12
SEQ_STEP = 2
HELD = 6
RELEASE = 3
VMEM_LIMIT = 64_000_000
F32 = jnp.float32
BF16 = jnp.bfloat16
LOG2E = 1.4426950408889634
MASKED = -1e30 * LOG2E


def dev(**axes):
    return dict(device_id=axes, device_id_type=pl.DeviceIdType.MESH)


def silu_mul(gate, up):
    gate = gate.astype(BF16).astype(F32)
    up = up.astype(BF16).astype(F32)
    return (jax.nn.silu(gate) * up).astype(BF16)


def project_kernel(
    n_q, n_ff, d_model, hidden, gain_in, wq, wkv, wg, wu,
    q_out, kv_out, keep_out, recv_out, send_out,
    gain, h_own, h_other, u, inv_all, sq_all, wq_buf, wbuf, wkv_buf, part, part_kv, near, near_kv, keep, keep_kv, far_src,
    far_src_kv, far, far_kv, z_rows, z_other,
    wq_sem, w_sem, wkv_sem, h_in, gain_sem, h_sems, sq_send, sq_recv, near_send, near_recv, qn_send, qn_recv, kn_send, kn_recv,
    far_send, far_recv, qf_send, qf_recv, kf_send, kf_recv, y_sems, out_sem, qkv_sem,
):
    xi = lax.axis_index("x")
    yj = lax.axis_index("yz")
    core = lax.rem(xi, 2)
    chip = xi // 2
    mate = xi + 1 - 2 * core
    across = lax.rem(xi + 2, 4)
    other_y = 1 - yj
    me = xi * 2 + yj
    half = hidden.shape[-1]
    n_all = n_q + n_ff
    n_far = n_q + EARLY
    to_mate = dev(x=mate, yz=yj)
    to_across = dev(x=across, yz=yj)

    barrier = pltpu.get_barrier_semaphore()
    for k in range(1, 8):
        peer = lax.rem(me + k, 8)
        pl.semaphore_signal(barrier, inc=1, **dev(x=peer // 2, yz=lax.rem(peer, 2)))
    h_load = pltpu.make_async_copy(hidden, h_own, h_in)
    h_load.start()
    gain_load = pltpu.make_async_copy(gain_in, gain, gain_sem)
    gain_load.start()

    def start_weights(g):
        slot = lax.rem(g, NBUF1)
        cols = pl.ds(pl.multiple_of((g - n_q) * W, W), W)
        pltpu.make_async_copy(wg.at[0, :, cols], wbuf.at[slot, 0], w_sem.at[slot, 0]).start()
        pltpu.make_async_copy(wu.at[0, :, cols], wbuf.at[slot, 1], w_sem.at[slot, 1]).start()

    def wait_weights(slot, k):
        pltpu.make_async_copy(wg.at[0, :, pl.ds(0, W)], wbuf.at[slot, k], w_sem.at[slot, k]).wait()

    def wq_copy(g):
        return pltpu.make_async_copy(wq.at[0, :, g * 2 * W:(g + 1) * 2 * W], wq_buf.at[g], wq_sem.at[g])

    h_load.wait()
    gain_load.wait()
    for g in range(n_q):
        wq_copy(g).start()
    kv_copy = pltpu.make_async_copy(wkv.at[0], wkv_buf, wkv_sem)
    kv_copy.start()

    folded = jnp.zeros((256, 128), F32)
    for k in range(half // 128):
        block = h_own[:, :, :, k * 128:(k + 1) * 128].reshape(256, 128).astype(F32)
        folded += block * block
    sq_all[me] = jnp.broadcast_to(jnp.sum(jnp.transpose(folded), axis=0, keepdims=True), (8, 256))
    pl.semaphore_wait(barrier, 7)

    def sq_copy(peer, src):
        return pltpu.make_async_remote_copy(
            src_ref=sq_all.at[src], dst_ref=sq_all.at[src], send_sem=sq_send.at[peer], recv_sem=sq_recv.at[src],
            **dev(x=peer // 2, yz=lax.rem(peer, 2)))

    def side_of(step):
        return 1 - chip if step < 2 else chip

    def piece(step):
        return pl.ds(32 * step, 32) if step < 2 else pl.ds(0, 64)

    def h_copy(step):
        block = (side_of(step), slice(None), piece(step))
        return pltpu.make_async_remote_copy(
            src_ref=h_own.at[block], dst_ref=h_other.at[block],
            send_sem=h_sems.at[step, 0], recv_sem=h_sems.at[step, 1], **dev(x=xi, yz=other_y))

    for k in range(1, 8):
        sq_copy(lax.rem(me + k, 8), me).start()
    for step in range(3):
        h_copy(step).start()
    for k in range(1, 8):
        peer = lax.rem(me + k, 8)
        sq_copy(peer, peer).wait_recv()
    total = jnp.sum(sq_all[...], axis=0)
    inv = lax.rsqrt(total / d_model + NORM_EPS)
    inv_all[...] = jnp.transpose(jnp.concatenate([inv] * 16, axis=0)).reshape(inv_all.shape)

    def normalize(values, step, which):
        cols = pl.ds(pl.multiple_of(which * half, 128), half)
        side, rows = side_of(step), piece(step)
        u[side, :, rows, cols] = (
            values[side, :, rows].astype(F32) * inv_all[side, :, rows, :1] * gain[:, cols].astype(F32)).astype(BF16)

    def near_copy(g):
        return pltpu.make_async_remote_copy(
            src_ref=part.at[g, :, 1 - core], dst_ref=near.at[g], send_sem=near_send.at[g],
            recv_sem=near_recv.at[g], **to_mate)

    def near_copy_q(g, step):
        side, rows = side_of(step), piece(step)
        return pltpu.make_async_remote_copy(
            src_ref=part.at[g, side, 1 - core, rows], dst_ref=near.at[g, side, rows],
            send_sem=qn_send.at[g, step], recv_sem=qn_recv.at[g, step], **to_mate)

    def near_copy_kv(step):
        side, rows = side_of(step), piece(step)
        return pltpu.make_async_remote_copy(
            src_ref=part_kv.at[side, 1 - core, rows], dst_ref=near_kv.at[side, rows],
            send_sem=kn_send.at[step], recv_sem=kn_recv.at[step], **to_mate)

    def far_copy(g):
        return pltpu.make_async_remote_copy(
            src_ref=far_src.at[g], dst_ref=recv_out.at[g - n_q], send_sem=far_send.at[g - n_q],
            recv_sem=far_recv.at[g - n_q], **to_across)

    def far_copy_q(g, step):
        rows = piece(step)
        return pltpu.make_async_remote_copy(
            src_ref=far_src.at[g, rows], dst_ref=far.at[g, rows], send_sem=qf_send.at[g, step],
            recv_sem=qf_recv.at[g, step], **to_across)

    def far_copy_kv(step):
        rows = piece(step)
        return pltpu.make_async_remote_copy(
            src_ref=far_src_kv.at[rows], dst_ref=far_kv.at[rows], send_sem=kf_send.at[step], recv_sem=kf_recv.at[step],
            **to_across)

    def keep_copy(g):
        return pltpu.make_async_copy(keep.at[g], keep_out.at[g - n_q], out_sem.at[g - n_q, 0])

    def send_copy(g):
        k = g - n_q
        return pltpu.make_async_copy(far_src.at[g], send_out.at[k - EARLY], out_sem.at[k, 1])

    def add(a, b):
        return (a.astype(F32) + b.astype(F32)).astype(BF16)

    def multiply(g):
        slot = lax.rem(g, NBUF1)
        for k in range(2):
            wait_weights(slot, k)
            res = jnp.dot(u[...].reshape(256, u.shape[-1]), wbuf[slot, k], preferred_element_type=F32).astype(BF16)
            part[g, :, :, :, k * W:(k + 1) * W] = res.reshape(2, 2, 64, W)
        near_copy(g).start()

        @pl.when(g + NBUF1 < n_all)
        def _():
            start_weights(g + NBUF1)

    def reduce_near(g):
        near_copy(g).wait_recv()
        far_src[g] = add(part[g, 1 - chip, core], near[g, 1 - chip])

        @pl.when((g < n_far) & ((core == 1) | (g < n_far - HELD)))
        def _():
            far_copy(g).start()

        @pl.when(g >= n_far)
        def _():
            send_copy(g).start()

        keep[g] = add(part[g, chip, core], near[g, chip])
        keep_copy(g).start()

    def multiply_q(step):
        side, rows = side_of(step), piece(step)
        lhs = u[side, :, rows].reshape(2 * rows.size, u.shape[-1])
        for g in range(n_q):
            if step == 0:
                wq_copy(g).wait()
            for k in range(2):
                res = jnp.dot(lhs, wq_buf[g, :, k * W:(k + 1) * W], preferred_element_type=F32).astype(BF16)
                part[g, side, :, rows, k * W:(k + 1) * W] = res.reshape(2, rows.size, W)
            near_copy_q(g, step).start()
            if step == 0 and g >= 1:
                reduce_q(0, g - 1)
        if step == 0:
            kv_copy.wait()
        res = jnp.dot(lhs, wkv_buf[...], preferred_element_type=F32).astype(BF16)
        part_kv[side, :, rows] = res.reshape(2, rows.size, res.shape[1])
        near_copy_kv(step).start()

    def reduce_q(step, g):
        side, rows = side_of(step), piece(step)
        near_copy_q(g, step).wait_recv()
        total_q = add(part[g, side, core, rows], near[g, side, rows])
        if step < 2:
            far_src[g, rows] = total_q
            far_copy_q(g, step).start()
        else:
            keep[g] = total_q

    def reduce_kv(step):
        side, rows = side_of(step), piece(step)
        near_copy_kv(step).wait_recv()
        total_kv = add(part_kv[side, core, rows], near_kv[side, rows])
        if step < 2:
            far_src_kv[rows] = total_kv
            far_copy_kv(step).start()
        else:
            keep_kv[...] = total_kv

    for step in range(3):
        normalize(h_own, step, yj)
        h_copy(step).wait_recv()
        normalize(h_other, step, other_y)
        if step < 2:
            multiply_q(step)
            for g in range(n_q - 1 if step == 0 else 0, n_q):
                reduce_q(step, g)
            reduce_kv(step)
        if step == 0:
            for g in range(n_q, n_q + NBUF1):
                start_weights(jnp.int32(g))

    @pl.loop(n_q, n_far)
    def _(g):
        multiply(g)

        @pl.when(g >= n_q + 1)
        def _():
            reduce_near(g - 1)

    q_cols = n_q * 2 * W
    multiply_q(2)
    for g in range(n_q):
        reduce_q(2, g)
        for step in range(2):
            far_copy_q(g, step).wait_recv()
        z_rows[:, :, g * 2 * W:(g + 1) * 2 * W] = add(keep[g], far[g]).reshape(2, 32, 2 * W)
    reduce_kv(2)
    for step in range(2):
        far_copy_kv(step).wait_recv()
    z_kv = add(keep_kv[...], far_kv[...])
    z_rows[:, :, q_cols:] = z_kv.reshape(2, 32, z_kv.shape[1])
    y_copy = pltpu.make_async_remote_copy(
        src_ref=z_rows.at[other_y], dst_ref=z_other, send_sem=y_sems.at[0], recv_sem=y_sems.at[1],
        **dev(x=xi, yz=other_y))
    y_copy.start()
    def qkv_copies(src, which):
        return (
            pltpu.make_async_copy(src.at[:, :q_cols], q_out.at[which], qkv_sem.at[0, 0 if src is z_other else 1]),
            pltpu.make_async_copy(src.at[:, q_cols:], kv_out.at[which], qkv_sem.at[1, 0 if src is z_other else 1]),
        )

    qkv_own = qkv_copies(z_rows.at[yj], yj)
    for copy in qkv_own:
        copy.start()

    @pl.loop(n_far, n_all)
    def _(g):
        multiply(g)
        reduce_near(g - 1)

        @pl.when((g == n_far + RELEASE) & (core == 0))
        def _():
            @pl.loop(n_far - HELD, n_far)
            def _(k):
                far_copy(k).start()

    reduce_near(jnp.int32(n_all - 1))
    y_copy.wait_recv()
    qkv_other = qkv_copies(z_other, other_y)
    for copy in qkv_other:
        copy.start()

    for step in range(3):
        h_copy(step).wait_send()
        near_copy_kv(step).wait_send()
        for g in range(n_q):
            near_copy_q(g, step).wait_send()
    for step in range(2):
        far_copy_kv(step).wait_send()
        for g in range(n_q):
            far_copy_q(g, step).wait_send()
    for k in range(1, 8):
        sq_copy(lax.rem(me + k, 8), me).wait_send()
    y_copy.wait_send()

    @pl.loop(n_q, n_all)
    def _(g):
        near_copy(g).wait_send()
        keep_copy(g).wait()

    @pl.loop(n_far, n_all)
    def _(g):
        send_copy(g).wait()

    for copy in qkv_own + qkv_other:
        copy.wait()

    @pl.loop(n_q, n_far)
    def _(g):
        far_copy(g).wait_send()
        far_copy(g).wait_recv()


def project(hidden, gain, w_q, w_kv, w_gate, w_up, d_model):
    rows, half = hidden.shape
    feats = w_q.shape[1]
    kv = w_kv.shape[2]
    n_q = w_q.shape[2] // (2 * W)
    n_ff = w_gate.shape[2] // W
    n_all = n_q + n_ff
    late = n_ff - EARLY
    dma = pltpu.SemaphoreType.DMA
    any_spec = pl.BlockSpec(memory_space=pl.ANY)
    cols = w_q.shape[2] + kv
    flops = 2 * rows * feats * (w_q.shape[2] + kv + 2 * w_gate.shape[2])
    return pl.pallas_call(
        functools.partial(project_kernel, n_q, n_ff, d_model),
        name="project",
        out_shape=(
            jax.ShapeDtypeStruct((2, 32, cols - kv), BF16),
            jax.ShapeDtypeStruct((2, 32, kv), BF16),
            jax.ShapeDtypeStruct((n_ff, 64, 2 * W), BF16),
            jax.ShapeDtypeStruct((EARLY, 64, 2 * W), BF16),
            jax.ShapeDtypeStruct((late, 64, 2 * W), BF16),
        ),
        in_specs=[any_spec] * 6,
        out_specs=(any_spec,) * 5,
        scratch_shapes=[
            pltpu.VMEM((1, feats), BF16),
            pltpu.VMEM((2, 2, 64, half), BF16),
            pltpu.VMEM((2, 2, 64, half), BF16),
            pltpu.VMEM((2, 2, 64, feats), BF16),
            pltpu.VMEM((2, 2, 64, 128), F32),
            pltpu.VMEM((8, 8, rows), F32),
            pltpu.VMEM((n_q, feats, 2 * W), BF16),
            pltpu.VMEM((NBUF1, 2, feats, W), BF16),
            pltpu.VMEM((feats, kv), BF16),
            pltpu.VMEM((n_all, 2, 2, 64, 2 * W), BF16),
            pltpu.VMEM((2, 2, 64, kv), BF16),
            pltpu.VMEM((n_all, 2, 64, 2 * W), BF16),
            pltpu.VMEM((2, 64, kv), BF16),
            pltpu.VMEM((n_all, 64, 2 * W), BF16),
            pltpu.VMEM((64, kv), BF16),
            pltpu.VMEM((n_all, 64, 2 * W), BF16),
            pltpu.VMEM((64, kv), BF16),
            pltpu.VMEM((n_q, 64, 2 * W), BF16),
            pltpu.VMEM((64, kv), BF16),
            pltpu.VMEM((2, 32, cols), BF16),
            pltpu.VMEM((32, cols), BF16),
            dma((n_q,)),
            dma((NBUF1, 2)),
            dma,
            dma,
            dma,
            dma((3, 2)),
            dma((8,)),
            dma((8,)),
            dma((n_all,)),
            dma((n_all,)),
            dma((n_q, 3)),
            dma((n_q, 3)),
            dma((3,)),
            dma((3,)),
            dma((EARLY,)),
            dma((EARLY,)),
            dma((n_q, 2)),
            dma((n_q, 2)),
            dma((2,)),
            dma((2,)),
            dma((2,)),
            dma((n_ff, 2)),
            dma((2, 2)),
        ],
        compiler_params=pltpu.CompilerParams(collective_id=0, has_side_effects=True, vmem_limit_bytes=VMEM_LIMIT),
        cost_estimate=pl.CostEstimate(flops=flops, bytes_accessed=feats * (flops // (rows * feats)), transcendentals=0),
    )(hidden.reshape(2, 2, 64, half), gain, w_q, w_kv, w_gate, w_up)


def attend_kernel(lens, q_ref, kv_ref, k_ref, v_ref, k_out, v_out, o_ref, fresh):
    step = pl.program_id(0)

    @pl.when(step == 0)
    def _():
        fresh[...] = kv_ref[...].astype(F32)

    n_pos = k_ref.shape[2]
    scale = q_ref.shape[2] ** -0.5 * LOG2E
    for s in range(SEQ_STEP):
        length = lens[step * SEQ_STEP + s]
        base = pl.multiple_of((length // 16) * 16, 16)
        k_out[0, s] = k_ref[0, s]
        v_out[0, s] = v_ref[0, s]
        hit = lax.broadcasted_iota(jnp.int32, (16, k_ref.shape[3]), 0) == length - base
        for src, dst, which in ((k_ref, k_out, 0), (v_ref, v_out, 1)):
            old = src[0, s, pl.ds(base, 16), :].astype(F32)
            new = fresh[which, pl.ds(step * SEQ_STEP + s, 1), :]
            dst[0, s, pl.ds(base, 16), :] = jnp.where(hit, new, old).astype(BF16)
        scores = lax.dot_general(q_ref[s], k_out[0, s], (((1,), (1,)), ((), ())), preferred_element_type=F32) * scale
        visible = lax.broadcasted_iota(jnp.int32, scores.shape, 1) <= length
        scores = jnp.where(visible, scores, MASKED)
        weights = jnp.exp2(scores - jnp.max(scores, axis=1, keepdims=True))
        probs = (weights * (1.0 / jnp.sum(weights, axis=1, keepdims=True))).astype(BF16)
        o_ref[s] = jnp.dot(probs, v_out[0, s], preferred_element_type=F32).astype(BF16)


def attend(lens, q, kv, k_cache, v_cache):
    seqs, heads, dim = q.shape
    n_pos = k_cache.shape[2]
    cache_spec = pl.BlockSpec((1, SEQ_STEP, n_pos, dim), lambda b, lens: (0, b, 0, 0))
    q_spec = pl.BlockSpec((SEQ_STEP, heads, dim), lambda b, lens: (b, 0, 0))
    return pl.pallas_call(
        attend_kernel,
        name="attend",
        out_shape=(
            jax.ShapeDtypeStruct(k_cache.shape, BF16),
            jax.ShapeDtypeStruct(v_cache.shape, BF16),
            jax.ShapeDtypeStruct(q.shape, BF16),
        ),
        grid_spec=pltpu.PrefetchScalarGridSpec(
            num_scalar_prefetch=1,
            grid=(seqs // SEQ_STEP,),
            in_specs=[q_spec, pl.BlockSpec((2, seqs, dim), lambda b, lens: (0, 0, 0)), cache_spec, cache_spec],
            out_specs=(cache_spec, cache_spec, q_spec),
            scratch_shapes=[pltpu.VMEM((2, seqs, dim), F32)],
        ),
        compiler_params=pltpu.CompilerParams(dimension_semantics=("arbitrary",), vmem_limit_bytes=66_000_000),
        cost_estimate=pl.CostEstimate(
            flops=10**10, bytes_accessed=8 * k_cache.size, transcendentals=seqs * heads * n_pos),
    )(lens, q, kv, k_cache, v_cache)


def output_kernel(
    n_ff, n_o, o_in, keep, recv_e, recv_l, hidden, w_o, w_down, out,
    acts, wbuf, acc, keep_v, recv_v, h_v, y_src, y_dst,
    w_sem, keep_sem, recv_sem, h_sem, oo_sems, on_send, on_recv, far_send, far_recv, near_send, near_recv, y_sems,
):
    xi = lax.axis_index("x")
    yj = lax.axis_index("yz")
    core = lax.rem(xi, 2)
    mate = xi + 1 - 2 * core
    across = lax.rem(xi + 2, 4)
    other_y = 1 - yj
    n_m = n_ff // GROUP
    n_g = n_m + n_o // GROUP
    n_early = EARLY // GROUP
    depth = GROUP * W
    d_out = w_down.shape[2]
    half = d_out // 2

    barrier = pltpu.get_barrier_semaphore()
    for x_, y_ in ((mate, yj), (across, yj), (xi, other_y)):
        pl.semaphore_signal(barrier, inc=1, **dev(x=x_, yz=y_))

    def keep_copy(g):
        return pltpu.make_async_copy(
            keep.at[pl.ds(GROUP * g, GROUP)], keep_v.at[pl.ds(GROUP * g, GROUP)], keep_sem.at[g])

    def recv_copy(g):
        src = recv_e.at[pl.ds(GROUP * g, GROUP)] if g < n_early else recv_l.at[pl.ds(GROUP * (g - n_early), GROUP)]
        return pltpu.make_async_copy(src, recv_v.at[pl.ds(GROUP * g, GROUP)], recv_sem.at[g])

    keep_copy(0).start()
    recv_copy(0).start()

    def rows_of(p, owner):
        off, size = PARTS[p]
        return pl.ds(pl.multiple_of(4 * off + owner * size, 16), size)

    def block(p, g, owner):
        return acts.at[pl.ds(GROUP * g, GROUP), rows_of(p, owner)]

    def o_rows(s):
        row = (1 - yj) * (32 * xi + 16 * s) + yj * (128 + 64 * s + 16 * xi)
        return acts.at[pl.ds(n_ff, n_o), pl.ds(pl.multiple_of(row, 16), 16)]

    def o_own(s):
        return pltpu.make_async_copy(o_in.at[yj, :, pl.ds(16 * s, 16)], o_rows(s), oo_sems.at[s])

    def o_copy(s):
        return pltpu.make_async_remote_copy(
            src_ref=o_in.at[other_y, :, pl.ds(16 * s, 16)], dst_ref=o_rows(s), send_sem=on_send.at[s],
            recv_sem=on_recv.at[s], **dev(x=xi, yz=other_y))

    h_load = pltpu.make_async_copy(hidden, h_v, h_sem)

    def load_weights(g):
        slot = lax.rem(g, NBUF3)

        @pl.when(g < n_m)
        def _():
            pltpu.make_async_copy(
                w_down.at[0, pl.ds(pl.multiple_of(g * depth, W), depth)], wbuf.at[slot], w_sem.at[slot]).start()

        @pl.when(g >= n_m)
        def _():
            pltpu.make_async_copy(
                w_o.at[0, pl.ds(pl.multiple_of((g - n_m) * depth, W), depth)], wbuf.at[slot], w_sem.at[slot]).start()

    def far_copy(p, g):
        return pltpu.make_async_remote_copy(
            src_ref=block(p, g, xi), dst_ref=block(p, g, xi), send_sem=far_send.at[p, g], recv_sem=far_recv.at[p, g],
            **dev(x=across, yz=yj))

    def near_copy(p, g, which):
        rows = block(p, g, xi if which == 0 else across)
        return pltpu.make_async_remote_copy(
            src_ref=rows, dst_ref=rows, send_sem=near_send.at[p, g, which], recv_sem=near_recv.at[p, g, which],
            **dev(x=mate, yz=yj))

    def give(p, g):
        far_copy(p, g).start()
        near_copy(p, g, 0).start()

    def give_m(p, g):
        off, size = PARTS[p]
        for k in range(GROUP):
            t = GROUP * g + k
            z = keep_v[t, off:off + size].astype(F32) + recv_v[t, off:off + size].astype(F32)
            acts[t, rows_of(p, xi)] = silu_mul(z[:, :W], z[:, W:])
        give(p, g)

    pl.semaphore_wait(barrier, 3)
    for g in range(n_m):
        keep_copy(g).wait()
        recv_copy(g).wait()
        give_m(0, g)
        if g == 0:
            for s in range(2):
                o_copy(s).start()
                o_own(s).start()
            for k in range(1, n_m):
                keep_copy(k).start()
                recv_copy(k).start()
    for s in range(NBUF3):
        load_weights(jnp.int32(s))
    h_load.start()
    acc[...] = jnp.zeros_like(acc)
    for s in range(2):
        o_own(s).wait()
        o_copy(s).wait_recv()

    def chunk(p, k):
        return k if p % 2 == 0 else n_g - 1 - k

    for g in range(n_m, n_g):
        give(0, g)
    for p in range(1, len(PARTS)):
        @pl.loop(0, n_g)
        def _(k):
            g = chunk(p, k)

            @pl.when(g < n_m)
            def _():
                give_m(p, g)

            @pl.when(g >= n_m)
            def _():
                give(p, g)

    def forward(p, k):
        g = chunk(p, k)
        far_copy(p, g).wait_recv()
        near_copy(p, g, 1).start()

    def multiply(p, k):
        g = chunk(p, k)
        slot = lax.rem(g, NBUF3)

        @pl.when(k >= (0 if p == 0 else NBUF3))
        def _():
            pltpu.make_async_copy(w_down.at[0, pl.ds(0, depth)], wbuf.at[slot], w_sem.at[slot]).wait()

        near_copy(p, g, 0).wait_recv()
        near_copy(p, g, 1).wait_recv()
        off, size = PARTS[p]
        rows = slice(4 * off, 4 * (off + size))
        for n in range(d_out // W):
            cols = slice(n * W, (n + 1) * W)
            total = acc[rows, cols]
            for j in range(GROUP):
                total += jnp.dot(
                    acts[GROUP * g + j, rows], wbuf[slot, j * W:(j + 1) * W, cols], preferred_element_type=F32)
            acc[rows, cols] = total

        @pl.when(k + NBUF3 < n_g)
        def _():
            load_weights(chunk(p, k + NBUF3))

    def cols_of(j):
        return pl.ds(pl.multiple_of(j * half, 128), half)

    def y_copy(p):
        rows = slice(4 * PARTS[p][0], 4 * sum(PARTS[p]))
        return pltpu.make_async_remote_copy(
            src_ref=y_src.at[rows], dst_ref=y_dst.at[rows], send_sem=y_sems.at[p, 0], recv_sem=y_sems.at[p, 1],
            **dev(x=xi, yz=other_y))

    def exchange(p):
        rows = slice(4 * PARTS[p][0], 4 * sum(PARTS[p]))
        y_src[rows] = acc[rows, cols_of(other_y)].astype(BF16)
        y_copy(p).start()

    def finalize(p):
        off, size = PARTS[p]
        rows = slice(4 * off, 4 * (off + size))
        y_copy(p).wait_recv()
        total = (acc[rows, cols_of(yj)] + y_dst[rows].astype(F32)).reshape(4, size, half)
        out[:, off:off + size] = (h_v[:, off:off + size].astype(F32) + total).astype(BF16)

    for p in range(len(PARTS)):
        forward(p, jnp.int32(0))
        if p > 0:
            multiply(p - 1, jnp.int32(n_g - 1))
            exchange(p - 1)
        if p == 1:
            h_load.wait()

        @pl.loop(1, n_g)
        def _(k):
            forward(p, k)
            multiply(p, k - 1)

        if p > 0:
            finalize(p - 1)

    last = len(PARTS) - 1
    g = chunk(last, n_g - 1)
    if n_g > NBUF3:
        pltpu.make_async_copy(w_down.at[0, pl.ds(0, depth)], wbuf.at[g % NBUF3], w_sem.at[g % NBUF3]).wait()
    near_copy(last, g, 0).wait_recv()
    near_copy(last, g, 1).wait_recv()
    rows = slice(4 * PARTS[last][0], 4 * sum(PARTS[last]))
    for j in (other_y, yj):
        for n in range(half // 256):
            cols = pl.ds(pl.multiple_of(j * half + n * 256, 256), 256)
            total = acc[rows, cols]
            for k in range(GROUP):
                total += jnp.dot(
                    acts[GROUP * g + k, rows], wbuf[g % NBUF3, k * W:(k + 1) * W, cols], preferred_element_type=F32)
            acc[rows, cols] = total
        if j is other_y:
            exchange(last)
    for s in range(2):
        o_copy(s).wait_send()
    for p in range(len(PARTS)):
        @pl.loop(0, n_g)
        def _(g):
            far_copy(p, g).wait_send()
            near_copy(p, g, 0).wait_send()
            near_copy(p, g, 1).wait_send()

    finalize(last)
    for p in range(len(PARTS)):
        y_copy(p).wait_send()


def finish(o, keep, recv_e, recv_l, hidden, w_o, w_down):
    rows, half = hidden.shape
    n_ff = w_down.shape[1] // W
    n_o = w_o.shape[1] // W
    n_m = n_ff // GROUP
    n_g = n_m + n_o // GROUP
    n_p = len(PARTS)
    d_out = w_down.shape[2]
    dma = pltpu.SemaphoreType.DMA
    any_spec = pl.BlockSpec(memory_space=pl.ANY)
    vmem = pl.BlockSpec(memory_space=pltpu.VMEM)
    flops = 2 * rows * d_out * (w_down.shape[1] + w_o.shape[1])
    out = pl.pallas_call(
        functools.partial(output_kernel, n_ff, n_o),
        name="finish",
        out_shape=jax.ShapeDtypeStruct((4, 64, half), BF16),
        in_specs=[any_spec] * 7,
        out_specs=vmem,
        scratch_shapes=[
            pltpu.VMEM((n_ff + n_o, rows, W), BF16),
            pltpu.VMEM((NBUF3, GROUP * W, d_out), BF16),
            pltpu.VMEM((rows, d_out), F32),
            pltpu.VMEM(keep.shape, BF16),
            pltpu.VMEM(keep.shape, BF16),
            pltpu.VMEM((4, 64, half), BF16),
            pltpu.VMEM((rows, half), BF16),
            pltpu.VMEM((rows, half), BF16),
            dma((NBUF3,)),
            dma((n_m,)),
            dma((n_m,)),
            dma,
            dma((2,)),
            dma((2,)),
            dma((2,)),
            dma((n_p, n_g)),
            dma((n_p, n_g)),
            dma((n_p, n_g, 2)),
            dma((n_p, n_g, 2)),
            dma((n_p, 2)),
        ],
        compiler_params=pltpu.CompilerParams(collective_id=1, has_side_effects=True, vmem_limit_bytes=56_000_000),
        cost_estimate=pl.CostEstimate(flops=flops, bytes_accessed=2 * d_out * (w_down.shape[1] + w_o.shape[1]), transcendentals=0),
    )(o, keep, recv_e, recv_l, hidden.reshape(4, 64, half), w_o, w_down)
    return out.reshape(rows, half)


def solution(mesh):
    x_size = mesh.shape["x"]
    y_size = mesh.shape["yz"]
    row_spec = P("dp", ("x", "yz"))
    tile_in = P(None, "x", "yz")
    tile_out = P(None, "yz", "x")
    cache_spec = P(None, ("dp", "x", "yz"))
    len_spec = P(("dp", "x", "yz"))

    def device_step(hidden, norm_gain, w_q, w_kv, w_gate, w_up, w_o, w_down, k_cache, v_cache, seq_len):
        d_model = hidden.shape[1] * x_size * y_size
        seqs = k_cache.shape[1]
        dim = k_cache.shape[3]
        q_cols = w_q.shape[2]
        heads = q_cols // dim
        q, kv, keep, recv_e, send = project(hidden, norm_gain, w_q, w_kv, w_gate, w_up, d_model)
        recv_l = lax.ppermute(send, "x", [(i, (i + x_size // 2) % x_size) for i in range(x_size)])
        q = q.reshape(y_size, seqs, heads, dim).transpose(1, 0, 2, 3).reshape(seqs, y_size * heads, dim)
        k_new, v_new, o = attend(seq_len, q, kv, k_cache, v_cache)
        o = o.reshape(seqs, y_size, q_cols // W, W).transpose(1, 2, 0, 3)
        hidden_out = finish(o, keep, recv_e, recv_l, hidden, w_o, w_down)
        return hidden_out, k_new, v_new

    return jax.shard_map(
        device_step,
        mesh=mesh,
        in_specs=(row_spec, P(None, "x"), tile_in, tile_in, tile_in, tile_in, tile_out, tile_out, cache_spec, cache_spec, len_spec),
        out_specs=(row_spec, cache_spec, cache_spec),
        check_vma=False,
    )
```

```python
import functools

import jax
import jax.numpy as jnp
from jax import lax
from jax.experimental import pallas as pl
from jax.experimental.pallas import tpu as pltpu
from jax.sharding import PartitionSpec as P

NORM_EPS = 1e-6
W = 512
NBUF1 = 4
NBUF3 = 6
GROUP = 3
PARTS = ((0, 32), (32, 16), (48, 16))
EARLY = 12
SEQ_STEP = 2
HELD = 6
RELEASE = 3
VMEM_LIMIT = 64_000_000
F32 = jnp.float32
BF16 = jnp.bfloat16
LOG2E = 1.4426950408889634
MASKED = -1e30 * LOG2E


def dev(**axes):
    return dict(device_id=axes, device_id_type=pl.DeviceIdType.MESH)


def silu_mul(gate, up):
    gate = gate.astype(BF16).astype(F32)
    up = up.astype(BF16).astype(F32)
    return (jax.nn.silu(gate) * up).astype(BF16)


def project_kernel(
    n_q, n_ff, d_model, hidden, gain_in, wq, wkv, wg, wu,
    q_out, kv_out, keep_out, recv_out, send_out,
    gain, h_own, h_other, u, inv_all, sq_all, wq_buf, wbuf, wkv_buf, part, part_kv, near, near_kv, keep, keep_kv, far_src,
    far_src_kv, far, far_kv, z_rows, z_other,
    wq_sem, w_sem, wkv_sem, h_in, gain_sem, h_sems, sq_send, sq_recv, near_send, near_recv, qn_send, qn_recv, kn_send, kn_recv,
    far_send, far_recv, qf_send, qf_recv, kf_send, kf_recv, y_sems, out_sem, qkv_sem,
):
    xi = lax.axis_index("x")
    yj = lax.axis_index("yz")
    core = lax.rem(xi, 2)
    chip = xi // 2
    mate = xi + 1 - 2 * core
    across = lax.rem(xi + 2, 4)
    other_y = 1 - yj
    me = xi * 2 + yj
    half = hidden.shape[-1]
    n_all = n_q + n_ff
    n_far = n_q + EARLY
    to_mate = dev(x=mate, yz=yj)
    to_across = dev(x=across, yz=yj)

    barrier = pltpu.get_barrier_semaphore()
    for k in range(1, 8):
        peer = lax.rem(me + k, 8)
        pl.semaphore_signal(barrier, inc=1, **dev(x=peer // 2, yz=lax.rem(peer, 2)))
    h_load = pltpu.make_async_copy(hidden, h_own, h_in)
    h_load.start()
    gain_load = pltpu.make_async_copy(gain_in, gain, gain_sem)
    gain_load.start()

    def start_weights(g):
        slot = lax.rem(g, NBUF1)
        cols = pl.ds(pl.multiple_of((g - n_q) * W, W), W)
        pltpu.make_async_copy(wg.at[0, :, cols], wbuf.at[slot, 0], w_sem.at[slot, 0]).start()
        pltpu.make_async_copy(wu.at[0, :, cols], wbuf.at[slot, 1], w_sem.at[slot, 1]).start()

    def wait_weights(slot, k):
        pltpu.make_async_copy(wg.at[0, :, pl.ds(0, W)], wbuf.at[slot, k], w_sem.at[slot, k]).wait()

    def wq_copy(g):
        return pltpu.make_async_copy(wq.at[0, :, g * 2 * W:(g + 1) * 2 * W], wq_buf.at[g], wq_sem.at[g])

    h_load.wait()
    gain_load.wait()
    for g in range(n_q):
        wq_copy(g).start()
    kv_copy = pltpu.make_async_copy(wkv.at[0], wkv_buf, wkv_sem)
    kv_copy.start()

    folded = jnp.zeros((256, 128), F32)
    for k in range(half // 128):
        block = h_own[:, :, :, k * 128:(k + 1) * 128].reshape(256, 128).astype(F32)
        folded += block * block
    sq_all[me] = jnp.broadcast_to(jnp.sum(jnp.transpose(folded), axis=0, keepdims=True), (8, 256))
    pl.semaphore_wait(barrier, 7)

    def sq_copy(peer, src):
        return pltpu.make_async_remote_copy(
            src_ref=sq_all.at[src], dst_ref=sq_all.at[src], send_sem=sq_send.at[peer], recv_sem=sq_recv.at[src],
            **dev(x=peer // 2, yz=lax.rem(peer, 2)))

    def side_of(step):
        return 1 - chip if step < 2 else chip

    def piece(step):
        return pl.ds(32 * step, 32) if step < 2 else pl.ds(0, 64)

    def h_copy(step):
        block = (side_of(step), slice(None), piece(step))
        return pltpu.make_async_remote_copy(
            src_ref=h_own.at[block], dst_ref=h_other.at[block],
            send_sem=h_sems.at[step, 0], recv_sem=h_sems.at[step, 1], **dev(x=xi, yz=other_y))

    for k in range(1, 8):
        sq_copy(lax.rem(me + k, 8), me).start()
    for step in range(3):
        h_copy(step).start()
    for k in range(1, 8):
        peer = lax.rem(me + k, 8)
        sq_copy(peer, peer).wait_recv()
    total = jnp.sum(sq_all[...], axis=0)
    inv = lax.rsqrt(total / d_model + NORM_EPS)
    inv_all[...] = jnp.transpose(jnp.concatenate([inv] * 16, axis=0)).reshape(inv_all.shape)

    def normalize(values, step, which):
        cols = pl.ds(pl.multiple_of(which * half, 128), half)
        side, rows = side_of(step), piece(step)
        u[side, :, rows, cols] = (
            values[side, :, rows].astype(F32) * inv_all[side, :, rows, :1] * gain[:, cols].astype(F32)).astype(BF16)

    def near_copy(g):
        return pltpu.make_async_remote_copy(
            src_ref=part.at[g, :, 1 - core], dst_ref=near.at[g], send_sem=near_send.at[g],
            recv_sem=near_recv.at[g], **to_mate)

    def near_copy_q(g, step):
        side, rows = side_of(step), piece(step)
        return pltpu.make_async_remote_copy(
            src_ref=part.at[g, side, 1 - core, rows], dst_ref=near.at[g, side, rows],
            send_sem=qn_send.at[g, step], recv_sem=qn_recv.at[g, step], **to_mate)

    def near_copy_kv(step):
        side, rows = side_of(step), piece(step)
        return pltpu.make_async_remote_copy(
            src_ref=part_kv.at[side, 1 - core, rows], dst_ref=near_kv.at[side, rows],
            send_sem=kn_send.at[step], recv_sem=kn_recv.at[step], **to_mate)

    def far_copy(g):
        return pltpu.make_async_remote_copy(
            src_ref=far_src.at[g], dst_ref=recv_out.at[g - n_q], send_sem=far_send.at[g - n_q],
            recv_sem=far_recv.at[g - n_q], **to_across)

    def far_copy_q(g, step):
        rows = piece(step)
        return pltpu.make_async_remote_copy(
            src_ref=far_src.at[g, rows], dst_ref=far.at[g, rows], send_sem=qf_send.at[g, step],
            recv_sem=qf_recv.at[g, step], **to_across)

    def far_copy_kv(step):
        rows = piece(step)
        return pltpu.make_async_remote_copy(
            src_ref=far_src_kv.at[rows], dst_ref=far_kv.at[rows], send_sem=kf_send.at[step], recv_sem=kf_recv.at[step],
            **to_across)

    def keep_copy(g):
        return pltpu.make_async_copy(keep.at[g], keep_out.at[g - n_q], out_sem.at[g - n_q, 0])

    def send_copy(g):
        k = g - n_q
        return pltpu.make_async_copy(far_src.at[g], send_out.at[k - EARLY], out_sem.at[k, 1])

    def add(a, b):
        return (a.astype(F32) + b.astype(F32)).astype(BF16)

    def multiply(g):
        slot = lax.rem(g, NBUF1)
        for k in range(2):
            wait_weights(slot, k)
            res = jnp.dot(u[...].reshape(256, u.shape[-1]), wbuf[slot, k], preferred_element_type=F32).astype(BF16)
            part[g, :, :, :, k * W:(k + 1) * W] = res.reshape(2, 2, 64, W)
        near_copy(g).start()

        @pl.when(g + NBUF1 < n_all)
        def _():
            start_weights(g + NBUF1)

    def reduce_near(g):
        near_copy(g).wait_recv()
        far_src[g] = add(part[g, 1 - chip, core], near[g, 1 - chip])

        @pl.when((g < n_far) & ((core == 1) | (g < n_far - HELD)))
        def _():
            far_copy(g).start()

        @pl.when(g >= n_far)
        def _():
            send_copy(g).start()

        keep[g] = add(part[g, chip, core], near[g, chip])
        keep_copy(g).start()

    def multiply_q(step):
        side, rows = side_of(step), piece(step)
        lhs = u[side, :, rows].reshape(2 * rows.size, u.shape[-1])
        for g in range(n_q):
            if step == 0:
                wq_copy(g).wait()
            for k in range(2):
                res = jnp.dot(lhs, wq_buf[g, :, k * W:(k + 1) * W], preferred_element_type=F32).astype(BF16)
                part[g, side, :, rows, k * W:(k + 1) * W] = res.reshape(2, rows.size, W)
            near_copy_q(g, step).start()
            if step == 0 and g >= 1:
                reduce_q(0, g - 1)
        if step == 0:
            kv_copy.wait()
        res = jnp.dot(lhs, wkv_buf[...], preferred_element_type=F32).astype(BF16)
        part_kv[side, :, rows] = res.reshape(2, rows.size, res.shape[1])
        near_copy_kv(step).start()

    def reduce_q(step, g):
        side, rows = side_of(step), piece(step)
        near_copy_q(g, step).wait_recv()
        total_q = add(part[g, side, core, rows], near[g, side, rows])
        if step < 2:
            far_src[g, rows] = total_q
            far_copy_q(g, step).start()
        else:
            keep[g] = total_q

    def reduce_kv(step):
        side, rows = side_of(step), piece(step)
        near_copy_kv(step).wait_recv()
        total_kv = add(part_kv[side, core, rows], near_kv[side, rows])
        if step < 2:
            far_src_kv[rows] = total_kv
            far_copy_kv(step).start()
        else:
            keep_kv[...] = total_kv

    for step in range(3):
        normalize(h_own, step, yj)
        h_copy(step).wait_recv()
        normalize(h_other, step, other_y)
        if step < 2:
            multiply_q(step)
            for g in range(n_q - 1 if step == 0 else 0, n_q):
                reduce_q(step, g)
            reduce_kv(step)
        if step == 0:
            for g in range(n_q, n_q + NBUF1):
                start_weights(jnp.int32(g))

    @pl.loop(n_q, n_far)
    def _(g):
        multiply(g)

        @pl.when(g >= n_q + 1)
        def _():
            reduce_near(g - 1)

    q_cols = n_q * 2 * W
    multiply_q(2)
    multiply(jnp.int32(n_far))
    reduce_near(jnp.int32(n_far - 1))
    for g in range(n_q):
        reduce_q(2, g)
        for step in range(2):
            far_copy_q(g, step).wait_recv()
        z_rows[:, :, g * 2 * W:(g + 1) * 2 * W] = add(keep[g], far[g]).reshape(2, 32, 2 * W)
    reduce_kv(2)
    for step in range(2):
        far_copy_kv(step).wait_recv()
    z_kv = add(keep_kv[...], far_kv[...])
    z_rows[:, :, q_cols:] = z_kv.reshape(2, 32, z_kv.shape[1])
    y_copy = pltpu.make_async_remote_copy(
        src_ref=z_rows.at[other_y], dst_ref=z_other, send_sem=y_sems.at[0], recv_sem=y_sems.at[1],
        **dev(x=xi, yz=other_y))
    y_copy.start()
    def qkv_copies(src, which):
        return (
            pltpu.make_async_copy(src.at[:, :q_cols], q_out.at[which], qkv_sem.at[0, 0 if src is z_other else 1]),
            pltpu.make_async_copy(src.at[:, q_cols:], kv_out.at[which], qkv_sem.at[1, 0 if src is z_other else 1]),
        )

    qkv_own = qkv_copies(z_rows.at[yj], yj)
    for copy in qkv_own:
        copy.start()

    @pl.loop(n_far + 1, n_all)
    def _(g):
        multiply(g)
        reduce_near(g - 1)

        @pl.when((g == n_far + RELEASE) & (core == 0))
        def _():
            @pl.loop(n_far - HELD, n_far)
            def _(k):
                far_copy(k).start()

    reduce_near(jnp.int32(n_all - 1))
    y_copy.wait_recv()
    qkv_other = qkv_copies(z_other, other_y)
    for copy in qkv_other:
        copy.start()

    for step in range(3):
        h_copy(step).wait_send()
        near_copy_kv(step).wait_send()
        for g in range(n_q):
            near_copy_q(g, step).wait_send()
    for step in range(2):
        far_copy_kv(step).wait_send()
        for g in range(n_q):
            far_copy_q(g, step).wait_send()
    for k in range(1, 8):
        sq_copy(lax.rem(me + k, 8), me).wait_send()
    y_copy.wait_send()

    @pl.loop(n_q, n_all)
    def _(g):
        near_copy(g).wait_send()
        keep_copy(g).wait()

    @pl.loop(n_far, n_all)
    def _(g):
        send_copy(g).wait()

    for copy in qkv_own + qkv_other:
        copy.wait()

    @pl.loop(n_q, n_far)
    def _(g):
        far_copy(g).wait_send()
        far_copy(g).wait_recv()


def project(hidden, gain, w_q, w_kv, w_gate, w_up, d_model):
    rows, half = hidden.shape
    feats = w_q.shape[1]
    kv = w_kv.shape[2]
    n_q = w_q.shape[2] // (2 * W)
    n_ff = w_gate.shape[2] // W
    n_all = n_q + n_ff
    late = n_ff - EARLY
    dma = pltpu.SemaphoreType.DMA
    any_spec = pl.BlockSpec(memory_space=pl.ANY)
    cols = w_q.shape[2] + kv
    flops = 2 * rows * feats * (w_q.shape[2] + kv + 2 * w_gate.shape[2])
    return pl.pallas_call(
        functools.partial(project_kernel, n_q, n_ff, d_model),
        name="project",
        out_shape=(
            jax.ShapeDtypeStruct((2, 32, cols - kv), BF16),
            jax.ShapeDtypeStruct((2, 32, kv), BF16),
            jax.ShapeDtypeStruct((n_ff, 64, 2 * W), BF16),
            jax.ShapeDtypeStruct((EARLY, 64, 2 * W), BF16),
            jax.ShapeDtypeStruct((late, 64, 2 * W), BF16),
        ),
        in_specs=[any_spec] * 6,
        out_specs=(any_spec,) * 5,
        scratch_shapes=[
            pltpu.VMEM((1, feats), BF16),
            pltpu.VMEM((2, 2, 64, half), BF16),
            pltpu.VMEM((2, 2, 64, half), BF16),
            pltpu.VMEM((2, 2, 64, feats), BF16),
            pltpu.VMEM((2, 2, 64, 128), F32),
            pltpu.VMEM((8, 8, rows), F32),
            pltpu.VMEM((n_q, feats, 2 * W), BF16),
            pltpu.VMEM((NBUF1, 2, feats, W), BF16),
            pltpu.VMEM((feats, kv), BF16),
            pltpu.VMEM((n_all, 2, 2, 64, 2 * W), BF16),
            pltpu.VMEM((2, 2, 64, kv), BF16),
            pltpu.VMEM((n_all, 2, 64, 2 * W), BF16),
            pltpu.VMEM((2, 64, kv), BF16),
            pltpu.VMEM((n_all, 64, 2 * W), BF16),
            pltpu.VMEM((64, kv), BF16),
            pltpu.VMEM((n_all, 64, 2 * W), BF16),
            pltpu.VMEM((64, kv), BF16),
            pltpu.VMEM((n_q, 64, 2 * W), BF16),
            pltpu.VMEM((64, kv), BF16),
            pltpu.VMEM((2, 32, cols), BF16),
            pltpu.VMEM((32, cols), BF16),
            dma((n_q,)),
            dma((NBUF1, 2)),
            dma,
            dma,
            dma,
            dma((3, 2)),
            dma((8,)),
            dma((8,)),
            dma((n_all,)),
            dma((n_all,)),
            dma((n_q, 3)),
            dma((n_q, 3)),
            dma((3,)),
            dma((3,)),
            dma((EARLY,)),
            dma((EARLY,)),
            dma((n_q, 2)),
            dma((n_q, 2)),
            dma((2,)),
            dma((2,)),
            dma((2,)),
            dma((n_ff, 2)),
            dma((2, 2)),
        ],
        compiler_params=pltpu.CompilerParams(collective_id=0, has_side_effects=True, vmem_limit_bytes=VMEM_LIMIT),
        cost_estimate=pl.CostEstimate(flops=flops, bytes_accessed=feats * (flops // (rows * feats)), transcendentals=0),
    )(hidden.reshape(2, 2, 64, half), gain, w_q, w_kv, w_gate, w_up)


def attend_kernel(lens, q_ref, kv_ref, k_ref, v_ref, k_out, v_out, o_ref, fresh):
    step = pl.program_id(0)

    @pl.when(step == 0)
    def _():
        fresh[...] = kv_ref[...].astype(F32)

    n_pos = k_ref.shape[2]
    scale = q_ref.shape[2] ** -0.5 * LOG2E
    for s in range(SEQ_STEP):
        length = lens[step * SEQ_STEP + s]
        base = pl.multiple_of((length // 16) * 16, 16)
        k_out[0, s] = k_ref[0, s]
        v_out[0, s] = v_ref[0, s]
        hit = lax.broadcasted_iota(jnp.int32, (16, k_ref.shape[3]), 0) == length - base
        for src, dst, which in ((k_ref, k_out, 0), (v_ref, v_out, 1)):
            old = src[0, s, pl.ds(base, 16), :].astype(F32)
            new = fresh[which, pl.ds(step * SEQ_STEP + s, 1), :]
            dst[0, s, pl.ds(base, 16), :] = jnp.where(hit, new, old).astype(BF16)
        scores = lax.dot_general(q_ref[s], k_ref[0, s], (((1,), (1,)), ((), ())), preferred_element_type=F32) * scale
        k_new = fresh[0, pl.ds(step * SEQ_STEP + s, 1), :]
        own = jnp.sum(q_ref[s].astype(F32) * k_new, axis=1, keepdims=True) * scale
        place = lax.broadcasted_iota(jnp.int32, scores.shape, 1)
        scores = jnp.where(place < length, scores, jnp.where(place == length, own, MASKED))
        weights = jnp.exp2(scores - jnp.max(scores, axis=1, keepdims=True))
        probs = (weights * (1.0 / jnp.sum(weights, axis=1, keepdims=True))).astype(BF16)
        o_ref[s] = jnp.dot(probs, v_out[0, s], preferred_element_type=F32).astype(BF16)


def attend(lens, q, kv, k_cache, v_cache):
    seqs, heads, dim = q.shape
    n_pos = k_cache.shape[2]
    cache_spec = pl.BlockSpec((1, SEQ_STEP, n_pos, dim), lambda b, lens: (0, b, 0, 0))
    q_spec = pl.BlockSpec((SEQ_STEP, heads, dim), lambda b, lens: (b, 0, 0))
    return pl.pallas_call(
        attend_kernel,
        name="attend",
        out_shape=(
            jax.ShapeDtypeStruct(k_cache.shape, BF16),
            jax.ShapeDtypeStruct(v_cache.shape, BF16),
            jax.ShapeDtypeStruct(q.shape, BF16),
        ),
        grid_spec=pltpu.PrefetchScalarGridSpec(
            num_scalar_prefetch=1,
            grid=(seqs // SEQ_STEP,),
            in_specs=[q_spec, pl.BlockSpec((2, seqs, dim), lambda b, lens: (0, 0, 0)), cache_spec, cache_spec],
            out_specs=(cache_spec, cache_spec, q_spec),
            scratch_shapes=[pltpu.VMEM((2, seqs, dim), F32)],
        ),
        compiler_params=pltpu.CompilerParams(dimension_semantics=("arbitrary",), vmem_limit_bytes=66_000_000),
        cost_estimate=pl.CostEstimate(
            flops=10**10, bytes_accessed=8 * k_cache.size, transcendentals=seqs * heads * n_pos),
    )(lens, q, kv, k_cache, v_cache)


def output_kernel(
    n_ff, n_o, o_in, keep, recv_e, recv_l, hidden, w_o, w_down, out,
    acts, wbuf, acc, keep_v, recv_v, h_v, y_src, y_dst,
    w_sem, keep_sem, recv_sem, h_sem, oo_sems, on_send, on_recv, far_send, far_recv, near_send, near_recv, y_sems,
):
    xi = lax.axis_index("x")
    yj = lax.axis_index("yz")
    core = lax.rem(xi, 2)
    mate = xi + 1 - 2 * core
    across = lax.rem(xi + 2, 4)
    other_y = 1 - yj
    n_m = n_ff // GROUP
    n_g = n_m + n_o // GROUP
    n_early = EARLY // GROUP
    depth = GROUP * W
    d_out = w_down.shape[2]
    half = d_out // 2

    barrier = pltpu.get_barrier_semaphore()
    for x_, y_ in ((mate, yj), (across, yj), (xi, other_y)):
        pl.semaphore_signal(barrier, inc=1, **dev(x=x_, yz=y_))

    def keep_copy(g):
        return pltpu.make_async_copy(
            keep.at[pl.ds(GROUP * g, GROUP)], keep_v.at[pl.ds(GROUP * g, GROUP)], keep_sem.at[g])

    def recv_copy(g):
        src = recv_e.at[pl.ds(GROUP * g, GROUP)] if g < n_early else recv_l.at[pl.ds(GROUP * (g - n_early), GROUP)]
        return pltpu.make_async_copy(src, recv_v.at[pl.ds(GROUP * g, GROUP)], recv_sem.at[g])

    keep_copy(0).start()
    recv_copy(0).start()

    def rows_of(p, owner):
        off, size = PARTS[p]
        return pl.ds(pl.multiple_of(4 * off + owner * size, 16), size)

    def block(p, g, owner):
        return acts.at[pl.ds(GROUP * g, GROUP), rows_of(p, owner)]

    def o_rows(s):
        row = (1 - yj) * (32 * xi + 16 * s) + yj * (128 + 64 * s + 16 * xi)
        return acts.at[pl.ds(n_ff, n_o), pl.ds(pl.multiple_of(row, 16), 16)]

    def o_own(s):
        return pltpu.make_async_copy(o_in.at[yj, :, pl.ds(16 * s, 16)], o_rows(s), oo_sems.at[s])

    def o_copy(s):
        return pltpu.make_async_remote_copy(
            src_ref=o_in.at[other_y, :, pl.ds(16 * s, 16)], dst_ref=o_rows(s), send_sem=on_send.at[s],
            recv_sem=on_recv.at[s], **dev(x=xi, yz=other_y))

    h_load = pltpu.make_async_copy(hidden, h_v, h_sem)

    def load_weights(g):
        slot = lax.rem(g, NBUF3)

        @pl.when(g < n_m)
        def _():
            pltpu.make_async_copy(
                w_down.at[0, pl.ds(pl.multiple_of(g * depth, W), depth)], wbuf.at[slot], w_sem.at[slot]).start()

        @pl.when(g >= n_m)
        def _():
            pltpu.make_async_copy(
                w_o.at[0, pl.ds(pl.multiple_of((g - n_m) * depth, W), depth)], wbuf.at[slot], w_sem.at[slot]).start()

    def far_copy(p, g):
        return pltpu.make_async_remote_copy(
            src_ref=block(p, g, xi), dst_ref=block(p, g, xi), send_sem=far_send.at[p, g], recv_sem=far_recv.at[p, g],
            **dev(x=across, yz=yj))

    def near_copy(p, g, which):
        rows = block(p, g, xi if which == 0 else across)
        return pltpu.make_async_remote_copy(
            src_ref=rows, dst_ref=rows, send_sem=near_send.at[p, g, which], recv_sem=near_recv.at[p, g, which],
            **dev(x=mate, yz=yj))

    def give(p, g):
        far_copy(p, g).start()
        near_copy(p, g, 0).start()

    def give_m(p, g):
        off, size = PARTS[p]
        for k in range(GROUP):
            t = GROUP * g + k
            z = keep_v[t, off:off + size].astype(F32) + recv_v[t, off:off + size].astype(F32)
            acts[t, rows_of(p, xi)] = silu_mul(z[:, :W], z[:, W:])
        give(p, g)

    pl.semaphore_wait(barrier, 3)
    for g in range(n_m):
        keep_copy(g).wait()
        recv_copy(g).wait()
        give_m(0, g)
        if g == 0:
            for s in range(2):
                o_copy(s).start()
                o_own(s).start()
            for k in range(1, n_m):
                keep_copy(k).start()
                recv_copy(k).start()
    for s in range(NBUF3):
        load_weights(jnp.int32(s))
    h_load.start()
    acc[...] = jnp.zeros_like(acc)
    for s in range(2):
        o_own(s).wait()
        o_copy(s).wait_recv()

    def chunk(p, k):
        return k if p % 2 == 0 else n_g - 1 - k

    for g in range(n_m, n_g):
        give(0, g)
    for p in range(1, len(PARTS)):
        @pl.loop(0, n_g)
        def _(k):
            g = chunk(p, k)

            @pl.when(g < n_m)
            def _():
                give_m(p, g)

            @pl.when(g >= n_m)
            def _():
                give(p, g)

    def forward(p, k):
        g = chunk(p, k)
        far_copy(p, g).wait_recv()
        near_copy(p, g, 1).start()

    def multiply(p, k):
        g = chunk(p, k)
        slot = lax.rem(g, NBUF3)

        @pl.when(k >= (0 if p == 0 else NBUF3))
        def _():
            pltpu.make_async_copy(w_down.at[0, pl.ds(0, depth)], wbuf.at[slot], w_sem.at[slot]).wait()

        near_copy(p, g, 0).wait_recv()
        near_copy(p, g, 1).wait_recv()
        off, size = PARTS[p]
        rows = slice(4 * off, 4 * (off + size))
        for n in range(d_out // W):
            cols = slice(n * W, (n + 1) * W)
            total = acc[rows, cols]
            for j in range(GROUP):
                total += jnp.dot(
                    acts[GROUP * g + j, rows], wbuf[slot, j * W:(j + 1) * W, cols], preferred_element_type=F32)
            acc[rows, cols] = total

        @pl.when(k + NBUF3 < n_g)
        def _():
            load_weights(chunk(p, k + NBUF3))

    def cols_of(j):
        return pl.ds(pl.multiple_of(j * half, 128), half)

    def y_copy(p):
        rows = slice(4 * PARTS[p][0], 4 * sum(PARTS[p]))
        return pltpu.make_async_remote_copy(
            src_ref=y_src.at[rows], dst_ref=y_dst.at[rows], send_sem=y_sems.at[p, 0], recv_sem=y_sems.at[p, 1],
            **dev(x=xi, yz=other_y))

    def exchange(p):
        rows = slice(4 * PARTS[p][0], 4 * sum(PARTS[p]))
        y_src[rows] = acc[rows, cols_of(other_y)].astype(BF16)
        y_copy(p).start()

    def finalize(p):
        off, size = PARTS[p]
        rows = slice(4 * off, 4 * (off + size))
        y_copy(p).wait_recv()
        total = (acc[rows, cols_of(yj)] + y_dst[rows].astype(F32)).reshape(4, size, half)
        out[:, off:off + size] = (h_v[:, off:off + size].astype(F32) + total).astype(BF16)

    for p in range(len(PARTS)):
        forward(p, jnp.int32(0))
        if p > 0:
            multiply(p - 1, jnp.int32(n_g - 1))
            exchange(p - 1)
        if p == 1:
            h_load.wait()

        @pl.loop(1, n_g)
        def _(k):
            forward(p, k)
            multiply(p, k - 1)

        if p > 0:
            finalize(p - 1)

    last = len(PARTS) - 1
    g = chunk(last, n_g - 1)
    if n_g > NBUF3:
        pltpu.make_async_copy(w_down.at[0, pl.ds(0, depth)], wbuf.at[g % NBUF3], w_sem.at[g % NBUF3]).wait()
    near_copy(last, g, 0).wait_recv()
    near_copy(last, g, 1).wait_recv()
    rows = slice(4 * PARTS[last][0], 4 * sum(PARTS[last]))
    for j in (other_y, yj):
        for n in range(half // 256):
            cols = pl.ds(pl.multiple_of(j * half + n * 256, 256), 256)
            total = acc[rows, cols]
            for k in range(GROUP):
                total += jnp.dot(
                    acts[GROUP * g + k, rows], wbuf[g % NBUF3, k * W:(k + 1) * W, cols], preferred_element_type=F32)
            acc[rows, cols] = total
        if j is other_y:
            exchange(last)
    for s in range(2):
        o_copy(s).wait_send()
    for p in range(len(PARTS)):
        @pl.loop(0, n_g)
        def _(g):
            far_copy(p, g).wait_send()
            near_copy(p, g, 0).wait_send()
            near_copy(p, g, 1).wait_send()

    finalize(last)
    for p in range(len(PARTS)):
        y_copy(p).wait_send()


def finish(o, keep, recv_e, recv_l, hidden, w_o, w_down):
    rows, half = hidden.shape
    n_ff = w_down.shape[1] // W
    n_o = w_o.shape[1] // W
    n_m = n_ff // GROUP
    n_g = n_m + n_o // GROUP
    n_p = len(PARTS)
    d_out = w_down.shape[2]
    dma = pltpu.SemaphoreType.DMA
    any_spec = pl.BlockSpec(memory_space=pl.ANY)
    vmem = pl.BlockSpec(memory_space=pltpu.VMEM)
    flops = 2 * rows * d_out * (w_down.shape[1] + w_o.shape[1])
    out = pl.pallas_call(
        functools.partial(output_kernel, n_ff, n_o),
        name="finish",
        out_shape=jax.ShapeDtypeStruct((4, 64, half), BF16),
        in_specs=[any_spec] * 7,
        out_specs=vmem,
        scratch_shapes=[
            pltpu.VMEM((n_ff + n_o, rows, W), BF16),
            pltpu.VMEM((NBUF3, GROUP * W, d_out), BF16),
            pltpu.VMEM((rows, d_out), F32),
            pltpu.VMEM(keep.shape, BF16),
            pltpu.VMEM(keep.shape, BF16),
            pltpu.VMEM((4, 64, half), BF16),
            pltpu.VMEM((rows, half), BF16),
            pltpu.VMEM((rows, half), BF16),
            dma((NBUF3,)),
            dma((n_m,)),
            dma((n_m,)),
            dma,
            dma((2,)),
            dma((2,)),
            dma((2,)),
            dma((n_p, n_g)),
            dma((n_p, n_g)),
            dma((n_p, n_g, 2)),
            dma((n_p, n_g, 2)),
            dma((n_p, 2)),
        ],
        compiler_params=pltpu.CompilerParams(collective_id=1, has_side_effects=True, vmem_limit_bytes=56_000_000),
        cost_estimate=pl.CostEstimate(flops=flops, bytes_accessed=2 * d_out * (w_down.shape[1] + w_o.shape[1]), transcendentals=0),
    )(o, keep, recv_e, recv_l, hidden.reshape(4, 64, half), w_o, w_down)
    return out.reshape(rows, half)


def solution(mesh):
    x_size = mesh.shape["x"]
    y_size = mesh.shape["yz"]
    row_spec = P("dp", ("x", "yz"))
    tile_in = P(None, "x", "yz")
    tile_out = P(None, "yz", "x")
    cache_spec = P(None, ("dp", "x", "yz"))
    len_spec = P(("dp", "x", "yz"))

    def device_step(hidden, norm_gain, w_q, w_kv, w_gate, w_up, w_o, w_down, k_cache, v_cache, seq_len):
        d_model = hidden.shape[1] * x_size * y_size
        seqs = k_cache.shape[1]
        dim = k_cache.shape[3]
        q_cols = w_q.shape[2]
        heads = q_cols // dim
        q, kv, keep, recv_e, send = project(hidden, norm_gain, w_q, w_kv, w_gate, w_up, d_model)
        recv_l = lax.ppermute(send, "x", [(i, (i + x_size // 2) % x_size) for i in range(x_size)])
        q = q.reshape(y_size, seqs, heads, dim).transpose(1, 0, 2, 3).reshape(seqs, y_size * heads, dim)
        k_new, v_new, o = attend(seq_len, q, kv, k_cache, v_cache)
        o = o.reshape(seqs, y_size, q_cols // W, W).transpose(1, 2, 0, 3)
        hidden_out = finish(o, keep, recv_e, recv_l, hidden, w_o, w_down)
        return hidden_out, k_new, v_new

    return jax.shard_map(
        device_step,
        mesh=mesh,
        in_specs=(row_spec, P(None, "x"), tile_in, tile_in, tile_in, tile_in, tile_out, tile_out, cache_spec, cache_spec, len_spec),
        out_specs=(row_spec, cache_spec, cache_spec),
        check_vma=False,
    )
```
